32 devices in a mesh: fsdp: 8 (over y, x, core), tp: 4 (over z).
Axes of the slice: x: 2, y: 2, z: 4, core: 2. Of those that a mesh axis runs over, the one named last changes fastest.
Arguments:
- tokens: bfloat16 [8192, 1536], P(('fsdp', 'tp')), may hold values from -6 to 6
- cotangent: bfloat16 [8192, 1536], P(('fsdp', 'tp')), may hold values from -6 to 6
- seq_start: int32 [32], P('fsdp'), may hold values from 0 to 1, as said below
- token_valid: int32 [8192], P('fsdp'), may hold values from 0 to 1, as said below
- norm_gain: float32 [1536], replicated, may hold values from 0.5 to 1.5
- proj_z: bfloat16 [1536, 3072], P('fsdp', 'tp'), may hold values from -0.15625 to 0.15625
- proj_x: bfloat16 [1536, 3072], P('fsdp', 'tp'), may hold values from -0.15625 to 0.15625
- proj_bc: bfloat16 [1536, 256], P('fsdp'), may hold values from -0.15625 to 0.15625
- proj_dt: bfloat16 [1536, 48], P('fsdp', 'tp'), may hold values from -0.15625 to 0.15625
- conv_chan: float32 [4, 3072], P(None, 'tp'), may hold values from -3 to 3
- bias_chan: float32 [3072], P('tp'), may hold values from -0.5 to 0.5
- conv_shared: float32 [4, 256], replicated, may hold values from -3 to 3
- bias_shared: float32 [256], replicated, may hold values from -0.5 to 0.5
- a_log: float32 [48], P('tp'), may hold values from -1 to 1.5
- dt_bias: float32 [48], P('tp'), may hold values from -8 to -2
- skip_gain: float32 [48], P('tp'), may hold values from 0.5 to 1.5
- gate_gain: float32 [3072], P('tp'), may hold values from 0.5 to 1.5
- proj_out: bfloat16 [3072, 1536], P('tp', 'fsdp'), may hold values from -0.109375 to 0.109375
Outputs:
- output: bfloat16 [8192, 1536], P(('fsdp', 'tp'))
- grad_tokens: bfloat16 [8192, 1536], P(('fsdp', 'tp'))
- grad_norm_gain: float32 [1536], replicated
- grad_proj_z: float32 [1536, 3072], P('fsdp', 'tp')
- grad_proj_x: float32 [1536, 3072], P('fsdp', 'tp')
- grad_proj_bc: float32 [1536, 256], P('fsdp')
- grad_proj_dt: float32 [1536, 48], P('fsdp', 'tp')
- grad_conv_chan: float32 [4, 3072], P(None, 'tp')
- grad_bias_chan: float32 [3072], P('tp')
- grad_conv_shared: float32 [4, 256], replicated
- grad_bias_shared: float32 [256], replicated
- grad_a_log: float32 [48], P('tp')
- grad_dt_bias: float32 [48], P('tp')
- grad_skip_gain: float32 [48], P('tp')
- grad_gate_gain: float32 [3072], P('tp')
- grad_proj_out: float32 [3072, 1536], P('tp', 'fsdp')
The draws below stay inside these ranges and needn't reach their ends.
Inputs may be any that keep to these rules, and one draw needn't show every extreme that they name: `seq_start`: each buffer of 4 blocks has 1 at its first block; a sequence spans 4 to min(15, 4) blocks and no sequence crosses a buffer; after a buffer's last sequence the flags are 0; some buffer is filled with sequences to its end. `token_valid`: within a sequence all tokens are 1 except between 0 and 127 tokens at the end of its last block; every token of the blocks after a buffer's last sequence is 0.
All inputs are finite; a program needn't handle non-finite values.
Results may differ from the reference program's by a relative error of at most 0.02.
Values may be sent and summed in bfloat16 or wider, within the bound.
A program may use at most 192 MiB of HBM per device.

```python
import jax
import jax.numpy as jnp
from jax import lax

D = 1536
HEADS = 48
HEAD = 64
STATE = 128
CONV = 4
STRETCH = 256
TOK_DEV = 256
INNER = 3072
TOKENS = 8192
N_FSDP = 8
N_TP = 4


def packing_layout(key):
    groups = N_FSDP
    stretch_count = TOK_DEV * N_TP // STRETCH
    subkeys = jax.random.split(jax.random.fold_in(key, 7), 4)
    least_filled = max(4, stretch_count // 2)
    filled = jax.random.randint(subkeys[0], (groups,), least_filled, stretch_count + 1)
    chosen = jax.random.randint(subkeys[1], (), 0, groups)
    filled = jnp.where(jnp.arange(groups) == chosen, stretch_count, filled)
    spacing = jax.random.randint(subkeys[2], (groups, stretch_count), 4, 13)
    offsets = jnp.cumsum(spacing, axis=1) - spacing
    allowed = offsets <= (filled - 4)[:, None]
    positions = jnp.arange(stretch_count)
    starting = jnp.any((offsets[:, :, None] == positions[None, None, :]) & allowed[:, :, None], axis=1)
    active = positions[None, :] < filled[:, None]
    following = jnp.concatenate([starting[:, 1:], jnp.ones((groups, 1), dtype=bool)], axis=1)
    closing = active & (following | (positions[None, :] + 1 == filled[:, None]))
    trimmed = jax.random.randint(subkeys[3], (groups, stretch_count), 0, STRETCH // 2)
    within = jnp.arange(STRETCH)
    kept_mask = active[:, :, None] & (jnp.logical_not(closing[:, :, None]) | (within[None, None, :] < STRETCH - trimmed[:, :, None]))
    return (starting.astype(jnp.int32).reshape(-1), kept_mask.astype(jnp.int32).reshape(-1))


def draw_seq_start(key, part):
    return packing_layout(key)[0]


def draw_token_valid(key, part):
    return packing_layout(key)[1]


def levels(rng, shape, cuts, low, largest):
    level, own = 1.0, jax.random.fold_in(rng, 6)
    for dim, parts in cuts:
        draws = jnp.exp(jax.random.uniform(jax.random.fold_in(own, dim), (parts,), jnp.float32, low / len(cuts), largest / len(cuts)))
        level = level * jnp.repeat(draws, shape[dim] // parts).reshape([-1 if axis == dim else 1 for axis in range(len(shape))])
    return level


def centred(own_key, extent, scale, most, pieces=(), held_as=jnp.bfloat16):
    array = jax.random.normal(own_key, extent, jnp.float32) * scale
    if len(pieces) > 0:
        array = levels(own_key, extent, pieces, -0.22, 0.18) * array
    return jnp.clip(array, min=-most, max=most).astype(held_as)


def setup_inputs(seed: int = 0) -> dict:
    key_of = jax.random.split(jax.random.key(seed), 19)
    tokens = centred(key_of[0], (TOKENS, D), 1.0, 6.0, ((0, 32),))
    cotangent = centred(key_of[1], (TOKENS, D), 1.0, 6.0, ((0, 32),))
    seq_start = draw_seq_start(jax.random.fold_in(key_of[18], 71), 0)
    token_valid = draw_token_valid(jax.random.fold_in(key_of[18], 71), 0)
    norm_gain = jnp.clip(1.0 + 0.1 * jax.random.normal(key_of[4], (D,), jnp.float32), 0.5, 1.5)
    proj_z = centred(key_of[5], (D, INNER), D ** -0.5, 0.15625, ((0, 8), (1, 4)))
    proj_x = centred(key_of[6], (D, INNER), D ** -0.5, 0.15625, ((0, 8), (1, 4)))
    proj_bc = centred(key_of[7], (D, 2 * STATE), D ** -0.5, 0.15625, ((0, 8),))
    proj_dt = centred(key_of[8], (D, HEADS), D ** -0.5, 0.15625, ((0, 8), (1, 4)))
    conv_chan = centred(key_of[9], (CONV, INNER), CONV ** -0.5, 3.0, ((1, 4),), jnp.float32)
    bias_chan = jnp.clip(jax.random.uniform(key_of[10], (INNER,), jnp.float32, -0.5, 0.5) * levels(key_of[10], (INNER,), ((0, 4),), -0.4, 0.0), -0.5, 0.5)
    conv_shared = centred(key_of[11], (CONV, 2 * STATE), CONV ** -0.5, 3.0, (), jnp.float32)
    bias_shared = jnp.clip(jax.random.uniform(key_of[12], (2 * STATE,), jnp.float32, -0.5, 0.5), -0.5, 0.5)
    a_log = jnp.clip(-1.0 + 2.5 * jax.random.uniform(key_of[13], (HEADS,), jnp.float32) ** levels(key_of[13], (HEADS,), ((0, 4),), -0.2, 0.2), -1.0, 1.5)
    dt_bias = jnp.clip(-8.0 + 6.0 * jax.random.uniform(key_of[14], (HEADS,), jnp.float32) ** levels(key_of[14], (HEADS,), ((0, 4),), -0.2, 0.2), -8.0, -2.0)
    skip_gain = jnp.clip(0.5 + 1.0 * jax.random.uniform(key_of[15], (HEADS,), jnp.float32) ** levels(key_of[15], (HEADS,), ((0, 4),), -0.2, 0.2), 0.5, 1.5)
    gate_gain = jnp.clip(1.0 + 0.1 * jax.random.normal(key_of[16], (INNER,), jnp.float32), 0.5, 1.5)
    proj_out = centred(key_of[17], (INNER, D), INNER ** -0.5, 0.109375, ((0, 4), (1, 8)))
    return {"tokens": tokens, "cotangent": cotangent, "seq_start": seq_start, "token_valid": token_valid, "norm_gain": norm_gain, "proj_z": proj_z, "proj_x": proj_x, "proj_bc": proj_bc, "proj_dt": proj_dt, "conv_chan": conv_chan, "bias_chan": bias_chan, "conv_shared": conv_shared, "bias_shared": bias_shared, "a_log": a_log, "dt_bias": dt_bias, "skip_gain": skip_gain, "gate_gain": gate_gain, "proj_out": proj_out}


EPSILON = 1e-05
PRECISE = lax.Precision.HIGHEST

@jax.custom_vjp
def low(v):
    return lax.optimization_barrier(v.astype(jnp.bfloat16)).astype(jnp.float32)

@jax.custom_vjp
def low_back(v):
    return v

def low_keep(v):
    return (low(v), None)

def low_pass(kept, grad):
    return (grad,)

def back_keep(v):
    return (v, None)

def back_low(kept, grad):
    return (low(grad),)
low.defvjp(low_keep, low_pass)
low_back.defvjp(back_keep, back_low)

def product(left, right):
    return jnp.dot(left, right, precision=PRECISE, preferred_element_type=jnp.float32)

def causal_conv(signal, kernel, offset_bias, openings):
    length = signal.shape[0]
    tap_count = kernel.shape[0]
    padded = jnp.concatenate([jnp.zeros((tap_count - 1, signal.shape[1]), jnp.float32), signal], axis=0)
    within = jnp.arange(length) % STRETCH
    opening = jnp.repeat(openings, STRETCH)
    result = jnp.zeros_like(signal) + offset_bias[None, :]
    for tap_index in range(tap_count):
        reach_back = tap_count - 1 - tap_index
        allowed = 1.0 - opening * (within < reach_back).astype(jnp.float32)
        result = result + allowed[:, None] * padded[tap_index:tap_index + length] * kernel[tap_index][None, :]
    return jax.nn.silu(result)

def state_scan(inputs, step_rates, decay_a, shared_b, shared_c, openings):
    seq_len, head_count, head_size = inputs.shape
    block_count = seq_len // STRETCH
    blocks_x = inputs.reshape(block_count, STRETCH, head_count, head_size)
    blocks_dt = step_rates.reshape(block_count, STRETCH, head_count)
    blocks_b = shared_b.reshape(block_count, STRETCH, shared_b.shape[1])
    blocks_c = shared_c.reshape(block_count, STRETCH, shared_c.shape[1])
    log_decay = blocks_dt * decay_a[None, None, :]
    lower = (jnp.arange(STRETCH)[:, None] >= jnp.arange(STRETCH)[None, :]).astype(jnp.float32)
    cumulative = jnp.einsum('ts,csh->cth', lower, log_decay, precision=PRECISE)
    spread = cumulative[:, :, None, :] - cumulative[:, None, :, :]
    weights = jnp.exp(jnp.where(lower[None, :, :, None] > 0, spread, -1e+30))
    intersection = jnp.einsum('ctn,csn->cts', blocks_c, blocks_b, precision=PRECISE)
    scaled_x = blocks_x * blocks_dt[..., None]
    within_block = jnp.einsum('ctsh,cshp->cthp', weights * intersection[..., None], scaled_x, precision=PRECISE)
    to_end = jnp.exp(cumulative[:, -1:, :] - cumulative)
    block_states = jnp.einsum('cshp,csn->chpn', scaled_x * to_end[..., None], blocks_b, precision=PRECISE)
    carry_decay = jnp.exp(cumulative[:, -1, :])

    def advance(carried, block_item):
        opening, factor, fresh_state = block_item
        entering = carried * (1.0 - opening)
        return (entering * factor[:, None, None] + fresh_state, entering)
    initial = jnp.zeros((head_count, head_size, blocks_b.shape[-1]), jnp.float32)
    _, entering = lax.scan(advance, initial, (openings, carry_decay, block_states))
    across_block = jnp.einsum('ctn,chpn->cthp', blocks_c, entering, precision=PRECISE) * jnp.exp(cumulative)[..., None]
    return (within_block + across_block).reshape(seq_len, head_count, head_size)

def gated_branch(pre_z, pre_x, pre_bc, pre_dt, conv_chan, bias_chan, conv_shared, bias_shared, a_log, dt_bias, skip_gain, validity, openings):
    length = pre_x.shape[0]
    head_count = pre_dt.shape[1]
    features = causal_conv(pre_x, conv_chan, bias_chan, openings)
    shared = causal_conv(pre_bc, conv_shared, bias_shared, openings)
    step_rates = jax.nn.softplus(pre_dt + dt_bias[None, :]) * validity[:, None]
    decay_a = -jnp.exp(a_log)
    heads_x = features.reshape(length, head_count, HEAD)
    mixed_out = state_scan(heads_x, step_rates, decay_a, shared[:, :STATE], shared[:, STATE:], openings)
    mixed_out = mixed_out + skip_gain[None, :, None] * heads_x
    return mixed_out.reshape(length, head_count * HEAD) * jax.nn.silu(pre_z) * validity[:, None]

def reference(tokens, cotangent, seq_start, token_valid, norm_gain, proj_z, proj_x, proj_bc, proj_dt, conv_chan, bias_chan, conv_shared, bias_shared, a_log, dt_bias, skip_gain, gate_gain, proj_out):
    group_len = TOK_DEV * N_TP
    validity = token_valid.astype(jnp.float32).reshape(N_FSDP, group_len)
    openings = seq_start.astype(jnp.float32).reshape(N_FSDP, group_len // STRETCH)
    params = tuple((weight_arg.astype(jnp.float32) for weight_arg in (norm_gain, proj_z, proj_x, proj_bc, proj_dt, conv_chan, bias_chan, conv_shared, bias_shared, a_log, dt_bias, skip_gain, gate_gain, proj_out)))
    resid = tokens.astype(jnp.float32).reshape(N_FSDP, group_len, D)

    def forward(resid_in, weight_set):
        gain_in, wz_full, wx_full, wbc_full, wdt_full, conv_c, bias_c, conv_s, bias_s, alog_in, dtb_in, skip_in, gate_in, wout_full = weight_set

        def one_group(carried, block_item):
            rows_in, valid_rows, open_rows = block_item
            rstd = lax.rsqrt(lax.optimization_barrier(jnp.mean(rows_in * rows_in, axis=1, keepdims=True)) + EPSILON)
            normed = low(rows_in * rstd * gain_in[None, :])
            pre_z = low_back(product(normed, wz_full))
            pre_x = low_back(product(normed, wx_full))
            pre_bc = low_back(product(normed, wbc_full))
            pre_dt = low_back(product(normed, wdt_full))
            gated = gated_branch(pre_z, pre_x, pre_bc, pre_dt, conv_c, bias_c, conv_s, bias_s, alog_in, dtb_in, skip_in, valid_rows, open_rows)
            grstd = lax.rsqrt(lax.optimization_barrier(jnp.mean(gated * gated, axis=1, keepdims=True)) + EPSILON)
            gnormed = low(gated * grstd * gate_in[None, :])
            return (carried, rows_in + product(gnormed, wout_full))
        _, outputs = lax.scan(jax.checkpoint(one_group), jnp.zeros((), jnp.float32), (resid_in, validity, openings))
        return outputs
    result, backward = jax.vjp(forward, resid, params)
    grad_resid, grad_params = backward(cotangent.astype(jnp.float32).reshape(N_FSDP, group_len, D))
    return (result.reshape(TOKENS, D).astype(jnp.bfloat16), grad_resid.reshape(TOKENS, D).astype(jnp.bfloat16), grad_params[0], grad_params[1], grad_params[2], grad_params[3], grad_params[4], grad_params[5], grad_params[6], grad_params[7], grad_params[8], grad_params[9], grad_params[10], grad_params[11], grad_params[12], grad_params[13])
```

```python
import functools
import jax
import jax.numpy as jnp
from jax import lax
from jax.experimental import pallas as pl
from jax.experimental.pallas import tpu as pltpu
from jax.sharding import PartitionSpec as P

HEAD = 64
STATE = 128
STRETCH = 256
LANES = 128
EPSILON = 1e-05
F32 = jnp.float32
BF16 = jnp.bfloat16
NN = (((1,), (0,)), ((), ()))
NT = (((1,), (1,)), ((), ()))
TN = (((0,), (0,)), ((), ()))


def mm(a, b, dims=NN):
    return lax.dot_general(a, b, dims, preferred_element_type=F32)


def exact(a, b):
    return lax.dot_general(a, b, NN, precision=lax.Precision.HIGHEST, preferred_element_type=F32)


def halves(v):
    high = v.astype(BF16)
    return high, (v - high.astype(F32)).astype(BF16)


def iota(shape, dim):
    return lax.broadcasted_iota(jnp.int32, shape, dim)


def spread_heads(v, chan):
    high, rest = halves(v)
    rows = iota((2 * LANES, chan), 0) & (LANES - 1)
    pick = jnp.where(rows == (iota((2 * LANES, chan), 1) >> 6), 1.0, 0.0).astype(BF16)
    return mm(jnp.concatenate([high, rest], axis=1), pick)


def gather_heads(v):
    chan = v.shape[1]
    high, rest = halves(v)
    pick = jnp.where((iota((chan, LANES), 0) >> 6) == iota((chan, LANES), 1), 1.0, 0.0).astype(BF16)
    return mm(high, pick) + mm(rest, pick)


def softplus(v):
    return jnp.maximum(v, 0.0) + jnp.log1p(jnp.exp(-jnp.abs(v)))


def sigmoid(v):
    return 1.0 / (1.0 + jnp.exp(-v))


def lower_mask():
    return iota((STRETCH, STRETCH), 0) >= iota((STRETCH, STRETCH), 1)


def convolve(xs_ref, taps_ref, bias_ref):
    total = bias_ref[...] + taps_ref[0:1, :] * xs_ref[5:5 + STRETCH, :]
    for tap in range(1, 4):
        total = total + taps_ref[tap:tap + 1, :] * xs_ref[5 + tap:5 + tap + STRETCH, :]
    return total


def decays(pre_dt, head_ref, valid):
    rates = softplus(pre_dt + head_ref[0:1, :]) * valid
    log_decay = rates * head_ref[1:2, :]
    lower = lower_mask().astype(F32)
    cumulative = exact(lower, log_decay)
    last = cumulative[STRETCH - 1:STRETCH, :]
    return rates, cumulative, jnp.exp(cumulative), jnp.exp(last - cumulative)


def weights_of(cumulative, across, head):
    return jnp.exp(jnp.minimum(cumulative[:, head:head + 1] - across[head:head + 1, :], 0.0))


def forward_kernel(
    open_ref, tok_ref, valid_ref, gain_ref, w_ref, taps_ref, bias_ref, head_ref, skip_ref,
    normed_ref, pre_ref, y_ref, gated_ref, sq_ref, enter_ref,
    state, xs,
):
    chan = y_ref.shape[1]
    block = pl.program_id(0)
    opening = open_ref[block] == 1

    @pl.when(opening)
    def _():
        state[...] = jnp.zeros_like(state)
        xs[0:8, :] = jnp.zeros((8, xs.shape[1]), F32)

    @pl.when(jnp.logical_not(opening))
    def _():
        xs[0:8, :] = xs[STRETCH:STRETCH + 8, :]

    valid = valid_ref[...]
    resid = tok_ref[...].astype(F32)
    rstd = lax.rsqrt(jnp.mean(resid * resid, axis=1, keepdims=True) + EPSILON)
    normed = (resid * rstd * gain_ref[...]).astype(BF16)
    normed_ref[...] = normed
    pre = mm(normed, w_ref[...])
    pre_ref[...] = pre
    xs[8:8 + STRETCH, :] = pre[:, chan:2 * chan + 2 * STATE]
    conv = convolve(xs, taps_ref, bias_ref)
    feats = conv * sigmoid(conv)
    x = feats[:, :chan]
    bs = feats[:, chan:chan + STATE].astype(BF16)
    cs = feats[:, chan + STATE:].astype(BF16)
    rates, cumulative, grown, to_end = decays(pre[:, 2 * chan + 2 * STATE:], head_ref, valid)
    across = cumulative.T
    grown_e = spread_heads(grown, chan)
    scaled = x * spread_heads(rates, chan)
    entering = state[...]
    enter_ref[0] = entering
    y_ref[...] = mm(cs, entering.astype(BF16)) * grown_e
    state[...] = entering * grown_e[STRETCH - 1:STRETCH, :] + mm(
        bs, (scaled * spread_heads(to_end, chan)).astype(BF16), TN
    )
    overlap = jnp.where(lower_mask(), mm(cs, bs, NT), 0.0)
    scaled_b = scaled.astype(BF16)
    first = iota((STRETCH, LANES), 1) < HEAD
    for pair in range(chan // LANES):
        cols = slice(pair * LANES, (pair + 1) * LANES)
        both = scaled_b[:, cols]
        mats = [
            (weights_of(cumulative, across, 2 * pair + side) * overlap).astype(BF16) for side in range(2)
        ]
        zero = jnp.zeros_like(both)
        y_ref[:, cols] += mm(
            jnp.concatenate(mats, axis=1),
            jnp.concatenate([jnp.where(first, both, zero), jnp.where(first, zero, both)], axis=0),
        )
    pre_z = pre[:, :chan]
    gated = (y_ref[...] + skip_ref[...] * x) * (pre_z * sigmoid(pre_z)) * valid
    gated_ref[...] = gated
    sq_ref[...] = jnp.sum(gated * gated, axis=1, keepdims=True)


def backward_kernel(
    open_ref, tok_ref, valid_ref, w_ref, taps_ref, bias_ref, head_ref, skip_ref, gate_ref,
    pre_ref, halo_ref, y_ref, enter_ref, dgn_ref, stats_ref,
    dpre_ref, dnormed_ref, dtaps_ref, dbias_ref, dhead_ref, dchan_ref, dgain_ref,
    dstate, xs, dus,
    *, inner,
):
    chan = y_ref.shape[1]
    wide = chan + 2 * STATE
    step = pl.program_id(0)
    block = pl.num_programs(0) - 1 - step
    opening = open_ref[block] == 1
    keep = jnp.where(opening, 0.0, 1.0).astype(F32)

    @pl.when(step == 0)
    def _():
        dstate[...] = jnp.zeros_like(dstate)
        dus[...] = jnp.zeros_like(dus)
        dtaps_ref[...] = jnp.zeros_like(dtaps_ref)
        dbias_ref[...] = jnp.zeros_like(dbias_ref)
        dhead_ref[...] = jnp.zeros_like(dhead_ref)
        dchan_ref[...] = jnp.zeros_like(dchan_ref)
        dgain_ref[...] = jnp.zeros_like(dgain_ref)

    valid = valid_ref[...]
    xs[0:8, :] = halo_ref[:, chan:2 * chan + 2 * STATE] * keep
    xs[8:8 + STRETCH, :] = pre_ref[:, chan:2 * chan + 2 * STATE]
    conv = convolve(xs, taps_ref, bias_ref)
    gate_u = sigmoid(conv)
    feats = conv * gate_u
    slope = gate_u * (1.0 + conv * (1.0 - gate_u))
    x = feats[:, :chan]
    bs = feats[:, chan:chan + STATE].astype(BF16)
    cs = feats[:, chan + STATE:].astype(BF16)
    pre_dt = pre_ref[:, 2 * chan + 2 * STATE:]
    rates, cumulative, grown, to_end = decays(pre_dt, head_ref, valid)
    across = cumulative.T
    grown_e = spread_heads(grown, chan)
    rates_e = spread_heads(rates, chan)
    to_end_e = spread_heads(to_end, chan)
    leave_e = grown_e[STRETCH - 1:STRETCH, :]

    pre_z = pre_ref[:, :chan]
    gate_z = sigmoid(pre_z)
    silu_z = pre_z * gate_z * valid
    y = y_ref[...]
    mixed = y + skip_ref[...] * x
    gated = mixed * silu_z
    grstd, cross = row_stats(stats_ref, inner)
    dgn = dgn_ref[...]
    d_gated = grstd * (gate_ref[...] * dgn) - gated * (grstd * grstd * grstd * cross * (1.0 / inner))
    d_mixed = d_gated * silu_z
    dpre_ref[:, :chan] = (
        d_gated * mixed * (valid * (gate_z * (1.0 + pre_z * (1.0 - gate_z))))
    ).astype(BF16)
    dchan_ref[0:1, :] += jnp.sum(dgn * gated * grstd, axis=0, keepdims=True)
    dchan_ref[1:2, :] += jnp.sum(d_mixed * x, axis=0, keepdims=True)

    dy_b = d_mixed.astype(BF16)
    dy = dy_b.astype(F32)
    scaled = x * rates_e
    scaled_b = scaled.astype(BF16)
    entering = enter_ref[0]
    d_leaving = dstate[...]
    d_leaving_b = d_leaving.astype(BF16)
    tail = mm(bs, d_leaving_b) * to_end_e
    overlap = jnp.where(lower_mask(), mm(cs, bs, NT), 0.0)
    first = iota((STRETCH, LANES), 1) < HEAD
    d_overlap = jnp.zeros((STRETCH, STRETCH), F32)
    parts = []
    for pair in range(chan // LANES):
        cols = slice(pair * LANES, (pair + 1) * LANES)
        dy_pair = dy_b[:, cols]
        x_pair = scaled_b[:, cols]
        zero = jnp.zeros_like(dy_pair)
        sides = [jnp.where(first, dy_pair, zero), jnp.where(first, zero, dy_pair)]
        mats = []
        for side in range(2):
            weight = weights_of(cumulative, across, 2 * pair + side)
            mats.append((weight * overlap).astype(BF16))
            d_overlap = d_overlap + mm(sides[side], x_pair, NT) * weight
        parts.append(mm(jnp.concatenate(mats, axis=0), jnp.concatenate(sides, axis=0), TN))
    d_scaled = jnp.concatenate(parts, axis=1) + tail
    scaled_r = scaled_b.astype(F32)
    d_cum = gather_heads(dy * y - scaled_r * d_scaled)
    d_last = jnp.sum(scaled_r * tail, axis=0, keepdims=True) + leave_e * jnp.sum(
        d_leaving * entering, axis=0, keepdims=True
    )
    d_last = gather_heads(jnp.broadcast_to(d_last, (8, chan)))[0:1, :]
    upper = (iota((STRETCH, STRETCH), 0) <= iota((STRETCH, STRETCH), 1)).astype(F32)
    d_log = exact(upper, d_cum) + d_last
    decay = head_ref[1:2, :]
    d_rates = d_log * decay + gather_heads(x * d_scaled)
    d_dt = d_rates * valid * sigmoid(pre_dt + head_ref[0:1, :])
    dhead_ref[0:1, :] += jnp.sum(d_log * rates, axis=0, keepdims=True) * decay
    dhead_ref[1:2, :] += jnp.sum(d_dt, axis=0, keepdims=True)
    dpre_ref[:, 2 * chan + 2 * STATE:] = d_dt.astype(BF16)

    d_x = d_scaled * rates_e + skip_ref[...] * d_mixed
    d_overlap_b = jnp.where(lower_mask(), d_overlap, 0.0).astype(BF16)
    dy_grown = (dy * grown_e).astype(BF16)
    x_end = (scaled * to_end_e).astype(BF16)
    d_b = mm(d_overlap_b, cs, TN) + mm(x_end, d_leaving_b, NT)
    d_c = mm(d_overlap_b, bs) + mm(dy_grown, entering.astype(BF16), NT)
    dstate[...] = (d_leaving * leave_e + mm(cs, dy_grown, TN)) * keep

    dus[0:STRETCH, :chan] = d_x * slope[:, :chan]
    dus[0:STRETCH, chan:chan + STATE] = d_b * slope[:, chan:chan + STATE]
    dus[0:STRETCH, chan + STATE:] = d_c * slope[:, chan + STATE:]
    d_conv = dus[0:STRETCH, :]
    dbias_ref[...] += jnp.sum(d_conv, axis=0, keepdims=True)
    d_pre = jnp.zeros((STRETCH, wide), F32)
    for tap in range(4):
        dtaps_ref[tap:tap + 1, :] += jnp.sum(d_conv * xs[5 + tap:5 + tap + STRETCH, :], axis=0, keepdims=True)
        d_pre = d_pre + taps_ref[tap:tap + 1, :] * dus[3 - tap:3 - tap + STRETCH, :]
    dpre_ref[:, chan:2 * chan + 2 * STATE] = d_pre.astype(BF16)
    dus[STRETCH:STRETCH + 8, :] = d_conv[0:8, :] * keep

    d_normed = mm(dpre_ref[...], w_ref[...], NT)
    dnormed_ref[...] = d_normed.astype(BF16)
    resid = tok_ref[...].astype(F32)
    rstd = lax.rsqrt(jnp.mean(resid * resid, axis=1, keepdims=True) + EPSILON)
    dgain_ref[...] += jnp.sum(d_normed * (resid * rstd), axis=0, keepdims=True)


def whole(shape):
    return pl.BlockSpec(shape, lambda *_: (0,) * len(shape), pipeline_mode=pl.Buffered(1))


def mixer_forward(openings, tok, valid, gain, w_in, taps, bias, heads, skip):
    tokens, width = tok.shape
    cols = w_in.shape[1]
    chan = skip.shape[1]
    blocks = tokens // STRETCH
    wide = chan + 2 * STATE
    rows = lambda n: pl.BlockSpec((STRETCH, n), lambda i, *_: (i, 0))
    return pl.pallas_call(
        forward_kernel,
        name="mixer_forward",
        grid_spec=pltpu.PrefetchScalarGridSpec(
            num_scalar_prefetch=1,
            grid=(blocks,),
            in_specs=[
                rows(width), rows(1), whole((1, width)), whole((width, cols)), whole((4, wide)), whole((1, wide)),
                whole((8, LANES)), whole((1, chan)),
            ],
            out_specs=[
                rows(width), rows(cols), rows(chan), rows(chan), rows(1),
                pl.BlockSpec((1, STATE, chan), lambda i, *_: (i, 0, 0)),
            ],
            scratch_shapes=[
                pltpu.VMEM((STATE, chan), F32),
                pltpu.VMEM((STRETCH + 8, wide), F32),
            ],
        ),
        out_shape=[
            jax.ShapeDtypeStruct((tokens, width), BF16),
            jax.ShapeDtypeStruct((tokens, cols), F32),
            jax.ShapeDtypeStruct((tokens, chan), F32),
            jax.ShapeDtypeStruct((tokens, chan), F32),
            jax.ShapeDtypeStruct((tokens, 1), F32),
            jax.ShapeDtypeStruct((blocks, STATE, chan), F32),
        ],
        cost_estimate=pl.CostEstimate(
            flops=2 * tokens * width * cols, bytes_accessed=tokens * cols * 12, transcendentals=tokens * chan
        ),
        compiler_params=pltpu.CompilerParams(vmem_limit_bytes=60 << 20, dimension_semantics=("arbitrary",)),
    )(openings, tok, valid, gain, w_in, taps, bias, heads, skip)


def mixer_backward(
    openings, tok, valid, w_in, taps, bias, heads, skip, gate, pre, y, enter, dgn, stats, inner
):
    tokens, width = tok.shape
    cols = w_in.shape[1]
    chan = skip.shape[1]
    blocks = tokens // STRETCH
    wide = chan + 2 * STATE
    per = STRETCH // 8
    rows = lambda n: pl.BlockSpec((STRETCH, n), lambda i, *_: (blocks - 1 - i, 0))
    return pl.pallas_call(
        functools.partial(backward_kernel, inner=inner),
        name="mixer_backward",
        grid_spec=pltpu.PrefetchScalarGridSpec(
            num_scalar_prefetch=1,
            grid=(blocks,),
            in_specs=[
                rows(width), rows(1), whole((width, cols)), whole((4, wide)), whole((1, wide)),
                whole((8, LANES)), whole((1, chan)), whole((1, chan)),
                rows(cols),
                pl.BlockSpec((8, cols), lambda i, *_: (jnp.maximum((blocks - 1 - i) * per - 1, 0), 0)),
                rows(chan),
                pl.BlockSpec((1, STATE, chan), lambda i, *_: (blocks - 1 - i, 0, 0)),
                rows(chan),
                pl.BlockSpec((8, STRETCH), lambda i, *_: (0, blocks - 1 - i)),
            ],
            out_specs=[
                rows(cols), rows(width),
                pl.BlockSpec((8, wide), lambda i, *_: (0, 0)),
                pl.BlockSpec((1, wide), lambda i, *_: (0, 0)),
                pl.BlockSpec((8, LANES), lambda i, *_: (0, 0)),
                pl.BlockSpec((8, chan), lambda i, *_: (0, 0)),
                pl.BlockSpec((1, width), lambda i, *_: (0, 0)),
            ],
            scratch_shapes=[
                pltpu.VMEM((STATE, chan), F32),
                pltpu.VMEM((STRETCH + 8, wide), F32),
                pltpu.VMEM((STRETCH + 8, wide), F32),
            ],
        ),
        out_shape=[
            jax.ShapeDtypeStruct((tokens, cols), BF16),
            jax.ShapeDtypeStruct((tokens, width), BF16),
            jax.ShapeDtypeStruct((8, wide), F32),
            jax.ShapeDtypeStruct((1, wide), F32),
            jax.ShapeDtypeStruct((8, LANES), F32),
            jax.ShapeDtypeStruct((8, chan), F32),
            jax.ShapeDtypeStruct((1, width), F32),
        ],
        cost_estimate=pl.CostEstimate(
            flops=4 * tokens * width * cols, bytes_accessed=tokens * cols * 12, transcendentals=tokens * chan
        ),
        compiler_params=pltpu.CompilerParams(vmem_limit_bytes=60 << 20, dimension_semantics=("arbitrary",)),
    )(openings, tok, valid, w_in, taps, bias, heads, skip, gate, pre, pre, y, enter, dgn, stats)


def stats_kernel(cot_ref, wout_ref, gate_ref, gated_ref, sq_ref, dgn_ref, stats_ref):
    dgn = mm(cot_ref[...], wout_ref[...])
    dgn_ref[...] = dgn
    cross = jnp.sum(gate_ref[...] * dgn * gated_ref[...], axis=1, keepdims=True)
    lane = iota((STRETCH, LANES), 1)
    both = jnp.where(lane == 0, sq_ref[...], 0.0) + jnp.where(lane == 1, cross, 0.0)
    stats_ref[...] = both.T[0:8, :]


def row_stats(stats_ref, inner):
    filled = jnp.concatenate([stats_ref[...], jnp.zeros((LANES - 8, STRETCH), F32)], axis=0).T
    grstd = lax.rsqrt(filled[:, 0:1] * (1.0 / inner) + EPSILON)
    return grstd, filled[:, 1:2]


def output_kernel(gated_ref, stats_ref, gate_ref, wout_ref, gnormed_ref, out_ref, *, inner):
    grstd, _ = row_stats(stats_ref, inner)
    gnormed = (gated_ref[...] * grstd * gate_ref[...]).astype(BF16)
    gnormed_ref[...] = gnormed
    out_ref[...] = mm(gnormed, wout_ref[...], NT).astype(BF16)


def gate_stats(cot, wout, gate, gated, sq):
    tokens, width = cot.shape
    chan = gate.shape[1]
    rows = lambda n: pl.BlockSpec((STRETCH, n), lambda i: (i, 0))
    return pl.pallas_call(
        stats_kernel,
        name="gate_stats",
        grid=(tokens // STRETCH,),
        in_specs=[rows(width), whole((width, chan)), whole((1, chan)), rows(chan), rows(1)],
        out_specs=[rows(chan), pl.BlockSpec((8, STRETCH), lambda i: (0, i))],
        out_shape=[jax.ShapeDtypeStruct((tokens, chan), F32), jax.ShapeDtypeStruct((8, tokens), F32)],
        cost_estimate=pl.CostEstimate(
            flops=2 * tokens * width * chan, bytes_accessed=tokens * (2 * width + 8 * chan), transcendentals=0
        ),
        compiler_params=pltpu.CompilerParams(vmem_limit_bytes=40 << 20),
    )(cot, wout, gate, gated, sq)


def output_part(gated, stats, gate, wout, inner):
    tokens, chan = gated.shape
    width = wout.shape[0]
    rows = lambda n: pl.BlockSpec((STRETCH, n), lambda i: (i, 0))
    return pl.pallas_call(
        functools.partial(output_kernel, inner=inner),
        name="output_part",
        grid=(tokens // STRETCH,),
        in_specs=[rows(chan), pl.BlockSpec((8, STRETCH), lambda i: (0, i)), whole((1, chan)), whole((width, chan))],
        out_specs=[rows(chan), rows(width)],
        out_shape=[jax.ShapeDtypeStruct((tokens, chan), BF16), jax.ShapeDtypeStruct((tokens, width), BF16)],
        cost_estimate=pl.CostEstimate(
            flops=2 * tokens * width * chan, bytes_accessed=tokens * (2 * width + 4 * chan), transcendentals=0
        ),
        compiler_params=pltpu.CompilerParams(vmem_limit_bytes=40 << 20),
    )(gated, stats, gate, wout)


def padded(v, fill):
    return jnp.pad(v[None, :], ((0, 0), (0, LANES - v.shape[0])), constant_values=fill)


def shards(
    tokens, cotangent, seq_start, token_valid, norm_gain, proj_z, proj_x, proj_bc, proj_dt, conv_chan, bias_chan,
    conv_shared, bias_shared, a_log, dt_bias, skip_gain, gate_gain, proj_out,
):
    chan = proj_z.shape[1]
    width = tokens.shape[1]
    heads_here = proj_dt.shape[1]
    inner = chan * lax.axis_size("tp")
    wide = chan + 2 * STATE
    valid = token_valid.astype(F32)[:, None]
    pack_in = jnp.concatenate(
        [proj_z, proj_x, proj_bc, jnp.pad(proj_dt, ((0, 0), (0, LANES - heads_here)))], axis=1
    )
    tok_all = lax.all_gather(tokens, "tp", axis=0, tiled=True)
    w_in = lax.all_gather(pack_in, "fsdp", axis=0, tiled=True)
    w_out = lax.all_gather(proj_out.T, "fsdp", axis=0, tiled=True)
    cot_all = lax.all_gather(cotangent, "tp", axis=0, tiled=True)
    decay = -jnp.exp(a_log)
    heads = jnp.concatenate([padded(dt_bias, -100.0), padded(decay, 0.0), jnp.zeros((6, LANES), F32)], axis=0)
    taps = jnp.concatenate([conv_chan, conv_shared], axis=1)
    bias = jnp.concatenate([bias_chan, bias_shared])[None, :]
    skip = jnp.repeat(skip_gain, HEAD)[None, :]
    gate = gate_gain[None, :]
    normed, pre, y, gated, sq, enter = mixer_forward(
        seq_start, tok_all, valid, norm_gain[None, :], w_in, taps, bias, heads, skip
    )
    dgn, stats = gate_stats(cot_all, w_out, gate, gated, sq)
    stats = lax.psum(stats, "tp")
    gnormed, out_rows = output_part(gated, stats, gate, w_out, inner)
    mixed = lax.psum_scatter(out_rows, "tp", scatter_dimension=0, tiled=True)
    dpre, dn_rows, dtaps, dbias, dhead, dchan, dgain = mixer_backward(
        seq_start, tok_all, valid, w_in, taps, bias, heads, skip, gate, pre, y, enter, dgn, stats, inner
    )
    d_normed = lax.psum_scatter(dn_rows, "tp", scatter_dimension=0, tiled=True).astype(F32)
    grad_in = jnp.einsum("td,tc->dc", normed, dpre, preferred_element_type=F32).astype(BF16)
    grad_out = jnp.einsum("td,tc->dc", cot_all, gnormed, preferred_element_type=F32).astype(BF16)
    own_in = lax.psum_scatter(grad_in, "fsdp", scatter_dimension=0, tiled=True).astype(F32)
    own_out = lax.psum_scatter(grad_out, "fsdp", scatter_dimension=0, tiled=True).astype(F32)
    mine = jnp.concatenate([v.reshape(-1) for v in (dtaps[0:4, :chan], dbias[:, :chan], dhead[0:2], dchan[0:2])])
    shared = jnp.concatenate([v.reshape(-1) for v in (dtaps[0:4, chan:], dbias[:, chan:], dgain)])
    split = mine.shape[0]
    both = lax.psum(jnp.concatenate([mine, shared]), "fsdp")
    mine = both[:split]
    shared, own_bc = lax.psum((both[split:], own_in[:, 2 * chan:wide + chan]), "tp")
    at = 0

    def take(source, *shape):
        nonlocal at
        size = 1
        for extent in shape:
            size *= extent
        part = source[at:at + size].reshape(shape)
        at += size
        return part

    g_taps, g_bias, g_heads, g_chan = (
        take(mine, 4, chan), take(mine, chan), take(mine, 2, LANES), take(mine, 2, chan),
    )
    at = 0
    g_taps_s, g_bias_s, g_gain = take(shared, 4, 2 * STATE), take(shared, 2 * STATE), take(shared, width)
    resid = tokens.astype(F32)
    rstd = lax.rsqrt(jnp.mean(resid * resid, axis=1, keepdims=True) + EPSILON)
    output = (resid + mixed.astype(F32)).astype(BF16)
    scaled_in = d_normed * norm_gain[None, :]
    grad_tokens = (
        cotangent.astype(F32) + rstd * scaled_in
        - resid * (rstd * rstd * rstd) * jnp.mean(scaled_in * resid, axis=1, keepdims=True)
    ).astype(BF16)
    return (
        output, grad_tokens, g_gain, own_in[:, :chan], own_in[:, chan:2 * chan], own_bc,
        own_in[:, wide + chan:wide + chan + heads_here], g_taps, g_bias, g_taps_s, g_bias_s,
        g_heads[0, :heads_here], g_heads[1, :heads_here], g_chan[1].reshape(heads_here, HEAD).sum(axis=1),
        g_chan[0], own_out.T,
    )


def solution(mesh):
    in_specs = (
        P(("fsdp", "tp"), None), P(("fsdp", "tp"), None), P("fsdp"), P("fsdp"), P(), P("fsdp", "tp"),
        P("fsdp", "tp"), P("fsdp", None), P("fsdp", "tp"), P(None, "tp"), P("tp"), P(), P(), P("tp"), P("tp"),
        P("tp"), P("tp"), P("tp", "fsdp"),
    )
    out_specs = (
        P(("fsdp", "tp"), None), P(("fsdp", "tp"), None), P(), P("fsdp", "tp"), P("fsdp", "tp"), P("fsdp", None),
        P("fsdp", "tp"), P(None, "tp"), P("tp"), P(), P(), P("tp"), P("tp"), P("tp"), P("tp"), P("tp", "fsdp"),
    )
    return jax.shard_map(shards, mesh=mesh, in_specs=in_specs, out_specs=out_specs, check_vma=False)
```

```python
import functools
import jax
import jax.numpy as jnp
from jax import lax
from jax.experimental import pallas as pl
from jax.experimental.pallas import tpu as pltpu
from jax.sharding import PartitionSpec as P

HEAD = 64
STATE = 128
STRETCH = 256
LANES = 128
EPSILON = 1e-05
F32 = jnp.float32
BF16 = jnp.bfloat16
NN = (((1,), (0,)), ((), ()))
NT = (((1,), (1,)), ((), ()))
TN = (((0,), (0,)), ((), ()))


def mm(a, b, dims=NN):
    return lax.dot_general(a, b, dims, preferred_element_type=F32)


def exact(a, b):
    return lax.dot_general(a, b, NN, precision=lax.Precision.HIGHEST, preferred_element_type=F32)


def halves(v):
    high = v.astype(BF16)
    return high, (v - high.astype(F32)).astype(BF16)


def iota(shape, dim):
    return lax.broadcasted_iota(jnp.int32, shape, dim)


def spread_heads(v, chan):
    high, rest = halves(v)
    rows = iota((2 * LANES, chan), 0) & (LANES - 1)
    pick = jnp.where(rows == (iota((2 * LANES, chan), 1) >> 6), 1.0, 0.0).astype(BF16)
    return mm(jnp.concatenate([high, rest], axis=1), pick)


def gather_heads(v):
    chan = v.shape[1]
    high, rest = halves(v)
    pick = jnp.where((iota((chan, LANES), 0) >> 6) == iota((chan, LANES), 1), 1.0, 0.0).astype(BF16)
    return mm(high, pick) + mm(rest, pick)


def softplus(v):
    return jnp.maximum(v, 0.0) + jnp.log1p(jnp.exp(-jnp.abs(v)))


def sigmoid(v):
    return 1.0 / (1.0 + jnp.exp(-v))


def lower_mask():
    return iota((STRETCH, STRETCH), 0) >= iota((STRETCH, STRETCH), 1)


def convolve(xs_ref, taps_ref, bias_ref):
    total = bias_ref[...] + taps_ref[0:1, :] * xs_ref[5:5 + STRETCH, :]
    for tap in range(1, 4):
        total = total + taps_ref[tap:tap + 1, :] * xs_ref[5 + tap:5 + tap + STRETCH, :]
    return total


def decays(pre_dt, head_ref, valid):
    rates = softplus(pre_dt + head_ref[0:1, :]) * valid
    log_decay = rates * head_ref[1:2, :]
    lower = lower_mask().astype(F32)
    cumulative = exact(lower, log_decay)
    last = cumulative[STRETCH - 1:STRETCH, :]
    return rates, cumulative, jnp.exp(cumulative), jnp.exp(last - cumulative)


def weights_of(cumulative, across, head):
    return jnp.exp(jnp.minimum(cumulative[:, head:head + 1] - across[head:head + 1, :], 0.0))


def forward_kernel(
    open_ref, tok_ref, valid_ref, gain_ref, w_ref, taps_ref, bias_ref, head_ref, skip_ref,
    normed_ref, pre_ref, y_ref, gated_ref, sq_ref, enter_ref,
    state, xs,
):
    chan = y_ref.shape[1]
    block = pl.program_id(0)
    opening = open_ref[block] == 1

    @pl.when(opening)
    def _():
        state[...] = jnp.zeros_like(state)
        xs[0:8, :] = jnp.zeros((8, xs.shape[1]), F32)

    @pl.when(jnp.logical_not(opening))
    def _():
        xs[0:8, :] = xs[STRETCH:STRETCH + 8, :]

    valid = valid_ref[...]
    resid = tok_ref[...].astype(F32)
    rstd = lax.rsqrt(jnp.mean(resid * resid, axis=1, keepdims=True) + EPSILON)
    normed = (resid * rstd * gain_ref[...]).astype(BF16)
    normed_ref[...] = normed
    pre = mm(normed, w_ref[...])
    pre_ref[...] = pre
    xs[8:8 + STRETCH, :] = pre[:, chan:2 * chan + 2 * STATE]
    conv = convolve(xs, taps_ref, bias_ref)
    feats = conv * sigmoid(conv)
    x = feats[:, :chan]
    bs = feats[:, chan:chan + STATE].astype(BF16)
    cs = feats[:, chan + STATE:].astype(BF16)
    rates, cumulative, grown, to_end = decays(pre[:, 2 * chan + 2 * STATE:], head_ref, valid)
    across = cumulative.T
    grown_e = spread_heads(grown, chan)
    scaled = x * spread_heads(rates, chan)
    entering = state[...]
    enter_ref[0] = entering
    y_ref[...] = mm(cs, entering.astype(BF16)) * grown_e
    state[...] = entering * grown_e[STRETCH - 1:STRETCH, :] + mm(
        bs, (scaled * spread_heads(to_end, chan)).astype(BF16), TN
    )
    overlap = jnp.where(lower_mask(), mm(cs, bs, NT), 0.0)
    scaled_b = scaled.astype(BF16)
    first = iota((STRETCH, LANES), 1) < HEAD
    for pair in range(chan // LANES):
        cols = slice(pair * LANES, (pair + 1) * LANES)
        both = scaled_b[:, cols]
        mats = [
            (weights_of(cumulative, across, 2 * pair + side) * overlap).astype(BF16) for side in range(2)
        ]
        zero = jnp.zeros_like(both)
        y_ref[:, cols] += mm(
            jnp.concatenate(mats, axis=1),
            jnp.concatenate([jnp.where(first, both, zero), jnp.where(first, zero, both)], axis=0),
        )
    pre_z = pre[:, :chan]
    gated = (y_ref[...] + skip_ref[...] * x) * (pre_z * sigmoid(pre_z)) * valid
    gated_ref[...] = gated
    sq_ref[...] = jnp.sum(gated * gated, axis=1, keepdims=True)


def backward_kernel(
    open_ref, tok_ref, valid_ref, w_ref, taps_ref, bias_ref, head_ref, skip_ref, gate_ref,
    pre_ref, halo_ref, y_ref, enter_ref, dgn_ref, stats_ref,
    dpre_ref, dnormed_ref, dtaps_ref, dbias_ref, dhead_ref, dchan_ref, dgain_ref,
    dstate, xs, dus,
    *, inner,
):
    chan = y_ref.shape[1]
    wide = chan + 2 * STATE
    step = pl.program_id(0)
    block = pl.num_programs(0) - 1 - step
    opening = open_ref[block] == 1
    keep = jnp.where(opening, 0.0, 1.0).astype(F32)

    @pl.when(step == 0)
    def _():
        dstate[...] = jnp.zeros_like(dstate)
        dus[...] = jnp.zeros_like(dus)
        dtaps_ref[...] = jnp.zeros_like(dtaps_ref)
        dbias_ref[...] = jnp.zeros_like(dbias_ref)
        dhead_ref[...] = jnp.zeros_like(dhead_ref)
        dchan_ref[...] = jnp.zeros_like(dchan_ref)
        dgain_ref[...] = jnp.zeros_like(dgain_ref)

    valid = valid_ref[...]
    xs[0:8, :] = halo_ref[:, chan:2 * chan + 2 * STATE] * keep
    xs[8:8 + STRETCH, :] = pre_ref[:, chan:2 * chan + 2 * STATE]
    conv = convolve(xs, taps_ref, bias_ref)
    gate_u = sigmoid(conv)
    feats = conv * gate_u
    slope = gate_u * (1.0 + conv * (1.0 - gate_u))
    x = feats[:, :chan]
    bs = feats[:, chan:chan + STATE].astype(BF16)
    cs = feats[:, chan + STATE:].astype(BF16)
    pre_dt = pre_ref[:, 2 * chan + 2 * STATE:]
    rates, cumulative, grown, to_end = decays(pre_dt, head_ref, valid)
    across = cumulative.T
    grown_e = spread_heads(grown, chan)
    rates_e = spread_heads(rates, chan)
    to_end_e = spread_heads(to_end, chan)
    leave_e = grown_e[STRETCH - 1:STRETCH, :]

    pre_z = pre_ref[:, :chan]
    gate_z = sigmoid(pre_z)
    silu_z = pre_z * gate_z * valid
    y = y_ref[...]
    mixed = y + skip_ref[...] * x
    gated = mixed * silu_z
    grstd, cross = row_stats(stats_ref, inner)
    dgn = dgn_ref[...]
    d_gated = grstd * (gate_ref[...] * dgn) - gated * (grstd * grstd * grstd * cross * (1.0 / inner))
    d_mixed = d_gated * silu_z
    dpre_ref[:, :chan] = (
        d_gated * mixed * (valid * (gate_z * (1.0 + pre_z * (1.0 - gate_z))))
    ).astype(BF16)
    dchan_ref[0:1, :] += jnp.sum(dgn * gated * grstd, axis=0, keepdims=True)
    dchan_ref[1:2, :] += jnp.sum(d_mixed * x, axis=0, keepdims=True)

    dy_b = d_mixed.astype(BF16)
    dy = dy_b.astype(F32)
    scaled = x * rates_e
    scaled_b = scaled.astype(BF16)
    entering = enter_ref[0]
    d_leaving = dstate[...]
    d_leaving_b = d_leaving.astype(BF16)
    tail = mm(bs, d_leaving_b) * to_end_e
    overlap = jnp.where(lower_mask(), mm(cs, bs, NT), 0.0)
    first = iota((STRETCH, LANES), 1) < HEAD
    d_overlap = jnp.zeros((STRETCH, STRETCH), F32)
    parts = []
    for pair in range(chan // LANES):
        cols = slice(pair * LANES, (pair + 1) * LANES)
        dy_pair = dy_b[:, cols]
        x_pair = scaled_b[:, cols]
        zero = jnp.zeros_like(dy_pair)
        sides = [jnp.where(first, dy_pair, zero), jnp.where(first, zero, dy_pair)]
        mats = []
        for side in range(2):
            weight = weights_of(cumulative, across, 2 * pair + side)
            mats.append((weight * overlap).astype(BF16))
            d_overlap = d_overlap + mm(sides[side], x_pair, NT) * weight
        parts.append(mm(jnp.concatenate(mats, axis=0), jnp.concatenate(sides, axis=0), TN))
    d_scaled = jnp.concatenate(parts, axis=1) + tail
    scaled_r = scaled_b.astype(F32)
    d_cum = gather_heads(dy * y - scaled_r * d_scaled)
    d_last = jnp.sum(scaled_r * tail, axis=0, keepdims=True) + leave_e * jnp.sum(
        d_leaving * entering, axis=0, keepdims=True
    )
    d_last = gather_heads(jnp.broadcast_to(d_last, (8, chan)))[0:1, :]
    upper = (iota((STRETCH, STRETCH), 0) <= iota((STRETCH, STRETCH), 1)).astype(F32)
    d_log = exact(upper, d_cum) + d_last
    decay = head_ref[1:2, :]
    d_rates = d_log * decay + gather_heads(x * d_scaled)
    d_dt = d_rates * valid * sigmoid(pre_dt + head_ref[0:1, :])
    dhead_ref[0:1, :] += jnp.sum(d_log * rates, axis=0, keepdims=True) * decay
    dhead_ref[1:2, :] += jnp.sum(d_dt, axis=0, keepdims=True)
    dpre_ref[:, 2 * chan + 2 * STATE:] = d_dt.astype(BF16)

    d_x = d_scaled * rates_e + skip_ref[...] * d_mixed
    d_overlap_b = jnp.where(lower_mask(), d_overlap, 0.0).astype(BF16)
    dy_grown = (dy * grown_e).astype(BF16)
    x_end = (scaled * to_end_e).astype(BF16)
    d_b = mm(d_overlap_b, cs, TN) + mm(x_end, d_leaving_b, NT)
    d_c = mm(d_overlap_b, bs) + mm(dy_grown, entering.astype(BF16), NT)
    dstate[...] = (d_leaving * leave_e + mm(cs, dy_grown, TN)) * keep

    dus[0:STRETCH, :chan] = d_x * slope[:, :chan]
    dus[0:STRETCH, chan:chan + STATE] = d_b * slope[:, chan:chan + STATE]
    dus[0:STRETCH, chan + STATE:] = d_c * slope[:, chan + STATE:]
    d_conv = dus[0:STRETCH, :]
    dbias_ref[...] += jnp.sum(d_conv, axis=0, keepdims=True)
    d_pre = jnp.zeros((STRETCH, wide), F32)
    for tap in range(4):
        dtaps_ref[tap:tap + 1, :] += jnp.sum(d_conv * xs[5 + tap:5 + tap + STRETCH, :], axis=0, keepdims=True)
        d_pre = d_pre + taps_ref[tap:tap + 1, :] * dus[3 - tap:3 - tap + STRETCH, :]
    dpre_ref[:, chan:2 * chan + 2 * STATE] = d_pre.astype(BF16)
    dus[STRETCH:STRETCH + 8, :] = d_conv[0:8, :] * keep

    d_normed = mm(dpre_ref[...], w_ref[...], NT)
    dnormed_ref[...] = d_normed.astype(BF16)
    resid = tok_ref[...].astype(F32)
    rstd = lax.rsqrt(jnp.mean(resid * resid, axis=1, keepdims=True) + EPSILON)
    dgain_ref[...] += jnp.sum(d_normed * (resid * rstd), axis=0, keepdims=True)


def whole(shape):
    return pl.BlockSpec(shape, lambda *_: (0,) * len(shape), pipeline_mode=pl.Buffered(1))


def mixer_forward(openings, tok, valid, gain, w_in, taps, bias, heads, skip):
    tokens, width = tok.shape
    cols = w_in.shape[1]
    chan = skip.shape[1]
    blocks = tokens // STRETCH
    wide = chan + 2 * STATE
    rows = lambda n: pl.BlockSpec((STRETCH, n), lambda i, *_: (i, 0))
    return pl.pallas_call(
        forward_kernel,
        name="mixer_forward",
        grid_spec=pltpu.PrefetchScalarGridSpec(
            num_scalar_prefetch=1,
            grid=(blocks,),
            in_specs=[
                rows(width), rows(1), whole((1, width)), whole((width, cols)), whole((4, wide)), whole((1, wide)),
                whole((8, LANES)), whole((1, chan)),
            ],
            out_specs=[
                rows(width), rows(cols), rows(chan), rows(chan), rows(1),
                pl.BlockSpec((1, STATE, chan), lambda i, *_: (i, 0, 0)),
            ],
            scratch_shapes=[
                pltpu.VMEM((STATE, chan), F32),
                pltpu.VMEM((STRETCH + 8, wide), F32),
            ],
        ),
        out_shape=[
            jax.ShapeDtypeStruct((tokens, width), BF16),
            jax.ShapeDtypeStruct((tokens, cols), F32),
            jax.ShapeDtypeStruct((tokens, chan), F32),
            jax.ShapeDtypeStruct((tokens, chan), F32),
            jax.ShapeDtypeStruct((tokens, 1), F32),
            jax.ShapeDtypeStruct((blocks, STATE, chan), F32),
        ],
        cost_estimate=pl.CostEstimate(
            flops=2 * tokens * width * cols, bytes_accessed=tokens * cols * 12, transcendentals=tokens * chan
        ),
        compiler_params=pltpu.CompilerParams(vmem_limit_bytes=60 << 20, dimension_semantics=("arbitrary",)),
    )(openings, tok, valid, gain, w_in, taps, bias, heads, skip)


def mixer_backward(
    openings, tok, valid, w_in, taps, bias, heads, skip, gate, pre, y, enter, dgn, stats, inner
):
    tokens, width = tok.shape
    cols = w_in.shape[1]
    chan = skip.shape[1]
    blocks = tokens // STRETCH
    wide = chan + 2 * STATE
    per = STRETCH // 8
    rows = lambda n: pl.BlockSpec((STRETCH, n), lambda i, *_: (blocks - 1 - i, 0))
    return pl.pallas_call(
        functools.partial(backward_kernel, inner=inner),
        name="mixer_backward",
        grid_spec=pltpu.PrefetchScalarGridSpec(
            num_scalar_prefetch=1,
            grid=(blocks,),
            in_specs=[
                rows(width), rows(1), whole((width, cols)), whole((4, wide)), whole((1, wide)),
                whole((8, LANES)), whole((1, chan)), whole((1, chan)),
                rows(cols),
                pl.BlockSpec((8, cols), lambda i, *_: (jnp.maximum((blocks - 1 - i) * per - 1, 0), 0)),
                rows(chan),
                pl.BlockSpec((1, STATE, chan), lambda i, *_: (blocks - 1 - i, 0, 0)),
                rows(chan),
                pl.BlockSpec((8, STRETCH), lambda i, *_: (0, blocks - 1 - i)),
            ],
            out_specs=[
                rows(cols), rows(width),
                pl.BlockSpec((8, wide), lambda i, *_: (0, 0)),
                pl.BlockSpec((1, wide), lambda i, *_: (0, 0)),
                pl.BlockSpec((8, LANES), lambda i, *_: (0, 0)),
                pl.BlockSpec((8, chan), lambda i, *_: (0, 0)),
                pl.BlockSpec((1, width), lambda i, *_: (0, 0)),
            ],
            scratch_shapes=[
                pltpu.VMEM((STATE, chan), F32),
                pltpu.VMEM((STRETCH + 8, wide), F32),
                pltpu.VMEM((STRETCH + 8, wide), F32),
            ],
        ),
        out_shape=[
            jax.ShapeDtypeStruct((tokens, cols), BF16),
            jax.ShapeDtypeStruct((tokens, width), BF16),
            jax.ShapeDtypeStruct((8, wide), F32),
            jax.ShapeDtypeStruct((1, wide), F32),
            jax.ShapeDtypeStruct((8, LANES), F32),
            jax.ShapeDtypeStruct((8, chan), F32),
            jax.ShapeDtypeStruct((1, width), F32),
        ],
        cost_estimate=pl.CostEstimate(
            flops=4 * tokens * width * cols, bytes_accessed=tokens * cols * 12, transcendentals=tokens * chan
        ),
        compiler_params=pltpu.CompilerParams(vmem_limit_bytes=60 << 20, dimension_semantics=("arbitrary",)),
    )(openings, tok, valid, w_in, taps, bias, heads, skip, gate, pre, pre, y, enter, dgn, stats)


def stats_kernel(cot_ref, wout_ref, gate_ref, gated_ref, sq_ref, dgn_ref, stats_ref):
    dgn = mm(cot_ref[...], wout_ref[...])
    dgn_ref[...] = dgn
    cross = jnp.sum(gate_ref[...] * dgn * gated_ref[...], axis=1, keepdims=True)
    lane = iota((STRETCH, LANES), 1)
    both = jnp.where(lane == 0, sq_ref[...], 0.0) + jnp.where(lane == 1, cross, 0.0)
    stats_ref[...] = both.T[0:8, :]


def row_stats(stats_ref, inner):
    filled = jnp.concatenate([stats_ref[...], jnp.zeros((LANES - 8, STRETCH), F32)], axis=0).T
    grstd = lax.rsqrt(filled[:, 0:1] * (1.0 / inner) + EPSILON)
    return grstd, filled[:, 1:2]


def output_kernel(gated_ref, stats_ref, gate_ref, wout_ref, gnormed_ref, out_ref, *, inner):
    grstd, _ = row_stats(stats_ref, inner)
    gnormed = (gated_ref[...] * grstd * gate_ref[...]).astype(BF16)
    gnormed_ref[...] = gnormed
    out_ref[...] = mm(gnormed, wout_ref[...], NT).astype(BF16)


def gate_stats(cot, wout, gate, gated, sq):
    tokens, width = cot.shape
    chan = gate.shape[1]
    rows = lambda n: pl.BlockSpec((STRETCH, n), lambda i: (i, 0))
    return pl.pallas_call(
        stats_kernel,
        name="gate_stats",
        grid=(tokens // STRETCH,),
        in_specs=[rows(width), whole((width, chan)), whole((1, chan)), rows(chan), rows(1)],
        out_specs=[rows(chan), pl.BlockSpec((8, STRETCH), lambda i: (0, i))],
        out_shape=[jax.ShapeDtypeStruct((tokens, chan), F32), jax.ShapeDtypeStruct((8, tokens), F32)],
        cost_estimate=pl.CostEstimate(
            flops=2 * tokens * width * chan, bytes_accessed=tokens * (2 * width + 8 * chan), transcendentals=0
        ),
        compiler_params=pltpu.CompilerParams(vmem_limit_bytes=40 << 20),
    )(cot, wout, gate, gated, sq)


def output_part(gated, stats, gate, wout, inner):
    tokens, chan = gated.shape
    width = wout.shape[0]
    rows = lambda n: pl.BlockSpec((STRETCH, n), lambda i: (i, 0))
    return pl.pallas_call(
        functools.partial(output_kernel, inner=inner),
        name="output_part",
        grid=(tokens // STRETCH,),
        in_specs=[rows(chan), pl.BlockSpec((8, STRETCH), lambda i: (0, i)), whole((1, chan)), whole((width, chan))],
        out_specs=[rows(chan), rows(width)],
        out_shape=[jax.ShapeDtypeStruct((tokens, chan), BF16), jax.ShapeDtypeStruct((tokens, width), BF16)],
        cost_estimate=pl.CostEstimate(
            flops=2 * tokens * width * chan, bytes_accessed=tokens * (2 * width + 4 * chan), transcendentals=0
        ),
        compiler_params=pltpu.CompilerParams(vmem_limit_bytes=40 << 20),
    )(gated, stats, gate, wout)


def padded(v, fill):
    return jnp.pad(v[None, :], ((0, 0), (0, LANES - v.shape[0])), constant_values=fill)


MESH = pl.DeviceIdType.MESH
TAGS = {"entry": 1, "stats": 2, "exit": 3}


def remote(source, target, send, recv, **where):
    return pltpu.make_async_remote_copy(
        src_ref=source, dst_ref=target, send_sem=send, recv_sem=recv, device_id=where, device_id_type=MESH
    )


def rows_at(ref, index, count):
    return ref.at[pl.ds(pl.multiple_of(index * count, count), count)]


def greet(axis, peers):
    barrier = pltpu.get_barrier_semaphore()
    for peer in peers:
        pl.semaphore_signal(barrier, inc=1, device_id={axis: peer}, device_id_type=MESH)


def greet_line(tp, n_tp):
    barrier = pltpu.get_barrier_semaphore()

    @pl.when(tp > 0)
    def _():
        pl.semaphore_signal(barrier, inc=1, device_id={"tp": tp - 1}, device_id_type=MESH)

    @pl.when(tp < n_tp - 1)
    def _():
        pl.semaphore_signal(barrier, inc=1, device_id={"tp": tp + 1}, device_id_type=MESH)

    return jnp.where(tp > 0, 1, 0) + jnp.where(tp < n_tp - 1, 1, 0)


class Line:
    def __init__(self, tp, n_tp, own, whole_ref, send, recv):
        self.tp, self.n, self.own, self.whole_ref, self.send, self.recv = tp, n_tp, own, whole_ref, send, recv
        self.count = own.shape[0]

    def copy(self, way, step, own=False):
        shift = -1 if way == 0 else 1
        index = self.tp + shift * step
        slot = rows_at(self.whole_ref, index, self.count)
        return remote(
            self.own if own else slot, slot, self.send.at[way, step], self.recv.at[way, step], tp=self.tp - shift
        )

    def sends(self, way, step):
        if way == 0:
            return jnp.logical_and(self.tp < self.n - 1, self.tp >= step)
        return jnp.logical_and(self.tp > 0, self.tp + step <= self.n - 1)

    def takes(self, way, step):
        return self.tp >= step + 1 if way == 0 else self.tp + step + 1 <= self.n - 1

    def start(self, way, step):
        @pl.when(self.sends(way, step))
        def _():
            self.copy(way, step, own=step == 0).start()

    def arrive(self, way, step):
        @pl.when(self.takes(way, step))
        def _():
            shift = -1 if way == 0 else 1
            slot = rows_at(self.whole_ref, self.tp + shift * (step + 1), self.count)
            remote(
                slot, slot, self.send.at[way, step], self.recv.at[way, step], tp=self.tp + shift
            ).wait_recv()

    def finish(self, way, step):
        @pl.when(self.sends(way, step))
        def _():
            self.copy(way, step, own=step == 0).wait_send()


def entry_kernel(
    tok_ref, pin_ref, pout_ref, tok_all, w_in, w_out, own_sem, z_send, z_recv, f_send, f_recv, p_send, p_recv,
    *, n_tp, n_fs,
):
    tp, me = lax.axis_index("tp"), lax.axis_index("fsdp")
    chip, core, chips = me // 2, me % 2, n_fs // 2
    partner = chip * 2 + 1 - core
    greet("fsdp", [((chip + d) % chips) * 2 + core for d in range(1, chips)] + [partner])
    line_count = greet_line(tp, n_tp)
    pl.semaphore_wait(pltpu.get_barrier_semaphore(), chips + line_count)

    packs = ((pin_ref, w_in), (pout_ref, w_out))
    count = pin_ref.shape[0]
    line = Line(tp, n_tp, tok_ref, tok_all, z_send, z_recv)
    for way in range(2):
        line.start(way, 0)
    for j, (pack, full) in enumerate(packs):
        for d in range(1, chips):
            remote(
                pack, rows_at(full, me, count), f_send.at[j, d], f_recv.at[j, d], fsdp=((chip + d) % chips) * 2 + core
            ).start()
        remote(pack, rows_at(full, me, count), p_send.at[j, 0], p_recv.at[j, 0], fsdp=partner).start()
    own = [
        pltpu.make_async_copy(tok_ref, rows_at(tok_all, tp, tok_ref.shape[0]), own_sem.at[0]),
        pltpu.make_async_copy(pin_ref, rows_at(w_in, me, count), own_sem.at[1]),
        pltpu.make_async_copy(pout_ref, rows_at(w_out, me, count), own_sem.at[2]),
    ]
    for copy in own:
        copy.start()
    for step in range(n_tp - 1):
        for way in range(2):
            line.arrive(way, step)
            if step + 1 < n_tp - 1:
                line.start(way, step + 1)
        if step == n_tp - 3 or n_tp < 3 and step == 0:
            for j, (pack, full) in enumerate(packs):
                for d in range(1, chips):
                    slot = rows_at(full, ((chip + chips - d) % chips) * 2 + core, count)
                    remote(slot, slot, f_send.at[j, d], f_recv.at[j, d], fsdp=partner).wait_recv()
                    remote(slot, slot, p_send.at[j, d], p_recv.at[j, d], fsdp=partner).start()
    for j, (pack, full) in enumerate(packs):
        for d in range(chips):
            slot = rows_at(full, ((chip + chips - d) % chips) * 2 + 1 - core, count)
            remote(slot, slot, p_send.at[j, d], p_recv.at[j, d], fsdp=partner).wait()
        for d in range(1, chips):
            remote(pack, rows_at(full, me, count), f_send.at[j, d], f_recv.at[j, d], fsdp=partner).wait_send()
    for step in range(n_tp - 1):
        for way in range(2):
            line.finish(way, step)
    for copy in own:
        copy.wait()


def entry(tokens, pack_in, pack_out, n_tp, n_fs):
    rows, width = tokens.shape
    count, cols = pack_in.shape
    chan = pack_out.shape[1]
    dma = pltpu.SemaphoreType.DMA
    anywhere = pl.BlockSpec(memory_space=pl.ANY)
    vmem = pl.BlockSpec(memory_space=pltpu.VMEM)
    chips = n_fs // 2
    sent = 2 * (n_tp * rows * width + n_fs * count * (cols + chan))
    return pl.pallas_call(
        functools.partial(entry_kernel, n_tp=n_tp, n_fs=n_fs),
        name="entry",
        in_specs=[vmem] * 3,
        out_specs=[anywhere] * 3,
        out_shape=[
            jax.ShapeDtypeStruct((rows * n_tp, width), BF16),
            jax.ShapeDtypeStruct((count * n_fs, cols), BF16),
            jax.ShapeDtypeStruct((count * n_fs, chan), BF16),
        ],
        scratch_shapes=[
            dma((3,)), dma((2, n_tp - 1)), dma((2, n_tp - 1)), dma((2, chips)), dma((2, chips)), dma((2, chips)),
            dma((2, chips)),
        ],
        cost_estimate=pl.CostEstimate(flops=0, bytes_accessed=sent * 8, transcendentals=0),
        compiler_params=pltpu.CompilerParams(
            collective_id=TAGS["entry"], has_side_effects=True, vmem_limit_bytes=16 << 20
        ),
    )(tokens, pack_in, pack_out)


def exchange_kernel(part_ref, total_ref, held, send, recv, *, n_tp):
    tp = lax.axis_index("tp")
    greet("tp", [(tp + d) % n_tp for d in range(1, n_tp)])
    pl.semaphore_wait(pltpu.get_barrier_semaphore(), n_tp - 1)
    copies = [
        remote(part_ref, held.at[tp], send.at[d], recv.at[d], tp=(tp + d) % n_tp) for d in range(1, n_tp)
    ]
    for copy in copies:
        copy.start()
    held[tp] = part_ref[...]
    for d in range(1, n_tp):
        slot = held.at[(tp + n_tp - d) % n_tp]
        remote(slot, slot, send.at[d], recv.at[d], tp=(tp + d) % n_tp).wait_recv()
    total = held[0]
    for peer in range(1, n_tp):
        total = total + held[peer]
    total_ref[...] = total
    for copy in copies:
        copy.wait_send()


def exchange(part, n_tp):
    dma = pltpu.SemaphoreType.DMA
    vmem = pl.BlockSpec(memory_space=pltpu.VMEM)
    return pl.pallas_call(
        functools.partial(exchange_kernel, n_tp=n_tp),
        name="stats_exchange",
        in_specs=[vmem],
        out_specs=vmem,
        out_shape=jax.ShapeDtypeStruct(part.shape, F32),
        scratch_shapes=[pltpu.VMEM((n_tp,) + part.shape, F32), dma((n_tp,)), dma((n_tp,))],
        compiler_params=pltpu.CompilerParams(
            collective_id=TAGS["stats"], has_side_effects=True, vmem_limit_bytes=4 << 20
        ),
    )(part)


def add_into(target, *sources):
    rows, tile = target.shape[0], 32

    @pl.loop(0, rows // tile)
    def _(i):
        at = pl.ds(pl.multiple_of(i * tile, tile), tile)
        total = sources[0][at, :].astype(F32)
        for source in sources[1:]:
            total = total + source[at, :].astype(F32)
        target[at, :] = total.astype(target.dtype)


def exit_kernel(
    dn_ref, gin_ref, gout_ref, mine_ref, shared_ref,
    dn_out, z_out, x_out, bc_out, dt_out, out_out, mine_out, shared_out,
    z_held, z_got, near_in, near_out, far_in, far_out, got_in, got_out, mine_got, shared_got, shared_held, shared_z,
    bc_held, bc_got,
    zs, zr, ns, nr, fs, fr, ms, mr, ss, sr, ts, tr, bs, br,
    *, n_tp, n_fs,
):
    tp, me = lax.axis_index("tp"), lax.axis_index("fsdp")
    chip, core, chips = me // 2, me % 2, n_fs // 2
    partner = chip * 2 + 1 - core
    chan = gout_ref.shape[1]
    cols = gin_ref.shape[1]
    block, count = dn_out.shape[0], z_out.shape[0]
    greet("fsdp", [(me + d) % n_fs for d in range(1, n_fs)])
    greet("tp", [(tp + d) % n_tp for d in range(1, n_tp)])
    pl.semaphore_wait(pltpu.get_barrier_semaphore(), n_fs - 1 + n_tp - 1)

    def ahead(way, step):
        return n_tp - 1 - step if way == 0 else step

    def passes(way, step):
        return ahead(way, step) > tp if way == 0 else ahead(way, step) < tp

    def first(way):
        return tp == 0 if way == 0 else tp == n_tp - 1

    def pass_on(way, step):
        towards = tp + 1 if way == 0 else tp - 1
        return remote(z_held.at[way, step], z_got.at[way, step], zs.at[way, step], zr.at[way, step], tp=towards)

    for way in range(2):
        @pl.when(first(way))
        def _():
            for step in range(n_tp - 1):
                towards = tp + 1 if way == 0 else tp - 1
                remote(
                    rows_at(dn_ref, ahead(way, step), block), z_got.at[way, step], zs.at[way, step], zr.at[way, step],
                    tp=towards,
                ).start()

    parts = (
        (gin_ref, slice(2 * chan, cols), near_in, far_in, got_in),
        (gin_ref, slice(0, 2 * chan), near_in, far_in, got_in),
        (gout_ref, slice(0, chan), near_out, far_out, got_out),
    )

    def near(j, d):
        source, span, held, _, _ = parts[j]
        rows = rows_at(source, ((chip + d) % chips) * 2 + 1 - core, count)
        return remote(rows.at[:, span], held.at[d, :, span], ns.at[j, d], nr.at[j, d], fsdp=partner)

    def far(j, d):
        _, span, _, held, got = parts[j]
        return remote(
            held.at[d, :, span], got.at[d, :, span], fs.at[j, d], fr.at[j, d], fsdp=((chip + d) % chips) * 2 + core
        )

    order = [d for d in range(1, chips)]
    for j in range(3):
        for d in order + [0]:
            near(j, d).start()

    def small(d):
        peer = (me + d) % n_fs
        return (
            remote(mine_ref, mine_got.at[me], ms.at[d], mr.at[d], fsdp=peer),
            remote(shared_ref, shared_got.at[me], ss.at[d], sr.at[d], fsdp=peer),
        )

    for d in range(1, n_fs):
        for copy in small(d):
            copy.start()
    mine_got[me] = mine_ref[...]
    shared_got[me] = shared_ref[...]

    for j in range(3):
        source, span, held, summed, _ = parts[j]
        for d in order:
            near(j, d).wait_recv()
            rows = rows_at(source, ((chip + d) % chips) * 2 + core, count)
            add_into(summed.at[d, :, span], rows.at[:, span], held.at[d, :, span])
            far(j, d).start()
        near(j, 0).wait_recv()

    def relay(step):
        for way in range(2):
            @pl.when(jnp.logical_and(passes(way, step), jnp.logical_not(first(way))))
            def _():
                pass_on(way, step).wait_recv()
                add_into(z_held.at[way, step], rows_at(dn_ref, ahead(way, step), block), z_got.at[way, step])
                pass_on(way, step).start()

    if n_tp > 2:
        relay(0)
    for d in range(1, n_fs):
        for copy in small(d):
            copy.wait_recv()
    total, again = mine_got[0], shared_got[0]
    for peer in range(1, n_fs):
        total, again = total + mine_got[peer], again + shared_got[peer]
    mine_out[...] = total
    shared_held[...] = again
    shared_z[tp] = again
    for d in range(1, n_tp):
        remote(shared_held, shared_z.at[tp], ts.at[d], tr.at[d], tp=(tp + d) % n_tp).start()
    for step in range(1, n_tp - 2):
        relay(step)

    def settle(j, target, span):
        source, _, held, _, got = parts[j]
        rows = rows_at(source, me, count)
        add_into(
            target, rows.at[:, span], held.at[0, :, span], *[got.at[d, :, span] for d in order]
        )

    for d in order:
        far(0, d).wait_recv()
    settle(0, bc_held, slice(2 * chan, 2 * chan + 2 * STATE))
    settle(0, dt_out, slice(2 * chan + 2 * STATE, cols))
    bc_got[tp] = bc_held[...]
    for d in range(1, n_tp):
        remote(bc_held, bc_got.at[tp], bs.at[d], br.at[d], tp=(tp + d) % n_tp).start()
    for j in (1, 2):
        for d in order:
            far(j, d).wait_recv()
    settle(1, z_out, slice(0, chan))
    settle(1, x_out, slice(chan, 2 * chan))
    settle(2, out_out, slice(0, chan))
    for d in range(1, n_tp):
        peer = (tp + n_tp - d) % n_tp
        remote(shared_held, shared_z.at[peer], ts.at[d], tr.at[d], tp=peer).wait_recv()
        remote(bc_held, bc_got.at[peer], bs.at[d], br.at[d], tp=peer).wait_recv()
    total = shared_z[0]
    for peer in range(1, n_tp):
        total = total + shared_z[peer]
    shared_out[...] = total
    add_into(bc_out, *[bc_got.at[peer] for peer in range(n_tp)])

    own = rows_at(dn_ref, tp, block)
    for way in range(2):
        for step in range(n_tp - 1):
            @pl.when(jnp.logical_and(ahead(way, step) == tp, jnp.logical_not(first(way))))
            def _():
                pass_on(way, step).wait_recv()

    for value in range(n_tp):
        @pl.when(tp == value)
        def _():
            incoming = []
            if value > 0:
                incoming.append(z_got.at[0, n_tp - 1 - value])
            if value < n_tp - 1:
                incoming.append(z_got.at[1, value])
            add_into(dn_out, own, *incoming)

    for way in range(2):
        for step in range(n_tp - 1):
            @pl.when(passes(way, step))
            def _():
                pass_on(way, step).wait_send()
    for j in range(3):
        for d in range(chips):
            near(j, d).wait_send()
        for d in order:
            far(j, d).wait_send()
    for d in range(1, n_fs):
        for copy in small(d):
            copy.wait_send()
    for d in range(1, n_tp):
        remote(shared_held, shared_z.at[tp], ts.at[d], tr.at[d], tp=(tp + d) % n_tp).wait_send()
        remote(bc_held, bc_got.at[tp], bs.at[d], br.at[d], tp=(tp + d) % n_tp).wait_send()


def leave(dn, grad_in, grad_out, mine, shared, n_tp, n_fs):
    block, width = dn.shape[0] // n_tp, dn.shape[1]
    count, cols = grad_in.shape[0] // n_fs, grad_in.shape[1]
    chan = grad_out.shape[1]
    chips = n_fs // 2
    dma = pltpu.SemaphoreType.DMA
    vmem = pl.BlockSpec(memory_space=pltpu.VMEM)
    room = lambda *shape: pltpu.VMEM(shape, BF16)
    shape = lambda *extents: jax.ShapeDtypeStruct(extents, F32)
    return pl.pallas_call(
        functools.partial(exit_kernel, n_tp=n_tp, n_fs=n_fs),
        name="exit",
        in_specs=[vmem] * 5,
        out_specs=[vmem] * 8,
        out_shape=[
            shape(block, width), shape(count, chan), shape(count, chan), shape(count, 2 * STATE), shape(count, LANES),
            shape(count, chan), shape(*mine.shape), shape(*shared.shape),
        ],
        scratch_shapes=[
            room(2, n_tp - 1, block, width), room(2, n_tp - 1, block, width),
            room(chips, count, cols), room(chips, count, chan), room(chips, count, cols), room(chips, count, chan),
            room(chips, count, cols), room(chips, count, chan),
            pltpu.VMEM((n_fs,) + mine.shape, F32), pltpu.VMEM((n_fs,) + shared.shape, F32),
            pltpu.VMEM(shared.shape, F32), pltpu.VMEM((n_tp,) + shared.shape, F32),
            room(count, 2 * STATE), room(n_tp, count, 2 * STATE),
            dma((2, n_tp - 1)), dma((2, n_tp - 1)), dma((3, chips)), dma((3, chips)), dma((3, chips)), dma((3, chips)),
            dma((n_fs,)), dma((n_fs,)), dma((n_fs,)), dma((n_fs,)), dma((n_tp,)), dma((n_tp,)), dma((n_tp,)),
            dma((n_tp,)),
        ],
        compiler_params=pltpu.CompilerParams(
            collective_id=TAGS["exit"], has_side_effects=True, vmem_limit_bytes=62 << 20
        ),
    )(dn, grad_in, grad_out, mine, shared)


def shards(
    tokens, cotangent, seq_start, token_valid, norm_gain, proj_z, proj_x, proj_bc, proj_dt, conv_chan, bias_chan,
    conv_shared, bias_shared, a_log, dt_bias, skip_gain, gate_gain, proj_out,
):
    chan = proj_z.shape[1]
    width = tokens.shape[1]
    heads_here = proj_dt.shape[1]
    inner = chan * lax.axis_size("tp")
    wide = chan + 2 * STATE
    valid = token_valid.astype(F32)[:, None]
    pack_in = jnp.concatenate(
        [proj_z, proj_x, proj_bc, jnp.pad(proj_dt, ((0, 0), (0, LANES - heads_here)))], axis=1
    )
    n_tp, n_fs = lax.axis_size("tp"), lax.axis_size("fsdp")
    tok_all, w_in, w_out = entry(tokens, pack_in, proj_out.T, n_tp, n_fs)
    late_cot, _ = lax.optimization_barrier((cotangent, tok_all))
    cot_all = lax.all_gather(late_cot, "tp", axis=0, tiled=True)
    decay = -jnp.exp(a_log)
    heads = jnp.concatenate([padded(dt_bias, -100.0), padded(decay, 0.0), jnp.zeros((6, LANES), F32)], axis=0)
    taps = jnp.concatenate([conv_chan, conv_shared], axis=1)
    bias = jnp.concatenate([bias_chan, bias_shared])[None, :]
    skip = jnp.repeat(skip_gain, HEAD)[None, :]
    gate = gate_gain[None, :]
    normed, pre, y, gated, sq, enter = mixer_forward(
        seq_start, tok_all, valid, norm_gain[None, :], w_in, taps, bias, heads, skip
    )
    dgn, stats = gate_stats(cot_all, w_out, gate, gated, sq)
    stats = exchange(stats, n_tp)
    gnormed, out_rows = output_part(gated, stats, gate, w_out, inner)
    mixed = lax.psum_scatter(out_rows, "tp", scatter_dimension=0, tiled=True)
    dpre, dn_rows, dtaps, dbias, dhead, dchan, dgain = mixer_backward(
        seq_start, tok_all, valid, w_in, taps, bias, heads, skip, gate, pre, y, enter, dgn, stats, inner
    )
    grad_in = jnp.einsum("td,tc->dc", normed, dpre, preferred_element_type=F32).astype(BF16)
    grad_out = jnp.einsum("td,tc->dc", cot_all, gnormed, preferred_element_type=F32).astype(BF16)
    pack = lambda *vs: jnp.concatenate([v.reshape(-1) for v in vs])
    mine = pack(dtaps[0:4, :chan], dbias[:, :chan], dhead[0:2], dchan[0:2])
    shared = pack(dtaps[0:4, chan:], dbias[:, chan:], dgain)
    tiles = lambda v: jnp.pad(v, (0, -v.shape[0] % (8 * LANES))).reshape(-1, LANES)
    d_normed, own_z, own_x, own_bc, own_dt, own_out, mine, shared = leave(
        dn_rows, grad_in, grad_out, tiles(mine), tiles(shared), n_tp, n_fs
    )
    mine, shared = mine.reshape(-1), shared.reshape(-1)
    at = 0

    def take(source, *shape):
        nonlocal at
        size = 1
        for extent in shape:
            size *= extent
        part = source[at:at + size].reshape(shape)
        at += size
        return part

    g_taps, g_bias, g_heads, g_chan = (
        take(mine, 4, chan), take(mine, chan), take(mine, 2, LANES), take(mine, 2, chan),
    )
    at = 0
    g_taps_s, g_bias_s, g_gain = take(shared, 4, 2 * STATE), take(shared, 2 * STATE), take(shared, width)
    resid = tokens.astype(F32)
    rstd = lax.rsqrt(jnp.mean(resid * resid, axis=1, keepdims=True) + EPSILON)
    output = (resid + mixed.astype(F32)).astype(BF16)
    scaled_in = d_normed * norm_gain[None, :]
    grad_tokens = (
        cotangent.astype(F32) + rstd * scaled_in
        - resid * (rstd * rstd * rstd) * jnp.mean(scaled_in * resid, axis=1, keepdims=True)
    ).astype(BF16)
    return (
        output, grad_tokens, g_gain, own_z, own_x, own_bc, own_dt[:, :heads_here], g_taps, g_bias, g_taps_s, g_bias_s,
        g_heads[0, :heads_here], g_heads[1, :heads_here], g_chan[1].reshape(heads_here, HEAD).sum(axis=1),
        g_chan[0], own_out.T,
    )


def solution(mesh):
    in_specs = (
        P(("fsdp", "tp"), None), P(("fsdp", "tp"), None), P("fsdp"), P("fsdp"), P(), P("fsdp", "tp"),
        P("fsdp", "tp"), P("fsdp", None), P("fsdp", "tp"), P(None, "tp"), P("tp"), P(), P(), P("tp"), P("tp"),
        P("tp"), P("tp"), P("tp", "fsdp"),
    )
    out_specs = (
        P(("fsdp", "tp"), None), P(("fsdp", "tp"), None), P(), P("fsdp", "tp"), P("fsdp", "tp"), P("fsdp", None),
        P("fsdp", "tp"), P(None, "tp"), P("tp"), P(), P(), P("tp"), P("tp"), P("tp"), P("tp"), P("tp", "fsdp"),
    )
    return jax.shard_map(shards, mesh=mesh, in_specs=in_specs, out_specs=out_specs, check_vma=False)
```

```python
import functools
import jax
import jax.numpy as jnp
from jax import lax
from jax.experimental import pallas as pl
from jax.experimental.pallas import tpu as pltpu
from jax.sharding import PartitionSpec as P

HEAD = 64
STATE = 128
STRETCH = 256
LANES = 128
EPSILON = 1e-05
F32 = jnp.float32
BF16 = jnp.bfloat16
NN = (((1,), (0,)), ((), ()))
NT = (((1,), (1,)), ((), ()))
TN = (((0,), (0,)), ((), ()))


def mm(a, b, dims=NN):
    return lax.dot_general(a, b, dims, preferred_element_type=F32)


def exact(a, b):
    return lax.dot_general(a, b, NN, precision=lax.Precision.HIGHEST, preferred_element_type=F32)


def halves(v):
    high = v.astype(BF16)
    return high, (v - high.astype(F32)).astype(BF16)


def iota(shape, dim):
    return lax.broadcasted_iota(jnp.int32, shape, dim)


def spread_heads(v, chan):
    high, rest = halves(v)
    rows = iota((2 * LANES, chan), 0) & (LANES - 1)
    pick = jnp.where(rows == (iota((2 * LANES, chan), 1) >> 6), 1.0, 0.0).astype(BF16)
    return mm(jnp.concatenate([high, rest], axis=1), pick)


def gather_heads(v):
    chan = v.shape[1]
    high, rest = halves(v)
    pick = jnp.where((iota((chan, LANES), 0) >> 6) == iota((chan, LANES), 1), 1.0, 0.0).astype(BF16)
    return mm(high, pick) + mm(rest, pick)


def softplus(v):
    return jnp.maximum(v, 0.0) + jnp.log1p(jnp.exp(-jnp.abs(v)))


def sigmoid(v):
    return 1.0 / (1.0 + jnp.exp(-v))


def lower_mask():
    return iota((STRETCH, STRETCH), 0) >= iota((STRETCH, STRETCH), 1)


def convolve(xs_ref, taps_ref, bias_ref):
    total = bias_ref[...] + taps_ref[0:1, :] * xs_ref[5:5 + STRETCH, :]
    for tap in range(1, 4):
        total = total + taps_ref[tap:tap + 1, :] * xs_ref[5 + tap:5 + tap + STRETCH, :]
    return total


def decays(pre_dt, head_ref, valid):
    rates = softplus(pre_dt + head_ref[0:1, :]) * valid
    log_decay = rates * head_ref[1:2, :]
    lower = lower_mask().astype(F32)
    cumulative = exact(lower, log_decay)
    last = cumulative[STRETCH - 1:STRETCH, :]
    return rates, cumulative, jnp.exp(cumulative), jnp.exp(last - cumulative)


def weights_of(cumulative, across, head):
    return jnp.exp(jnp.minimum(cumulative[:, head:head + 1] - across[head:head + 1, :], 0.0))


def forward_kernel(
    open_ref, tok_ref, valid_ref, gain_ref, w_ref, taps_ref, bias_ref, head_ref, skip_ref,
    normed_ref, pre_ref, y_ref, gated_ref, sq_ref, enter_ref,
    state, xs,
):
    chan = y_ref.shape[1]
    block = pl.program_id(0)
    opening = open_ref[block] == 1

    @pl.when(opening)
    def _():
        state[...] = jnp.zeros_like(state)
        xs[0:8, :] = jnp.zeros((8, xs.shape[1]), F32)

    @pl.when(jnp.logical_not(opening))
    def _():
        xs[0:8, :] = xs[STRETCH:STRETCH + 8, :]

    valid = valid_ref[...]
    resid = tok_ref[...].astype(F32)
    rstd = lax.rsqrt(jnp.mean(resid * resid, axis=1, keepdims=True) + EPSILON)
    normed = (resid * rstd * gain_ref[...]).astype(BF16)
    normed_ref[...] = normed
    pre = mm(normed, w_ref[...])
    pre_ref[...] = pre
    xs[8:8 + STRETCH, :] = pre[:, chan:2 * chan + 2 * STATE]
    conv = convolve(xs, taps_ref, bias_ref)
    feats = conv * sigmoid(conv)
    x = feats[:, :chan]
    bs = feats[:, chan:chan + STATE].astype(BF16)
    cs = feats[:, chan + STATE:].astype(BF16)
    rates, cumulative, grown, to_end = decays(pre[:, 2 * chan + 2 * STATE:], head_ref, valid)
    across = cumulative.T
    grown_e = spread_heads(grown, chan)
    scaled = x * spread_heads(rates, chan)
    entering = state[...]
    enter_ref[0] = entering
    y_ref[...] = mm(cs, entering.astype(BF16)) * grown_e
    state[...] = entering * grown_e[STRETCH - 1:STRETCH, :] + mm(
        bs, (scaled * spread_heads(to_end, chan)).astype(BF16), TN
    )
    overlap = jnp.where(lower_mask(), mm(cs, bs, NT), 0.0)
    scaled_b = scaled.astype(BF16)
    first = iota((STRETCH, LANES), 1) < HEAD
    for pair in range(chan // LANES):
        cols = slice(pair * LANES, (pair + 1) * LANES)
        both = scaled_b[:, cols]
        mats = [
            (weights_of(cumulative, across, 2 * pair + side) * overlap).astype(BF16) for side in range(2)
        ]
        zero = jnp.zeros_like(both)
        y_ref[:, cols] += mm(
            jnp.concatenate(mats, axis=1),
            jnp.concatenate([jnp.where(first, both, zero), jnp.where(first, zero, both)], axis=0),
        )
    pre_z = pre[:, :chan]
    gated = (y_ref[...] + skip_ref[...] * x) * (pre_z * sigmoid(pre_z)) * valid
    gated_ref[...] = gated
    sq_ref[...] = jnp.sum(gated * gated, axis=1, keepdims=True)


def backward_kernel(
    open_ref, tok_ref, valid_ref, w_ref, taps_ref, bias_ref, head_ref, skip_ref, gate_ref,
    pre_ref, halo_ref, y_ref, enter_ref, dgn_ref, stats_ref,
    dpre_ref, dnormed_ref, dtaps_ref, dbias_ref, dhead_ref, dchan_ref, dgain_ref,
    dstate, xs, dus,
    *, inner,
):
    chan = y_ref.shape[1]
    wide = chan + 2 * STATE
    step = pl.program_id(0)
    block = pl.num_programs(0) - 1 - step
    opening = open_ref[block] == 1
    keep = jnp.where(opening, 0.0, 1.0).astype(F32)

    @pl.when(step == 0)
    def _():
        dstate[...] = jnp.zeros_like(dstate)
        dus[...] = jnp.zeros_like(dus)
        dtaps_ref[...] = jnp.zeros_like(dtaps_ref)
        dbias_ref[...] = jnp.zeros_like(dbias_ref)
        dhead_ref[...] = jnp.zeros_like(dhead_ref)
        dchan_ref[...] = jnp.zeros_like(dchan_ref)
        dgain_ref[...] = jnp.zeros_like(dgain_ref)

    valid = valid_ref[...]
    xs[0:8, :] = halo_ref[:, chan:2 * chan + 2 * STATE] * keep
    xs[8:8 + STRETCH, :] = pre_ref[:, chan:2 * chan + 2 * STATE]
    conv = convolve(xs, taps_ref, bias_ref)
    gate_u = sigmoid(conv)
    feats = conv * gate_u
    slope = gate_u * (1.0 + conv * (1.0 - gate_u))
    x = feats[:, :chan]
    bs = feats[:, chan:chan + STATE].astype(BF16)
    cs = feats[:, chan + STATE:].astype(BF16)
    pre_dt = pre_ref[:, 2 * chan + 2 * STATE:]
    rates, cumulative, grown, to_end = decays(pre_dt, head_ref, valid)
    across = cumulative.T
    grown_e = spread_heads(grown, chan)
    rates_e = spread_heads(rates, chan)
    to_end_e = spread_heads(to_end, chan)
    leave_e = grown_e[STRETCH - 1:STRETCH, :]

    pre_z = pre_ref[:, :chan]
    gate_z = sigmoid(pre_z)
    silu_z = pre_z * gate_z * valid
    y = y_ref[...]
    mixed = y + skip_ref[...] * x
    gated = mixed * silu_z
    grstd, cross = row_stats(stats_ref, inner)
    dgn = dgn_ref[...]
    d_gated = grstd * (gate_ref[...] * dgn) - gated * (grstd * grstd * grstd * cross * (1.0 / inner))
    d_mixed = d_gated * silu_z
    dpre_ref[:, :chan] = (
        d_gated * mixed * (valid * (gate_z * (1.0 + pre_z * (1.0 - gate_z))))
    ).astype(BF16)
    dchan_ref[0:1, :] += jnp.sum(dgn * gated * grstd, axis=0, keepdims=True)
    dchan_ref[1:2, :] += jnp.sum(d_mixed * x, axis=0, keepdims=True)

    dy_b = d_mixed.astype(BF16)
    dy = dy_b.astype(F32)
    scaled = x * rates_e
    scaled_b = scaled.astype(BF16)
    entering = enter_ref[0]
    d_leaving = dstate[...]
    d_leaving_b = d_leaving.astype(BF16)
    tail = mm(bs, d_leaving_b) * to_end_e
    overlap = jnp.where(lower_mask(), mm(cs, bs, NT), 0.0)
    first = iota((STRETCH, LANES), 1) < HEAD
    d_overlap = jnp.zeros((STRETCH, STRETCH), F32)
    parts = []
    for pair in range(chan // LANES):
        cols = slice(pair * LANES, (pair + 1) * LANES)
        dy_pair = dy_b[:, cols]
        x_pair = scaled_b[:, cols]
        zero = jnp.zeros_like(dy_pair)
        sides = [jnp.where(first, dy_pair, zero), jnp.where(first, zero, dy_pair)]
        mats = []
        for side in range(2):
            weight = weights_of(cumulative, across, 2 * pair + side)
            mats.append((weight * overlap).astype(BF16))
            d_overlap = d_overlap + mm(sides[side], x_pair, NT) * weight
        parts.append(mm(jnp.concatenate(mats, axis=0), jnp.concatenate(sides, axis=0), TN))
    d_scaled = jnp.concatenate(parts, axis=1) + tail
    scaled_r = scaled_b.astype(F32)
    d_cum = gather_heads(dy * y - scaled_r * d_scaled)
    d_last = jnp.sum(scaled_r * tail, axis=0, keepdims=True) + leave_e * jnp.sum(
        d_leaving * entering, axis=0, keepdims=True
    )
    d_last = gather_heads(jnp.broadcast_to(d_last, (8, chan)))[0:1, :]
    upper = (iota((STRETCH, STRETCH), 0) <= iota((STRETCH, STRETCH), 1)).astype(F32)
    d_log = exact(upper, d_cum) + d_last
    decay = head_ref[1:2, :]
    d_rates = d_log * decay + gather_heads(x * d_scaled)
    d_dt = d_rates * valid * sigmoid(pre_dt + head_ref[0:1, :])
    dhead_ref[0:1, :] += jnp.sum(d_log * rates, axis=0, keepdims=True) * decay
    dhead_ref[1:2, :] += jnp.sum(d_dt, axis=0, keepdims=True)
    dpre_ref[:, 2 * chan + 2 * STATE:] = d_dt.astype(BF16)

    d_x = d_scaled * rates_e + skip_ref[...] * d_mixed
    d_overlap_b = jnp.where(lower_mask(), d_overlap, 0.0).astype(BF16)
    dy_grown = (dy * grown_e).astype(BF16)
    x_end = (scaled * to_end_e).astype(BF16)
    d_b = mm(d_overlap_b, cs, TN) + mm(x_end, d_leaving_b, NT)
    d_c = mm(d_overlap_b, bs) + mm(dy_grown, entering.astype(BF16), NT)
    dstate[...] = (d_leaving * leave_e + mm(cs, dy_grown, TN)) * keep

    dus[0:STRETCH, :chan] = d_x * slope[:, :chan]
    dus[0:STRETCH, chan:chan + STATE] = d_b * slope[:, chan:chan + STATE]
    dus[0:STRETCH, chan + STATE:] = d_c * slope[:, chan + STATE:]
    d_conv = dus[0:STRETCH, :]
    dbias_ref[...] += jnp.sum(d_conv, axis=0, keepdims=True)
    d_pre = jnp.zeros((STRETCH, wide), F32)
    for tap in range(4):
        dtaps_ref[tap:tap + 1, :] += jnp.sum(d_conv * xs[5 + tap:5 + tap + STRETCH, :], axis=0, keepdims=True)
        d_pre = d_pre + taps_ref[tap:tap + 1, :] * dus[3 - tap:3 - tap + STRETCH, :]
    dpre_ref[:, chan:2 * chan + 2 * STATE] = d_pre.astype(BF16)
    dus[STRETCH:STRETCH + 8, :] = d_conv[0:8, :] * keep

    d_normed = mm(dpre_ref[...], w_ref[...], NT)
    dnormed_ref[...] = d_normed.astype(BF16)
    resid = tok_ref[...].astype(F32)
    rstd = lax.rsqrt(jnp.mean(resid * resid, axis=1, keepdims=True) + EPSILON)
    dgain_ref[...] += jnp.sum(d_normed * (resid * rstd), axis=0, keepdims=True)


def whole(shape):
    return pl.BlockSpec(shape, lambda *_: (0,) * len(shape), pipeline_mode=pl.Buffered(1))


def mixer_forward(openings, tok, valid, gain, w_in, taps, bias, heads, skip):
    tokens, width = tok.shape
    cols = w_in.shape[1]
    chan = skip.shape[1]
    blocks = tokens // STRETCH
    wide = chan + 2 * STATE
    rows = lambda n: pl.BlockSpec((STRETCH, n), lambda i, *_: (i, 0))
    return pl.pallas_call(
        forward_kernel,
        name="mixer_forward",
        grid_spec=pltpu.PrefetchScalarGridSpec(
            num_scalar_prefetch=1,
            grid=(blocks,),
            in_specs=[
                rows(width), rows(1), whole((1, width)), whole((width, cols)), whole((4, wide)), whole((1, wide)),
                whole((8, LANES)), whole((1, chan)),
            ],
            out_specs=[
                rows(width), rows(cols), rows(chan), rows(chan), rows(1),
                pl.BlockSpec((1, STATE, chan), lambda i, *_: (i, 0, 0)),
            ],
            scratch_shapes=[
                pltpu.VMEM((STATE, chan), F32),
                pltpu.VMEM((STRETCH + 8, wide), F32),
            ],
        ),
        out_shape=[
            jax.ShapeDtypeStruct((tokens, width), BF16),
            jax.ShapeDtypeStruct((tokens, cols), F32),
            jax.ShapeDtypeStruct((tokens, chan), F32),
            jax.ShapeDtypeStruct((tokens, chan), F32),
            jax.ShapeDtypeStruct((tokens, 1), F32),
            jax.ShapeDtypeStruct((blocks, STATE, chan), F32),
        ],
        cost_estimate=pl.CostEstimate(
            flops=2 * tokens * width * cols, bytes_accessed=tokens * cols * 12, transcendentals=tokens * chan
        ),
        compiler_params=pltpu.CompilerParams(vmem_limit_bytes=60 << 20, dimension_semantics=("arbitrary",)),
    )(openings, tok, valid, gain, w_in, taps, bias, heads, skip)


def mixer_backward(
    openings, tok, valid, w_in, taps, bias, heads, skip, gate, pre, y, enter, dgn, stats, inner
):
    tokens, width = tok.shape
    cols = w_in.shape[1]
    chan = skip.shape[1]
    blocks = tokens // STRETCH
    wide = chan + 2 * STATE
    per = STRETCH // 8
    rows = lambda n: pl.BlockSpec((STRETCH, n), lambda i, *_: (blocks - 1 - i, 0))
    return pl.pallas_call(
        functools.partial(backward_kernel, inner=inner),
        name="mixer_backward",
        grid_spec=pltpu.PrefetchScalarGridSpec(
            num_scalar_prefetch=1,
            grid=(blocks,),
            in_specs=[
                rows(width), rows(1), whole((width, cols)), whole((4, wide)), whole((1, wide)),
                whole((8, LANES)), whole((1, chan)), whole((1, chan)),
                rows(cols),
                pl.BlockSpec((8, cols), lambda i, *_: (jnp.maximum((blocks - 1 - i) * per - 1, 0), 0)),
                rows(chan),
                pl.BlockSpec((1, STATE, chan), lambda i, *_: (blocks - 1 - i, 0, 0)),
                rows(chan),
                pl.BlockSpec((8, STRETCH), lambda i, *_: (0, blocks - 1 - i)),
            ],
            out_specs=[
                rows(cols), rows(width),
                pl.BlockSpec((8, wide), lambda i, *_: (0, 0)),
                pl.BlockSpec((1, wide), lambda i, *_: (0, 0)),
                pl.BlockSpec((8, LANES), lambda i, *_: (0, 0)),
                pl.BlockSpec((8, chan), lambda i, *_: (0, 0)),
                pl.BlockSpec((1, width), lambda i, *_: (0, 0)),
            ],
            scratch_shapes=[
                pltpu.VMEM((STATE, chan), F32),
                pltpu.VMEM((STRETCH + 8, wide), F32),
                pltpu.VMEM((STRETCH + 8, wide), F32),
            ],
        ),
        out_shape=[
            jax.ShapeDtypeStruct((tokens, cols), BF16),
            jax.ShapeDtypeStruct((tokens, width), BF16),
            jax.ShapeDtypeStruct((8, wide), F32),
            jax.ShapeDtypeStruct((1, wide), F32),
            jax.ShapeDtypeStruct((8, LANES), F32),
            jax.ShapeDtypeStruct((8, chan), F32),
            jax.ShapeDtypeStruct((1, width), F32),
        ],
        cost_estimate=pl.CostEstimate(
            flops=4 * tokens * width * cols, bytes_accessed=tokens * cols * 12, transcendentals=tokens * chan
        ),
        compiler_params=pltpu.CompilerParams(vmem_limit_bytes=60 << 20, dimension_semantics=("arbitrary",)),
    )(openings, tok, valid, w_in, taps, bias, heads, skip, gate, pre, pre, y, enter, dgn, stats)


def stats_kernel(cot_ref, wout_ref, gate_ref, gated_ref, sq_ref, dgn_ref, stats_ref):
    dgn = mm(cot_ref[...], wout_ref[...])
    dgn_ref[...] = dgn
    cross = jnp.sum(gate_ref[...] * dgn * gated_ref[...], axis=1, keepdims=True)
    lane = iota((STRETCH, LANES), 1)
    both = jnp.where(lane == 0, sq_ref[...], 0.0) + jnp.where(lane == 1, cross, 0.0)
    stats_ref[...] = both.T[0:8, :]


def row_stats(stats_ref, inner):
    filled = jnp.concatenate([stats_ref[...], jnp.zeros((LANES - 8, STRETCH), F32)], axis=0).T
    grstd = lax.rsqrt(filled[:, 0:1] * (1.0 / inner) + EPSILON)
    return grstd, filled[:, 1:2]


def output_kernel(gated_ref, stats_ref, gate_ref, wout_ref, gnormed_ref, out_ref, *, inner):
    grstd, _ = row_stats(stats_ref, inner)
    gnormed = (gated_ref[...] * grstd * gate_ref[...]).astype(BF16)
    gnormed_ref[...] = gnormed
    out_ref[...] = mm(gnormed, wout_ref[...], NT).astype(BF16)


def gate_stats(cot, wout, gate, gated, sq):
    tokens, width = cot.shape
    chan = gate.shape[1]
    rows = lambda n: pl.BlockSpec((STRETCH, n), lambda i: (i, 0))
    return pl.pallas_call(
        stats_kernel,
        name="gate_stats",
        grid=(tokens // STRETCH,),
        in_specs=[rows(width), whole((width, chan)), whole((1, chan)), rows(chan), rows(1)],
        out_specs=[rows(chan), pl.BlockSpec((8, STRETCH), lambda i: (0, i))],
        out_shape=[jax.ShapeDtypeStruct((tokens, chan), F32), jax.ShapeDtypeStruct((8, tokens), F32)],
        cost_estimate=pl.CostEstimate(
            flops=2 * tokens * width * chan, bytes_accessed=tokens * (2 * width + 8 * chan), transcendentals=0
        ),
        compiler_params=pltpu.CompilerParams(vmem_limit_bytes=40 << 20),
    )(cot, wout, gate, gated, sq)


def output_part(gated, stats, gate, wout, inner):
    tokens, chan = gated.shape
    width = wout.shape[0]
    rows = lambda n: pl.BlockSpec((STRETCH, n), lambda i: (i, 0))
    return pl.pallas_call(
        functools.partial(output_kernel, inner=inner),
        name="output_part",
        grid=(tokens // STRETCH,),
        in_specs=[rows(chan), pl.BlockSpec((8, STRETCH), lambda i: (0, i)), whole((1, chan)), whole((width, chan))],
        out_specs=[rows(chan), rows(width)],
        out_shape=[jax.ShapeDtypeStruct((tokens, chan), BF16), jax.ShapeDtypeStruct((tokens, width), BF16)],
        cost_estimate=pl.CostEstimate(
            flops=2 * tokens * width * chan, bytes_accessed=tokens * (2 * width + 4 * chan), transcendentals=0
        ),
        compiler_params=pltpu.CompilerParams(vmem_limit_bytes=40 << 20),
    )(gated, stats, gate, wout)


def padded(v, fill):
    return jnp.pad(v[None, :], ((0, 0), (0, LANES - v.shape[0])), constant_values=fill)


MESH = pl.DeviceIdType.MESH
CHUNKS = 4
TAGS = {"entry": 1, "stats": 2, "exit": 3}


def remote(source, target, send, recv, **where):
    return pltpu.make_async_remote_copy(
        src_ref=source, dst_ref=target, send_sem=send, recv_sem=recv, device_id=where, device_id_type=MESH
    )


def rows_at(ref, index, count):
    return ref.at[pl.ds(pl.multiple_of(index * count, count), count)]


def greet(axis, peers):
    barrier = pltpu.get_barrier_semaphore()
    for peer in peers:
        pl.semaphore_signal(barrier, inc=1, device_id={axis: peer}, device_id_type=MESH)


def greet_line(tp, n_tp):
    barrier = pltpu.get_barrier_semaphore()

    @pl.when(tp > 0)
    def _():
        pl.semaphore_signal(barrier, inc=1, device_id={"tp": tp - 1}, device_id_type=MESH)

    @pl.when(tp < n_tp - 1)
    def _():
        pl.semaphore_signal(barrier, inc=1, device_id={"tp": tp + 1}, device_id_type=MESH)

    return jnp.where(tp > 0, 1, 0) + jnp.where(tp < n_tp - 1, 1, 0)


class Line:
    def __init__(self, tp, n_tp, own, whole_ref, send, recv):
        self.tp, self.n, self.own, self.whole_ref, self.send, self.recv = tp, n_tp, own, whole_ref, send, recv
        self.count = own.shape[0]

    def copy(self, way, step, own=False):
        shift = -1 if way == 0 else 1
        index = self.tp + shift * step
        slot = rows_at(self.whole_ref, index, self.count)
        return remote(
            self.own if own else slot, slot, self.send.at[way, step], self.recv.at[way, step], tp=self.tp - shift
        )

    def sends(self, way, step):
        if way == 0:
            return jnp.logical_and(self.tp < self.n - 1, self.tp >= step)
        return jnp.logical_and(self.tp > 0, self.tp + step <= self.n - 1)

    def takes(self, way, step):
        return self.tp >= step + 1 if way == 0 else self.tp + step + 1 <= self.n - 1

    def start(self, way, step):
        @pl.when(self.sends(way, step))
        def _():
            self.copy(way, step, own=step == 0).start()

    def arrive(self, way, step):
        @pl.when(self.takes(way, step))
        def _():
            shift = -1 if way == 0 else 1
            slot = rows_at(self.whole_ref, self.tp + shift * (step + 1), self.count)
            remote(
                slot, slot, self.send.at[way, step], self.recv.at[way, step], tp=self.tp + shift
            ).wait_recv()

    def finish(self, way, step):
        @pl.when(self.sends(way, step))
        def _():
            self.copy(way, step, own=step == 0).wait_send()


def entry_kernel(
    tok_ref, pin_ref, pout_ref, tok_all, w_in, w_out, own_sem, z_send, z_recv, f_send, f_recv, p_send, p_recv,
    *, n_tp, n_fs,
):
    tp, me = lax.axis_index("tp"), lax.axis_index("fsdp")
    chip, core, chips = me // 2, me % 2, n_fs // 2
    partner = chip * 2 + 1 - core
    greet("fsdp", [((chip + d) % chips) * 2 + core for d in range(1, chips)] + [partner])
    line_count = greet_line(tp, n_tp)
    pl.semaphore_wait(pltpu.get_barrier_semaphore(), chips + line_count)

    packs = ((pin_ref, w_in), (pout_ref, w_out))
    count = pin_ref.shape[0]
    line = Line(tp, n_tp, tok_ref, tok_all, z_send, z_recv)
    for way in range(2):
        line.start(way, 0)
    for j, (pack, full) in enumerate(packs):
        for d in range(1, chips):
            remote(
                pack, rows_at(full, me, count), f_send.at[j, d], f_recv.at[j, d], fsdp=((chip + d) % chips) * 2 + core
            ).start()
        remote(pack, rows_at(full, me, count), p_send.at[j, 0], p_recv.at[j, 0], fsdp=partner).start()
    own = [
        pltpu.make_async_copy(tok_ref, rows_at(tok_all, tp, tok_ref.shape[0]), own_sem.at[0]),
        pltpu.make_async_copy(pin_ref, rows_at(w_in, me, count), own_sem.at[1]),
        pltpu.make_async_copy(pout_ref, rows_at(w_out, me, count), own_sem.at[2]),
    ]
    for copy in own:
        copy.start()
    for step in range(n_tp - 1):
        for way in range(2):
            line.arrive(way, step)
            if step + 1 < n_tp - 1:
                line.start(way, step + 1)
        if step == n_tp - 3 or n_tp < 3 and step == 0:
            for j, (pack, full) in enumerate(packs):
                for d in range(1, chips):
                    slot = rows_at(full, ((chip + chips - d) % chips) * 2 + core, count)
                    remote(slot, slot, f_send.at[j, d], f_recv.at[j, d], fsdp=partner).wait_recv()
                    remote(slot, slot, p_send.at[j, d], p_recv.at[j, d], fsdp=partner).start()
    for j, (pack, full) in enumerate(packs):
        for d in range(chips):
            slot = rows_at(full, ((chip + chips - d) % chips) * 2 + 1 - core, count)
            remote(slot, slot, p_send.at[j, d], p_recv.at[j, d], fsdp=partner).wait()
        for d in range(1, chips):
            remote(pack, rows_at(full, me, count), f_send.at[j, d], f_recv.at[j, d], fsdp=partner).wait_send()
    for step in range(n_tp - 1):
        for way in range(2):
            line.finish(way, step)
    for copy in own:
        copy.wait()


def entry(tokens, pack_in, pack_out, n_tp, n_fs):
    rows, width = tokens.shape
    count, cols = pack_in.shape
    chan = pack_out.shape[1]
    dma = pltpu.SemaphoreType.DMA
    anywhere = pl.BlockSpec(memory_space=pl.ANY)
    vmem = pl.BlockSpec(memory_space=pltpu.VMEM)
    chips = n_fs // 2
    sent = 2 * (n_tp * rows * width + n_fs * count * (cols + chan))
    return pl.pallas_call(
        functools.partial(entry_kernel, n_tp=n_tp, n_fs=n_fs),
        name="entry",
        in_specs=[vmem] * 3,
        out_specs=[anywhere] * 3,
        out_shape=[
            jax.ShapeDtypeStruct((rows * n_tp, width), BF16),
            jax.ShapeDtypeStruct((count * n_fs, cols), BF16),
            jax.ShapeDtypeStruct((count * n_fs, chan), BF16),
        ],
        scratch_shapes=[
            dma((3,)), dma((2, n_tp - 1)), dma((2, n_tp - 1)), dma((2, chips)), dma((2, chips)), dma((2, chips)),
            dma((2, chips)),
        ],
        cost_estimate=pl.CostEstimate(flops=0, bytes_accessed=sent * 8, transcendentals=0),
        compiler_params=pltpu.CompilerParams(
            collective_id=TAGS["entry"], has_side_effects=True, vmem_limit_bytes=16 << 20
        ),
    )(tokens, pack_in, pack_out)


def exchange_kernel(part_ref, total_ref, held, send, recv, *, n_tp):
    tp = lax.axis_index("tp")
    greet("tp", [(tp + d) % n_tp for d in range(1, n_tp)])
    pl.semaphore_wait(pltpu.get_barrier_semaphore(), n_tp - 1)
    copies = [
        remote(part_ref, held.at[tp], send.at[d], recv.at[d], tp=(tp + d) % n_tp) for d in range(1, n_tp)
    ]
    for copy in copies:
        copy.start()
    held[tp] = part_ref[...]
    for d in range(1, n_tp):
        slot = held.at[(tp + n_tp - d) % n_tp]
        remote(slot, slot, send.at[d], recv.at[d], tp=(tp + d) % n_tp).wait_recv()
    total = held[0]
    for peer in range(1, n_tp):
        total = total + held[peer]
    total_ref[...] = total
    for copy in copies:
        copy.wait_send()


def exchange(part, n_tp):
    dma = pltpu.SemaphoreType.DMA
    vmem = pl.BlockSpec(memory_space=pltpu.VMEM)
    return pl.pallas_call(
        functools.partial(exchange_kernel, n_tp=n_tp),
        name="stats_exchange",
        in_specs=[vmem],
        out_specs=vmem,
        out_shape=jax.ShapeDtypeStruct(part.shape, F32),
        scratch_shapes=[pltpu.VMEM((n_tp,) + part.shape, F32), dma((n_tp,)), dma((n_tp,))],
        compiler_params=pltpu.CompilerParams(
            collective_id=TAGS["stats"], has_side_effects=True, vmem_limit_bytes=4 << 20
        ),
    )(part)


def add_into(target, *sources):
    rows, tile = target.shape[0], 32

    @pl.loop(0, rows // tile)
    def _(i):
        at = pl.ds(pl.multiple_of(i * tile, tile), tile)
        total = sources[0][at, :].astype(F32)
        for source in sources[1:]:
            total = total + source[at, :].astype(F32)
        target[at, :] = total.astype(target.dtype)


def fill_rows(target, pieces):
    places, at = [], 0
    for source, row, start, length in pieces:
        places.append(at)
        for k in range(length // LANES):
            target[at:at + 1, :] = source[row:row + 1, start + k * LANES:start + (k + 1) * LANES]
            at += 1
    if at < target.shape[0]:
        target[at:, :] = jnp.zeros((target.shape[0] - at, LANES), F32)
    return places


def spill_row(target, row, source, at):
    for k in range(target.shape[1] // LANES):
        target[row:row + 1, k * LANES:(k + 1) * LANES] = source[at + k:at + k + 1, :]


def exit_kernel(
    dn_ref, normed_ref, dpre_ref, cot_ref, gn_ref, dtaps_ref, dbias_ref, dhead_ref, dchan_ref, dgain_ref,
    dn_out, z_out, x_out, bc_out, dt_out, out_out,
    taps_out, bias_out, taps_s_out, bias_s_out, log_out, step_out, skip_out, gate_out, gain_out,
    gin_ref, gout_ref, mine_ref, shared_ref,
    z_held, z_got, near_in, near_out, far_in, far_out, got_in, got_out, mine_got, shared_got, shared_held, shared_z,
    bc_held, bc_got,
    zs, zr, ns, nr, fs, fr, ms, mr, ss, sr, ts, tr, bs, br,
    *, n_tp, n_fs,
):
    tp, me = lax.axis_index("tp"), lax.axis_index("fsdp")
    chip, core, chips = me // 2, me % 2, n_fs // 2
    partner = chip * 2 + 1 - core
    chan = gout_ref.shape[1]
    cols = gin_ref.shape[1]
    width = gin_ref.shape[0]
    mine_at = fill_rows(
        mine_ref, [(dtaps_ref, tap, 0, chan) for tap in range(4)] + [(dbias_ref, 0, 0, chan)]
        + [(dchan_ref, row, 0, chan) for row in range(2)] + [(dhead_ref, row, 0, LANES) for row in range(2)]
    )
    shared_at = fill_rows(
        shared_ref, [(dtaps_ref, tap, chan, 2 * STATE) for tap in range(4)] + [(dbias_ref, 0, chan, 2 * STATE)]
        + [(dgain_ref, 0, 0, width)]
    )
    block, count = dn_out.shape[0], z_out.shape[0]
    greet("fsdp", [(me + d) % n_fs for d in range(1, n_fs)])
    greet("tp", [(tp + d) % n_tp for d in range(1, n_tp)])
    pl.semaphore_wait(pltpu.get_barrier_semaphore(), n_fs - 1 + n_tp - 1)

    chunk = block // CHUNKS
    steps = (n_tp - 1) * CHUNKS

    def ahead(way, step):
        return n_tp - 1 - step // CHUNKS if way == 0 else step // CHUNKS

    def passes(way, step):
        return ahead(way, step) > tp if way == 0 else ahead(way, step) < tp

    def first(way):
        return tp == 0 if way == 0 else tp == n_tp - 1

    def local(way, step):
        return dn_ref.at[pl.ds(pl.multiple_of(ahead(way, step) * block + step % CHUNKS * chunk, chunk), chunk)]

    def pass_on(way, step, direct=False):
        towards = tp + 1 if way == 0 else tp - 1
        source = local(way, step) if direct else z_held.at[way, step]
        return remote(source, z_got.at[way, step], zs.at[way, step], zr.at[way, step], tp=towards)

    def advance(turn):
        for way in range(2):
            lag = jnp.maximum(tp - 1 if way == 0 else n_tp - 2 - tp, 0)
            step = turn - lag
            live = jnp.logical_and(step >= 0, step < steps)

            @pl.when(jnp.logical_and(first(way), live))
            def _():
                @pl.when(step >= 2)
                def _():
                    pass_on(way, step - 2, True).wait_send()

                pass_on(way, step, True).start()

            @pl.when(jnp.logical_and(jnp.logical_and(passes(way, step), live), jnp.logical_not(first(way))))
            def _():
                pass_on(way, step).wait_recv()
                add_into(z_held.at[way, step], local(way, step), z_got.at[way, step])
                pass_on(way, step).start()

    parts = (
        (gin_ref, slice(2 * chan, cols), near_in, far_in, got_in),
        (gin_ref, slice(0, 2 * chan), near_in, far_in, got_in),
        (gout_ref, slice(0, chan), near_out, far_out, got_out),
    )

    def near(j, d):
        source, span, held, _, _ = parts[j]
        rows = rows_at(source, ((chip + d) % chips) * 2 + 1 - core, count)
        return remote(rows.at[:, span], held.at[d, :, span], ns.at[j, d], nr.at[j, d], fsdp=partner)

    def far(j, d):
        _, span, _, held, got = parts[j]
        return remote(
            held.at[d, :, span], got.at[d, :, span], fs.at[j, d], fr.at[j, d], fsdp=((chip + d) % chips) * 2 + core
        )

    order = [d for d in range(1, chips)]

    def small(d):
        peer = (me + d) % n_fs
        return (
            remote(mine_ref, mine_got.at[me], ms.at[d], mr.at[d], fsdp=peer),
            remote(shared_ref, shared_got.at[me], ss.at[d], sr.at[d], fsdp=peer),
        )

    for d in range(1, n_fs):
        for copy in small(d):
            copy.start()
    mine_got[me] = mine_ref[...]
    shared_got[me] = shared_ref[...]

    advance(0)
    tile = 256
    pieces = width // tile
    for piece in range(pieces):
        rows = slice(piece * tile, (piece + 1) * tile)
        gin_ref[rows, :] = mm(normed_ref[:, rows], dpre_ref[...], TN).astype(BF16)
        gout_ref[rows, :] = mm(cot_ref[:, rows], gn_ref[...], TN).astype(BF16)
        if piece % 2 == 1:
            advance(piece // 2 + 1)
    at = pieces // 2 + 1
    for j in range(3):
        for d in order + [0]:
            near(j, d).start()
    for j in range(3):
        source, span, held, summed, _ = parts[j]
        for d in order:
            near(j, d).wait_recv()
            rows = rows_at(source, ((chip + d) % chips) * 2 + core, count)
            add_into(summed.at[d, :, span], rows.at[:, span], held.at[d, :, span])
            far(j, d).start()
        near(j, 0).wait_recv()
        if j == 0:
            advance(at)
    turns = steps + max(n_tp - 3, 0)
    for d in range(1, n_fs):
        for copy in small(d):
            copy.wait_recv()
    total, again = mine_got[0], shared_got[0]
    for peer in range(1, n_fs):
        total, again = total + mine_got[peer], again + shared_got[peer]
    skip_sum = gather_heads(jnp.concatenate(
        [total[at_row:at_row + 1, :] for at_row in range(mine_at[6], mine_at[6] + chan // LANES)] , axis=1
    ) + jnp.zeros((8, chan), F32))
    heads_here = log_out.shape[1]
    for tap in range(4):
        spill_row(taps_out, tap, total, mine_at[tap])
    spill_row(bias_out, 0, total, mine_at[4])
    spill_row(gate_out, 0, total, mine_at[5])
    skip_out[...] = skip_sum[0:1, :heads_here]
    log_out[...] = total[mine_at[7]:mine_at[7] + 1, :heads_here]
    step_out[...] = total[mine_at[8]:mine_at[8] + 1, :heads_here]
    shared_held[...] = again
    shared_z[tp] = again
    for d in range(1, n_tp):
        remote(shared_held, shared_z.at[tp], ts.at[d], tr.at[d], tp=(tp + d) % n_tp).start()
    pl.loop(at + 1, at + 5)(advance)

    def settle(j, target, span):
        source, _, held, _, got = parts[j]
        rows = rows_at(source, me, count)
        add_into(
            target, rows.at[:, span], held.at[0, :, span], *[got.at[d, :, span] for d in order]
        )

    for d in order:
        far(0, d).wait_recv()
    settle(0, bc_held, slice(2 * chan, 2 * chan + 2 * STATE))
    settle(0, dt_out, slice(2 * chan + 2 * STATE, cols))
    bc_got[tp] = bc_held[...]
    for d in range(1, n_tp):
        remote(bc_held, bc_got.at[tp], bs.at[d], br.at[d], tp=(tp + d) % n_tp).start()
    pl.loop(at + 5, turns)(advance)
    for j in (1, 2):
        for d in order:
            far(j, d).wait_recv()
    settle(1, z_out, slice(0, chan))
    settle(1, x_out, slice(chan, 2 * chan))
    settle(2, out_out, slice(0, chan))
    for d in range(1, n_tp):
        peer = (tp + n_tp - d) % n_tp
        remote(shared_held, shared_z.at[peer], ts.at[d], tr.at[d], tp=peer).wait_recv()
        remote(bc_held, bc_got.at[peer], bs.at[d], br.at[d], tp=peer).wait_recv()
    total = shared_z[0]
    for peer in range(1, n_tp):
        total = total + shared_z[peer]
    for tap in range(4):
        spill_row(taps_s_out, tap, total, shared_at[tap])
    spill_row(bias_s_out, 0, total, shared_at[4])
    spill_row(gain_out, 0, total, shared_at[5])
    add_into(bc_out, *[bc_got.at[peer] for peer in range(n_tp)])

    own = rows_at(dn_ref, tp, block)
    for way in range(2):
        for step in range(steps):
            @pl.when(jnp.logical_and(ahead(way, step) == tp, jnp.logical_not(first(way))))
            def _():
                pass_on(way, step).wait_recv()

    for value in range(n_tp):
        @pl.when(tp == value)
        def _():
            for part in range(CHUNKS):
                span = pl.ds(part * chunk, chunk)
                incoming = []
                if value > 0:
                    incoming.append(z_got.at[0, (n_tp - 1 - value) * CHUNKS + part])
                if value < n_tp - 1:
                    incoming.append(z_got.at[1, value * CHUNKS + part])
                add_into(dn_out.at[span], own.at[span], *incoming)

    for way in range(2):
        @pl.when(first(way))
        def _():
            for step in range(steps - 2, steps):
                pass_on(way, step, True).wait_send()

        for step in range(steps):
            @pl.when(jnp.logical_and(passes(way, step), jnp.logical_not(first(way))))
            def _():
                pass_on(way, step).wait_send()
    for j in range(3):
        for d in range(chips):
            near(j, d).wait_send()
        for d in order:
            far(j, d).wait_send()
    for d in range(1, n_fs):
        for copy in small(d):
            copy.wait_send()
    for d in range(1, n_tp):
        remote(shared_held, shared_z.at[tp], ts.at[d], tr.at[d], tp=(tp + d) % n_tp).wait_send()
        remote(bc_held, bc_got.at[tp], bs.at[d], br.at[d], tp=(tp + d) % n_tp).wait_send()


def leave(dn, normed, dpre, cot, gnormed, small, heads_here, n_tp, n_fs):
    block, width = dn.shape[0] // n_tp, dn.shape[1]
    count, cols = width // n_fs, dpre.shape[1]
    chan = gnormed.shape[1]
    chips, steps = n_fs // 2, (n_tp - 1) * CHUNKS
    dma = pltpu.SemaphoreType.DMA
    vmem = pl.BlockSpec(memory_space=pltpu.VMEM)
    room = lambda *shape: pltpu.VMEM(shape, BF16)
    shape = lambda *extents: jax.ShapeDtypeStruct(extents, F32)
    up = lambda n: -(-n // 8) * 8
    mine = (up(7 * chan // LANES + 2), LANES)
    shared = (up((10 * STATE + width) // LANES), LANES)
    outs = [
        shape(block, width), shape(count, chan), shape(count, chan), shape(count, 2 * STATE), shape(count, LANES),
        shape(count, chan), shape(4, chan), shape(1, chan), shape(4, 2 * STATE), shape(1, 2 * STATE),
        shape(1, heads_here), shape(1, heads_here), shape(1, heads_here), shape(1, chan), shape(1, width),
    ]
    return pl.pallas_call(
        functools.partial(exit_kernel, n_tp=n_tp, n_fs=n_fs),
        name="exit",
        in_specs=[vmem] * 10,
        out_specs=[vmem] * len(outs),
        out_shape=outs,
        scratch_shapes=[
            room(width, cols), room(width, chan), pltpu.VMEM(mine, F32), pltpu.VMEM(shared, F32),
            room(2, steps, block // CHUNKS, width), room(2, steps, block // CHUNKS, width),
            room(chips, count, cols), room(chips, count, chan), room(chips, count, cols), room(chips, count, chan),
            room(chips, count, cols), room(chips, count, chan),
            pltpu.VMEM((n_fs,) + mine, F32), pltpu.VMEM((n_fs,) + shared, F32),
            pltpu.VMEM(shared, F32), pltpu.VMEM((n_tp,) + shared, F32),
            room(count, 2 * STATE), room(n_tp, count, 2 * STATE),
            dma((2, steps)), dma((2, steps)), dma((3, chips)), dma((3, chips)), dma((3, chips)), dma((3, chips)),
            dma((n_fs,)), dma((n_fs,)), dma((n_fs,)), dma((n_fs,)), dma((n_tp,)), dma((n_tp,)), dma((n_tp,)),
            dma((n_tp,)),
        ],
        compiler_params=pltpu.CompilerParams(
            collective_id=TAGS["exit"], has_side_effects=True, vmem_limit_bytes=62 << 20
        ),
    )(dn, normed, dpre, cot, gnormed, *small)


def shards(
    tokens, cotangent, seq_start, token_valid, norm_gain, proj_z, proj_x, proj_bc, proj_dt, conv_chan, bias_chan,
    conv_shared, bias_shared, a_log, dt_bias, skip_gain, gate_gain, proj_out,
):
    chan = proj_z.shape[1]
    width = tokens.shape[1]
    heads_here = proj_dt.shape[1]
    inner = chan * lax.axis_size("tp")
    valid = token_valid.astype(F32)[:, None]
    pack_in = jnp.concatenate(
        [proj_z, proj_x, proj_bc, jnp.pad(proj_dt, ((0, 0), (0, LANES - heads_here)))], axis=1
    )
    n_tp, n_fs = lax.axis_size("tp"), lax.axis_size("fsdp")
    tok_all, w_in, w_out = entry(tokens, pack_in, proj_out.T, n_tp, n_fs)
    late_cot, _ = lax.optimization_barrier((cotangent, tok_all))
    cot_all = lax.all_gather(late_cot, "tp", axis=0, tiled=True)
    decay = -jnp.exp(a_log)
    heads = jnp.concatenate([padded(dt_bias, -100.0), padded(decay, 0.0), jnp.zeros((6, LANES), F32)], axis=0)
    taps = jnp.concatenate([conv_chan, conv_shared], axis=1)
    bias = jnp.concatenate([bias_chan, bias_shared])[None, :]
    skip = jnp.repeat(skip_gain, HEAD)[None, :]
    gate = gate_gain[None, :]
    normed, pre, y, gated, sq, enter = mixer_forward(
        seq_start, tok_all, valid, norm_gain[None, :], w_in, taps, bias, heads, skip
    )
    dgn, stats = gate_stats(cot_all, w_out, gate, gated, sq)
    stats = exchange(stats, n_tp)
    gnormed, out_rows = output_part(gated, stats, gate, w_out, inner)
    mixed = lax.psum_scatter(out_rows, "tp", scatter_dimension=0, tiled=True)
    dpre, dn_rows, dtaps, dbias, dhead, dchan, dgain = mixer_backward(
        seq_start, tok_all, valid, w_in, taps, bias, heads, skip, gate, pre, y, enter, dgn, stats, inner
    )
    (
        d_normed, own_z, own_x, own_bc, own_dt, own_out, g_taps, g_bias, g_taps_s, g_bias_s, g_log, g_step, g_skip,
        g_gate, g_gain,
    ) = leave(
        dn_rows, normed, dpre, cot_all, gnormed, (dtaps, dbias, dhead, dchan, dgain), heads_here, n_tp, n_fs
    )
    resid = tokens.astype(F32)
    rstd = lax.rsqrt(jnp.mean(resid * resid, axis=1, keepdims=True) + EPSILON)
    output = (resid + mixed.astype(F32)).astype(BF16)
    scaled_in = d_normed * norm_gain[None, :]
    grad_tokens = (
        cotangent.astype(F32) + rstd * scaled_in
        - resid * (rstd * rstd * rstd) * jnp.mean(scaled_in * resid, axis=1, keepdims=True)
    ).astype(BF16)
    return (
        output, grad_tokens, g_gain[0], own_z, own_x, own_bc, own_dt[:, :heads_here], g_taps, g_bias[0], g_taps_s,
        g_bias_s[0], g_log[0], g_step[0], g_skip[0], g_gate[0], own_out.T,
    )


def solution(mesh):
    in_specs = (
        P(("fsdp", "tp"), None), P(("fsdp", "tp"), None), P("fsdp"), P("fsdp"), P(), P("fsdp", "tp"),
        P("fsdp", "tp"), P("fsdp", None), P("fsdp", "tp"), P(None, "tp"), P("tp"), P(), P(), P("tp"), P("tp"),
        P("tp"), P("tp"), P("tp", "fsdp"),
    )
    out_specs = (
        P(("fsdp", "tp"), None), P(("fsdp", "tp"), None), P(), P("fsdp", "tp"), P("fsdp", "tp"), P("fsdp", None),
        P("fsdp", "tp"), P(None, "tp"), P("tp"), P(), P(), P("tp"), P("tp"), P("tp"), P("tp"), P("tp", "fsdp"),
    )
    return jax.shard_map(shards, mesh=mesh, in_specs=in_specs, out_specs=out_specs, check_vma=False)
```

```python
import functools
import jax
import jax.numpy as jnp
from jax import lax
from jax.experimental import pallas as pl
from jax.experimental.pallas import tpu as pltpu
from jax.sharding import PartitionSpec as P

HEAD = 64
STATE = 128
STRETCH = 256
LANES = 128
EPSILON = 1e-05
F32 = jnp.float32
BF16 = jnp.bfloat16
NN = (((1,), (0,)), ((), ()))
NT = (((1,), (1,)), ((), ()))
TN = (((0,), (0,)), ((), ()))


def mm(a, b, dims=NN):
    return lax.dot_general(a, b, dims, preferred_element_type=F32)


def exact(a, b):
    return lax.dot_general(a, b, NN, precision=lax.Precision.HIGHEST, preferred_element_type=F32)


def halves(v):
    high = v.astype(BF16)
    return high, (v - high.astype(F32)).astype(BF16)


def iota(shape, dim):
    return lax.broadcasted_iota(jnp.int32, shape, dim)


def spread_heads(v, chan):
    high, rest = halves(v)
    rows = iota((2 * LANES, chan), 0) & (LANES - 1)
    pick = jnp.where(rows == (iota((2 * LANES, chan), 1) >> 6), 1.0, 0.0).astype(BF16)
    return mm(jnp.concatenate([high, rest], axis=1), pick)


def gather_heads(v):
    chan = v.shape[1]
    high, rest = halves(v)
    pick = jnp.where((iota((chan, LANES), 0) >> 6) == iota((chan, LANES), 1), 1.0, 0.0).astype(BF16)
    return mm(high, pick) + mm(rest, pick)


def softplus(v):
    return jnp.maximum(v, 0.0) + jnp.log1p(jnp.exp(-jnp.abs(v)))


def sigmoid(v):
    return 1.0 / (1.0 + jnp.exp(-v))


def lower_mask():
    return iota((STRETCH, STRETCH), 0) >= iota((STRETCH, STRETCH), 1)


def convolve(xs_ref, taps_ref, bias_ref):
    total = bias_ref[...] + taps_ref[0:1, :] * xs_ref[5:5 + STRETCH, :]
    for tap in range(1, 4):
        total = total + taps_ref[tap:tap + 1, :] * xs_ref[5 + tap:5 + tap + STRETCH, :]
    return total


def decays(pre_dt, head_ref, valid):
    rates = softplus(pre_dt + head_ref[0:1, :]) * valid
    log_decay = rates * head_ref[1:2, :]
    lower = lower_mask().astype(F32)
    cumulative = exact(lower, log_decay)
    last = cumulative[STRETCH - 1:STRETCH, :]
    return rates, cumulative, jnp.exp(cumulative), jnp.exp(last - cumulative)


def weights_of(cumulative, across, head):
    return jnp.exp(jnp.minimum(cumulative[:, head:head + 1] - across[head:head + 1, :], 0.0))


def backward_kernel(
    open_ref, tok_ref, w_ref, taps_ref, bias_ref, head_ref, skip_ref, gate_ref,
    pre_ref, halo_ref, y_ref, enter_ref, dgn_ref, stats_ref,
    dpre_ref, dnormed_ref, dtaps_ref, dbias_ref, dhead_ref, dchan_ref, dgain_ref,
    dstate, xs, dus,
    *, inner,
):
    chan = y_ref.shape[1]
    wide = chan + 2 * STATE
    step = pl.program_id(0)
    block = pl.num_programs(0) - 1 - step
    opening = open_ref[block] == 1
    keep = jnp.where(opening, 0.0, 1.0).astype(F32)

    @pl.when(step == 0)
    def _():
        dstate[...] = jnp.zeros_like(dstate)
        dus[...] = jnp.zeros_like(dus)
        dtaps_ref[...] = jnp.zeros_like(dtaps_ref)
        dbias_ref[...] = jnp.zeros_like(dbias_ref)
        dhead_ref[...] = jnp.zeros_like(dhead_ref)
        dchan_ref[...] = jnp.zeros_like(dchan_ref)
        dgain_ref[...] = jnp.zeros_like(dgain_ref)

    grstd, cross, valid = row_stats(stats_ref, inner)
    xs[0:8, :] = halo_ref[:, chan:2 * chan + 2 * STATE] * keep
    xs[8:8 + STRETCH, :] = pre_ref[:, chan:2 * chan + 2 * STATE]
    conv = convolve(xs, taps_ref, bias_ref)
    gate_u = sigmoid(conv)
    feats = conv * gate_u
    slope = gate_u * (1.0 + conv * (1.0 - gate_u))
    x = feats[:, :chan]
    bs = feats[:, chan:chan + STATE].astype(BF16)
    cs = feats[:, chan + STATE:].astype(BF16)
    pre_dt = pre_ref[:, 2 * chan + 2 * STATE:]
    rates, cumulative, grown, to_end = decays(pre_dt, head_ref, valid)
    across = cumulative.T
    grown_e = spread_heads(grown, chan)
    rates_e = spread_heads(rates, chan)
    to_end_e = spread_heads(to_end, chan)
    leave_e = grown_e[STRETCH - 1:STRETCH, :]

    pre_z = pre_ref[:, :chan]
    gate_z = sigmoid(pre_z)
    silu_z = pre_z * gate_z * valid
    y = y_ref[...]
    mixed = y + skip_ref[...] * x
    gated = mixed * silu_z
    dgn = dgn_ref[...]
    d_gated = grstd * (gate_ref[...] * dgn) - gated * (grstd * grstd * grstd * cross * (1.0 / inner))
    d_mixed = d_gated * silu_z
    dpre_ref[:, :chan] = (
        d_gated * mixed * (valid * (gate_z * (1.0 + pre_z * (1.0 - gate_z))))
    ).astype(BF16)
    dchan_ref[0:1, :] += jnp.sum(dgn * gated * grstd, axis=0, keepdims=True)
    dchan_ref[1:2, :] += jnp.sum(d_mixed * x, axis=0, keepdims=True)

    dy_b = d_mixed.astype(BF16)
    dy = dy_b.astype(F32)
    scaled = x * rates_e
    scaled_b = scaled.astype(BF16)
    entering = enter_ref[0]
    d_leaving = dstate[...]
    d_leaving_b = d_leaving.astype(BF16)
    tail = mm(bs, d_leaving_b) * to_end_e
    overlap = jnp.where(lower_mask(), mm(cs, bs, NT), 0.0)
    first = iota((STRETCH, LANES), 1) < HEAD
    d_overlap = jnp.zeros((STRETCH, STRETCH), F32)
    parts = []
    for pair in range(chan // LANES):
        cols = slice(pair * LANES, (pair + 1) * LANES)
        dy_pair = dy_b[:, cols]
        x_pair = scaled_b[:, cols]
        zero = jnp.zeros_like(dy_pair)
        sides = [jnp.where(first, dy_pair, zero), jnp.where(first, zero, dy_pair)]
        mats = []
        for side in range(2):
            weight = weights_of(cumulative, across, 2 * pair + side)
            mats.append((weight * overlap).astype(BF16))
            d_overlap = d_overlap + mm(sides[side], x_pair, NT) * weight
        parts.append(mm(jnp.concatenate(mats, axis=0), jnp.concatenate(sides, axis=0), TN))
    d_scaled = jnp.concatenate(parts, axis=1) + tail
    scaled_r = scaled_b.astype(F32)
    d_cum = gather_heads(dy * y - scaled_r * d_scaled)
    d_last = jnp.sum(scaled_r * tail, axis=0, keepdims=True) + leave_e * jnp.sum(
        d_leaving * entering, axis=0, keepdims=True
    )
    d_last = gather_heads(jnp.broadcast_to(d_last, (8, chan)))[0:1, :]
    upper = (iota((STRETCH, STRETCH), 0) <= iota((STRETCH, STRETCH), 1)).astype(F32)
    d_log = exact(upper, d_cum) + d_last
    decay = head_ref[1:2, :]
    d_rates = d_log * decay + gather_heads(x * d_scaled)
    d_dt = d_rates * valid * sigmoid(pre_dt + head_ref[0:1, :])
    dhead_ref[0:1, :] += jnp.sum(d_log * rates, axis=0, keepdims=True) * decay
    dhead_ref[1:2, :] += jnp.sum(d_dt, axis=0, keepdims=True)
    dpre_ref[:, 2 * chan + 2 * STATE:] = d_dt.astype(BF16)

    d_x = d_scaled * rates_e + skip_ref[...] * d_mixed
    d_overlap_b = jnp.where(lower_mask(), d_overlap, 0.0).astype(BF16)
    dy_grown = (dy * grown_e).astype(BF16)
    x_end = (scaled * to_end_e).astype(BF16)
    d_b = mm(d_overlap_b, cs, TN) + mm(x_end, d_leaving_b, NT)
    d_c = mm(d_overlap_b, bs) + mm(dy_grown, entering.astype(BF16), NT)
    dstate[...] = (d_leaving * leave_e + mm(cs, dy_grown, TN)) * keep

    dus[0:STRETCH, :chan] = d_x * slope[:, :chan]
    dus[0:STRETCH, chan:chan + STATE] = d_b * slope[:, chan:chan + STATE]
    dus[0:STRETCH, chan + STATE:] = d_c * slope[:, chan + STATE:]
    d_conv = dus[0:STRETCH, :]
    dbias_ref[...] += jnp.sum(d_conv, axis=0, keepdims=True)
    d_pre = jnp.zeros((STRETCH, wide), F32)
    for tap in range(4):
        dtaps_ref[tap:tap + 1, :] += jnp.sum(d_conv * xs[5 + tap:5 + tap + STRETCH, :], axis=0, keepdims=True)
        d_pre = d_pre + taps_ref[tap:tap + 1, :] * dus[3 - tap:3 - tap + STRETCH, :]
    dpre_ref[:, chan:2 * chan + 2 * STATE] = d_pre.astype(BF16)
    dus[STRETCH:STRETCH + 8, :] = d_conv[0:8, :] * keep

    d_normed = mm(dpre_ref[...], w_ref[...], NT)
    dnormed_ref[...] = d_normed.astype(BF16)
    resid = tok_ref[...].astype(F32)
    rstd = lax.rsqrt(jnp.mean(resid * resid, axis=1, keepdims=True) + EPSILON)
    dgain_ref[...] += jnp.sum(d_normed * (resid * rstd), axis=0, keepdims=True)


def whole(shape):
    return pl.BlockSpec(shape, lambda *_: (0,) * len(shape), pipeline_mode=pl.Buffered(1))


def mixer_backward(
    openings, tok, w_in, taps, bias, heads, skip, gate, pre, y, enter, dgn, stats, inner
):
    tokens, width = tok.shape
    cols = w_in.shape[1]
    chan = skip.shape[1]
    blocks = tokens // STRETCH
    wide = chan + 2 * STATE
    per = STRETCH // 8
    rows = lambda n: pl.BlockSpec((STRETCH, n), lambda i, *_: (blocks - 1 - i, 0))
    return pl.pallas_call(
        functools.partial(backward_kernel, inner=inner),
        name="mixer_backward",
        grid_spec=pltpu.PrefetchScalarGridSpec(
            num_scalar_prefetch=1,
            grid=(blocks,),
            in_specs=[
                rows(width), whole((width, cols)), whole((4, wide)), whole((1, wide)),
                whole((8, LANES)), whole((1, chan)), whole((1, chan)),
                rows(cols),
                pl.BlockSpec((8, cols), lambda i, *_: (jnp.maximum((blocks - 1 - i) * per - 1, 0), 0)),
                rows(chan),
                pl.BlockSpec((1, STATE, chan), lambda i, *_: (blocks - 1 - i, 0, 0)),
                rows(chan),
                pl.BlockSpec((8, STRETCH), lambda i, *_: (0, blocks - 1 - i)),
            ],
            out_specs=[
                rows(cols), rows(width),
                pl.BlockSpec((8, wide), lambda i, *_: (0, 0)),
                pl.BlockSpec((1, wide), lambda i, *_: (0, 0)),
                pl.BlockSpec((8, LANES), lambda i, *_: (0, 0)),
                pl.BlockSpec((8, chan), lambda i, *_: (0, 0)),
                pl.BlockSpec((1, width), lambda i, *_: (0, 0)),
            ],
            scratch_shapes=[
                pltpu.VMEM((STATE, chan), F32),
                pltpu.VMEM((STRETCH + 8, wide), F32),
                pltpu.VMEM((STRETCH + 8, wide), F32),
            ],
        ),
        out_shape=[
            jax.ShapeDtypeStruct((tokens, cols), BF16),
            jax.ShapeDtypeStruct((tokens, width), BF16),
            jax.ShapeDtypeStruct((8, wide), F32),
            jax.ShapeDtypeStruct((1, wide), F32),
            jax.ShapeDtypeStruct((8, LANES), F32),
            jax.ShapeDtypeStruct((8, chan), F32),
            jax.ShapeDtypeStruct((1, width), F32),
        ],
        cost_estimate=pl.CostEstimate(
            flops=4 * tokens * width * cols, bytes_accessed=tokens * cols * 12, transcendentals=tokens * chan
        ),
        compiler_params=pltpu.CompilerParams(vmem_limit_bytes=60 << 20, dimension_semantics=("arbitrary",)),
    )(openings, tok, w_in, taps, bias, heads, skip, gate, pre, pre, y, enter, dgn, stats)


MESH = pl.DeviceIdType.MESH
CHUNKS = 4
TAGS = {"ahead": 1, "exit": 2}


def remote(source, target, send, recv, **where):
    return pltpu.make_async_remote_copy(
        src_ref=source, dst_ref=target, send_sem=send, recv_sem=recv, device_id=where, device_id_type=MESH
    )


def rows_at(ref, index, count):
    return ref.at[pl.ds(pl.multiple_of(index * count, count), count)]


def greet(axis, peers):
    barrier = pltpu.get_barrier_semaphore()
    for peer in peers:
        pl.semaphore_signal(barrier, inc=1, device_id={axis: peer}, device_id_type=MESH)


class Line:
    def __init__(self, tp, n_tp, own, whole_ref, send, recv):
        self.tp, self.n, self.own, self.whole_ref, self.send, self.recv = tp, n_tp, own, whole_ref, send, recv
        self.count = own.shape[0]

    def copy(self, way, step, own=False):
        shift = -1 if way == 0 else 1
        index = self.tp + shift * step
        slot = rows_at(self.whole_ref, index, self.count)
        return remote(
            self.own if own else slot, slot, self.send.at[way, step], self.recv.at[way, step], tp=self.tp - shift
        )

    def sends(self, way, step):
        if way == 0:
            return jnp.logical_and(self.tp < self.n - 1, self.tp >= step)
        return jnp.logical_and(self.tp > 0, self.tp + step <= self.n - 1)

    def takes(self, way, step):
        return self.tp >= step + 1 if way == 0 else self.tp + step + 1 <= self.n - 1

    def start(self, way, step):
        @pl.when(self.sends(way, step))
        def _():
            self.copy(way, step, own=step == 0).start()

    def arrive(self, way, step):
        @pl.when(self.takes(way, step))
        def _():
            shift = -1 if way == 0 else 1
            slot = rows_at(self.whole_ref, self.tp + shift * (step + 1), self.count)
            remote(
                slot, slot, self.send.at[way, step], self.recv.at[way, step], tp=self.tp + shift
            ).wait_recv()

    def finish(self, way, step):
        @pl.when(self.sends(way, step))
        def _():
            self.copy(way, step, own=step == 0).wait_send()


def forward_block(keep, tok, valid, gain_ref, w_ref, taps_ref, bias_ref, head_ref, skip_ref,
                  normed_ref, pre_ref, y_ref, gated_ref, enter_ref, state, xs):
    chan = y_ref.shape[1]
    xs[0:8, :] = xs[STRETCH:STRETCH + 8, :] * keep
    resid = tok.astype(F32)
    rstd = lax.rsqrt(jnp.mean(resid * resid, axis=1, keepdims=True) + EPSILON)
    normed = (resid * rstd * gain_ref[...]).astype(BF16)
    normed_ref[...] = normed
    pre_ref[...] = mm(normed, w_ref[...])
    xs[8:8 + STRETCH, :] = pre_ref[:, chan:2 * chan + 2 * STATE]
    conv = convolve(xs, taps_ref, bias_ref)
    feats = conv * sigmoid(conv)
    x = feats[:, :chan]
    bs = feats[:, chan:chan + STATE].astype(BF16)
    cs = feats[:, chan + STATE:].astype(BF16)
    rates, cumulative, grown, to_end = decays(pre_ref[:, 2 * chan + 2 * STATE:], head_ref, valid)
    across = cumulative.T
    grown_e = spread_heads(grown, chan)
    scaled = x * spread_heads(rates, chan)
    entering = state[...] * keep
    enter_ref[...] = entering
    y_ref[...] = mm(cs, entering.astype(BF16)) * grown_e
    state[...] = entering * grown_e[STRETCH - 1:STRETCH, :] + mm(
        bs, (scaled * spread_heads(to_end, chan)).astype(BF16), TN
    )
    overlap = jnp.where(lower_mask(), mm(cs, bs, NT), 0.0)
    scaled_b = scaled.astype(BF16)
    first = iota((STRETCH, LANES), 1) < HEAD
    for pair in range(chan // LANES):
        cols = slice(pair * LANES, (pair + 1) * LANES)
        both = scaled_b[:, cols]
        mats = [
            (weights_of(cumulative, across, 2 * pair + side) * overlap).astype(BF16) for side in range(2)
        ]
        zero = jnp.zeros_like(both)
        y_ref[:, cols] += mm(
            jnp.concatenate(mats, axis=1),
            jnp.concatenate([jnp.where(first, both, zero), jnp.where(first, zero, both)], axis=0),
        )
    pre_z = pre_ref[:, :chan]
    gated = (y_ref[...] + skip_ref[...] * x) * (pre_z * sigmoid(pre_z)) * valid
    gated_ref[...] = gated
    return jnp.sum(gated * gated, axis=1, keepdims=True)


def as_row(column):
    lane = iota((STRETCH, LANES), 1)
    return jnp.where(lane == 0, column, 0.0).T[0:8, :]


def as_column(row):
    return jnp.concatenate([row, jnp.zeros((LANES - 8, STRETCH), F32)], axis=0).T


def row_stats(stats_ref, inner):
    filled = as_column(stats_ref[...])
    return lax.rsqrt(filled[:, 0:1] * (1.0 / inner) + EPSILON), filled[:, 1:2], filled[:, 2:3]


def ahead_kernel(
    open_ref, step_bias, log_rate, direct, tok_ref, cot_ref, pz_ref, px_ref, pbc_ref, pdt_ref, pout_ref, mask_ref,
    norm_gain, conv_chan, bias_chan, conv_shared, bias_shared, gate_gain,
    tok_out, cot_out, win_out, normed_out, pre_out, y_out, enter_out, dgn_out, gn_out, rows_out, stats_ref,
    taps_ref, bias_ref, head_ref, skip_ref, gate_ref,
    pin_ref, gain_ref, tok_all, cot_all, w_in, w_out, normed, pre, y, gated, enter, dgn, gnormed, rows, state, xs, squares, crosses,
    squares_got, crosses_got,
    own_sem, z_send, z_recv, c_send, c_recv, f_send, f_recv, p_send, p_recv, q_send, q_recv, r_send, r_recv,
    all_sem, out_sem,
    *, n_tp, n_fs, inner,
):
    tp, me = lax.axis_index("tp"), lax.axis_index("fsdp")
    chip, core, chips = me // 2, me % 2, n_fs // 2
    partner = chip * 2 + 1 - core
    blocks = tok_all.shape[0] // STRETCH
    per = tok_ref.shape[0]
    chan = pout_ref.shape[1]
    pin_ref[:, :chan] = pz_ref[...]
    pin_ref[:, chan:2 * chan] = px_ref[...]
    pin_ref[:, 2 * chan:2 * chan + 2 * STATE] = pbc_ref[...]
    heads_here, rows_dt = pdt_ref.shape
    pin_ref[:, 2 * chan + 2 * STATE:] = jnp.concatenate(
        [pdt_ref[...].astype(F32), jnp.zeros((LANES - heads_here, rows_dt), F32)], axis=0
    ).T.astype(BF16)
    greet("fsdp", [((chip + d) % chips) * 2 + core for d in range(1, chips)] + [partner])
    greet("tp", [(tp + d) % n_tp for d in range(1, n_tp)])
    pl.semaphore_wait(pltpu.get_barrier_semaphore(), chips + n_tp - 1)

    packs = ((pin_ref, w_in), (pout_ref, w_out))
    count = pin_ref.shape[0]
    line = Line(tp, n_tp, tok_ref, tok_all, z_send, z_recv)
    late = Line(tp, n_tp, cot_ref, cot_all, c_send, c_recv)
    for way in range(2):
        line.start(way, 0)
    for j, (pack, full) in enumerate(packs):
        for d in range(1, chips):
            remote(
                pack, rows_at(full, me, count), f_send.at[j, d], f_recv.at[j, d], fsdp=((chip + d) % chips) * 2 + core
            ).start()
        remote(pack, rows_at(full, me, count), p_send.at[j, 0], p_recv.at[j, 0], fsdp=partner).start()
    own = [
        pltpu.make_async_copy(tok_ref, rows_at(tok_all, tp, per), own_sem.at[0]),
        pltpu.make_async_copy(pin_ref, rows_at(w_in, me, count), own_sem.at[1]),
        pltpu.make_async_copy(pout_ref, rows_at(w_out, me, count), own_sem.at[2]),
        pltpu.make_async_copy(cot_ref, rows_at(cot_all, tp, per), own_sem.at[3]),
    ]
    for copy in own:
        copy.start()
    state[...] = jnp.zeros_like(state)
    xs[...] = jnp.zeros_like(xs)
    lane = iota((8, LANES), 1)
    place = iota((8, LANES), 0)
    step_row, rate_row, skip_row = (
        sum(jnp.where(lane == head, source[head], 0.0) for head in range(heads_here))
        for source in (step_bias, log_rate, direct)
    )
    live = lane < heads_here
    head_ref[...] = jnp.where(
        place == 0, jnp.where(live, step_row, -100.0), jnp.where(live & (place == 1), -jnp.exp(rate_row), 0.0)
    )
    skip_ref[...] = spread_heads(skip_row, chan)[0:1, :]
    gain_ref[...] = norm_gain[...].reshape(gain_ref.shape)
    gate_ref[...] = gate_gain[...].reshape(gate_ref.shape)
    taps_ref[:, :chan] = conv_chan[...]
    taps_ref[:, chan:] = conv_shared[...]
    bias_ref[:, :chan] = bias_chan[...].reshape(1, chan)
    bias_ref[:, chan:] = bias_shared[...].reshape(1, 2 * STATE)
    for step in range(n_tp - 1):
        for way in range(2):
            line.arrive(way, step)
            if step + 1 < n_tp - 1:
                line.start(way, step + 1)
        if step == n_tp - 3 or n_tp < 3 and step == 0:
            for j, (pack, full) in enumerate(packs):
                for d in range(1, chips):
                    slot = rows_at(full, ((chip + chips - d) % chips) * 2 + core, count)
                    remote(slot, slot, f_send.at[j, d], f_recv.at[j, d], fsdp=partner).wait_recv()
                    remote(slot, slot, p_send.at[j, d], p_recv.at[j, d], fsdp=partner).start()
    for step in range(n_tp - 1):
        for way in range(2):
            line.finish(way, step)
    for way in range(2):
        late.start(way, 0)
    for j, (pack, full) in enumerate(packs):
        for d in range(chips):
            slot = rows_at(full, ((chip + chips - d) % chips) * 2 + 1 - core, count)
            remote(slot, slot, p_send.at[j, d], p_recv.at[j, d], fsdp=partner).wait()
        for d in range(1, chips):
            remote(pack, rows_at(full, me, count), f_send.at[j, d], f_recv.at[j, d], fsdp=partner).wait_send()
    for copy in own:
        copy.wait()
    wholes = [
        pltpu.make_async_copy(tok_all, tok_out, all_sem.at[0]), pltpu.make_async_copy(w_in, win_out, all_sem.at[1]),
    ]
    for copy in wholes:
        copy.start()

    def span(block):
        return pl.ds(pl.multiple_of(block * STRETCH, STRETCH), STRETCH)

    def out(k, block):
        at = span(block)
        pairs = (
            (normed.at[at], normed_out.at[at]), (pre.at[block % 2], pre_out.at[at]), (y.at[at], y_out.at[at]),
            (enter.at[block], enter_out.at[block]), (gnormed.at[at], gn_out.at[at]),
            (rows.at[block % 2], rows_out.at[at]), (dgn.at[at], dgn_out.at[at]), (cot_all.at[at], cot_out.at[at]),
        )
        return pltpu.make_async_copy(*pairs[k], out_sem.at[k, block])

    @pl.loop(0, blocks)
    def _(block):
        at = span(block)
        keep = jnp.where(open_ref[block] == 1, 0.0, 1.0).astype(F32)

        @pl.when(block >= 2)
        def _():
            out(1, block - 2).wait()

        valid = mask_ref[at].reshape(1, STRETCH).astype(F32)
        squares[:, at] = jnp.where(iota((8, STRETCH), 0) == 2, valid, 0.0)
        total = forward_block(
            keep, tok_all[at, :], as_column(squares[:, at])[:, 2:3], gain_ref, w_in, taps_ref, bias_ref, head_ref, skip_ref,
            normed.at[at], pre.at[block % 2], y.at[at], gated.at[at], enter.at[block], state, xs,
        )
        squares[0:1, at] = as_row(total)[0:1, :]
        for k in range(4):
            out(k, block).start()

        @pl.when(block == max(blocks - 2, 0))
        def _():
            for way in range(2):
                late.arrive(way, 0)
                if n_tp > 2:
                    late.start(way, 1)

    def swap(part, got, send, recv):
        for d in range(1, n_tp):
            remote(part, got.at[tp], send.at[d], recv.at[d], tp=(tp + d) % n_tp).start()
        got[tp] = part[...]
        for d in range(1, n_tp):
            slot = got.at[(tp + n_tp - d) % n_tp]
            remote(slot, slot, send.at[d], recv.at[d], tp=(tp + d) % n_tp).wait_recv()
        total = got[0]
        for peer in range(1, n_tp):
            total = total + got[peer]
        return total

    stats_ref[...] = swap(squares, squares_got, q_send, q_recv)

    @pl.loop(0, blocks)
    def _(block):
        at = span(block)

        @pl.when(block >= 2)
        def _():
            out(5, block - 2).wait()

        grstd, _, _ = row_stats(stats_ref.at[:, at], inner)
        value = (gated[at, :] * grstd * gate_ref[...]).astype(BF16)
        gnormed[at, :] = value
        rows[block % 2] = mm(value, w_out[...], NT).astype(BF16)
        out(4, block).start()
        out(5, block).start()

    def gradient(block):
        at = span(block)
        value = mm(cot_all[at, :], w_out[...])
        dgn[at, :] = value
        crosses[:, at] = as_row(jnp.sum(gate_ref[...] * value * gated[at, :], axis=1, keepdims=True))
        out(6, block).start()
        out(7, block).start()

    ratio = per // STRETCH

    def gradients(index):
        for k in range(ratio):
            gradient(index * ratio + k)

    gradients(tp)
    for step in range(n_tp - 1):
        for way in range(2):
            if step > 0:
                late.arrive(way, step)
                if step + 1 < n_tp - 1:
                    late.start(way, step + 1)
        for way in range(2):
            @pl.when(late.takes(way, step))
            def _():
                gradients(tp - step - 1 if way == 0 else tp + step + 1)

    total = swap(crosses, crosses_got, r_send, r_recv)
    stats_ref[1:2, :] = total[0:1, :]
    stats_ref[2:3, :] = squares[2:3, :]

    for copy in wholes:
        copy.wait()

    @pl.loop(0, blocks)
    def _(block):
        for k in (0, 2, 3, 4, 6, 7):
            out(k, block).wait()

    for block in range(max(blocks - 2, 0), blocks):
        out(1, block).wait()
        out(5, block).wait()
    for step in range(n_tp - 1):
        for way in range(2):
            late.finish(way, step)
    for d in range(1, n_tp):
        remote(squares, squares_got.at[tp], q_send.at[d], q_recv.at[d], tp=(tp + d) % n_tp).wait_send()
        remote(crosses, crosses_got.at[tp], r_send.at[d], r_recv.at[d], tp=(tp + d) % n_tp).wait_send()


def ahead(
    openings, heads, tokens, cotangent, projections, mask, vectors, n_tp, n_fs
):
    per, width = tokens.shape
    total = per * n_tp
    count, chan = projections[0].shape
    wide = chan + 2 * STATE
    cols = chan + wide + LANES
    blocks = total // STRETCH
    chips = n_fs // 2
    dma = pltpu.SemaphoreType.DMA
    anywhere = pl.BlockSpec(memory_space=pl.ANY)
    vmem = pl.BlockSpec(memory_space=pltpu.VMEM)
    shape = jax.ShapeDtypeStruct
    return pl.pallas_call(
        functools.partial(ahead_kernel, n_tp=n_tp, n_fs=n_fs, inner=chan * n_tp),
        name="ahead",
        in_specs=[pl.BlockSpec(memory_space=pltpu.SMEM)] * 4 + [vmem] * 14,
        out_specs=[anywhere] * 10 + [vmem] * 6,
        out_shape=[
            shape((total, width), BF16), shape((total, width), BF16), shape((count * n_fs, cols), BF16),
            shape((total, width), BF16), shape((total, cols), F32), shape((total, chan), F32),
            shape((blocks, STATE, chan), F32), shape((total, chan), F32), shape((total, chan), BF16),
            shape((total, width), BF16), shape((8, total), F32), shape((4, wide), F32), shape((1, wide), F32),
            shape((8, LANES), F32), shape((1, chan), F32), shape((1, chan), F32),
        ],
        scratch_shapes=[
            pltpu.VMEM((count, cols), BF16), pltpu.VMEM((1, width), F32),
            pltpu.VMEM((total, width), BF16), pltpu.VMEM((total, width), BF16),
            pltpu.VMEM((count * n_fs, cols), BF16), pltpu.VMEM((count * n_fs, chan), BF16),
            pltpu.VMEM((total, width), BF16), pltpu.VMEM((2, STRETCH, cols), F32), pltpu.VMEM((total, chan), F32),
            pltpu.VMEM((total, chan), F32), pltpu.VMEM((blocks, STATE, chan), F32), pltpu.VMEM((total, chan), F32),
            pltpu.VMEM((total, chan), BF16), pltpu.VMEM((2, STRETCH, width), BF16),
            pltpu.VMEM((STATE, chan), F32), pltpu.VMEM((STRETCH + 8, wide), F32),
            pltpu.VMEM((8, total), F32), pltpu.VMEM((8, total), F32),
            pltpu.VMEM((n_tp, 8, total), F32), pltpu.VMEM((n_tp, 8, total), F32),
            dma((4,)), dma((2, n_tp - 1)), dma((2, n_tp - 1)), dma((2, n_tp - 1)), dma((2, n_tp - 1)),
            dma((2, chips)), dma((2, chips)), dma((2, chips)), dma((2, chips)),
            dma((n_tp,)), dma((n_tp,)), dma((n_tp,)), dma((n_tp,)), dma((2,)), dma((8, blocks)),
        ],
        compiler_params=pltpu.CompilerParams(
            collective_id=TAGS["ahead"], has_side_effects=True, vmem_limit_bytes=63 << 20
        ),
    )(openings, *heads, tokens, cotangent, *projections, mask, *vectors)


def add_into(target, *sources):
    rows, tile = target.shape[0], 32

    @pl.loop(0, rows // tile)
    def _(i):
        at = pl.ds(pl.multiple_of(i * tile, tile), tile)
        total = sources[0][at, :].astype(F32)
        for source in sources[1:]:
            total = total + source[at, :].astype(F32)
        target[at, :] = total.astype(target.dtype)


def fill_rows(target, pieces):
    at = 0
    for source, row, start, length in pieces:
        for k in range(length // LANES):
            target[at:at + 1, :] = source[row:row + 1, start + k * LANES:start + (k + 1) * LANES]
            at += 1
    if at < target.shape[0]:
        target[at:, :] = jnp.zeros((target.shape[0] - at, LANES), F32)


def finish_kernel(
    tok_ref, cot_ref, mixed_ref, gain_ref, dn_ref, own_ref, bc_ref, mine_ref, shared_ref,
    output, grad_tokens, g_gain, g_z, g_x, g_bc, g_dt, g_taps, g_bias, g_taps_s, g_bias_s, g_log, g_step, g_skip, g_gate,
    g_out,
):
    chan, heads_here = g_z.shape[1], g_log.shape[0]
    resid = tok_ref[...].astype(F32)
    output[...] = (resid + mixed_ref[...].astype(F32)).astype(BF16)
    rstd = lax.rsqrt(jnp.mean(resid * resid, axis=1, keepdims=True) + EPSILON)
    scaled = dn_ref[...] * gain_ref[...].reshape(1, resid.shape[1])
    grad_tokens[...] = (
        cot_ref[...].astype(F32) + rstd * scaled
        - resid * (rstd * rstd * rstd) * jnp.mean(scaled * resid, axis=1, keepdims=True)
    ).astype(BF16)
    g_z[...] = own_ref[:, :chan]
    g_x[...] = own_ref[:, chan:2 * chan]
    g_dt[...] = own_ref[:, 2 * chan:2 * chan + LANES].T[0:heads_here, :]
    g_out[...] = own_ref[:, 2 * chan + LANES:]
    g_bc[...] = bc_ref[...]

    def row(source, at, length):
        return jnp.concatenate([source[at + k:at + k + 1, :] for k in range(length // LANES)], axis=1)

    per = chan // LANES
    for tap in range(4):
        g_taps[tap:tap + 1, :] = row(mine_ref, tap * per, chan)
        g_taps_s[tap:tap + 1, :] = row(shared_ref, tap * 2, 2 * STATE)
    g_bias[...] = row(mine_ref, 4 * per, chan).reshape(chan)
    g_gate[...] = row(mine_ref, 5 * per, chan).reshape(chan)
    skip = gather_heads(jnp.broadcast_to(row(mine_ref, 6 * per, chan), (8, chan)))
    g_skip[...] = skip[0:1, :heads_here].reshape(heads_here)
    g_log[...] = mine_ref[7 * per:7 * per + 1, :heads_here].reshape(heads_here)
    g_step[...] = mine_ref[7 * per + 1:7 * per + 2, :heads_here].reshape(heads_here)
    g_bias_s[...] = row(shared_ref, 8, 2 * STATE).reshape(2 * STATE)
    g_gain[...] = row(shared_ref, 10, g_gain.shape[0]).reshape(g_gain.shape[0])


def finish(tokens, cotangent, mixed, gain, dn, own, bc, mine, shared, heads_here):
    rows, width = tokens.shape
    count = own.shape[0]
    chan = (own.shape[1] - LANES) // 3
    vmem = pl.BlockSpec(memory_space=pltpu.VMEM)
    shape = lambda *extents: jax.ShapeDtypeStruct(extents, F32)
    outs = [
        jax.ShapeDtypeStruct((rows, width), BF16), jax.ShapeDtypeStruct((rows, width), BF16), shape(width),
        shape(count, chan), shape(count, chan), shape(count, 2 * STATE), shape(heads_here, count), shape(4, chan),
        shape(chan), shape(4, 2 * STATE), shape(2 * STATE), shape(heads_here), shape(heads_here), shape(heads_here),
        shape(chan), shape(count, chan),
    ]
    return pl.pallas_call(
        finish_kernel, name="finish", in_specs=[vmem] * 9, out_specs=[vmem] * len(outs), out_shape=outs,
        compiler_params=pltpu.CompilerParams(vmem_limit_bytes=40 << 20),
    )(tokens, cotangent, mixed, gain, dn, own, bc, mine, shared)


def exit_kernel(
    dn_ref, normed_ref, dpre_ref, cot_ref, gn_ref, dtaps_ref, dbias_ref, dhead_ref, dchan_ref, dgain_ref,
    dn_out, own_out, bc_out, mine_out, shared_out,
    gin_ref, gout_ref, mine_ref, shared_ref,
    z_held, z_got, near_in, near_out, far_in, far_out, got_in, got_out, mine_got, shared_got, shared_held, shared_z,
    bc_held, bc_got,
    zs, zr, ns, nr, fs, fr, ms, mr, ss, sr, ts, tr, bs, br,
    *, n_tp, n_fs,
):
    tp, me = lax.axis_index("tp"), lax.axis_index("fsdp")
    chip, core, chips = me // 2, me % 2, n_fs // 2
    partner = chip * 2 + 1 - core
    chan = gout_ref.shape[1]
    cols = gin_ref.shape[1]
    width = gin_ref.shape[0]
    fill_rows(
        mine_ref, [(dtaps_ref, tap, 0, chan) for tap in range(4)] + [(dbias_ref, 0, 0, chan)]
        + [(dchan_ref, row, 0, chan) for row in range(2)] + [(dhead_ref, row, 0, LANES) for row in range(2)]
    )
    fill_rows(
        shared_ref, [(dtaps_ref, tap, chan, 2 * STATE) for tap in range(4)] + [(dbias_ref, 0, chan, 2 * STATE)]
        + [(dgain_ref, 0, 0, width)]
    )
    block, count = dn_out.shape[0], own_out.shape[0]
    greet("fsdp", [(me + d) % n_fs for d in range(1, n_fs)])
    greet("tp", [(tp + d) % n_tp for d in range(1, n_tp)])
    pl.semaphore_wait(pltpu.get_barrier_semaphore(), n_fs - 1 + n_tp - 1)

    chunk = block // CHUNKS
    steps = (n_tp - 1) * CHUNKS

    def ahead(way, step):
        return n_tp - 1 - step // CHUNKS if way == 0 else step // CHUNKS

    def passes(way, step):
        return ahead(way, step) > tp if way == 0 else ahead(way, step) < tp

    def first(way):
        return tp == 0 if way == 0 else tp == n_tp - 1

    def local(way, step):
        return dn_ref.at[pl.ds(pl.multiple_of(ahead(way, step) * block + step % CHUNKS * chunk, chunk), chunk)]

    def pass_on(way, step, direct=False):
        towards = tp + 1 if way == 0 else tp - 1
        source = local(way, step) if direct else z_held.at[way, step]
        return remote(source, z_got.at[way, step], zs.at[way, step], zr.at[way, step], tp=towards)

    for way in range(2):
        @pl.when(first(way))
        def _():
            for step in range(2):
                pass_on(way, step, True).start()

    def advance(turn):
        for way in range(2):
            lag = jnp.maximum(tp - 1 if way == 0 else n_tp - 2 - tp, 0)
            step = turn - lag
            live = jnp.logical_and(step >= 0, step < steps)

            @pl.when(jnp.logical_and(first(way), live))
            def _():
                pass_on(way, step, True).wait_send()

                @pl.when(step + 2 < steps)
                def _():
                    pass_on(way, step + 2, True).start()

            @pl.when(jnp.logical_and(jnp.logical_and(passes(way, step), live), jnp.logical_not(first(way))))
            def _():
                pass_on(way, step).wait_recv()
                add_into(z_held.at[way, step], local(way, step), z_got.at[way, step])
                pass_on(way, step).start()

    parts = (
        (gin_ref, slice(2 * chan, cols), near_in, far_in, got_in),
        (gout_ref, slice(0, chan), near_out, far_out, got_out),
        (gin_ref, slice(chan, 2 * chan), near_in, far_in, got_in),
        (gin_ref, slice(0, chan), near_in, far_in, got_in),
    )

    def near(j, d):
        source, span, held, _, _ = parts[j]
        rows = rows_at(source, ((chip + d) % chips) * 2 + 1 - core, count)
        return remote(rows.at[:, span], held.at[d, :, span], ns.at[j, d], nr.at[j, d], fsdp=partner)

    def far(j, d):
        _, span, _, held, got = parts[j]
        return remote(
            held.at[d, :, span], got.at[d, :, span], fs.at[j, d], fr.at[j, d], fsdp=((chip + d) % chips) * 2 + core
        )

    order = [d for d in range(1, chips)]

    def small(d):
        peer = (me + d) % n_fs
        return (
            remote(mine_ref, mine_got.at[me], ms.at[d], mr.at[d], fsdp=peer),
            remote(shared_ref, shared_got.at[me], ss.at[d], sr.at[d], fsdp=peer),
        )

    for d in range(1, n_fs):
        for copy in small(d):
            copy.start()
    mine_got[me] = mine_ref[...]
    shared_got[me] = shared_ref[...]

    def differentiate(j):
        _, span, *_ = parts[j]
        left, right, target = (cot_ref, gn_ref, gout_ref) if j == 1 else (normed_ref, dpre_ref, gin_ref)
        tile = 256

        @pl.loop(0, width // tile)
        def _(piece):
            at = pl.ds(pl.multiple_of(piece * tile, tile), tile)
            target[at, span] = mm(left[:, at], right[:, span], TN).astype(BF16)

        for d in order + [0]:
            near(j, d).start()

    def send_sums(j):
        source, span, held, summed, _ = parts[j]
        for d in order:
            near(j, d).wait_recv()
            rows = rows_at(source, ((chip + d) % chips) * 2 + core, count)
            add_into(summed.at[d, :, span], rows.at[:, span], held.at[d, :, span])
            far(j, d).start()
        near(j, 0).wait_recv()

    differentiate(0)
    advance(0)
    differentiate(1)
    send_sums(0)
    advance(1)
    differentiate(2)
    send_sums(1)
    advance(2)
    differentiate(3)
    send_sums(2)
    advance(3)
    send_sums(3)
    at = 3
    turns = steps + max(n_tp - 3, 0)
    for d in range(1, n_fs):
        for copy in small(d):
            copy.wait_recv()
    total, again = mine_got[0], shared_got[0]
    for peer in range(1, n_fs):
        total, again = total + mine_got[peer], again + shared_got[peer]
    mine_out[...] = total
    shared_held[...] = again
    shared_z[tp] = again
    for d in range(1, n_tp):
        remote(shared_held, shared_z.at[tp], ts.at[d], tr.at[d], tp=(tp + d) % n_tp).start()
    pl.loop(at + 1, at + 5)(advance)

    def settle(j, target, span):
        source, _, held, _, got = parts[j]
        rows = rows_at(source, me, count)
        add_into(
            target, rows.at[:, span], held.at[0, :, span], *[got.at[d, :, span] for d in order]
        )

    for d in order:
        far(0, d).wait_recv()
    settle(0, bc_held, slice(2 * chan, 2 * chan + 2 * STATE))
    bc_got[tp] = bc_held[...]
    for d in range(1, n_tp):
        remote(bc_held, bc_got.at[tp], bs.at[d], br.at[d], tp=(tp + d) % n_tp).start()
    pl.loop(at + 5, turns)(advance)
    settle(0, own_out.at[:, 2 * chan:2 * chan + LANES], slice(2 * chan + 2 * STATE, cols))
    for j in (1, 2, 3):
        for d in order:
            far(j, d).wait_recv()
    settle(1, own_out.at[:, 2 * chan + LANES:], slice(0, chan))
    settle(2, own_out.at[:, chan:2 * chan], slice(chan, 2 * chan))
    settle(3, own_out.at[:, :chan], slice(0, chan))
    for d in range(1, n_tp):
        peer = (tp + n_tp - d) % n_tp
        remote(shared_held, shared_z.at[peer], ts.at[d], tr.at[d], tp=peer).wait_recv()
        remote(bc_held, bc_got.at[peer], bs.at[d], br.at[d], tp=peer).wait_recv()
    total = shared_z[0]
    for peer in range(1, n_tp):
        total = total + shared_z[peer]
    shared_out[...] = total
    add_into(bc_out, *[bc_got.at[peer] for peer in range(n_tp)])

    own = rows_at(dn_ref, tp, block)
    for way in range(2):
        for step in range(steps):
            @pl.when(jnp.logical_and(ahead(way, step) == tp, jnp.logical_not(first(way))))
            def _():
                pass_on(way, step).wait_recv()

    for value in range(n_tp):
        @pl.when(tp == value)
        def _():
            for part in range(CHUNKS):
                span = pl.ds(part * chunk, chunk)
                incoming = []
                if value > 0:
                    incoming.append(z_got.at[0, (n_tp - 1 - value) * CHUNKS + part])
                if value < n_tp - 1:
                    incoming.append(z_got.at[1, value * CHUNKS + part])
                add_into(dn_out.at[span], own.at[span], *incoming)

    for way in range(2):
        for step in range(steps):
            @pl.when(jnp.logical_and(passes(way, step), jnp.logical_not(first(way))))
            def _():
                pass_on(way, step).wait_send()
    for j in range(4):
        for d in range(chips):
            near(j, d).wait_send()
        for d in order:
            far(j, d).wait_send()
    for d in range(1, n_fs):
        for copy in small(d):
            copy.wait_send()
    for d in range(1, n_tp):
        remote(shared_held, shared_z.at[tp], ts.at[d], tr.at[d], tp=(tp + d) % n_tp).wait_send()
        remote(bc_held, bc_got.at[tp], bs.at[d], br.at[d], tp=(tp + d) % n_tp).wait_send()


def leave(dn, normed, dpre, cot, gnormed, small, n_tp, n_fs):
    block, width = dn.shape[0] // n_tp, dn.shape[1]
    count, cols = width // n_fs, dpre.shape[1]
    chan = gnormed.shape[1]
    chips, steps = n_fs // 2, (n_tp - 1) * CHUNKS
    dma = pltpu.SemaphoreType.DMA
    vmem = pl.BlockSpec(memory_space=pltpu.VMEM)
    room = lambda *shape: pltpu.VMEM(shape, BF16)
    shape = lambda *extents: jax.ShapeDtypeStruct(extents, F32)
    up = lambda n: -(-n // 8) * 8
    mine = (up(7 * chan // LANES + 2), LANES)
    shared = (up((10 * STATE + width) // LANES), LANES)
    outs = [
        shape(block, width), shape(count, 3 * chan + LANES), shape(count, 2 * STATE), shape(*mine), shape(*shared),
    ]
    return pl.pallas_call(
        functools.partial(exit_kernel, n_tp=n_tp, n_fs=n_fs),
        name="exit",
        in_specs=[vmem] * 10,
        out_specs=[vmem] * len(outs),
        out_shape=outs,
        scratch_shapes=[
            room(width, cols), room(width, chan), pltpu.VMEM(mine, F32), pltpu.VMEM(shared, F32),
            room(2, steps, block // CHUNKS, width), room(2, steps, block // CHUNKS, width),
            room(chips, count, cols), room(chips, count, chan), room(chips, count, cols), room(chips, count, chan),
            room(chips, count, cols), room(chips, count, chan),
            pltpu.VMEM((n_fs,) + mine, F32), pltpu.VMEM((n_fs,) + shared, F32),
            pltpu.VMEM(shared, F32), pltpu.VMEM((n_tp,) + shared, F32),
            room(count, 2 * STATE), room(n_tp, count, 2 * STATE),
            dma((2, steps)), dma((2, steps)), dma((4, chips)), dma((4, chips)), dma((4, chips)), dma((4, chips)),
            dma((n_fs,)), dma((n_fs,)), dma((n_fs,)), dma((n_fs,)), dma((n_tp,)), dma((n_tp,)), dma((n_tp,)),
            dma((n_tp,)),
        ],
        compiler_params=pltpu.CompilerParams(
            collective_id=TAGS["exit"], has_side_effects=True, vmem_limit_bytes=62 << 20
        ),
    )(dn, normed, dpre, cot, gnormed, *small)


def shards(
    tokens, cotangent, seq_start, token_valid, norm_gain, proj_z, proj_x, proj_bc, proj_dt, conv_chan, bias_chan,
    conv_shared, bias_shared, a_log, dt_bias, skip_gain, gate_gain, proj_out,
):
    chan, heads_here = proj_z.shape[1], proj_dt.shape[1]
    n_tp, n_fs = lax.axis_size("tp"), lax.axis_size("fsdp")
    tok_all, cot_all, w_in, normed, pre, y, enter, dgn, gnormed, out_rows, stats, taps, bias, heads, skip, gate = ahead(
        seq_start, (dt_bias, a_log, skip_gain), tokens, cotangent,
        (proj_z, proj_x, proj_bc, proj_dt.T, proj_out.T), token_valid,
        (norm_gain, conv_chan, bias_chan, conv_shared, bias_shared, gate_gain), n_tp, n_fs,
    )
    mixed = lax.psum_scatter(out_rows, "tp", scatter_dimension=0, tiled=True)
    dpre, dn_rows, *small = mixer_backward(
        seq_start, tok_all, w_in, taps, bias, heads, skip, gate, pre, y, enter, dgn, stats, chan * n_tp
    )
    sums = leave(dn_rows, normed, dpre, cot_all, gnormed, small, n_tp, n_fs)
    grads = list(finish(tokens, cotangent, mixed, norm_gain, *sums, heads_here))
    grads[6], grads[15] = grads[6].T, grads[15].T
    return tuple(grads)


def solution(mesh):
    in_specs = (
        P(("fsdp", "tp"), None), P(("fsdp", "tp"), None), P("fsdp"), P("fsdp"), P(), P("fsdp", "tp"),
        P("fsdp", "tp"), P("fsdp", None), P("fsdp", "tp"), P(None, "tp"), P("tp"), P(), P(), P("tp"), P("tp"),
        P("tp"), P("tp"), P("tp", "fsdp"),
    )
    out_specs = (
        P(("fsdp", "tp"), None), P(("fsdp", "tp"), None), P(), P("fsdp", "tp"), P("fsdp", "tp"), P("fsdp", None),
        P("fsdp", "tp"), P(None, "tp"), P("tp"), P(), P(), P("tp"), P("tp"), P("tp"), P("tp"), P("tp", "fsdp"),
    )
    return jax.shard_map(shards, mesh=mesh, in_specs=in_specs, out_specs=out_specs, check_vma=False)
```

```python
import functools
import jax
import jax.numpy as jnp
from jax import lax
from jax.experimental import pallas as pl
from jax.experimental.pallas import tpu as pltpu
from jax.sharding import PartitionSpec as P

HEAD = 64
STATE = 128
STRETCH = 256
LANES = 128
EPSILON = 1e-05
PLACES = 3
F32 = jnp.float32
BF16 = jnp.bfloat16
NN = (((1,), (0,)), ((), ()))
NT = (((1,), (1,)), ((), ()))
TN = (((0,), (0,)), ((), ()))


def mm(a, b, dims=NN):
    return lax.dot_general(a, b, dims, preferred_element_type=F32)


def exact(a, b):
    return lax.dot_general(a, b, NN, precision=lax.Precision.HIGHEST, preferred_element_type=F32)


def halves(v):
    high = v.astype(BF16)
    return high, (v - high.astype(F32)).astype(BF16)


def iota(shape, dim):
    return lax.broadcasted_iota(jnp.int32, shape, dim)


def spread_heads(v, chan):
    high, rest = halves(v)
    rows = iota((2 * LANES, chan), 0) & (LANES - 1)
    pick = jnp.where(rows == (iota((2 * LANES, chan), 1) >> 6), 1.0, 0.0).astype(BF16)
    return mm(jnp.concatenate([high, rest], axis=1), pick)


def gather_heads(v):
    chan = v.shape[1]
    high, rest = halves(v)
    pick = jnp.where((iota((chan, LANES), 0) >> 6) == iota((chan, LANES), 1), 1.0, 0.0).astype(BF16)
    return mm(high, pick) + mm(rest, pick)


def softplus(v):
    return jnp.maximum(v, 0.0) + jnp.log1p(jnp.exp(-jnp.abs(v)))


def sigmoid(v):
    return 1.0 / (1.0 + jnp.exp(-v))


def lower_mask():
    return iota((STRETCH, STRETCH), 0) >= iota((STRETCH, STRETCH), 1)


def convolve(xs_ref, taps_ref, bias_ref):
    total = bias_ref[...] + taps_ref[0:1, :] * xs_ref[5:5 + STRETCH, :]
    for tap in range(1, 4):
        total = total + taps_ref[tap:tap + 1, :] * xs_ref[5 + tap:5 + tap + STRETCH, :]
    return total


def decays(pre_dt, head_ref, valid):
    rates = softplus(pre_dt + head_ref[0:1, :]) * valid
    log_decay = rates * head_ref[1:2, :]
    lower = lower_mask().astype(F32)
    cumulative = exact(lower, log_decay)
    last = cumulative[STRETCH - 1:STRETCH, :]
    return rates, cumulative, jnp.exp(cumulative), jnp.exp(last - cumulative)


def weights_of(cumulative, across, head):
    return jnp.exp(jnp.minimum(cumulative[:, head:head + 1] - across[head:head + 1, :], 0.0))


def backward_kernel(
    open_ref, tok_ref, w_hbm, taps_ref, bias_ref, head_ref, skip_ref, gate_ref,
    pre_ref, halo_ref, y_ref, enter_ref, dgn_ref, stats_ref, rows_ref,
    dpre_ref, dnormed_ref, dtaps_ref, dbias_ref, dhead_ref, dchan_ref, dgain_ref, mixed_ref,
    dstate, xs, dus, rows, w_ref, o_got, fetch_sem, o_send, o_recv,
    *, inner, n_tp,
):
    chan = y_ref.shape[1]
    wide = chan + 2 * STATE
    step = pl.program_id(0)
    block = pl.num_programs(0) - 1 - step
    opening = open_ref[block] == 1
    keep = jnp.where(opening, 0.0, 1.0).astype(F32)
    tp = lax.axis_index("tp")
    per = rows.shape[0] // n_tp
    chunk = per // CHUNKS
    sums = LineSum(
        tp, n_tp, CHUNKS - EARLY, lambda index, part: chunk_of(rows, index, per, part + EARLY, chunk),
        lambda index, part: chunk_of(rows_ref, index, per, part + EARLY, chunk), o_got, o_send, o_recv,
    )

    fetches = (
        pltpu.make_async_copy(rows_ref, rows, fetch_sem.at[0]), pltpu.make_async_copy(w_hbm, w_ref, fetch_sem.at[1])
    )

    def turn(place):
        at = step * PLACES + place - 2

        @pl.when(jnp.logical_and(at >= 0, at < sums.turns))
        def _():
            sums.advance(at)

    @pl.when(step == 0)
    def _():
        for fetch in fetches:
            fetch.start()
        line_greeting(tp, n_tp)
        sums.kick()

    @pl.when(step == 0)
    def _():
        dstate[...] = jnp.zeros_like(dstate)
        dus[...] = jnp.zeros_like(dus)
        dtaps_ref[...] = jnp.zeros_like(dtaps_ref)
        dbias_ref[...] = jnp.zeros_like(dbias_ref)
        dhead_ref[...] = jnp.zeros_like(dhead_ref)
        dchan_ref[...] = jnp.zeros_like(dchan_ref)
        dgain_ref[...] = jnp.zeros_like(dgain_ref)

    grstd, cross, valid = row_stats(stats_ref, inner)
    xs[0:8, :] = halo_ref[:, chan:2 * chan + 2 * STATE] * keep
    xs[8:8 + STRETCH, :] = pre_ref[:, chan:2 * chan + 2 * STATE]
    conv = convolve(xs, taps_ref, bias_ref)
    gate_u = sigmoid(conv)
    feats = conv * gate_u
    slope = gate_u * (1.0 + conv * (1.0 - gate_u))
    x = feats[:, :chan]
    bs = feats[:, chan:chan + STATE].astype(BF16)
    cs = feats[:, chan + STATE:].astype(BF16)
    pre_dt = pre_ref[:, 2 * chan + 2 * STATE:]
    rates, cumulative, grown, to_end = decays(pre_dt, head_ref, valid)
    across = cumulative.T
    grown_e = spread_heads(grown, chan)
    rates_e = spread_heads(rates, chan)
    to_end_e = spread_heads(to_end, chan)
    leave_e = grown_e[STRETCH - 1:STRETCH, :]

    pre_z = pre_ref[:, :chan]
    gate_z = sigmoid(pre_z)
    silu_z = pre_z * gate_z * valid
    y = y_ref[...]
    mixed = y + skip_ref[...] * x
    gated = mixed * silu_z
    dgn = dgn_ref[...]
    d_gated = grstd * (gate_ref[...] * dgn) - gated * (grstd * grstd * grstd * cross * (1.0 / inner))
    d_mixed = d_gated * silu_z
    dpre_ref[:, :chan] = (
        d_gated * mixed * (valid * (gate_z * (1.0 + pre_z * (1.0 - gate_z))))
    ).astype(BF16)
    dchan_ref[0:1, :] += jnp.sum(dgn * gated * grstd, axis=0, keepdims=True)
    dchan_ref[1:2, :] += jnp.sum(d_mixed * x, axis=0, keepdims=True)

    turn(0)
    dy_b = d_mixed.astype(BF16)
    dy = dy_b.astype(F32)
    scaled = x * rates_e
    scaled_b = scaled.astype(BF16)
    entering = enter_ref[0]
    d_leaving = dstate[...]
    d_leaving_b = d_leaving.astype(BF16)
    tail = mm(bs, d_leaving_b) * to_end_e
    overlap = jnp.where(lower_mask(), mm(cs, bs, NT), 0.0)
    first = iota((STRETCH, LANES), 1) < HEAD
    d_overlap = jnp.zeros((STRETCH, STRETCH), F32)
    parts = []
    for pair in range(chan // LANES):
        cols = slice(pair * LANES, (pair + 1) * LANES)
        dy_pair = dy_b[:, cols]
        x_pair = scaled_b[:, cols]
        zero = jnp.zeros_like(dy_pair)
        sides = [jnp.where(first, dy_pair, zero), jnp.where(first, zero, dy_pair)]
        mats = []
        for side in range(2):
            weight = weights_of(cumulative, across, 2 * pair + side)
            mats.append((weight * overlap).astype(BF16))
            d_overlap = d_overlap + mm(sides[side], x_pair, NT) * weight
        parts.append(mm(jnp.concatenate(mats, axis=0), jnp.concatenate(sides, axis=0), TN))
    turn(1)
    d_scaled = jnp.concatenate(parts, axis=1) + tail
    scaled_r = scaled_b.astype(F32)
    d_cum = gather_heads(dy * y - scaled_r * d_scaled)
    d_last = jnp.sum(scaled_r * tail, axis=0, keepdims=True) + leave_e * jnp.sum(
        d_leaving * entering, axis=0, keepdims=True
    )
    d_last = gather_heads(jnp.broadcast_to(d_last, (8, chan)))[0:1, :]
    upper = (iota((STRETCH, STRETCH), 0) <= iota((STRETCH, STRETCH), 1)).astype(F32)
    d_log = exact(upper, d_cum) + d_last
    decay = head_ref[1:2, :]
    d_rates = d_log * decay + gather_heads(x * d_scaled)
    d_dt = d_rates * valid * sigmoid(pre_dt + head_ref[0:1, :])
    dhead_ref[0:1, :] += jnp.sum(d_log * rates, axis=0, keepdims=True) * decay
    dhead_ref[1:2, :] += jnp.sum(d_dt, axis=0, keepdims=True)
    dpre_ref[:, 2 * chan + 2 * STATE:] = d_dt.astype(BF16)

    d_x = d_scaled * rates_e + skip_ref[...] * d_mixed
    d_overlap_b = jnp.where(lower_mask(), d_overlap, 0.0).astype(BF16)
    dy_grown = (dy * grown_e).astype(BF16)
    x_end = (scaled * to_end_e).astype(BF16)
    d_b = mm(d_overlap_b, cs, TN) + mm(x_end, d_leaving_b, NT)
    d_c = mm(d_overlap_b, bs) + mm(dy_grown, entering.astype(BF16), NT)
    dstate[...] = (d_leaving * leave_e + mm(cs, dy_grown, TN)) * keep

    dus[0:STRETCH, :chan] = d_x * slope[:, :chan]
    dus[0:STRETCH, chan:chan + STATE] = d_b * slope[:, chan:chan + STATE]
    dus[0:STRETCH, chan + STATE:] = d_c * slope[:, chan + STATE:]
    d_conv = dus[0:STRETCH, :]
    dbias_ref[...] += jnp.sum(d_conv, axis=0, keepdims=True)
    d_pre = jnp.zeros((STRETCH, wide), F32)
    for tap in range(4):
        dtaps_ref[tap:tap + 1, :] += jnp.sum(d_conv * xs[5 + tap:5 + tap + STRETCH, :], axis=0, keepdims=True)
        d_pre = d_pre + taps_ref[tap:tap + 1, :] * dus[3 - tap:3 - tap + STRETCH, :]
    dpre_ref[:, chan:2 * chan + 2 * STATE] = d_pre.astype(BF16)
    dus[STRETCH:STRETCH + 8, :] = d_conv[0:8, :] * keep

    @pl.when(step == 0)
    def _():
        for fetch in fetches:
            fetch.wait()

    turn(2)
    d_normed = mm(dpre_ref[...], w_ref[...], NT)
    dnormed_ref[...] = d_normed.astype(BF16)
    resid = tok_ref[...].astype(F32)
    rstd = lax.rsqrt(jnp.mean(resid * resid, axis=1, keepdims=True) + EPSILON)
    dgain_ref[...] += jnp.sum(d_normed * (resid * rstd), axis=0, keepdims=True)

    @pl.when(step == pl.num_programs(0) - 1)
    def _():
        pl.loop(jnp.minimum(step * PLACES + 1, sums.turns), sums.turns)(sums.advance)
        sums.settle(lambda part: mixed_ref.at[pl.ds(part * chunk, chunk)])
        sums.drain()


def whole(shape):
    return pl.BlockSpec(shape, lambda *_: (0,) * len(shape), pipeline_mode=pl.Buffered(1))


def mixer_backward(
    openings, tok, w_in, taps, bias, heads, skip, gate, pre, y, enter, dgn, stats, out_rows, inner, n_tp
):
    tokens, width = tok.shape
    cols = w_in.shape[1]
    chan = skip.shape[1]
    blocks = tokens // STRETCH
    wide = chan + 2 * STATE
    per = STRETCH // 8
    steps = (n_tp - 1) * (CHUNKS - EARLY)
    kept = tokens // n_tp // CHUNKS * (CHUNKS - EARLY)
    rows = lambda n: pl.BlockSpec((STRETCH, n), lambda i, *_: (blocks - 1 - i, 0))
    return pl.pallas_call(
        functools.partial(backward_kernel, inner=inner, n_tp=n_tp),
        name="mixer_backward",
        grid_spec=pltpu.PrefetchScalarGridSpec(
            num_scalar_prefetch=1,
            grid=(blocks,),
            in_specs=[
                rows(width), pl.BlockSpec(memory_space=pl.ANY), whole((4, wide)), whole((1, wide)),
                whole((8, LANES)), whole((1, chan)), whole((1, chan)),
                rows(cols),
                pl.BlockSpec((8, cols), lambda i, *_: (jnp.maximum((blocks - 1 - i) * per - 1, 0), 0)),
                rows(chan),
                pl.BlockSpec((1, STATE, chan), lambda i, *_: (blocks - 1 - i, 0, 0)),
                rows(chan),
                pl.BlockSpec((8, STRETCH), lambda i, *_: (0, blocks - 1 - i)),
                pl.BlockSpec(memory_space=pl.ANY),
            ],
            out_specs=[
                rows(cols), rows(width),
                pl.BlockSpec((8, wide), lambda i, *_: (0, 0)),
                pl.BlockSpec((1, wide), lambda i, *_: (0, 0)),
                pl.BlockSpec((8, LANES), lambda i, *_: (0, 0)),
                pl.BlockSpec((8, chan), lambda i, *_: (0, 0)),
                pl.BlockSpec((1, width), lambda i, *_: (0, 0)),
                pl.BlockSpec((kept, width), lambda i, *_: (0, 0)),
            ],
            scratch_shapes=[
                pltpu.VMEM((STATE, chan), F32),
                pltpu.VMEM((STRETCH + 8, wide), F32),
                pltpu.VMEM((STRETCH + 8, wide), F32),
                pltpu.VMEM((tokens, width), BF16),
                pltpu.VMEM((width, cols), BF16),
                pltpu.VMEM((2, steps, tokens // n_tp // CHUNKS, width), BF16),
                pltpu.SemaphoreType.DMA((2,)),
                pltpu.SemaphoreType.DMA((2, steps)),
                pltpu.SemaphoreType.DMA((2, steps)),
            ],
        ),
        out_shape=[
            jax.ShapeDtypeStruct((tokens, cols), BF16),
            jax.ShapeDtypeStruct((tokens, width), BF16),
            jax.ShapeDtypeStruct((8, wide), F32),
            jax.ShapeDtypeStruct((1, wide), F32),
            jax.ShapeDtypeStruct((8, LANES), F32),
            jax.ShapeDtypeStruct((8, chan), F32),
            jax.ShapeDtypeStruct((1, width), F32),
            jax.ShapeDtypeStruct((kept, width), F32),
        ],
        cost_estimate=pl.CostEstimate(
            flops=4 * tokens * width * cols, bytes_accessed=tokens * cols * 12, transcendentals=tokens * chan
        ),
        compiler_params=pltpu.CompilerParams(
            collective_id=TAGS["backward"], has_side_effects=True, vmem_limit_bytes=60 << 20,
            dimension_semantics=("arbitrary",),
        ),
    )(openings, tok, w_in, taps, bias, heads, skip, gate, pre, pre, y, enter, dgn, stats, out_rows)


MESH = pl.DeviceIdType.MESH
CHUNKS = 4
EARLY = 1
TAGS = {"ahead": 1, "backward": 2, "exit": 3}


def remote(source, target, send, recv, **where):
    return pltpu.make_async_remote_copy(
        src_ref=source, dst_ref=target, send_sem=send, recv_sem=recv, device_id=where, device_id_type=MESH
    )


def rows_at(ref, index, count):
    return ref.at[pl.ds(pl.multiple_of(index * count, count), count)]


def greet(axis, peers):
    barrier = pltpu.get_barrier_semaphore()
    for peer in peers:
        pl.semaphore_signal(barrier, inc=1, device_id={axis: peer}, device_id_type=MESH)


class Line:
    def __init__(self, tp, n_tp, own, whole_ref, send, recv):
        self.tp, self.n, self.own, self.whole_ref, self.send, self.recv = tp, n_tp, own, whole_ref, send, recv
        self.count = own.shape[0]

    def copy(self, way, step, own=False):
        shift = -1 if way == 0 else 1
        index = self.tp + shift * step
        slot = rows_at(self.whole_ref, index, self.count)
        return remote(
            self.own if own else slot, slot, self.send.at[way, step], self.recv.at[way, step], tp=self.tp - shift
        )

    def sends(self, way, step):
        if way == 0:
            return jnp.logical_and(self.tp < self.n - 1, self.tp >= step)
        return jnp.logical_and(self.tp > 0, self.tp + step <= self.n - 1)

    def takes(self, way, step):
        return self.tp >= step + 1 if way == 0 else self.tp + step + 1 <= self.n - 1

    def start(self, way, step):
        @pl.when(self.sends(way, step))
        def _():
            self.copy(way, step, own=step == 0).start()

    def arrive(self, way, step):
        @pl.when(self.takes(way, step))
        def _():
            shift = -1 if way == 0 else 1
            slot = rows_at(self.whole_ref, self.tp + shift * (step + 1), self.count)
            remote(
                slot, slot, self.send.at[way, step], self.recv.at[way, step], tp=self.tp + shift
            ).wait_recv()

    def finish(self, way, step):
        @pl.when(self.sends(way, step))
        def _():
            self.copy(way, step, own=step == 0).wait_send()


class LineSum:
    def __init__(self, tp, n_tp, per, local, origin, got, send, recv):
        self.tp, self.n, self.per, self.local_of, self.origin = tp, n_tp, per, local, origin
        self.got, self.send, self.recv = got, send, recv
        self.steps = (n_tp - 1) * per
        self.paced = max(n_tp - 2, 0) * per
        self.turns = self.paced + max(n_tp - 3, 0)

    def ahead(self, way, step):
        return self.n - 1 - step // self.per if way == 0 else step // self.per

    def passes(self, way, step):
        return self.ahead(way, step) > self.tp if way == 0 else self.ahead(way, step) < self.tp

    def first(self, way):
        return self.tp == 0 if way == 0 else self.tp == self.n - 1

    def local(self, way, step):
        return self.local_of(self.ahead(way, step), step % self.per)

    def copy(self, way, step, direct):
        source = (self.origin if direct else self.local_of)(self.ahead(way, step), step % self.per)
        return remote(
            source, self.got.at[way, step], self.send.at[way, step], self.recv.at[way, step],
            tp=self.tp + 1 if way == 0 else self.tp - 1,
        )

    def kick(self):
        for way in range(2):
            @pl.when(self.first(way))
            def _():
                for step in range(min(2, self.steps) if self.paced else self.steps):
                    self.copy(way, step, True).start()

    def advance(self, turn):
        for way in range(2):
            lag = jnp.maximum(self.tp - 1 if way == 0 else self.n - 2 - self.tp, 0)
            step = turn - lag
            live = jnp.logical_and(step >= 0, step < self.paced)

            @pl.when(jnp.logical_and(self.first(way), live))
            def _():
                self.copy(way, step, True).wait_send()

                @pl.when(step + 2 < self.steps)
                def _():
                    self.copy(way, step + 2, True).start()

                @pl.when(step == self.paced - 1)
                def _():
                    for rest in range(self.paced + 2, self.steps):
                        self.copy(way, rest, True).start()

            @pl.when(jnp.logical_and(jnp.logical_and(self.passes(way, step), live), jnp.logical_not(self.first(way))))
            def _():
                copy = self.copy(way, step, False)
                copy.wait_recv()
                add_into(self.local(way, step), self.local(way, step), self.got.at[way, step])
                copy.start()

    def settle(self, target):
        for way in range(2):
            for step in range(self.steps):
                @pl.when(jnp.logical_and(self.ahead(way, step) == self.tp, jnp.logical_not(self.first(way))))
                def _():
                    self.copy(way, step, False).wait_recv()

        for value in range(self.n):
            @pl.when(self.tp == value)
            def _():
                for part in range(self.per):
                    incoming = []
                    if value > 0:
                        incoming.append(self.got.at[0, (self.n - 1 - value) * self.per + part])
                    if value < self.n - 1:
                        incoming.append(self.got.at[1, value * self.per + part])
                    add_into(target(part), self.local_of(value, part), *incoming)

    def drain(self):
        for way in range(2):
            @pl.when(self.first(way))
            def _():
                for step in range(self.paced, self.steps):
                    self.copy(way, step, True).wait_send()

            for step in range(self.steps):
                @pl.when(jnp.logical_and(self.passes(way, step), jnp.logical_not(self.first(way))))
                def _():
                    self.copy(way, step, False).wait_send()


def chunk_of(ref, block, rows, part, chunk):
    return ref.at[pl.ds(pl.multiple_of(block * rows + part * chunk, chunk), chunk)]


def line_greeting(tp, n_tp):
    barrier = pltpu.get_barrier_semaphore()
    for near, there in ((tp - 1, tp > 0), (tp + 1, tp < n_tp - 1)):
        @pl.when(there)
        def _():
            pl.semaphore_signal(barrier, inc=1, device_id={"tp": near}, device_id_type=MESH)
    pl.semaphore_wait(barrier, jnp.where(tp > 0, 1, 0) + jnp.where(tp < n_tp - 1, 1, 0))


def forward_block(keep, tok, valid, gain_ref, w_ref, taps_ref, bias_ref, head_ref, skip_ref,
                  normed_ref, pre_ref, y_ref, gated_ref, enter_ref, state, xs):
    chan = y_ref.shape[1]
    xs[0:8, :] = xs[STRETCH:STRETCH + 8, :] * keep
    resid = tok.astype(F32)
    rstd = lax.rsqrt(jnp.mean(resid * resid, axis=1, keepdims=True) + EPSILON)
    normed = (resid * rstd * gain_ref[...]).astype(BF16)
    normed_ref[...] = normed
    pre_ref[...] = mm(normed, w_ref[...])
    xs[8:8 + STRETCH, :] = pre_ref[:, chan:2 * chan + 2 * STATE]
    conv = convolve(xs, taps_ref, bias_ref)
    feats = conv * sigmoid(conv)
    x = feats[:, :chan]
    bs = feats[:, chan:chan + STATE].astype(BF16)
    cs = feats[:, chan + STATE:].astype(BF16)
    rates, cumulative, grown, to_end = decays(pre_ref[:, 2 * chan + 2 * STATE:], head_ref, valid)
    across = cumulative.T
    grown_e = spread_heads(grown, chan)
    scaled = x * spread_heads(rates, chan)
    entering = state[...] * keep
    enter_ref[...] = entering
    y_ref[...] = mm(cs, entering.astype(BF16)) * grown_e
    state[...] = entering * grown_e[STRETCH - 1:STRETCH, :] + mm(
        bs, (scaled * spread_heads(to_end, chan)).astype(BF16), TN
    )
    overlap = jnp.where(lower_mask(), mm(cs, bs, NT), 0.0)
    scaled_b = scaled.astype(BF16)
    first = iota((STRETCH, LANES), 1) < HEAD
    for pair in range(chan // LANES):
        cols = slice(pair * LANES, (pair + 1) * LANES)
        both = scaled_b[:, cols]
        mats = [
            (weights_of(cumulative, across, 2 * pair + side) * overlap).astype(BF16) for side in range(2)
        ]
        zero = jnp.zeros_like(both)
        y_ref[:, cols] += mm(
            jnp.concatenate(mats, axis=1),
            jnp.concatenate([jnp.where(first, both, zero), jnp.where(first, zero, both)], axis=0),
        )
    pre_z = pre_ref[:, :chan]
    gated = (y_ref[...] + skip_ref[...] * x) * (pre_z * sigmoid(pre_z)) * valid
    gated_ref[...] = gated
    return jnp.sum(gated * gated, axis=1, keepdims=True)


def as_row(column):
    lane = iota((STRETCH, LANES), 1)
    return jnp.where(lane == 0, column, 0.0).T[0:8, :]


def as_column(row):
    return jnp.concatenate([row, jnp.zeros((LANES - 8, STRETCH), F32)], axis=0).T


def row_stats(stats_ref, inner):
    filled = as_column(stats_ref[...])
    return lax.rsqrt(filled[:, 0:1] * (1.0 / inner) + EPSILON), filled[:, 1:2], filled[:, 2:3]


def ahead_kernel(
    open_ref, step_bias, log_rate, direct, tok_ref, cot_ref, pz_ref, px_ref, pbc_ref, pdt_ref, pout_ref, mask_ref,
    norm_gain, conv_chan, bias_chan, conv_shared, bias_shared, gate_gain,
    tok_out, cot_out, win_out, normed_out, pre_out, y_out, enter_out, dgn_out, gn_out, rows_out, mixed_out, stats_ref,
    taps_ref, bias_ref, head_ref, skip_ref, gate_ref,
    pin_ref, gain_ref, tok_all, cot_all, w_in, w_out, normed, pre, y, gated, enter, dgn, gnormed, rows, state, xs, squares, crosses,
    squares_got, crosses_got, o_got,
    own_sem, z_send, z_recv, c_send, c_recv, f_send, f_recv, p_send, p_recv, q_send, q_recv, r_send, r_recv,
    all_sem, out_sem, o_send, o_recv,
    *, n_tp, n_fs, inner,
):
    tp, me = lax.axis_index("tp"), lax.axis_index("fsdp")
    chip, core, chips = me // 2, me % 2, n_fs // 2
    partner = chip * 2 + 1 - core
    blocks = tok_all.shape[0] // STRETCH
    per = tok_ref.shape[0]
    chan = pout_ref.shape[1]
    pin_ref[:, :chan] = pz_ref[...]
    pin_ref[:, chan:2 * chan] = px_ref[...]
    pin_ref[:, 2 * chan:2 * chan + 2 * STATE] = pbc_ref[...]
    heads_here, rows_dt = pdt_ref.shape
    pin_ref[:, 2 * chan + 2 * STATE:] = jnp.concatenate(
        [pdt_ref[...].astype(F32), jnp.zeros((LANES - heads_here, rows_dt), F32)], axis=0
    ).T.astype(BF16)
    greet("fsdp", [((chip + d) % chips) * 2 + core for d in range(1, chips)] + [partner])
    greet("tp", [(tp + d) % n_tp for d in range(1, n_tp)])
    pl.semaphore_wait(pltpu.get_barrier_semaphore(), chips + n_tp - 1)

    packs = ((pin_ref, w_in), (pout_ref, w_out))
    count = pin_ref.shape[0]
    line = Line(tp, n_tp, tok_ref, tok_all, z_send, z_recv)
    late = Line(tp, n_tp, cot_ref, cot_all, c_send, c_recv)
    for way in range(2):
        line.start(way, 0)
    for j, (pack, full) in enumerate(packs):
        for d in range(1, chips):
            remote(
                pack, rows_at(full, me, count), f_send.at[j, d], f_recv.at[j, d], fsdp=((chip + d) % chips) * 2 + core
            ).start()
        remote(pack, rows_at(full, me, count), p_send.at[j, 0], p_recv.at[j, 0], fsdp=partner).start()
    own = [
        pltpu.make_async_copy(tok_ref, rows_at(tok_all, tp, per), own_sem.at[0]),
        pltpu.make_async_copy(pin_ref, rows_at(w_in, me, count), own_sem.at[1]),
        pltpu.make_async_copy(pout_ref, rows_at(w_out, me, count), own_sem.at[2]),
        pltpu.make_async_copy(cot_ref, rows_at(cot_all, tp, per), own_sem.at[3]),
    ]
    for copy in own:
        copy.start()
    state[...] = jnp.zeros_like(state)
    xs[...] = jnp.zeros_like(xs)
    lane = iota((8, LANES), 1)
    place = iota((8, LANES), 0)
    step_row, rate_row, skip_row = (
        sum(jnp.where(lane == head, source[head], 0.0) for head in range(heads_here))
        for source in (step_bias, log_rate, direct)
    )
    live = lane < heads_here
    head_ref[...] = jnp.where(
        place == 0, jnp.where(live, step_row, -100.0), jnp.where(live & (place == 1), -jnp.exp(rate_row), 0.0)
    )
    skip_ref[...] = spread_heads(skip_row, chan)[0:1, :]
    gain_ref[...] = norm_gain[...].reshape(gain_ref.shape)
    gate_ref[...] = gate_gain[...].reshape(gate_ref.shape)
    taps_ref[:, :chan] = conv_chan[...]
    taps_ref[:, chan:] = conv_shared[...]
    bias_ref[:, :chan] = bias_chan[...].reshape(1, chan)
    bias_ref[:, chan:] = bias_shared[...].reshape(1, 2 * STATE)
    for step in range(n_tp - 1):
        for way in range(2):
            line.arrive(way, step)
            if step + 1 < n_tp - 1:
                line.start(way, step + 1)
        if step == n_tp - 3 or n_tp < 3 and step == 0:
            for j, (pack, full) in enumerate(packs):
                for d in range(1, chips):
                    slot = rows_at(full, ((chip + chips - d) % chips) * 2 + core, count)
                    remote(slot, slot, f_send.at[j, d], f_recv.at[j, d], fsdp=partner).wait_recv()
                    remote(slot, slot, p_send.at[j, d], p_recv.at[j, d], fsdp=partner).start()
    for step in range(n_tp - 1):
        for way in range(2):
            line.finish(way, step)
    for way in range(2):
        late.start(way, 0)
    for j, (pack, full) in enumerate(packs):
        for d in range(chips):
            slot = rows_at(full, ((chip + chips - d) % chips) * 2 + 1 - core, count)
            remote(slot, slot, p_send.at[j, d], p_recv.at[j, d], fsdp=partner).wait()
        for d in range(1, chips):
            remote(pack, rows_at(full, me, count), f_send.at[j, d], f_recv.at[j, d], fsdp=partner).wait_send()
    for copy in own:
        copy.wait()
    wholes = [
        pltpu.make_async_copy(tok_all, tok_out, all_sem.at[0]), pltpu.make_async_copy(w_in, win_out, all_sem.at[1]),
    ]
    for copy in wholes:
        copy.start()

    def span(block):
        return pl.ds(pl.multiple_of(block * STRETCH, STRETCH), STRETCH)

    def out(k, block):
        at = span(block)
        chunk = per // CHUNKS * EARLY
        kept = pl.ds(pl.multiple_of(block * STRETCH + chunk, chunk), STRETCH - chunk)
        pairs = (
            (normed.at[at], normed_out.at[at]), (pre.at[block % 2], pre_out.at[at]), (y.at[at], y_out.at[at]),
            (enter.at[block], enter_out.at[block]), (gnormed.at[at], gn_out.at[at]),
            (rows.at[kept], rows_out.at[kept]), (dgn.at[at], dgn_out.at[at]), (cot_all.at[at], cot_out.at[at]),
        )
        return pltpu.make_async_copy(*pairs[k], out_sem.at[k, block])

    @pl.loop(0, blocks)
    def _(block):
        at = span(block)
        keep = jnp.where(open_ref[block] == 1, 0.0, 1.0).astype(F32)

        @pl.when(block >= 2)
        def _():
            out(1, block - 2).wait()

        valid = mask_ref[at].reshape(1, STRETCH).astype(F32)
        squares[:, at] = jnp.where(iota((8, STRETCH), 0) == 2, valid, 0.0)
        total = forward_block(
            keep, tok_all[at, :], as_column(squares[:, at])[:, 2:3], gain_ref, w_in, taps_ref, bias_ref, head_ref, skip_ref,
            normed.at[at], pre.at[block % 2], y.at[at], gated.at[at], enter.at[block], state, xs,
        )
        squares[0:1, at] = as_row(total)[0:1, :]
        for k in range(4):
            out(k, block).start()

        @pl.when(block == max(blocks - 2, 0))
        def _():
            for way in range(2):
                late.arrive(way, 0)
                if n_tp > 2:
                    late.start(way, 1)

    def swap(part, got, send, recv):
        for d in range(1, n_tp):
            remote(part, got.at[tp], send.at[d], recv.at[d], tp=(tp + d) % n_tp).start()
        got[tp] = part[...]
        for d in range(1, n_tp):
            slot = got.at[(tp + n_tp - d) % n_tp]
            remote(slot, slot, send.at[d], recv.at[d], tp=(tp + d) % n_tp).wait_recv()
        total = got[0]
        for peer in range(1, n_tp):
            total = total + got[peer]
        return total

    stats_ref[...] = swap(squares, squares_got, q_send, q_recv)

    @pl.loop(0, blocks)
    def _(block):
        at = span(block)

        grstd, _, _ = row_stats(stats_ref.at[:, at], inner)
        value = (gated[at, :] * grstd * gate_ref[...]).astype(BF16)
        gnormed[at, :] = value
        rows[at, :] = mm(value, w_out[...], NT).astype(BF16)
        out(4, block).start()
        out(5, block).start()

    chunk = per // CHUNKS
    piece = lambda index, part: chunk_of(rows, index, per, part, chunk)
    sums = LineSum(tp, n_tp, EARLY, piece, piece, o_got, o_send, o_recv)
    sums.kick()

    def gradient(block):
        at = span(block)
        value = mm(cot_all[at, :], w_out[...])
        dgn[at, :] = value
        crosses[:, at] = as_row(jnp.sum(gate_ref[...] * value * gated[at, :], axis=1, keepdims=True))
        out(6, block).start()
        out(7, block).start()

    ratio = per // STRETCH

    def gradients(index):
        for k in range(ratio):
            gradient(index * ratio + k)

    gradients(tp)
    middle = min(sums.turns, 3)
    for step in range(n_tp - 1):
        for way in range(2):
            if step > 0:
                late.arrive(way, step)
                if step + 1 < n_tp - 1:
                    late.start(way, step + 1)
        for way in range(2):
            @pl.when(late.takes(way, step))
            def _():
                gradients(tp - step - 1 if way == 0 else tp + step + 1)
        if step == max(n_tp - 3, 0):
            pl.loop(0, middle)(sums.advance)

    total = swap(crosses, crosses_got, r_send, r_recv)
    if middle < sums.turns:
        pl.loop(middle, sums.turns)(sums.advance)
    sums.settle(lambda part: mixed_out.at[pl.ds(part * chunk, chunk)])

    stats_ref[1:2, :] = total[0:1, :]
    stats_ref[2:3, :] = squares[2:3, :]

    for copy in wholes:
        copy.wait()

    @pl.loop(0, blocks)
    def _(block):
        for k in (0, 2, 3, 4, 5, 6, 7):
            out(k, block).wait()

    for block in range(max(blocks - 2, 0), blocks):
        out(1, block).wait()
    for step in range(n_tp - 1):
        for way in range(2):
            late.finish(way, step)
    sums.drain()
    for d in range(1, n_tp):
        remote(squares, squares_got.at[tp], q_send.at[d], q_recv.at[d], tp=(tp + d) % n_tp).wait_send()
        remote(crosses, crosses_got.at[tp], r_send.at[d], r_recv.at[d], tp=(tp + d) % n_tp).wait_send()


def ahead(
    openings, heads, tokens, cotangent, projections, mask, vectors, n_tp, n_fs
):
    per, width = tokens.shape
    total = per * n_tp
    count, chan = projections[0].shape
    wide = chan + 2 * STATE
    cols = chan + wide + LANES
    blocks = total // STRETCH
    chips = n_fs // 2
    dma = pltpu.SemaphoreType.DMA
    anywhere = pl.BlockSpec(memory_space=pl.ANY)
    vmem = pl.BlockSpec(memory_space=pltpu.VMEM)
    shape = jax.ShapeDtypeStruct
    return pl.pallas_call(
        functools.partial(ahead_kernel, n_tp=n_tp, n_fs=n_fs, inner=chan * n_tp),
        name="ahead",
        in_specs=[pl.BlockSpec(memory_space=pltpu.SMEM)] * 4 + [vmem] * 14,
        out_specs=[anywhere] * 10 + [vmem] * 7,
        out_shape=[
            shape((total, width), BF16), shape((total, width), BF16), shape((count * n_fs, cols), BF16),
            shape((total, width), BF16), shape((total, cols), F32), shape((total, chan), F32),
            shape((blocks, STATE, chan), F32), shape((total, chan), F32), shape((total, chan), BF16),
            shape((total, width), BF16), shape((per // CHUNKS * EARLY, width), F32), shape((8, total), F32),
            shape((4, wide), F32), shape((1, wide), F32),
            shape((8, LANES), F32), shape((1, chan), F32), shape((1, chan), F32),
        ],
        scratch_shapes=[
            pltpu.VMEM((count, cols), BF16), pltpu.VMEM((1, width), F32),
            pltpu.VMEM((total, width), BF16), pltpu.VMEM((total, width), BF16),
            pltpu.VMEM((count * n_fs, cols), BF16), pltpu.VMEM((count * n_fs, chan), BF16),
            pltpu.VMEM((total, width), BF16), pltpu.VMEM((2, STRETCH, cols), F32), pltpu.VMEM((total, chan), F32),
            pltpu.VMEM((total, chan), F32), pltpu.VMEM((blocks, STATE, chan), F32), pltpu.VMEM((total, chan), F32),
            pltpu.VMEM((total, chan), BF16), pltpu.VMEM((total, width), BF16),
            pltpu.VMEM((STATE, chan), F32), pltpu.VMEM((STRETCH + 8, wide), F32),
            pltpu.VMEM((8, total), F32), pltpu.VMEM((8, total), F32),
            pltpu.VMEM((n_tp, 8, total), F32), pltpu.VMEM((n_tp, 8, total), F32),
            pltpu.VMEM((2, (n_tp - 1) * EARLY, per // CHUNKS, width), BF16),
            dma((4,)), dma((2, n_tp - 1)), dma((2, n_tp - 1)), dma((2, n_tp - 1)), dma((2, n_tp - 1)),
            dma((2, chips)), dma((2, chips)), dma((2, chips)), dma((2, chips)),
            dma((n_tp,)), dma((n_tp,)), dma((n_tp,)), dma((n_tp,)), dma((2,)), dma((8, blocks)),
            dma((2, (n_tp - 1) * EARLY)), dma((2, (n_tp - 1) * EARLY)),
        ],
        compiler_params=pltpu.CompilerParams(
            collective_id=TAGS["ahead"], has_side_effects=True, vmem_limit_bytes=63 << 20
        ),
    )(openings, *heads, tokens, cotangent, *projections, mask, *vectors)


def add_into(target, *sources):
    rows, tile = target.shape[0], 32

    @pl.loop(0, rows // tile)
    def _(i):
        at = pl.ds(pl.multiple_of(i * tile, tile), tile)
        total = sources[0][at, :].astype(F32)
        for source in sources[1:]:
            total = total + source[at, :].astype(F32)
        target[at, :] = total.astype(target.dtype)


def fill_rows(target, pieces):
    at = 0
    for source, row, start, length in pieces:
        for k in range(length // LANES):
            target[at:at + 1, :] = source[row:row + 1, start + k * LANES:start + (k + 1) * LANES]
            at += 1
    if at < target.shape[0]:
        target[at:, :] = jnp.zeros((target.shape[0] - at, LANES), F32)


def finish_kernel(
    tok_ref, cot_ref, early_ref, mixed_ref, gain_ref, dn_ref, own_ref, bc_ref, mine_ref, shared_ref,
    output, grad_tokens, g_gain, g_z, g_x, g_bc, g_dt, g_taps, g_bias, g_taps_s, g_bias_s, g_log, g_step, g_skip, g_gate,
    g_out,
):
    chan, heads_here = g_z.shape[1], g_log.shape[0]
    resid = tok_ref[...].astype(F32)
    early = early_ref.shape[0]
    output[0:early, :] = (resid[0:early, :] + early_ref[...]).astype(BF16)
    output[early:, :] = (resid[early:, :] + mixed_ref[...]).astype(BF16)
    rstd = lax.rsqrt(jnp.mean(resid * resid, axis=1, keepdims=True) + EPSILON)
    scaled = dn_ref[...].astype(F32) * gain_ref[...].reshape(1, resid.shape[1])
    grad_tokens[...] = (
        cot_ref[...].astype(F32) + rstd * scaled
        - resid * (rstd * rstd * rstd) * jnp.mean(scaled * resid, axis=1, keepdims=True)
    ).astype(BF16)
    g_z[...] = own_ref[:, :chan].astype(F32)
    g_x[...] = own_ref[:, chan:2 * chan].astype(F32)
    g_dt[...] = own_ref[:, 2 * chan:2 * chan + LANES].astype(F32).T[0:heads_here, :]
    g_out[...] = own_ref[:, 2 * chan + LANES:].astype(F32)
    g_bc[...] = bc_ref[...].astype(F32)

    def row(source, at, length):
        return jnp.concatenate([source[at + k:at + k + 1, :] for k in range(length // LANES)], axis=1)

    per = chan // LANES
    for tap in range(4):
        g_taps[tap:tap + 1, :] = row(mine_ref, tap * per, chan)
        g_taps_s[tap:tap + 1, :] = row(shared_ref, tap * 2, 2 * STATE)
    g_bias[...] = row(mine_ref, 4 * per, chan).reshape(chan)
    g_gate[...] = row(mine_ref, 5 * per, chan).reshape(chan)
    skip = gather_heads(jnp.broadcast_to(row(mine_ref, 6 * per, chan), (8, chan)))
    g_skip[...] = skip[0:1, :heads_here].reshape(heads_here)
    g_log[...] = mine_ref[7 * per:7 * per + 1, :heads_here].reshape(heads_here)
    g_step[...] = mine_ref[7 * per + 1:7 * per + 2, :heads_here].reshape(heads_here)
    g_bias_s[...] = row(shared_ref, 8, 2 * STATE).reshape(2 * STATE)
    g_gain[...] = row(shared_ref, 10, g_gain.shape[0]).reshape(g_gain.shape[0])


def finish(tokens, cotangent, early, mixed, gain, dn, own, bc, mine, shared, heads_here):
    rows, width = tokens.shape
    count = own.shape[0]
    chan = (own.shape[1] - LANES) // 3
    vmem = pl.BlockSpec(memory_space=pltpu.VMEM)
    shape = lambda *extents: jax.ShapeDtypeStruct(extents, F32)
    outs = [
        jax.ShapeDtypeStruct((rows, width), BF16), jax.ShapeDtypeStruct((rows, width), BF16), shape(width),
        shape(count, chan), shape(count, chan), shape(count, 2 * STATE), shape(heads_here, count), shape(4, chan),
        shape(chan), shape(4, 2 * STATE), shape(2 * STATE), shape(heads_here), shape(heads_here), shape(heads_here),
        shape(chan), shape(count, chan),
    ]
    return pl.pallas_call(
        finish_kernel, name="finish", in_specs=[vmem] * 10, out_specs=[vmem] * len(outs), out_shape=outs,
        compiler_params=pltpu.CompilerParams(vmem_limit_bytes=40 << 20),
    )(tokens, cotangent, early, mixed, gain, dn, own, bc, mine, shared)


def exit_kernel(
    dn_ref, normed_ref, dpre_ref, cot_ref, gn_ref, dtaps_ref, dbias_ref, dhead_ref, dchan_ref, dgain_ref,
    dn_out, own_out, bc_out, mine_out, shared_out,
    dn, normed, dpre, cot, gn, fetch_sem,
    gin_ref, gout_ref, mine_ref, shared_ref,
    z_got, near_in, near_out, far_in, far_out, got_in, got_out, mine_got, shared_got, shared_held, shared_z,
    bc_held, bc_got,
    zs, zr, ns, nr, fs, fr, ms, mr, ss, sr, ts, tr, bs, br,
    *, n_tp, n_fs,
):
    tp, me = lax.axis_index("tp"), lax.axis_index("fsdp")
    chip, core, chips = me // 2, me % 2, n_fs // 2
    partner = chip * 2 + 1 - core
    chan = gout_ref.shape[1]
    cols = gin_ref.shape[1]
    width = gin_ref.shape[0]
    fetches = [
        pltpu.make_async_copy(source, target, fetch_sem.at[k])
        for k, (source, target) in enumerate(
            [(normed_ref, normed), (dpre_ref, dpre), (cot_ref, cot), (gn_ref, gn), (dn_ref, dn)]
        )
    ]
    for fetch in fetches:
        fetch.start()
    fill_rows(
        mine_ref, [(dtaps_ref, tap, 0, chan) for tap in range(4)] + [(dbias_ref, 0, 0, chan)]
        + [(dchan_ref, row, 0, chan) for row in range(2)] + [(dhead_ref, row, 0, LANES) for row in range(2)]
    )
    fill_rows(
        shared_ref, [(dtaps_ref, tap, chan, 2 * STATE) for tap in range(4)] + [(dbias_ref, 0, chan, 2 * STATE)]
        + [(dgain_ref, 0, 0, width)]
    )
    block, count = dn_out.shape[0], own_out.shape[0]
    greet("fsdp", [(me + d) % n_fs for d in range(1, n_fs)])
    greet("tp", [(tp + d) % n_tp for d in range(1, n_tp)])
    pl.semaphore_wait(pltpu.get_barrier_semaphore(), n_fs - 1 + n_tp - 1)

    chunk = block // CHUNKS
    sums = LineSum(
        tp, n_tp, CHUNKS, lambda index, part: chunk_of(dn, index, block, part, chunk),
        lambda index, part: chunk_of(dn_ref, index, block, part, chunk), z_got, zs, zr,
    )
    sums.kick()
    for k in (0, 1):
        fetches[k].wait()
    advance = sums.advance
    parts = (
        (gin_ref, slice(2 * chan, cols), near_in, far_in, got_in),
        (gout_ref, slice(0, chan), near_out, far_out, got_out),
        (gin_ref, slice(chan, 2 * chan), near_in, far_in, got_in),
        (gin_ref, slice(0, chan), near_in, far_in, got_in),
    )

    def near(j, d):
        source, span, held, _, _ = parts[j]
        rows = rows_at(source, ((chip + d) % chips) * 2 + 1 - core, count)
        return remote(rows.at[:, span], held.at[d, :, span], ns.at[j, d], nr.at[j, d], fsdp=partner)

    def far(j, d):
        _, span, _, held, got = parts[j]
        return remote(
            held.at[d, :, span], got.at[d, :, span], fs.at[j, d], fr.at[j, d], fsdp=((chip + d) % chips) * 2 + core
        )

    order = [d for d in range(1, chips)]

    def small(d):
        peer = (me + d) % n_fs
        return (
            remote(mine_ref, mine_got.at[me], ms.at[d], mr.at[d], fsdp=peer),
            remote(shared_ref, shared_got.at[me], ss.at[d], sr.at[d], fsdp=peer),
        )

    for d in range(1, n_fs):
        for copy in small(d):
            copy.start()
    mine_got[me] = mine_ref[...]
    shared_got[me] = shared_ref[...]

    def differentiate(j):
        _, span, *_ = parts[j]
        left, right, target = (cot, gn, gout_ref) if j == 1 else (normed, dpre, gin_ref)
        tile = 256

        @pl.loop(0, width // tile)
        def _(piece):
            at = pl.ds(pl.multiple_of(piece * tile, tile), tile)
            target[at, span] = mm(left[:, at], right[:, span], TN).astype(BF16)

        for d in order + [0]:
            near(j, d).start()

    def send_sums(j):
        source, span, held, summed, _ = parts[j]
        for d in order:
            near(j, d).wait_recv()
            rows = rows_at(source, ((chip + d) % chips) * 2 + core, count)
            add_into(summed.at[d, :, span], rows.at[:, span], held.at[d, :, span])
            far(j, d).start()
        near(j, 0).wait_recv()

    differentiate(0)
    for k in (2, 3, 4):
        fetches[k].wait()
    advance(0)
    differentiate(1)
    send_sums(0)
    advance(1)
    differentiate(2)
    send_sums(1)
    advance(2)
    differentiate(3)
    send_sums(2)
    advance(3)
    send_sums(3)
    at = 3
    turns = sums.turns
    for d in range(1, n_fs):
        for copy in small(d):
            copy.wait_recv()
    total, again = mine_got[0], shared_got[0]
    for peer in range(1, n_fs):
        total, again = total + mine_got[peer], again + shared_got[peer]
    mine_out[...] = total
    shared_held[...] = again
    shared_z[tp] = again
    for d in range(1, n_tp):
        remote(shared_held, shared_z.at[tp], ts.at[d], tr.at[d], tp=(tp + d) % n_tp).start()
    pl.loop(at + 1, turns)(advance)

    def settle(j, target, span):
        source, _, held, _, got = parts[j]
        rows = rows_at(source, me, count)
        add_into(
            target, rows.at[:, span], held.at[0, :, span], *[got.at[d, :, span] for d in order]
        )

    for d in order:
        far(0, d).wait_recv()
    settle(0, bc_held, slice(2 * chan, 2 * chan + 2 * STATE))
    bc_got[tp] = bc_held[...]
    for d in range(1, n_tp):
        remote(bc_held, bc_got.at[tp], bs.at[d], br.at[d], tp=(tp + d) % n_tp).start()
    settle(0, own_out.at[:, 2 * chan:2 * chan + LANES], slice(2 * chan + 2 * STATE, cols))
    for j in (1, 2, 3):
        for d in order:
            far(j, d).wait_recv()
    settle(1, own_out.at[:, 2 * chan + LANES:], slice(0, chan))
    settle(2, own_out.at[:, chan:2 * chan], slice(chan, 2 * chan))
    settle(3, own_out.at[:, :chan], slice(0, chan))
    for d in range(1, n_tp):
        peer = (tp + n_tp - d) % n_tp
        remote(shared_held, shared_z.at[peer], ts.at[d], tr.at[d], tp=peer).wait_recv()
        remote(bc_held, bc_got.at[peer], bs.at[d], br.at[d], tp=peer).wait_recv()
    total = shared_z[0]
    for peer in range(1, n_tp):
        total = total + shared_z[peer]
    shared_out[...] = total
    add_into(bc_out, *[bc_got.at[peer] for peer in range(n_tp)])

    sums.settle(lambda part: dn_out.at[pl.ds(part * chunk, chunk)])
    sums.drain()
    for j in range(4):
        for d in range(chips):
            near(j, d).wait_send()
        for d in order:
            far(j, d).wait_send()
    for d in range(1, n_fs):
        for copy in small(d):
            copy.wait_send()
    for d in range(1, n_tp):
        remote(shared_held, shared_z.at[tp], ts.at[d], tr.at[d], tp=(tp + d) % n_tp).wait_send()
        remote(bc_held, bc_got.at[tp], bs.at[d], br.at[d], tp=(tp + d) % n_tp).wait_send()


def leave(dn, normed, dpre, cot, gnormed, small, n_tp, n_fs):
    block, width = dn.shape[0] // n_tp, dn.shape[1]
    count, cols = width // n_fs, dpre.shape[1]
    chan = gnormed.shape[1]
    chips, steps = n_fs // 2, (n_tp - 1) * CHUNKS
    dma = pltpu.SemaphoreType.DMA
    vmem = pl.BlockSpec(memory_space=pltpu.VMEM)
    room = lambda *shape: pltpu.VMEM(shape, BF16)
    shape = lambda *extents: jax.ShapeDtypeStruct(extents, F32)
    up = lambda n: -(-n // 8) * 8
    mine = (up(7 * chan // LANES + 2), LANES)
    shared = (up((10 * STATE + width) // LANES), LANES)
    low = lambda *extents: jax.ShapeDtypeStruct(extents, BF16)
    outs = [low(block, width), low(count, 3 * chan + LANES), low(count, 2 * STATE), shape(*mine), shape(*shared)]
    return pl.pallas_call(
        functools.partial(exit_kernel, n_tp=n_tp, n_fs=n_fs),
        name="exit",
        in_specs=[pl.BlockSpec(memory_space=pl.ANY)] * 5 + [vmem] * 5,
        out_specs=[vmem] * len(outs),
        out_shape=outs,
        scratch_shapes=[
            room(*dn.shape), room(*normed.shape), room(*dpre.shape), room(*cot.shape), room(*gnormed.shape), dma((5,)),
            room(width, cols), room(width, chan), pltpu.VMEM(mine, F32), pltpu.VMEM(shared, F32),
            room(2, steps, block // CHUNKS, width),
            room(chips, count, cols), room(chips, count, chan), room(chips, count, cols), room(chips, count, chan),
            room(chips, count, cols), room(chips, count, chan),
            pltpu.VMEM((n_fs,) + mine, F32), pltpu.VMEM((n_fs,) + shared, F32),
            pltpu.VMEM(shared, F32), pltpu.VMEM((n_tp,) + shared, F32),
            room(count, 2 * STATE), room(n_tp, count, 2 * STATE),
            dma((2, steps)), dma((2, steps)), dma((4, chips)), dma((4, chips)), dma((4, chips)), dma((4, chips)),
            dma((n_fs,)), dma((n_fs,)), dma((n_fs,)), dma((n_fs,)), dma((n_tp,)), dma((n_tp,)), dma((n_tp,)),
            dma((n_tp,)),
        ],
        compiler_params=pltpu.CompilerParams(
            collective_id=TAGS["exit"], has_side_effects=True, vmem_limit_bytes=62 << 20
        ),
    )(dn, normed, dpre, cot, gnormed, *small)


def shards(
    tokens, cotangent, seq_start, token_valid, norm_gain, proj_z, proj_x, proj_bc, proj_dt, conv_chan, bias_chan,
    conv_shared, bias_shared, a_log, dt_bias, skip_gain, gate_gain, proj_out,
):
    chan, heads_here = proj_z.shape[1], proj_dt.shape[1]
    n_tp, n_fs = lax.axis_size("tp"), lax.axis_size("fsdp")
    (
        tok_all, cot_all, w_in, normed, pre, y, enter, dgn, gnormed, out_rows, early, stats, taps, bias, heads, skip,
        gate,
    ) = ahead(
        seq_start, (dt_bias, a_log, skip_gain), tokens, cotangent,
        (proj_z, proj_x, proj_bc, proj_dt.T, proj_out.T), token_valid,
        (norm_gain, conv_chan, bias_chan, conv_shared, bias_shared, gate_gain), n_tp, n_fs,
    )
    dpre, dn_rows, *small, mixed = mixer_backward(
        seq_start, tok_all, w_in, taps, bias, heads, skip, gate, pre, y, enter, dgn, stats, out_rows, chan * n_tp,
        n_tp,
    )
    sums = leave(dn_rows, normed, dpre, cot_all, gnormed, small, n_tp, n_fs)
    grads = list(finish(tokens, cotangent, early, mixed, norm_gain, *sums, heads_here))
    grads[6], grads[15] = grads[6].T, grads[15].T
    return tuple(grads)


def solution(mesh):
    in_specs = (
        P(("fsdp", "tp"), None), P(("fsdp", "tp"), None), P("fsdp"), P("fsdp"), P(), P("fsdp", "tp"),
        P("fsdp", "tp"), P("fsdp", None), P("fsdp", "tp"), P(None, "tp"), P("tp"), P(), P(), P("tp"), P("tp"),
        P("tp"), P("tp"), P("tp", "fsdp"),
    )
    out_specs = (
        P(("fsdp", "tp"), None), P(("fsdp", "tp"), None), P(), P("fsdp", "tp"), P("fsdp", "tp"), P("fsdp", None),
        P("fsdp", "tp"), P(None, "tp"), P("tp"), P(), P(), P("tp"), P("tp"), P("tp"), P("tp"), P("tp", "fsdp"),
    )
    return jax.shard_map(shards, mesh=mesh, in_specs=in_specs, out_specs=out_specs, check_vma=False)
```

```python
import functools
import jax
import jax.numpy as jnp
from jax import lax
from jax.experimental import pallas as pl
from jax.experimental.pallas import tpu as pltpu
from jax.sharding import PartitionSpec as P

HEAD = 64
STATE = 128
STRETCH = 256
LANES = 128
EPSILON = 1e-05
PLACES = 3
F32 = jnp.float32
BF16 = jnp.bfloat16
NN = (((1,), (0,)), ((), ()))
NT = (((1,), (1,)), ((), ()))
TN = (((0,), (0,)), ((), ()))


def mm(a, b, dims=NN):
    return lax.dot_general(a, b, dims, preferred_element_type=F32)


def exact(a, b):
    return lax.dot_general(a, b, NN, precision=lax.Precision.HIGHEST, preferred_element_type=F32)


def halves(v):
    high = v.astype(BF16)
    return high, (v - high.astype(F32)).astype(BF16)


def iota(shape, dim):
    return lax.broadcasted_iota(jnp.int32, shape, dim)


def spread_heads(v, chan):
    high, rest = halves(v)
    rows = iota((2 * LANES, chan), 0) & (LANES - 1)
    pick = jnp.where(rows == (iota((2 * LANES, chan), 1) >> 6), 1.0, 0.0).astype(BF16)
    return mm(jnp.concatenate([high, rest], axis=1), pick)


def gather_heads(v):
    chan = v.shape[1]
    high, rest = halves(v)
    pick = jnp.where((iota((chan, LANES), 0) >> 6) == iota((chan, LANES), 1), 1.0, 0.0).astype(BF16)
    return mm(high, pick) + mm(rest, pick)


def softplus(v):
    return jnp.maximum(v, 0.0) + jnp.log1p(jnp.exp(-jnp.abs(v)))


def sigmoid(v):
    return 1.0 / (1.0 + jnp.exp(-v))


def lower_mask():
    return iota((STRETCH, STRETCH), 0) >= iota((STRETCH, STRETCH), 1)


def convolve(xs_ref, taps_ref, bias_ref):
    total = bias_ref[...] + taps_ref[0:1, :] * xs_ref[5:5 + STRETCH, :]
    for tap in range(1, 4):
        total = total + taps_ref[tap:tap + 1, :] * xs_ref[5 + tap:5 + tap + STRETCH, :]
    return total


def decays(pre_dt, head_ref, valid):
    rates = softplus(pre_dt + head_ref[0:1, :]) * valid
    log_decay = rates * head_ref[1:2, :]
    lower = lower_mask().astype(F32)
    cumulative = exact(lower, log_decay)
    last = cumulative[STRETCH - 1:STRETCH, :]
    return rates, cumulative, jnp.exp(cumulative), jnp.exp(last - cumulative)


def weights_of(cumulative, across, head):
    return jnp.exp(jnp.minimum(cumulative[:, head:head + 1] - across[head:head + 1, :], 0.0))


def backward_kernel(
    open_ref, tok_ref, w_hbm, taps_ref, bias_ref, head_ref, skip_ref, gate_ref,
    pre_ref, halo_ref, y_ref, enter_ref, dgn_ref, stats_ref, rows_ref,
    dpre_ref, dnormed_ref, dtaps_ref, dbias_ref, dhead_ref, dchan_ref, dgain_ref, mixed_ref,
    dstate, xs, dus, rows, w_ref, o_got, fetch_sem, o_send, o_recv,
    *, inner, n_tp,
):
    chan = y_ref.shape[1]
    wide = chan + 2 * STATE
    step = pl.program_id(0)
    block = pl.num_programs(0) - 1 - step
    opening = open_ref[block] == 1
    keep = jnp.where(opening, 0.0, 1.0).astype(F32)
    tp = lax.axis_index("tp")
    per = rows.shape[0] // n_tp
    chunk = per // CHUNKS
    sums = LineSum(
        tp, n_tp, CHUNKS - EARLY, lambda index, part: chunk_of(rows, index, per, part + EARLY, chunk),
        lambda index, part: chunk_of(rows_ref, index, per, part + EARLY, chunk), o_got, o_send, o_recv,
    )

    fetches = (
        pltpu.make_async_copy(rows_ref, rows, fetch_sem.at[0]), pltpu.make_async_copy(w_hbm, w_ref, fetch_sem.at[1])
    )

    def turn(place):
        at = step * PLACES + place - 2

        @pl.when(jnp.logical_and(at >= 0, at < sums.turns))
        def _():
            sums.advance(at)

    @pl.when(step == 0)
    def _():
        for fetch in fetches:
            fetch.start()
        line_greeting(tp, n_tp)
        sums.kick()

    @pl.when(step == 0)
    def _():
        dstate[...] = jnp.zeros_like(dstate)
        dus[...] = jnp.zeros_like(dus)
        dtaps_ref[...] = jnp.zeros_like(dtaps_ref)
        dbias_ref[...] = jnp.zeros_like(dbias_ref)
        dhead_ref[...] = jnp.zeros_like(dhead_ref)
        dchan_ref[...] = jnp.zeros_like(dchan_ref)
        dgain_ref[...] = jnp.zeros_like(dgain_ref)

    grstd, cross, valid = row_stats(stats_ref, inner)
    xs[0:8, :] = halo_ref[:, chan:2 * chan + 2 * STATE] * keep
    xs[8:8 + STRETCH, :] = pre_ref[:, chan:2 * chan + 2 * STATE]
    conv = convolve(xs, taps_ref, bias_ref)
    gate_u = sigmoid(conv)
    feats = conv * gate_u
    slope = gate_u * (1.0 + conv * (1.0 - gate_u))
    x = feats[:, :chan]
    bs = feats[:, chan:chan + STATE].astype(BF16)
    cs = feats[:, chan + STATE:].astype(BF16)
    pre_dt = pre_ref[:, 2 * chan + 2 * STATE:]
    rates, cumulative, grown, to_end = decays(pre_dt, head_ref, valid)
    across = cumulative.T
    grown_e = spread_heads(grown, chan)
    rates_e = spread_heads(rates, chan)
    to_end_e = spread_heads(to_end, chan)
    leave_e = grown_e[STRETCH - 1:STRETCH, :]

    pre_z = pre_ref[:, :chan]
    gate_z = sigmoid(pre_z)
    silu_z = pre_z * gate_z * valid
    y = y_ref[...]
    mixed = y + skip_ref[...] * x
    gated = mixed * silu_z
    dgn = dgn_ref[...]
    d_gated = grstd * (gate_ref[...] * dgn) - gated * (grstd * grstd * grstd * cross * (1.0 / inner))
    d_mixed = d_gated * silu_z
    dpre_ref[:, :chan] = (
        d_gated * mixed * (valid * (gate_z * (1.0 + pre_z * (1.0 - gate_z))))
    ).astype(BF16)
    dchan_ref[0:1, :] += jnp.sum(dgn * gated * grstd, axis=0, keepdims=True)
    dchan_ref[1:2, :] += jnp.sum(d_mixed * x, axis=0, keepdims=True)

    turn(0)
    dy_b = d_mixed.astype(BF16)
    dy = dy_b.astype(F32)
    scaled = x * rates_e
    scaled_b = scaled.astype(BF16)
    entering = enter_ref[0]
    d_leaving = dstate[...]
    d_leaving_b = d_leaving.astype(BF16)
    tail = mm(bs, d_leaving_b) * to_end_e
    overlap = jnp.where(lower_mask(), mm(cs, bs, NT), 0.0)
    first = iota((STRETCH, LANES), 1) < HEAD
    d_overlap = jnp.zeros((STRETCH, STRETCH), F32)
    parts = []
    for pair in range(chan // LANES):
        cols = slice(pair * LANES, (pair + 1) * LANES)
        dy_pair = dy_b[:, cols]
        x_pair = scaled_b[:, cols]
        zero = jnp.zeros_like(dy_pair)
        sides = [jnp.where(first, dy_pair, zero), jnp.where(first, zero, dy_pair)]
        mats = []
        for side in range(2):
            weight = weights_of(cumulative, across, 2 * pair + side)
            mats.append((weight * overlap).astype(BF16))
            d_overlap = d_overlap + mm(sides[side], x_pair, NT) * weight
        parts.append(mm(jnp.concatenate(mats, axis=0), jnp.concatenate(sides, axis=0), TN))
    turn(1)
    d_scaled = jnp.concatenate(parts, axis=1) + tail
    scaled_r = scaled_b.astype(F32)
    d_cum = gather_heads(dy * y - scaled_r * d_scaled)
    d_last = jnp.sum(scaled_r * tail, axis=0, keepdims=True) + leave_e * jnp.sum(
        d_leaving * entering, axis=0, keepdims=True
    )
    d_last = gather_heads(jnp.broadcast_to(d_last, (8, chan)))[0:1, :]
    upper = (iota((STRETCH, STRETCH), 0) <= iota((STRETCH, STRETCH), 1)).astype(F32)
    d_log = exact(upper, d_cum) + d_last
    decay = head_ref[1:2, :]
    d_rates = d_log * decay + gather_heads(x * d_scaled)
    d_dt = d_rates * valid * sigmoid(pre_dt + head_ref[0:1, :])
    dhead_ref[0:1, :] += jnp.sum(d_log * rates, axis=0, keepdims=True) * decay
    dhead_ref[1:2, :] += jnp.sum(d_dt, axis=0, keepdims=True)
    dpre_ref[:, 2 * chan + 2 * STATE:] = d_dt.astype(BF16)

    d_x = d_scaled * rates_e + skip_ref[...] * d_mixed
    d_overlap_b = jnp.where(lower_mask(), d_overlap, 0.0).astype(BF16)
    dy_grown = (dy * grown_e).astype(BF16)
    x_end = (scaled * to_end_e).astype(BF16)
    d_b = mm(d_overlap_b, cs, TN) + mm(x_end, d_leaving_b, NT)
    d_c = mm(d_overlap_b, bs) + mm(dy_grown, entering.astype(BF16), NT)
    dstate[...] = (d_leaving * leave_e + mm(cs, dy_grown, TN)) * keep

    dus[0:STRETCH, :chan] = d_x * slope[:, :chan]
    dus[0:STRETCH, chan:chan + STATE] = d_b * slope[:, chan:chan + STATE]
    dus[0:STRETCH, chan + STATE:] = d_c * slope[:, chan + STATE:]
    d_conv = dus[0:STRETCH, :]
    dbias_ref[...] += jnp.sum(d_conv, axis=0, keepdims=True)
    d_pre = jnp.zeros((STRETCH, wide), F32)
    for tap in range(4):
        dtaps_ref[tap:tap + 1, :] += jnp.sum(d_conv * xs[5 + tap:5 + tap + STRETCH, :], axis=0, keepdims=True)
        d_pre = d_pre + taps_ref[tap:tap + 1, :] * dus[3 - tap:3 - tap + STRETCH, :]
    dpre_ref[:, chan:2 * chan + 2 * STATE] = d_pre.astype(BF16)
    dus[STRETCH:STRETCH + 8, :] = d_conv[0:8, :] * keep

    @pl.when(step == 0)
    def _():
        for fetch in fetches:
            fetch.wait()

    turn(2)
    d_normed = mm(dpre_ref[...], w_ref[...], NT)
    dnormed_ref[...] = d_normed.astype(BF16)
    resid = tok_ref[...].astype(F32)
    rstd = lax.rsqrt(jnp.mean(resid * resid, axis=1, keepdims=True) + EPSILON)
    dgain_ref[...] += jnp.sum(d_normed * (resid * rstd), axis=0, keepdims=True)

    @pl.when(step == pl.num_programs(0) - 1)
    def _():
        pl.loop(jnp.minimum(step * PLACES + 1, sums.turns), sums.turns)(sums.advance)
        sums.settle(lambda part: mixed_ref.at[pl.ds(part * chunk, chunk)])
        sums.drain()


def whole(shape):
    return pl.BlockSpec(shape, lambda *_: (0,) * len(shape), pipeline_mode=pl.Buffered(1))


def mixer_backward(
    openings, tok, w_in, taps, bias, heads, skip, gate, pre, y, enter, dgn, stats, out_rows, inner, n_tp
):
    tokens, width = tok.shape
    cols = w_in.shape[1]
    chan = skip.shape[1]
    blocks = tokens // STRETCH
    wide = chan + 2 * STATE
    per = STRETCH // 8
    steps = (n_tp - 1) * (CHUNKS - EARLY)
    kept = tokens // n_tp // CHUNKS * (CHUNKS - EARLY)
    rows = lambda n: pl.BlockSpec((STRETCH, n), lambda i, *_: (blocks - 1 - i, 0))
    return pl.pallas_call(
        functools.partial(backward_kernel, inner=inner, n_tp=n_tp),
        name="mixer_backward",
        grid_spec=pltpu.PrefetchScalarGridSpec(
            num_scalar_prefetch=1,
            grid=(blocks,),
            in_specs=[
                rows(width), pl.BlockSpec(memory_space=pl.ANY), whole((4, wide)), whole((1, wide)),
                whole((8, LANES)), whole((1, chan)), whole((1, chan)),
                rows(cols),
                pl.BlockSpec((8, cols), lambda i, *_: (jnp.maximum((blocks - 1 - i) * per - 1, 0), 0)),
                rows(chan),
                pl.BlockSpec((1, STATE, chan), lambda i, *_: (blocks - 1 - i, 0, 0)),
                rows(chan),
                pl.BlockSpec((8, STRETCH), lambda i, *_: (0, blocks - 1 - i)),
                pl.BlockSpec(memory_space=pl.ANY),
            ],
            out_specs=[
                rows(cols), rows(width),
                pl.BlockSpec((8, wide), lambda i, *_: (0, 0)),
                pl.BlockSpec((1, wide), lambda i, *_: (0, 0)),
                pl.BlockSpec((8, LANES), lambda i, *_: (0, 0)),
                pl.BlockSpec((8, chan), lambda i, *_: (0, 0)),
                pl.BlockSpec((1, width), lambda i, *_: (0, 0)),
                pl.BlockSpec((kept, width), lambda i, *_: (0, 0)),
            ],
            scratch_shapes=[
                pltpu.VMEM((STATE, chan), F32),
                pltpu.VMEM((STRETCH + 8, wide), F32),
                pltpu.VMEM((STRETCH + 8, wide), F32),
                pltpu.VMEM((tokens, width), BF16),
                pltpu.VMEM((width, cols), BF16),
                pltpu.VMEM((2, steps, tokens // n_tp // CHUNKS, width), BF16),
                pltpu.SemaphoreType.DMA((2,)),
                pltpu.SemaphoreType.DMA((2, steps)),
                pltpu.SemaphoreType.DMA((2, steps)),
            ],
        ),
        out_shape=[
            jax.ShapeDtypeStruct((tokens, cols), BF16),
            jax.ShapeDtypeStruct((tokens, width), BF16),
            jax.ShapeDtypeStruct((8, wide), F32),
            jax.ShapeDtypeStruct((1, wide), F32),
            jax.ShapeDtypeStruct((8, LANES), F32),
            jax.ShapeDtypeStruct((8, chan), F32),
            jax.ShapeDtypeStruct((1, width), F32),
            jax.ShapeDtypeStruct((kept, width), BF16),
        ],
        cost_estimate=pl.CostEstimate(
            flops=4 * tokens * width * cols, bytes_accessed=tokens * cols * 12, transcendentals=tokens * chan
        ),
        compiler_params=pltpu.CompilerParams(
            collective_id=TAGS["backward"], has_side_effects=True, vmem_limit_bytes=60 << 20,
            dimension_semantics=("arbitrary",),
        ),
    )(openings, tok, w_in, taps, bias, heads, skip, gate, pre, pre, y, enter, dgn, stats, out_rows)


MESH = pl.DeviceIdType.MESH
CHUNKS = 4
EARLY = 1
TAGS = {"ahead": 1, "backward": 2, "exit": 3}


def remote(source, target, send, recv, **where):
    return pltpu.make_async_remote_copy(
        src_ref=source, dst_ref=target, send_sem=send, recv_sem=recv, device_id=where, device_id_type=MESH
    )


def rows_at(ref, index, count):
    return ref.at[pl.ds(pl.multiple_of(index * count, count), count)]


def greet(axis, peers):
    barrier = pltpu.get_barrier_semaphore()
    for peer in peers:
        pl.semaphore_signal(barrier, inc=1, device_id={axis: peer}, device_id_type=MESH)


class Line:
    def __init__(self, tp, n_tp, own, whole_ref, send, recv):
        self.tp, self.n, self.own, self.whole_ref, self.send, self.recv = tp, n_tp, own, whole_ref, send, recv
        self.count = own.shape[0]

    def copy(self, way, step, own=False):
        shift = -1 if way == 0 else 1
        index = self.tp + shift * step
        slot = rows_at(self.whole_ref, index, self.count)
        return remote(
            self.own if own else slot, slot, self.send.at[way, step], self.recv.at[way, step], tp=self.tp - shift
        )

    def sends(self, way, step):
        if way == 0:
            return jnp.logical_and(self.tp < self.n - 1, self.tp >= step)
        return jnp.logical_and(self.tp > 0, self.tp + step <= self.n - 1)

    def takes(self, way, step):
        return self.tp >= step + 1 if way == 0 else self.tp + step + 1 <= self.n - 1

    def start(self, way, step):
        @pl.when(self.sends(way, step))
        def _():
            self.copy(way, step, own=step == 0).start()

    def arrive(self, way, step):
        @pl.when(self.takes(way, step))
        def _():
            shift = -1 if way == 0 else 1
            slot = rows_at(self.whole_ref, self.tp + shift * (step + 1), self.count)
            remote(
                slot, slot, self.send.at[way, step], self.recv.at[way, step], tp=self.tp + shift
            ).wait_recv()

    def finish(self, way, step):
        @pl.when(self.sends(way, step))
        def _():
            self.copy(way, step, own=step == 0).wait_send()


class LineSum:
    def __init__(self, tp, n_tp, per, local, origin, got, send, recv):
        self.tp, self.n, self.per, self.local_of, self.origin = tp, n_tp, per, local, origin
        self.got, self.send, self.recv = got, send, recv
        self.steps = (n_tp - 1) * per
        self.paced = max(n_tp - 2, 0) * per
        self.turns = self.paced + max(n_tp - 3, 0)

    def ahead(self, way, step):
        return self.n - 1 - step // self.per if way == 0 else step // self.per

    def passes(self, way, step):
        return self.ahead(way, step) > self.tp if way == 0 else self.ahead(way, step) < self.tp

    def first(self, way):
        return self.tp == 0 if way == 0 else self.tp == self.n - 1

    def local(self, way, step):
        return self.local_of(self.ahead(way, step), step % self.per)

    def copy(self, way, step, direct):
        source = (self.origin if direct else self.local_of)(self.ahead(way, step), step % self.per)
        return remote(
            source, self.got.at[way, step], self.send.at[way, step], self.recv.at[way, step],
            tp=self.tp + 1 if way == 0 else self.tp - 1,
        )

    def kick(self):
        for way in range(2):
            @pl.when(self.first(way))
            def _():
                for step in range(min(2, self.steps) if self.paced else self.steps):
                    self.copy(way, step, True).start()

    def advance(self, turn):
        for way in range(2):
            lag = jnp.maximum(self.tp - 1 if way == 0 else self.n - 2 - self.tp, 0)
            step = turn - lag
            live = jnp.logical_and(step >= 0, step < self.paced)

            @pl.when(jnp.logical_and(self.first(way), live))
            def _():
                self.copy(way, step, True).wait_send()

                @pl.when(step + 2 < self.steps)
                def _():
                    self.copy(way, step + 2, True).start()

                @pl.when(step == self.paced - 1)
                def _():
                    for rest in range(self.paced + 2, self.steps):
                        self.copy(way, rest, True).start()

            @pl.when(jnp.logical_and(jnp.logical_and(self.passes(way, step), live), jnp.logical_not(self.first(way))))
            def _():
                copy = self.copy(way, step, False)
                copy.wait_recv()
                add_into(self.local(way, step), self.local(way, step), self.got.at[way, step])
                copy.start()

    def settle(self, target):
        for way in range(2):
            for step in range(self.steps):
                @pl.when(jnp.logical_and(self.ahead(way, step) == self.tp, jnp.logical_not(self.first(way))))
                def _():
                    self.copy(way, step, False).wait_recv()

        for value in range(self.n):
            @pl.when(self.tp == value)
            def _():
                for part in range(self.per):
                    incoming = []
                    if value > 0:
                        incoming.append(self.got.at[0, (self.n - 1 - value) * self.per + part])
                    if value < self.n - 1:
                        incoming.append(self.got.at[1, value * self.per + part])
                    add_into(target(part), self.local_of(value, part), *incoming)

    def drain(self):
        for way in range(2):
            @pl.when(self.first(way))
            def _():
                for step in range(self.paced, self.steps):
                    self.copy(way, step, True).wait_send()

            for step in range(self.steps):
                @pl.when(jnp.logical_and(self.passes(way, step), jnp.logical_not(self.first(way))))
                def _():
                    self.copy(way, step, False).wait_send()


def chunk_of(ref, block, rows, part, chunk):
    return ref.at[pl.ds(pl.multiple_of(block * rows + part * chunk, chunk), chunk)]


def line_greeting(tp, n_tp):
    barrier = pltpu.get_barrier_semaphore()
    for near, there in ((tp - 1, tp > 0), (tp + 1, tp < n_tp - 1)):
        @pl.when(there)
        def _():
            pl.semaphore_signal(barrier, inc=1, device_id={"tp": near}, device_id_type=MESH)
    pl.semaphore_wait(barrier, jnp.where(tp > 0, 1, 0) + jnp.where(tp < n_tp - 1, 1, 0))


def forward_block(keep, tok, valid, gain_ref, w_ref, taps_ref, bias_ref, head_ref, skip_ref,
                  normed_ref, pre_ref, y_ref, gated_ref, enter_ref, state, xs):
    chan = y_ref.shape[1]
    xs[0:8, :] = xs[STRETCH:STRETCH + 8, :] * keep
    resid = tok.astype(F32)
    rstd = lax.rsqrt(jnp.mean(resid * resid, axis=1, keepdims=True) + EPSILON)
    normed = (resid * rstd * gain_ref[...]).astype(BF16)
    normed_ref[...] = normed
    pre_ref[...] = mm(normed, w_ref[...])
    xs[8:8 + STRETCH, :] = pre_ref[:, chan:2 * chan + 2 * STATE]
    conv = convolve(xs, taps_ref, bias_ref)
    feats = conv * sigmoid(conv)
    x = feats[:, :chan]
    bs = feats[:, chan:chan + STATE].astype(BF16)
    cs = feats[:, chan + STATE:].astype(BF16)
    rates, cumulative, grown, to_end = decays(pre_ref[:, 2 * chan + 2 * STATE:], head_ref, valid)
    across = cumulative.T
    grown_e = spread_heads(grown, chan)
    scaled = x * spread_heads(rates, chan)
    entering = state[...] * keep
    enter_ref[...] = entering
    y_ref[...] = mm(cs, entering.astype(BF16)) * grown_e
    state[...] = entering * grown_e[STRETCH - 1:STRETCH, :] + mm(
        bs, (scaled * spread_heads(to_end, chan)).astype(BF16), TN
    )
    overlap = jnp.where(lower_mask(), mm(cs, bs, NT), 0.0)
    scaled_b = scaled.astype(BF16)
    first = iota((STRETCH, LANES), 1) < HEAD
    for pair in range(chan // LANES):
        cols = slice(pair * LANES, (pair + 1) * LANES)
        both = scaled_b[:, cols]
        mats = [
            (weights_of(cumulative, across, 2 * pair + side) * overlap).astype(BF16) for side in range(2)
        ]
        zero = jnp.zeros_like(both)
        y_ref[:, cols] += mm(
            jnp.concatenate(mats, axis=1),
            jnp.concatenate([jnp.where(first, both, zero), jnp.where(first, zero, both)], axis=0),
        )
    pre_z = pre_ref[:, :chan]
    gated = (y_ref[...] + skip_ref[...] * x) * (pre_z * sigmoid(pre_z)) * valid
    gated_ref[...] = gated
    return jnp.sum(gated * gated, axis=1, keepdims=True)


def as_row(column):
    lane = iota((STRETCH, LANES), 1)
    return jnp.where(lane == 0, column, 0.0).T[0:8, :]


def as_column(row):
    return jnp.concatenate([row, jnp.zeros((LANES - 8, STRETCH), F32)], axis=0).T


def row_stats(stats_ref, inner):
    filled = as_column(stats_ref[...])
    return lax.rsqrt(filled[:, 0:1] * (1.0 / inner) + EPSILON), filled[:, 1:2], filled[:, 2:3]


def ahead_kernel(
    open_ref, step_bias, log_rate, direct, tok_ref, cot_ref, pz_ref, px_ref, pbc_ref, pdt_ref, pout_ref, mask_ref,
    norm_gain, conv_chan, bias_chan, conv_shared, bias_shared, gate_gain,
    tok_out, cot_out, win_out, normed_out, pre_out, y_out, enter_out, dgn_out, gn_out, rows_out, mixed_out, stats_ref,
    taps_ref, bias_ref, head_ref, skip_ref, gate_ref,
    pin_ref, gain_ref, tok_all, cot_all, w_in, w_out, normed, pre, y, gated, enter, dgn, gnormed, rows, state, xs, squares, crosses,
    squares_got, crosses_got, o_got,
    own_sem, z_send, z_recv, c_send, c_recv, f_send, f_recv, p_send, p_recv, q_send, q_recv, r_send, r_recv,
    all_sem, out_sem, o_send, o_recv,
    *, n_tp, n_fs, inner,
):
    tp, me = lax.axis_index("tp"), lax.axis_index("fsdp")
    chip, core, chips = me // 2, me % 2, n_fs // 2
    partner = chip * 2 + 1 - core
    blocks = tok_all.shape[0] // STRETCH
    per = tok_ref.shape[0]
    chan = pout_ref.shape[1]
    pin_ref[:, :chan] = pz_ref[...]
    pin_ref[:, chan:2 * chan] = px_ref[...]
    pin_ref[:, 2 * chan:2 * chan + 2 * STATE] = pbc_ref[...]
    heads_here, rows_dt = pdt_ref.shape
    pin_ref[:, 2 * chan + 2 * STATE:] = jnp.concatenate(
        [pdt_ref[...].astype(F32), jnp.zeros((LANES - heads_here, rows_dt), F32)], axis=0
    ).T.astype(BF16)
    greet("fsdp", [((chip + d) % chips) * 2 + core for d in range(1, chips)] + [partner])
    greet("tp", [(tp + d) % n_tp for d in range(1, n_tp)])
    pl.semaphore_wait(pltpu.get_barrier_semaphore(), chips + n_tp - 1)

    packs = ((pin_ref, w_in), (pout_ref, w_out))
    count = pin_ref.shape[0]
    line = Line(tp, n_tp, tok_ref, tok_all, z_send, z_recv)
    late = Line(tp, n_tp, cot_ref, cot_all, c_send, c_recv)
    for way in range(2):
        line.start(way, 0)
    for j, (pack, full) in enumerate(packs):
        for d in range(1, chips):
            remote(
                pack, rows_at(full, me, count), f_send.at[j, d], f_recv.at[j, d], fsdp=((chip + d) % chips) * 2 + core
            ).start()
        remote(pack, rows_at(full, me, count), p_send.at[j, 0], p_recv.at[j, 0], fsdp=partner).start()
    own = [
        pltpu.make_async_copy(tok_ref, rows_at(tok_all, tp, per), own_sem.at[0]),
        pltpu.make_async_copy(pin_ref, rows_at(w_in, me, count), own_sem.at[1]),
        pltpu.make_async_copy(pout_ref, rows_at(w_out, me, count), own_sem.at[2]),
        pltpu.make_async_copy(cot_ref, rows_at(cot_all, tp, per), own_sem.at[3]),
    ]
    for copy in own:
        copy.start()
    state[...] = jnp.zeros_like(state)
    xs[...] = jnp.zeros_like(xs)
    lane = iota((8, LANES), 1)
    place = iota((8, LANES), 0)
    step_row, rate_row, skip_row = (
        sum(jnp.where(lane == head, source[head], 0.0) for head in range(heads_here))
        for source in (step_bias, log_rate, direct)
    )
    live = lane < heads_here
    head_ref[...] = jnp.where(
        place == 0, jnp.where(live, step_row, -100.0), jnp.where(live & (place == 1), -jnp.exp(rate_row), 0.0)
    )
    skip_ref[...] = spread_heads(skip_row, chan)[0:1, :]
    gain_ref[...] = norm_gain[...].reshape(gain_ref.shape)
    gate_ref[...] = gate_gain[...].reshape(gate_ref.shape)
    taps_ref[:, :chan] = conv_chan[...]
    taps_ref[:, chan:] = conv_shared[...]
    bias_ref[:, :chan] = bias_chan[...].reshape(1, chan)
    bias_ref[:, chan:] = bias_shared[...].reshape(1, 2 * STATE)
    for step in range(n_tp - 1):
        for way in range(2):
            line.arrive(way, step)
            if step + 1 < n_tp - 1:
                line.start(way, step + 1)
        if step == n_tp - 3 or n_tp < 3 and step == 0:
            for j, (pack, full) in enumerate(packs):
                for d in range(1, chips):
                    slot = rows_at(full, ((chip + chips - d) % chips) * 2 + core, count)
                    remote(slot, slot, f_send.at[j, d], f_recv.at[j, d], fsdp=partner).wait_recv()
                    remote(slot, slot, p_send.at[j, d], p_recv.at[j, d], fsdp=partner).start()
    for way in range(2):
        for step in range(n_tp - 1):
            line.finish(way, step)
        late.start(way, 0)
    for j, (pack, full) in enumerate(packs):
        for d in range(chips):
            slot = rows_at(full, ((chip + chips - d) % chips) * 2 + 1 - core, count)
            remote(slot, slot, p_send.at[j, d], p_recv.at[j, d], fsdp=partner).wait()
        for d in range(1, chips):
            remote(pack, rows_at(full, me, count), f_send.at[j, d], f_recv.at[j, d], fsdp=partner).wait_send()
    for copy in own:
        copy.wait()
    wholes = [
        pltpu.make_async_copy(tok_all, tok_out, all_sem.at[0]), pltpu.make_async_copy(w_in, win_out, all_sem.at[1]),
    ]
    for copy in wholes:
        copy.start()

    def span(block):
        return pl.ds(pl.multiple_of(block * STRETCH, STRETCH), STRETCH)

    def out(k, block):
        at = span(block)
        chunk = per // CHUNKS * EARLY
        kept = pl.ds(pl.multiple_of(block * STRETCH + chunk, chunk), STRETCH - chunk)
        pairs = (
            (normed.at[at], normed_out.at[at]), (pre.at[block % 2], pre_out.at[at]), (y.at[at], y_out.at[at]),
            (enter.at[block], enter_out.at[block]), (gnormed.at[at], gn_out.at[at]),
            (rows.at[kept], rows_out.at[kept]), (dgn.at[at], dgn_out.at[at]), (cot_all.at[at], cot_out.at[at]),
        )
        return pltpu.make_async_copy(*pairs[k], out_sem.at[k, block])

    @pl.loop(0, blocks)
    def _(block):
        at = span(block)
        keep = jnp.where(open_ref[block] == 1, 0.0, 1.0).astype(F32)

        @pl.when(block >= 2)
        def _():
            out(1, block - 2).wait()

        valid = mask_ref[at].reshape(1, STRETCH).astype(F32)
        squares[:, at] = jnp.where(iota((8, STRETCH), 0) == 2, valid, 0.0)
        total = forward_block(
            keep, tok_all[at, :], as_column(squares[:, at])[:, 2:3], gain_ref, w_in, taps_ref, bias_ref, head_ref, skip_ref,
            normed.at[at], pre.at[block % 2], y.at[at], gated.at[at], enter.at[block], state, xs,
        )
        squares[0:1, at] = as_row(total)[0:1, :]
        for k in range(4):
            out(k, block).start()

        @pl.when(block == max(blocks - 2, 0))
        def _():
            for way in range(2):
                late.arrive(way, 0)
                if n_tp > 2:
                    late.start(way, 1)

    def swap(part, got, send, recv):
        for d in range(1, n_tp):
            remote(part, got.at[tp], send.at[d], recv.at[d], tp=(tp + d) % n_tp).start()
        got[tp] = part[...]
        for d in range(1, n_tp):
            slot = got.at[(tp + n_tp - d) % n_tp]
            remote(slot, slot, send.at[d], recv.at[d], tp=(tp + d) % n_tp).wait_recv()
        total = got[0]
        for peer in range(1, n_tp):
            total = total + got[peer]
        return total

    stats_ref[...] = swap(squares, squares_got, q_send, q_recv)

    @pl.loop(0, blocks)
    def _(block):
        at = span(block)

        grstd, _, _ = row_stats(stats_ref.at[:, at], inner)
        value = (gated[at, :] * grstd * gate_ref[...]).astype(BF16)
        gnormed[at, :] = value
        rows[at, :] = mm(value, w_out[...], NT).astype(BF16)
        out(4, block).start()
        out(5, block).start()

    chunk = per // CHUNKS
    piece = lambda index, part: chunk_of(rows, index, per, part, chunk)
    sums = LineSum(tp, n_tp, EARLY, piece, piece, o_got, o_send, o_recv)
    sums.kick()

    def gradient(block):
        at = span(block)
        value = mm(cot_all[at, :], w_out[...])
        dgn[at, :] = value
        crosses[:, at] = as_row(jnp.sum(gate_ref[...] * value * gated[at, :], axis=1, keepdims=True))
        out(6, block).start()
        out(7, block).start()

    ratio = per // STRETCH

    def gradients(index):
        for k in range(ratio):
            gradient(index * ratio + k)

    gradients(tp)
    middle = min(sums.turns, 3)
    for step in range(n_tp - 1):
        for way in range(2):
            if step > 0:
                late.arrive(way, step)
                if step + 1 < n_tp - 1:
                    late.start(way, step + 1)
        for way in range(2):
            @pl.when(late.takes(way, step))
            def _():
                gradients(tp - step - 1 if way == 0 else tp + step + 1)
        if step == max(n_tp - 3, 0):
            pl.loop(0, middle)(sums.advance)

    total = swap(crosses, crosses_got, r_send, r_recv)
    if middle < sums.turns:
        pl.loop(middle, sums.turns)(sums.advance)
    sums.settle(lambda part: mixed_out.at[pl.ds(part * chunk, chunk)])

    stats_ref[1:2, :] = total[0:1, :]
    stats_ref[2:3, :] = squares[2:3, :]

    for copy in wholes:
        copy.wait()

    @pl.loop(0, blocks)
    def _(block):
        for k in (0, 2, 3, 4, 5, 6, 7):
            out(k, block).wait()

    for block in range(max(blocks - 2, 0), blocks):
        out(1, block).wait()
    for step in range(n_tp - 1):
        for way in range(2):
            late.finish(way, step)
    sums.drain()
    for d in range(1, n_tp):
        remote(squares, squares_got.at[tp], q_send.at[d], q_recv.at[d], tp=(tp + d) % n_tp).wait_send()
        remote(crosses, crosses_got.at[tp], r_send.at[d], r_recv.at[d], tp=(tp + d) % n_tp).wait_send()


def ahead(
    openings, heads, tokens, cotangent, projections, mask, vectors, n_tp, n_fs
):
    per, width = tokens.shape
    total = per * n_tp
    count, chan = projections[0].shape
    wide = chan + 2 * STATE
    cols = chan + wide + LANES
    blocks = total // STRETCH
    chips = n_fs // 2
    dma = pltpu.SemaphoreType.DMA
    anywhere = pl.BlockSpec(memory_space=pl.ANY)
    vmem = pl.BlockSpec(memory_space=pltpu.VMEM)
    shape = jax.ShapeDtypeStruct
    return pl.pallas_call(
        functools.partial(ahead_kernel, n_tp=n_tp, n_fs=n_fs, inner=chan * n_tp),
        name="ahead",
        in_specs=[pl.BlockSpec(memory_space=pltpu.SMEM)] * 4 + [vmem] * 14,
        out_specs=[anywhere] * 10 + [vmem] * 7,
        out_shape=[
            shape((total, width), BF16), shape((total, width), BF16), shape((count * n_fs, cols), BF16),
            shape((total, width), BF16), shape((total, cols), F32), shape((total, chan), F32),
            shape((blocks, STATE, chan), F32), shape((total, chan), F32), shape((total, chan), BF16),
            shape((total, width), BF16), shape((per // CHUNKS * EARLY, width), BF16), shape((8, total), F32),
            shape((4, wide), F32), shape((1, wide), F32),
            shape((8, LANES), F32), shape((1, chan), F32), shape((1, chan), F32),
        ],
        scratch_shapes=[
            pltpu.VMEM((count, cols), BF16), pltpu.VMEM((1, width), F32),
            pltpu.VMEM((total, width), BF16), pltpu.VMEM((total, width), BF16),
            pltpu.VMEM((count * n_fs, cols), BF16), pltpu.VMEM((count * n_fs, chan), BF16),
            pltpu.VMEM((total, width), BF16), pltpu.VMEM((2, STRETCH, cols), F32), pltpu.VMEM((total, chan), F32),
            pltpu.VMEM((total, chan), F32), pltpu.VMEM((blocks, STATE, chan), F32), pltpu.VMEM((total, chan), F32),
            pltpu.VMEM((total, chan), BF16), pltpu.VMEM((total, width), BF16),
            pltpu.VMEM((STATE, chan), F32), pltpu.VMEM((STRETCH + 8, wide), F32),
            pltpu.VMEM((8, total), F32), pltpu.VMEM((8, total), F32),
            pltpu.VMEM((n_tp, 8, total), F32), pltpu.VMEM((n_tp, 8, total), F32),
            pltpu.VMEM((2, (n_tp - 1) * EARLY, per // CHUNKS, width), BF16),
            dma((4,)), dma((2, n_tp - 1)), dma((2, n_tp - 1)), dma((2, n_tp - 1)), dma((2, n_tp - 1)),
            dma((2, chips)), dma((2, chips)), dma((2, chips)), dma((2, chips)),
            dma((n_tp,)), dma((n_tp,)), dma((n_tp,)), dma((n_tp,)), dma((2,)), dma((8, blocks)),
            dma((2, (n_tp - 1) * EARLY)), dma((2, (n_tp - 1) * EARLY)),
        ],
        compiler_params=pltpu.CompilerParams(
            collective_id=TAGS["ahead"], has_side_effects=True, vmem_limit_bytes=63 << 20
        ),
    )(openings, *heads, tokens, cotangent, *projections, mask, *vectors)


def add_into(target, *sources):
    rows, tile = target.shape[0], 32

    @pl.loop(0, rows // tile)
    def _(i):
        at = pl.ds(pl.multiple_of(i * tile, tile), tile)
        total = sources[0][at, :].astype(F32)
        for source in sources[1:]:
            total = total + source[at, :].astype(F32)
        target[at, :] = total.astype(target.dtype)


def fill_rows(target, pieces):
    at = 0
    for source, row, start, length in pieces:
        for k in range(length // LANES):
            target[at:at + 1, :] = source[row:row + 1, start + k * LANES:start + (k + 1) * LANES]
            at += 1
    if at < target.shape[0]:
        target[at:, :] = jnp.zeros((target.shape[0] - at, LANES), F32)


def finish_kernel(
    *refs,
):
    sources, refs = refs[:10], refs[10:]
    results, copies, sem = refs[:16], refs[16:26], refs[26]
    fetches = [pltpu.make_async_copy(source, copy, sem.at[k]) for k, (source, copy) in enumerate(zip(sources, copies))]
    for fetch in fetches:
        fetch.start()
    for fetch in fetches:
        fetch.wait()
    write_results(*copies, *results)


def write_results(
    tok_ref, cot_ref, early_ref, mixed_ref, gain_ref, dn_ref, own_ref, bc_ref, mine_ref, shared_ref,
    output, grad_tokens, g_gain, g_z, g_x, g_bc, g_dt, g_taps, g_bias, g_taps_s, g_bias_s, g_log, g_step, g_skip, g_gate,
    g_out,
):
    chan, heads_here = g_z.shape[1], g_log.shape[0]
    resid = tok_ref[...].astype(F32)
    early = early_ref.shape[0]
    output[0:early, :] = (resid[0:early, :] + early_ref[...].astype(F32)).astype(BF16)
    output[early:, :] = (resid[early:, :] + mixed_ref[...].astype(F32)).astype(BF16)
    rstd = lax.rsqrt(jnp.mean(resid * resid, axis=1, keepdims=True) + EPSILON)
    scaled = dn_ref[...].astype(F32) * gain_ref[...].reshape(1, resid.shape[1])
    grad_tokens[...] = (
        cot_ref[...].astype(F32) + rstd * scaled
        - resid * (rstd * rstd * rstd) * jnp.mean(scaled * resid, axis=1, keepdims=True)
    ).astype(BF16)
    g_z[...] = own_ref[:, :chan].astype(F32)
    g_x[...] = own_ref[:, chan:2 * chan].astype(F32)
    g_dt[...] = own_ref[:, 2 * chan:2 * chan + LANES].astype(F32).T[0:heads_here, :]
    g_out[...] = own_ref[:, 2 * chan + LANES:].astype(F32)
    g_bc[...] = bc_ref[...].astype(F32)

    def row(source, at, length):
        return jnp.concatenate([source[at + k:at + k + 1, :] for k in range(length // LANES)], axis=1)

    per = chan // LANES
    for tap in range(4):
        g_taps[tap:tap + 1, :] = row(mine_ref, tap * per, chan)
        g_taps_s[tap:tap + 1, :] = row(shared_ref, tap * 2, 2 * STATE)
    g_bias[...] = row(mine_ref, 4 * per, chan).reshape(chan)
    g_gate[...] = row(mine_ref, 5 * per, chan).reshape(chan)
    skip = gather_heads(jnp.broadcast_to(row(mine_ref, 6 * per, chan), (8, chan)))
    g_skip[...] = skip[0:1, :heads_here].reshape(heads_here)
    g_log[...] = mine_ref[7 * per:7 * per + 1, :heads_here].reshape(heads_here)
    g_step[...] = mine_ref[7 * per + 1:7 * per + 2, :heads_here].reshape(heads_here)
    g_bias_s[...] = row(shared_ref, 8, 2 * STATE).reshape(2 * STATE)
    g_gain[...] = row(shared_ref, 10, g_gain.shape[0]).reshape(g_gain.shape[0])


def finish(tokens, cotangent, early, mixed, gain, dn, own, bc, mine, shared, heads_here):
    operands = (tokens, cotangent, early, mixed, gain, dn, own, bc, mine, shared)
    rows, width = tokens.shape
    count = own.shape[0]
    chan = (own.shape[1] - LANES) // 3
    vmem = pl.BlockSpec(memory_space=pltpu.VMEM)
    shape = lambda *extents: jax.ShapeDtypeStruct(extents, F32)
    outs = [
        jax.ShapeDtypeStruct((rows, width), BF16), jax.ShapeDtypeStruct((rows, width), BF16), shape(width),
        shape(count, chan), shape(count, chan), shape(count, 2 * STATE), shape(heads_here, count), shape(4, chan),
        shape(chan), shape(4, 2 * STATE), shape(2 * STATE), shape(heads_here), shape(heads_here), shape(heads_here),
        shape(chan), shape(count, chan),
    ]
    return pl.pallas_call(
        finish_kernel, name="finish", in_specs=[pl.BlockSpec(memory_space=pltpu.HBM)] * 10,
        out_specs=[vmem] * len(outs), out_shape=outs,
        scratch_shapes=[pltpu.VMEM(v.shape, v.dtype) for v in operands] + [pltpu.SemaphoreType.DMA((10,))],
        compiler_params=pltpu.CompilerParams(vmem_limit_bytes=63 << 20),
    )(*operands)


def exit_kernel(
    dn_ref, normed_ref, dpre_ref, cot_ref, gn_ref, dtaps_ref, dbias_ref, dhead_ref, dchan_ref, dgain_ref,
    dn_out, own_out, bc_out, mine_out, shared_out,
    dn, normed, dpre, cot, gn, fetch_sem,
    gin_ref, gout_ref, mine_ref, shared_ref,
    z_got, near_in, near_out, far_in, far_out, got_in, got_out, mine_got, shared_got, shared_held, shared_z,
    bc_held, bc_got,
    zs, zr, ns, nr, fs, fr, ms, mr, ss, sr, ts, tr, bs, br,
    *, n_tp, n_fs,
):
    tp, me = lax.axis_index("tp"), lax.axis_index("fsdp")
    chip, core, chips = me // 2, me % 2, n_fs // 2
    partner = chip * 2 + 1 - core
    chan = gout_ref.shape[1]
    cols = gin_ref.shape[1]
    width = gin_ref.shape[0]
    fetches = [
        pltpu.make_async_copy(source, target, fetch_sem.at[k])
        for k, (source, target) in enumerate(
            [(normed_ref, normed), (dpre_ref, dpre), (cot_ref, cot), (gn_ref, gn), (dn_ref, dn)]
        )
    ]
    for fetch in fetches:
        fetch.start()
    fill_rows(
        mine_ref, [(dtaps_ref, tap, 0, chan) for tap in range(4)] + [(dbias_ref, 0, 0, chan)]
        + [(dchan_ref, row, 0, chan) for row in range(2)] + [(dhead_ref, row, 0, LANES) for row in range(2)]
    )
    fill_rows(
        shared_ref, [(dtaps_ref, tap, chan, 2 * STATE) for tap in range(4)] + [(dbias_ref, 0, chan, 2 * STATE)]
        + [(dgain_ref, 0, 0, width)]
    )
    block, count = dn_out.shape[0], own_out.shape[0]
    greet("fsdp", [(me + d) % n_fs for d in range(1, n_fs)])
    greet("tp", [(tp + d) % n_tp for d in range(1, n_tp)])
    pl.semaphore_wait(pltpu.get_barrier_semaphore(), n_fs - 1 + n_tp - 1)

    chunk = block // CHUNKS
    sums = LineSum(
        tp, n_tp, CHUNKS, lambda index, part: chunk_of(dn, index, block, part, chunk),
        lambda index, part: chunk_of(dn_ref, index, block, part, chunk), z_got, zs, zr,
    )
    sums.kick()
    for k in (0, 1):
        fetches[k].wait()
    advance = sums.advance
    parts = (
        (gin_ref, slice(2 * chan, cols), near_in, far_in, got_in),
        (gout_ref, slice(0, chan), near_out, far_out, got_out),
        (gin_ref, slice(chan, 2 * chan), near_in, far_in, got_in),
        (gin_ref, slice(0, chan), near_in, far_in, got_in),
    )

    def near(j, d):
        source, span, held, _, _ = parts[j]
        rows = rows_at(source, ((chip + d) % chips) * 2 + 1 - core, count)
        return remote(rows.at[:, span], held.at[d, :, span], ns.at[j, d], nr.at[j, d], fsdp=partner)

    def far(j, d):
        _, span, _, held, got = parts[j]
        return remote(
            held.at[d, :, span], got.at[d, :, span], fs.at[j, d], fr.at[j, d], fsdp=((chip + d) % chips) * 2 + core
        )

    order = [d for d in range(1, chips)]

    def small(d):
        peer = (me + d) % n_fs
        return (
            remote(mine_ref, mine_got.at[me], ms.at[d], mr.at[d], fsdp=peer),
            remote(shared_ref, shared_got.at[me], ss.at[d], sr.at[d], fsdp=peer),
        )

    for d in range(1, n_fs):
        for copy in small(d):
            copy.start()
    mine_got[me] = mine_ref[...]
    shared_got[me] = shared_ref[...]

    def differentiate(j):
        _, span, *_ = parts[j]
        left, right, target = (cot, gn, gout_ref) if j == 1 else (normed, dpre, gin_ref)
        tile = 256

        @pl.loop(0, width // tile)
        def _(piece):
            at = pl.ds(pl.multiple_of(piece * tile, tile), tile)
            target[at, span] = mm(left[:, at], right[:, span], TN).astype(BF16)

        for d in order + [0]:
            near(j, d).start()

    def send_sums(j):
        source, span, held, summed, _ = parts[j]
        for d in order:
            near(j, d).wait_recv()
            rows = rows_at(source, ((chip + d) % chips) * 2 + core, count)
            add_into(summed.at[d, :, span], rows.at[:, span], held.at[d, :, span])
            far(j, d).start()
        near(j, 0).wait_recv()

    differentiate(0)
    for k in (2, 3, 4):
        fetches[k].wait()
    advance(0)
    differentiate(1)
    send_sums(0)
    advance(1)
    differentiate(2)
    send_sums(1)
    advance(2)
    differentiate(3)
    send_sums(2)
    advance(3)
    send_sums(3)
    at = 3
    turns = sums.turns
    for d in range(1, n_fs):
        for copy in small(d):
            copy.wait_recv()
    total, again = mine_got[0], shared_got[0]
    for peer in range(1, n_fs):
        total, again = total + mine_got[peer], again + shared_got[peer]
    mine_out[...] = total
    shared_held[...] = again
    shared_z[tp] = again
    for d in range(1, n_tp):
        remote(shared_held, shared_z.at[tp], ts.at[d], tr.at[d], tp=(tp + d) % n_tp).start()
    pl.loop(at + 1, turns)(advance)

    def settle(j, target, span):
        source, _, held, _, got = parts[j]
        rows = rows_at(source, me, count)
        add_into(
            target, rows.at[:, span], held.at[0, :, span], *[got.at[d, :, span] for d in order]
        )

    for d in order:
        far(0, d).wait_recv()
    settle(0, bc_held, slice(2 * chan, 2 * chan + 2 * STATE))
    bc_got[tp] = bc_held[...]
    for d in range(1, n_tp):
        remote(bc_held, bc_got.at[tp], bs.at[d], br.at[d], tp=(tp + d) % n_tp).start()
    settle(0, own_out.at[:, 2 * chan:2 * chan + LANES], slice(2 * chan + 2 * STATE, cols))
    for j in (1, 2, 3):
        for d in order:
            far(j, d).wait_recv()
    settle(1, own_out.at[:, 2 * chan + LANES:], slice(0, chan))
    settle(2, own_out.at[:, chan:2 * chan], slice(chan, 2 * chan))
    settle(3, own_out.at[:, :chan], slice(0, chan))
    for d in range(1, n_tp):
        peer = (tp + n_tp - d) % n_tp
        remote(shared_held, shared_z.at[peer], ts.at[d], tr.at[d], tp=peer).wait_recv()
        remote(bc_held, bc_got.at[peer], bs.at[d], br.at[d], tp=peer).wait_recv()
    total = shared_z[0]
    for peer in range(1, n_tp):
        total = total + shared_z[peer]
    shared_out[...] = total
    add_into(bc_out, *[bc_got.at[peer] for peer in range(n_tp)])

    sums.settle(lambda part: dn_out.at[pl.ds(part * chunk, chunk)])
    sums.drain()
    for j in range(4):
        for d in range(chips):
            near(j, d).wait_send()
        for d in order:
            far(j, d).wait_send()
    for d in range(1, n_fs):
        for copy in small(d):
            copy.wait_send()
    for d in range(1, n_tp):
        remote(shared_held, shared_z.at[tp], ts.at[d], tr.at[d], tp=(tp + d) % n_tp).wait_send()
        remote(bc_held, bc_got.at[tp], bs.at[d], br.at[d], tp=(tp + d) % n_tp).wait_send()


def leave(dn, normed, dpre, cot, gnormed, small, n_tp, n_fs):
    block, width = dn.shape[0] // n_tp, dn.shape[1]
    count, cols = width // n_fs, dpre.shape[1]
    chan = gnormed.shape[1]
    chips, steps = n_fs // 2, (n_tp - 1) * CHUNKS
    dma = pltpu.SemaphoreType.DMA
    vmem = pl.BlockSpec(memory_space=pltpu.VMEM)
    room = lambda *shape: pltpu.VMEM(shape, BF16)
    shape = lambda *extents: jax.ShapeDtypeStruct(extents, F32)
    up = lambda n: -(-n // 8) * 8
    mine = (up(7 * chan // LANES + 2), LANES)
    shared = (up((10 * STATE + width) // LANES), LANES)
    low = lambda *extents: jax.ShapeDtypeStruct(extents, BF16)
    outs = [low(block, width), low(count, 3 * chan + LANES), low(count, 2 * STATE), shape(*mine), shape(*shared)]
    return pl.pallas_call(
        functools.partial(exit_kernel, n_tp=n_tp, n_fs=n_fs),
        name="exit",
        in_specs=[pl.BlockSpec(memory_space=pl.ANY)] * 5 + [vmem] * 5,
        out_specs=[vmem] * len(outs),
        out_shape=outs,
        scratch_shapes=[
            room(*dn.shape), room(*normed.shape), room(*dpre.shape), room(*cot.shape), room(*gnormed.shape), dma((5,)),
            room(width, cols), room(width, chan), pltpu.VMEM(mine, F32), pltpu.VMEM(shared, F32),
            room(2, steps, block // CHUNKS, width),
            room(chips, count, cols), room(chips, count, chan), room(chips, count, cols), room(chips, count, chan),
            room(chips, count, cols), room(chips, count, chan),
            pltpu.VMEM((n_fs,) + mine, F32), pltpu.VMEM((n_fs,) + shared, F32),
            pltpu.VMEM(shared, F32), pltpu.VMEM((n_tp,) + shared, F32),
            room(count, 2 * STATE), room(n_tp, count, 2 * STATE),
            dma((2, steps)), dma((2, steps)), dma((4, chips)), dma((4, chips)), dma((4, chips)), dma((4, chips)),
            dma((n_fs,)), dma((n_fs,)), dma((n_fs,)), dma((n_fs,)), dma((n_tp,)), dma((n_tp,)), dma((n_tp,)),
            dma((n_tp,)),
        ],
        compiler_params=pltpu.CompilerParams(
            collective_id=TAGS["exit"], has_side_effects=True, vmem_limit_bytes=62 << 20
        ),
    )(dn, normed, dpre, cot, gnormed, *small)


def shards(
    tokens, cotangent, seq_start, token_valid, norm_gain, proj_z, proj_x, proj_bc, proj_dt, conv_chan, bias_chan,
    conv_shared, bias_shared, a_log, dt_bias, skip_gain, gate_gain, proj_out,
):
    chan, heads_here = proj_z.shape[1], proj_dt.shape[1]
    n_tp, n_fs = lax.axis_size("tp"), lax.axis_size("fsdp")
    (
        tok_all, cot_all, w_in, normed, pre, y, enter, dgn, gnormed, out_rows, early, stats, taps, bias, heads, skip,
        gate,
    ) = ahead(
        seq_start, (dt_bias, a_log, skip_gain), tokens, cotangent,
        (proj_z, proj_x, proj_bc, proj_dt.T, proj_out.T), token_valid,
        (norm_gain, conv_chan, bias_chan, conv_shared, bias_shared, gate_gain), n_tp, n_fs,
    )
    dpre, dn_rows, *small, mixed = mixer_backward(
        seq_start, tok_all, w_in, taps, bias, heads, skip, gate, pre, y, enter, dgn, stats, out_rows, chan * n_tp,
        n_tp,
    )
    sums = leave(dn_rows, normed, dpre, cot_all, gnormed, small, n_tp, n_fs)
    grads = list(finish(tokens, cotangent, early, mixed, norm_gain, *sums, heads_here))
    grads[6], grads[15] = grads[6].T, grads[15].T
    return tuple(grads)


def solution(mesh):
    in_specs = (
        P(("fsdp", "tp"), None), P(("fsdp", "tp"), None), P("fsdp"), P("fsdp"), P(), P("fsdp", "tp"),
        P("fsdp", "tp"), P("fsdp", None), P("fsdp", "tp"), P(None, "tp"), P("tp"), P(), P(), P("tp"), P("tp"),
        P("tp"), P("tp"), P("tp", "fsdp"),
    )
    out_specs = (
        P(("fsdp", "tp"), None), P(("fsdp", "tp"), None), P(), P("fsdp", "tp"), P("fsdp", "tp"), P("fsdp", None),
        P("fsdp", "tp"), P(None, "tp"), P("tp"), P(), P(), P("tp"), P("tp"), P("tp"), P("tp"), P("tp", "fsdp"),
    )
    return jax.shard_map(shards, mesh=mesh, in_specs=in_specs, out_specs=out_specs, check_vma=False)
```

```python
import functools
import jax
import jax.numpy as jnp
from jax import lax
from jax.experimental import pallas as pl
from jax.experimental.pallas import tpu as pltpu
from jax.sharding import PartitionSpec as P

HEAD = 64
STATE = 128
STRETCH = 256
LANES = 128
EPSILON = 1e-05
PLACES = 3
F32 = jnp.float32
BF16 = jnp.bfloat16
NN = (((1,), (0,)), ((), ()))
NT = (((1,), (1,)), ((), ()))
TN = (((0,), (0,)), ((), ()))


def mm(a, b, dims=NN):
    return lax.dot_general(a, b, dims, preferred_element_type=F32)


def exact(a, b):
    return lax.dot_general(a, b, NN, precision=lax.Precision.HIGHEST, preferred_element_type=F32)


def halves(v):
    high = v.astype(BF16)
    return high, (v - high.astype(F32)).astype(BF16)


def iota(shape, dim):
    return lax.broadcasted_iota(jnp.int32, shape, dim)


def spread_heads(v, chan):
    high, rest = halves(v)
    rows = iota((2 * LANES, chan), 0) & (LANES - 1)
    pick = jnp.where(rows == (iota((2 * LANES, chan), 1) >> 6), 1.0, 0.0).astype(BF16)
    return mm(jnp.concatenate([high, rest], axis=1), pick)


def gather_heads(v):
    chan = v.shape[1]
    high, rest = halves(v)
    pick = jnp.where((iota((chan, LANES), 0) >> 6) == iota((chan, LANES), 1), 1.0, 0.0).astype(BF16)
    return mm(high, pick) + mm(rest, pick)


def softplus(v):
    return jnp.maximum(v, 0.0) + jnp.log1p(jnp.exp(-jnp.abs(v)))


def sigmoid(v):
    return 1.0 / (1.0 + jnp.exp(-v))


def lower_mask():
    return iota((STRETCH, STRETCH), 0) >= iota((STRETCH, STRETCH), 1)


def convolve(xs_ref, taps_ref, bias_ref):
    total = bias_ref[...] + taps_ref[0:1, :] * xs_ref[5:5 + STRETCH, :]
    for tap in range(1, 4):
        total = total + taps_ref[tap:tap + 1, :] * xs_ref[5 + tap:5 + tap + STRETCH, :]
    return total


def decays(pre_dt, head_ref, valid):
    rates = softplus(pre_dt + head_ref[0:1, :]) * valid
    log_decay = rates * head_ref[1:2, :]
    lower = lower_mask().astype(F32)
    cumulative = exact(lower, log_decay)
    last = cumulative[STRETCH - 1:STRETCH, :]
    return rates, cumulative, jnp.exp(cumulative), jnp.exp(last - cumulative)


def weights_of(cumulative, across, head):
    return jnp.exp(jnp.minimum(cumulative[:, head:head + 1] - across[head:head + 1, :], 0.0))


def backward_kernel(
    open_ref, tok_ref, w_hbm, taps_ref, bias_ref, head_ref, skip_ref, gate_ref,
    pre_ref, halo_ref, y_ref, enter_ref, dgn_ref, stats_ref, rows_ref,
    dpre_ref, dnormed_ref, dtaps_ref, dbias_ref, dhead_ref, dchan_ref, dgain_ref, mixed_ref,
    dstate, xs, dus, rows, w_ref, o_got, fetch_sem, o_send, o_recv,
    *, inner, n_tp,
):
    chan = y_ref.shape[1]
    wide = chan + 2 * STATE
    step = pl.program_id(0)
    block = pl.num_programs(0) - 1 - step
    opening = open_ref[block] == 1
    keep = jnp.where(opening, 0.0, 1.0).astype(F32)
    tp = lax.axis_index("tp")
    per = rows.shape[0] // n_tp
    chunk = per // CHUNKS
    sums = LineSum(
        tp, n_tp, CHUNKS - EARLY, lambda index, part: chunk_of(rows, index, per, part + EARLY, chunk),
        lambda index, part: chunk_of(rows_ref, index, per, part + EARLY, chunk), o_got, o_send, o_recv,
    )

    fetches = (
        pltpu.make_async_copy(rows_ref, rows, fetch_sem.at[0]), pltpu.make_async_copy(w_hbm, w_ref, fetch_sem.at[1])
    )

    def turn(place):
        at = step * PLACES + place - 2

        @pl.when(jnp.logical_and(at >= 0, at < sums.turns))
        def _():
            sums.advance(at)

    @pl.when(step == 0)
    def _():
        for fetch in fetches:
            fetch.start()
        line_greeting(tp, n_tp)
        sums.kick()

    @pl.when(step == 0)
    def _():
        dstate[...] = jnp.zeros_like(dstate)
        dus[...] = jnp.zeros_like(dus)
        dtaps_ref[...] = jnp.zeros_like(dtaps_ref)
        dbias_ref[...] = jnp.zeros_like(dbias_ref)
        dhead_ref[...] = jnp.zeros_like(dhead_ref)
        dchan_ref[...] = jnp.zeros_like(dchan_ref)
        dgain_ref[...] = jnp.zeros_like(dgain_ref)

    grstd, cross, valid = row_stats(stats_ref, inner)
    xs[0:8, :] = halo_ref[:, chan:2 * chan + 2 * STATE] * keep
    xs[8:8 + STRETCH, :] = pre_ref[:, chan:2 * chan + 2 * STATE]
    conv = convolve(xs, taps_ref, bias_ref)
    gate_u = sigmoid(conv)
    feats = conv * gate_u
    slope = gate_u * (1.0 + conv * (1.0 - gate_u))
    x = feats[:, :chan]
    bs = feats[:, chan:chan + STATE].astype(BF16)
    cs = feats[:, chan + STATE:].astype(BF16)
    pre_dt = pre_ref[:, 2 * chan + 2 * STATE:]
    rates, cumulative, grown, to_end = decays(pre_dt, head_ref, valid)
    across = cumulative.T
    grown_e = spread_heads(grown, chan)
    rates_e = spread_heads(rates, chan)
    to_end_e = spread_heads(to_end, chan)
    leave_e = grown_e[STRETCH - 1:STRETCH, :]

    pre_z = pre_ref[:, :chan]
    gate_z = sigmoid(pre_z)
    silu_z = pre_z * gate_z * valid
    y = y_ref[...]
    mixed = y + skip_ref[...] * x
    gated = mixed * silu_z
    dgn = dgn_ref[...]
    d_gated = grstd * (gate_ref[...] * dgn) - gated * (grstd * grstd * grstd * cross * (1.0 / inner))
    d_mixed = d_gated * silu_z
    dpre_ref[:, :chan] = (
        d_gated * mixed * (valid * (gate_z * (1.0 + pre_z * (1.0 - gate_z))))
    ).astype(BF16)
    dchan_ref[0:1, :] += jnp.sum(dgn * gated * grstd, axis=0, keepdims=True)
    dchan_ref[1:2, :] += jnp.sum(d_mixed * x, axis=0, keepdims=True)

    turn(0)
    dy_b = d_mixed.astype(BF16)
    dy = dy_b.astype(F32)
    scaled = x * rates_e
    scaled_b = scaled.astype(BF16)
    entering = enter_ref[0]
    d_leaving = dstate[...]
    d_leaving_b = d_leaving.astype(BF16)
    tail = mm(bs, d_leaving_b) * to_end_e
    overlap = jnp.where(lower_mask(), mm(cs, bs, NT), 0.0)
    first = iota((STRETCH, LANES), 1) < HEAD
    d_overlap = jnp.zeros((STRETCH, STRETCH), F32)
    parts = []
    for pair in range(chan // LANES):
        cols = slice(pair * LANES, (pair + 1) * LANES)
        dy_pair = dy_b[:, cols]
        x_pair = scaled_b[:, cols]
        zero = jnp.zeros_like(dy_pair)
        sides = [jnp.where(first, dy_pair, zero), jnp.where(first, zero, dy_pair)]
        mats = []
        for side in range(2):
            weight = weights_of(cumulative, across, 2 * pair + side)
            mats.append((weight * overlap).astype(BF16))
            d_overlap = d_overlap + mm(sides[side], x_pair, NT) * weight
        parts.append(mm(jnp.concatenate(mats, axis=0), jnp.concatenate(sides, axis=0), TN))
    turn(1)
    d_scaled = jnp.concatenate(parts, axis=1) + tail
    scaled_r = scaled_b.astype(F32)
    d_cum = gather_heads(dy * y - scaled_r * d_scaled)
    d_last = jnp.sum(scaled_r * tail, axis=0, keepdims=True) + leave_e * jnp.sum(
        d_leaving * entering, axis=0, keepdims=True
    )
    d_last = gather_heads(jnp.broadcast_to(d_last, (8, chan)))[0:1, :]
    upper = (iota((STRETCH, STRETCH), 0) <= iota((STRETCH, STRETCH), 1)).astype(F32)
    d_log = exact(upper, d_cum) + d_last
    decay = head_ref[1:2, :]
    d_rates = d_log * decay + gather_heads(x * d_scaled)
    d_dt = d_rates * valid * sigmoid(pre_dt + head_ref[0:1, :])
    dhead_ref[0:1, :] += jnp.sum(d_log * rates, axis=0, keepdims=True) * decay
    dhead_ref[1:2, :] += jnp.sum(d_dt, axis=0, keepdims=True)
    dpre_ref[:, 2 * chan + 2 * STATE:] = d_dt.astype(BF16)

    d_x = d_scaled * rates_e + skip_ref[...] * d_mixed
    d_overlap_b = jnp.where(lower_mask(), d_overlap, 0.0).astype(BF16)
    dy_grown = (dy * grown_e).astype(BF16)
    x_end = (scaled * to_end_e).astype(BF16)
    d_b = mm(d_overlap_b, cs, TN) + mm(x_end, d_leaving_b, NT)
    d_c = mm(d_overlap_b, bs) + mm(dy_grown, entering.astype(BF16), NT)
    dstate[...] = (d_leaving * leave_e + mm(cs, dy_grown, TN)) * keep

    dus[0:STRETCH, :chan] = d_x * slope[:, :chan]
    dus[0:STRETCH, chan:chan + STATE] = d_b * slope[:, chan:chan + STATE]
    dus[0:STRETCH, chan + STATE:] = d_c * slope[:, chan + STATE:]
    d_conv = dus[0:STRETCH, :]
    dbias_ref[...] += jnp.sum(d_conv, axis=0, keepdims=True)
    d_pre = jnp.zeros((STRETCH, wide), F32)
    for tap in range(4):
        dtaps_ref[tap:tap + 1, :] += jnp.sum(d_conv * xs[5 + tap:5 + tap + STRETCH, :], axis=0, keepdims=True)
        d_pre = d_pre + taps_ref[tap:tap + 1, :] * dus[3 - tap:3 - tap + STRETCH, :]
    dpre_ref[:, chan:2 * chan + 2 * STATE] = d_pre.astype(BF16)
    dus[STRETCH:STRETCH + 8, :] = d_conv[0:8, :] * keep

    @pl.when(step == 0)
    def _():
        for fetch in fetches:
            fetch.wait()

    turn(2)
    d_normed = mm(dpre_ref[...], w_ref[...], NT)
    dnormed_ref[...] = d_normed.astype(BF16)
    resid = tok_ref[...].astype(F32)
    rstd = lax.rsqrt(jnp.mean(resid * resid, axis=1, keepdims=True) + EPSILON)
    dgain_ref[...] += jnp.sum(d_normed * (resid * rstd), axis=0, keepdims=True)

    @pl.when(step == pl.num_programs(0) - 1)
    def _():
        pl.loop(jnp.minimum(step * PLACES + 1, sums.turns), sums.turns)(sums.advance)
        sums.settle(lambda part: mixed_ref.at[pl.ds(part * chunk, chunk)])
        sums.drain()


def whole(shape):
    return pl.BlockSpec(shape, lambda *_: (0,) * len(shape), pipeline_mode=pl.Buffered(1))


def mixer_backward(
    openings, tok, w_in, taps, bias, heads, skip, gate, pre, y, enter, dgn, stats, out_rows, inner, n_tp
):
    tokens, width = tok.shape
    cols = w_in.shape[1]
    chan = skip.shape[1]
    blocks = tokens // STRETCH
    wide = chan + 2 * STATE
    per = STRETCH // 8
    steps = (n_tp - 1) * (CHUNKS - EARLY)
    kept = tokens // n_tp // CHUNKS * (CHUNKS - EARLY)
    rows = lambda n: pl.BlockSpec((STRETCH, n), lambda i, *_: (blocks - 1 - i, 0))
    return pl.pallas_call(
        functools.partial(backward_kernel, inner=inner, n_tp=n_tp),
        name="mixer_backward",
        grid_spec=pltpu.PrefetchScalarGridSpec(
            num_scalar_prefetch=1,
            grid=(blocks,),
            in_specs=[
                rows(width), pl.BlockSpec(memory_space=pl.ANY), whole((4, wide)), whole((1, wide)),
                whole((8, LANES)), whole((1, chan)), whole((1, chan)),
                rows(cols),
                pl.BlockSpec((8, cols), lambda i, *_: (jnp.maximum((blocks - 1 - i) * per - 1, 0), 0)),
                rows(chan),
                pl.BlockSpec((1, STATE, chan), lambda i, *_: (blocks - 1 - i, 0, 0)),
                rows(chan),
                pl.BlockSpec((8, STRETCH), lambda i, *_: (0, blocks - 1 - i)),
                pl.BlockSpec(memory_space=pl.ANY),
            ],
            out_specs=[
                rows(cols), rows(width),
                pl.BlockSpec((8, wide), lambda i, *_: (0, 0)),
                pl.BlockSpec((1, wide), lambda i, *_: (0, 0)),
                pl.BlockSpec((8, LANES), lambda i, *_: (0, 0)),
                pl.BlockSpec((8, chan), lambda i, *_: (0, 0)),
                pl.BlockSpec((1, width), lambda i, *_: (0, 0)),
                pl.BlockSpec((kept, width), lambda i, *_: (0, 0)),
            ],
            scratch_shapes=[
                pltpu.VMEM((STATE, chan), F32),
                pltpu.VMEM((STRETCH + 8, wide), F32),
                pltpu.VMEM((STRETCH + 8, wide), F32),
                pltpu.VMEM((tokens, width), BF16),
                pltpu.VMEM((width, cols), BF16),
                pltpu.VMEM((2, steps, tokens // n_tp // CHUNKS, width), BF16),
                pltpu.SemaphoreType.DMA((2,)),
                pltpu.SemaphoreType.DMA((2, steps)),
                pltpu.SemaphoreType.DMA((2, steps)),
            ],
        ),
        out_shape=[
            jax.ShapeDtypeStruct((tokens, cols), BF16),
            jax.ShapeDtypeStruct((tokens, width), BF16),
            jax.ShapeDtypeStruct((8, wide), F32),
            jax.ShapeDtypeStruct((1, wide), F32),
            jax.ShapeDtypeStruct((8, LANES), F32),
            jax.ShapeDtypeStruct((8, chan), F32),
            jax.ShapeDtypeStruct((1, width), F32),
            jax.ShapeDtypeStruct((kept, width), BF16),
        ],
        cost_estimate=pl.CostEstimate(
            flops=4 * tokens * width * cols, bytes_accessed=tokens * cols * 12, transcendentals=tokens * chan
        ),
        compiler_params=pltpu.CompilerParams(
            collective_id=TAGS["backward"], has_side_effects=True, vmem_limit_bytes=60 << 20,
            dimension_semantics=("arbitrary",),
        ),
    )(openings, tok, w_in, taps, bias, heads, skip, gate, pre, pre, y, enter, dgn, stats, out_rows)


MESH = pl.DeviceIdType.MESH
CHUNKS = 4
EARLY = 1
TAGS = {"ahead": 1, "backward": 2, "exit": 3}


def remote(source, target, send, recv, **where):
    return pltpu.make_async_remote_copy(
        src_ref=source, dst_ref=target, send_sem=send, recv_sem=recv, device_id=where, device_id_type=MESH
    )


def rows_at(ref, index, count):
    return ref.at[pl.ds(pl.multiple_of(index * count, count), count)]


def greet(axis, peers):
    barrier = pltpu.get_barrier_semaphore()
    for peer in peers:
        pl.semaphore_signal(barrier, inc=1, device_id={axis: peer}, device_id_type=MESH)


class Line:
    def __init__(self, tp, n_tp, own, whole_ref, send, recv, split=1):
        self.tp, self.n, self.own, self.whole_ref, self.send, self.recv = tp, n_tp, own, whole_ref, send, recv
        self.count = own.shape[0]
        self.split, self.part = split, own.shape[0] // split

    def piece(self, index, step):
        return self.whole_ref.at[
            pl.ds(pl.multiple_of(index * self.count + step % self.split * self.part, self.part), self.part)
        ]

    def copy(self, way, step, own=False):
        shift = -1 if way == 0 else 1
        slot = self.piece(self.tp + shift * (step // self.split), step)
        source = self.own.at[pl.ds(step % self.split * self.part, self.part)] if own else slot
        return remote(source, slot, self.send.at[way, step], self.recv.at[way, step], tp=self.tp - shift)

    def sends(self, way, step):
        step = step // self.split
        if way == 0:
            return jnp.logical_and(self.tp < self.n - 1, self.tp >= step)
        return jnp.logical_and(self.tp > 0, self.tp + step <= self.n - 1)

    def takes(self, way, step):
        step = step // self.split
        return self.tp >= step + 1 if way == 0 else self.tp + step + 1 <= self.n - 1

    def start(self, way, step):
        @pl.when(self.sends(way, step))
        def _():
            self.copy(way, step, own=step < self.split).start()

    def arrive(self, way, step):
        @pl.when(self.takes(way, step))
        def _():
            shift = -1 if way == 0 else 1
            slot = self.piece(self.tp + shift * (step // self.split + 1), step)
            remote(
                slot, slot, self.send.at[way, step], self.recv.at[way, step], tp=self.tp + shift
            ).wait_recv()

    def finish(self, way, step):
        @pl.when(self.sends(way, step))
        def _():
            self.copy(way, step, own=step < self.split).wait_send()


class LineSum:
    def __init__(self, tp, n_tp, per, local, origin, got, send, recv):
        self.tp, self.n, self.per, self.local_of, self.origin = tp, n_tp, per, local, origin
        self.got, self.send, self.recv = got, send, recv
        self.steps = (n_tp - 1) * per
        self.paced = max(n_tp - 2, 0) * per
        self.turns = self.paced + max(n_tp - 3, 0)

    def ahead(self, way, step):
        return self.n - 1 - step // self.per if way == 0 else step // self.per

    def passes(self, way, step):
        return self.ahead(way, step) > self.tp if way == 0 else self.ahead(way, step) < self.tp

    def first(self, way):
        return self.tp == 0 if way == 0 else self.tp == self.n - 1

    def local(self, way, step):
        return self.local_of(self.ahead(way, step), step % self.per)

    def copy(self, way, step, direct):
        source = (self.origin if direct else self.local_of)(self.ahead(way, step), step % self.per)
        return remote(
            source, self.got.at[way, step], self.send.at[way, step], self.recv.at[way, step],
            tp=self.tp + 1 if way == 0 else self.tp - 1,
        )

    def kick(self):
        for way in range(2):
            @pl.when(self.first(way))
            def _():
                for step in range(min(2, self.steps) if self.paced else self.steps):
                    self.copy(way, step, True).start()

    def advance(self, turn):
        for way in range(2):
            lag = jnp.maximum(self.tp - 1 if way == 0 else self.n - 2 - self.tp, 0)
            step = turn - lag
            live = jnp.logical_and(step >= 0, step < self.paced)

            @pl.when(jnp.logical_and(self.first(way), live))
            def _():
                self.copy(way, step, True).wait_send()

                @pl.when(step + 2 < self.steps)
                def _():
                    self.copy(way, step + 2, True).start()

                @pl.when(step == self.paced - 1)
                def _():
                    for rest in range(self.paced + 2, self.steps):
                        self.copy(way, rest, True).start()

            @pl.when(jnp.logical_and(jnp.logical_and(self.passes(way, step), live), jnp.logical_not(self.first(way))))
            def _():
                copy = self.copy(way, step, False)
                copy.wait_recv()
                add_into(self.local(way, step), self.local(way, step), self.got.at[way, step])
                copy.start()

    def settle(self, target):
        for way in range(2):
            for step in range(self.steps):
                @pl.when(jnp.logical_and(self.ahead(way, step) == self.tp, jnp.logical_not(self.first(way))))
                def _():
                    self.copy(way, step, False).wait_recv()

        for value in range(self.n):
            @pl.when(self.tp == value)
            def _():
                for part in range(self.per):
                    incoming = []
                    if value > 0:
                        incoming.append(self.got.at[0, (self.n - 1 - value) * self.per + part])
                    if value < self.n - 1:
                        incoming.append(self.got.at[1, value * self.per + part])
                    add_into(target(part), self.local_of(value, part), *incoming)

    def drain(self):
        for way in range(2):
            @pl.when(self.first(way))
            def _():
                for step in range(self.paced, self.steps):
                    self.copy(way, step, True).wait_send()

            for step in range(self.steps):
                @pl.when(jnp.logical_and(self.passes(way, step), jnp.logical_not(self.first(way))))
                def _():
                    self.copy(way, step, False).wait_send()


def chunk_of(ref, block, rows, part, chunk):
    return ref.at[pl.ds(pl.multiple_of(block * rows + part * chunk, chunk), chunk)]


def line_greeting(tp, n_tp):
    barrier = pltpu.get_barrier_semaphore()
    for near, there in ((tp - 1, tp > 0), (tp + 1, tp < n_tp - 1)):
        @pl.when(there)
        def _():
            pl.semaphore_signal(barrier, inc=1, device_id={"tp": near}, device_id_type=MESH)
    pl.semaphore_wait(barrier, jnp.where(tp > 0, 1, 0) + jnp.where(tp < n_tp - 1, 1, 0))


def forward_block(keep, tok, valid, gain_ref, w_ref, taps_ref, bias_ref, head_ref, skip_ref,
                  normed_ref, pre_ref, y_ref, gated_ref, enter_ref, state, xs):
    chan = y_ref.shape[1]
    xs[0:8, :] = xs[STRETCH:STRETCH + 8, :] * keep
    resid = tok.astype(F32)
    rstd = lax.rsqrt(jnp.mean(resid * resid, axis=1, keepdims=True) + EPSILON)
    normed = (resid * rstd * gain_ref[...]).astype(BF16)
    normed_ref[...] = normed
    pre_ref[...] = mm(normed, w_ref[...])
    xs[8:8 + STRETCH, :] = pre_ref[:, chan:2 * chan + 2 * STATE]
    conv = convolve(xs, taps_ref, bias_ref)
    feats = conv * sigmoid(conv)
    x = feats[:, :chan]
    bs = feats[:, chan:chan + STATE].astype(BF16)
    cs = feats[:, chan + STATE:].astype(BF16)
    rates, cumulative, grown, to_end = decays(pre_ref[:, 2 * chan + 2 * STATE:], head_ref, valid)
    across = cumulative.T
    grown_e = spread_heads(grown, chan)
    scaled = x * spread_heads(rates, chan)
    entering = state[...] * keep
    enter_ref[...] = entering
    y_ref[...] = mm(cs, entering.astype(BF16)) * grown_e
    state[...] = entering * grown_e[STRETCH - 1:STRETCH, :] + mm(
        bs, (scaled * spread_heads(to_end, chan)).astype(BF16), TN
    )
    overlap = jnp.where(lower_mask(), mm(cs, bs, NT), 0.0)
    scaled_b = scaled.astype(BF16)
    first = iota((STRETCH, LANES), 1) < HEAD
    for pair in range(chan // LANES):
        cols = slice(pair * LANES, (pair + 1) * LANES)
        both = scaled_b[:, cols]
        mats = [
            (weights_of(cumulative, across, 2 * pair + side) * overlap).astype(BF16) for side in range(2)
        ]
        zero = jnp.zeros_like(both)
        y_ref[:, cols] += mm(
            jnp.concatenate(mats, axis=1),
            jnp.concatenate([jnp.where(first, both, zero), jnp.where(first, zero, both)], axis=0),
        )
    pre_z = pre_ref[:, :chan]
    gated = (y_ref[...] + skip_ref[...] * x) * (pre_z * sigmoid(pre_z)) * valid
    gated_ref[...] = gated
    return jnp.sum(gated * gated, axis=1, keepdims=True)


def as_row(column):
    lane = iota((STRETCH, LANES), 1)
    return jnp.where(lane == 0, column, 0.0).T[0:8, :]


def as_column(row):
    return jnp.concatenate([row, jnp.zeros((LANES - 8, STRETCH), F32)], axis=0).T


def row_stats(stats_ref, inner):
    filled = as_column(stats_ref[...])
    return lax.rsqrt(filled[:, 0:1] * (1.0 / inner) + EPSILON), filled[:, 1:2], filled[:, 2:3]


def ahead_kernel(
    open_ref, step_bias, log_rate, direct, tok_ref, cot_ref, pz_ref, px_ref, pbc_ref, pdt_ref, pout_ref, mask_ref,
    norm_gain, conv_chan, bias_chan, conv_shared, bias_shared, gate_gain,
    tok_out, cot_out, win_out, normed_out, pre_out, y_out, enter_out, dgn_out, gn_out, rows_out, mixed_out, stats_ref,
    taps_ref, bias_ref, head_ref, skip_ref, gate_ref,
    pin_ref, gain_ref, tok_all, cot_all, w_in, w_out, normed, pre, y, gated, enter, dgn, gnormed, rows, state, xs, squares, crosses,
    squares_got, crosses_got, o_got,
    own_sem, z_send, z_recv, c_send, c_recv, f_send, f_recv, p_send, p_recv, q_send, q_recv, r_send, r_recv,
    all_sem, out_sem, o_send, o_recv,
    *, n_tp, n_fs, inner,
):
    tp, me = lax.axis_index("tp"), lax.axis_index("fsdp")
    chip, core, chips = me // 2, me % 2, n_fs // 2
    partner = chip * 2 + 1 - core
    blocks = tok_all.shape[0] // STRETCH
    per = tok_ref.shape[0]
    chan = pout_ref.shape[1]
    pin_ref[:, :chan] = pz_ref[...]
    pin_ref[:, chan:2 * chan] = px_ref[...]
    pin_ref[:, 2 * chan:2 * chan + 2 * STATE] = pbc_ref[...]
    heads_here, rows_dt = pdt_ref.shape
    pin_ref[:, 2 * chan + 2 * STATE:] = jnp.concatenate(
        [pdt_ref[...].astype(F32), jnp.zeros((LANES - heads_here, rows_dt), F32)], axis=0
    ).T.astype(BF16)
    greet("fsdp", [((chip + d) % chips) * 2 + core for d in range(1, chips)] + [partner])
    greet("tp", [(tp + d) % n_tp for d in range(1, n_tp)])
    pl.semaphore_wait(pltpu.get_barrier_semaphore(), chips + n_tp - 1)

    packs = ((pin_ref, w_in), (pout_ref, w_out))
    count = pin_ref.shape[0]
    line = Line(tp, n_tp, tok_ref, tok_all, z_send, z_recv, split=2)
    late = Line(tp, n_tp, cot_ref, cot_all, c_send, c_recv)
    for way in range(2):
        line.start(way, 0)
    for j, (pack, full) in enumerate(packs):
        for d in range(1, chips):
            remote(
                pack, rows_at(full, me, count), f_send.at[j, d], f_recv.at[j, d], fsdp=((chip + d) % chips) * 2 + core
            ).start()
        remote(pack, rows_at(full, me, count), p_send.at[j, 0], p_recv.at[j, 0], fsdp=partner).start()
    own = [
        pltpu.make_async_copy(tok_ref, rows_at(tok_all, tp, per), own_sem.at[0]),
        pltpu.make_async_copy(pin_ref, rows_at(w_in, me, count), own_sem.at[1]),
        pltpu.make_async_copy(pout_ref, rows_at(w_out, me, count), own_sem.at[2]),
        pltpu.make_async_copy(cot_ref, rows_at(cot_all, tp, per), own_sem.at[3]),
    ]
    for copy in own:
        copy.start()
    state[...] = jnp.zeros_like(state)
    xs[...] = jnp.zeros_like(xs)
    lane = iota((8, LANES), 1)
    place = iota((8, LANES), 0)
    step_row, rate_row, skip_row = (
        sum(jnp.where(lane == head, source[head], 0.0) for head in range(heads_here))
        for source in (step_bias, log_rate, direct)
    )
    live = lane < heads_here
    head_ref[...] = jnp.where(
        place == 0, jnp.where(live, step_row, -100.0), jnp.where(live & (place == 1), -jnp.exp(rate_row), 0.0)
    )
    skip_ref[...] = spread_heads(skip_row, chan)[0:1, :]
    gain_ref[...] = norm_gain[...].reshape(gain_ref.shape)
    gate_ref[...] = gate_gain[...].reshape(gate_ref.shape)
    taps_ref[:, :chan] = conv_chan[...]
    taps_ref[:, chan:] = conv_shared[...]
    bias_ref[:, :chan] = bias_chan[...].reshape(1, chan)
    bias_ref[:, chan:] = bias_shared[...].reshape(1, 2 * STATE)
    last = 2 * (n_tp - 1)
    for step in range(1, last):
        for way in range(2):
            if step >= 2:
                line.arrive(way, step - 2)
            line.finish(way, step - 1)
            line.start(way, step)
    for j, (pack, full) in enumerate(packs):
        for d in range(1, chips):
            slot = rows_at(full, ((chip + chips - d) % chips) * 2 + core, count)
            remote(slot, slot, f_send.at[j, d], f_recv.at[j, d], fsdp=partner).wait_recv()
            remote(slot, slot, p_send.at[j, d], p_recv.at[j, d], fsdp=partner).start()
    for way in range(2):
        line.finish(way, last - 1)
        late.start(way, 0)
    for way in range(2):
        line.arrive(way, last - 2)
        line.arrive(way, last - 1)
    for j, (pack, full) in enumerate(packs):
        for d in range(chips):
            slot = rows_at(full, ((chip + chips - d) % chips) * 2 + 1 - core, count)
            remote(slot, slot, p_send.at[j, d], p_recv.at[j, d], fsdp=partner).wait()
        for d in range(1, chips):
            remote(pack, rows_at(full, me, count), f_send.at[j, d], f_recv.at[j, d], fsdp=partner).wait_send()
    for copy in own:
        copy.wait()
    wholes = [
        pltpu.make_async_copy(tok_all, tok_out, all_sem.at[0]), pltpu.make_async_copy(w_in, win_out, all_sem.at[1]),
    ]
    for copy in wholes:
        copy.start()

    def span(block):
        return pl.ds(pl.multiple_of(block * STRETCH, STRETCH), STRETCH)

    def out(k, block):
        at = span(block)
        chunk = per // CHUNKS * EARLY
        kept = pl.ds(pl.multiple_of(block * STRETCH + chunk, chunk), STRETCH - chunk)
        pairs = (
            (normed.at[at], normed_out.at[at]), (pre.at[block % 2], pre_out.at[at]), (y.at[at], y_out.at[at]),
            (enter.at[block], enter_out.at[block]), (gnormed.at[at], gn_out.at[at]),
            (rows.at[kept], rows_out.at[kept]), (dgn.at[at], dgn_out.at[at]), (cot_all.at[at], cot_out.at[at]),
        )
        return pltpu.make_async_copy(*pairs[k], out_sem.at[k, block])

    @pl.loop(0, blocks)
    def _(block):
        at = span(block)
        keep = jnp.where(open_ref[block] == 1, 0.0, 1.0).astype(F32)

        @pl.when(block >= 2)
        def _():
            out(1, block - 2).wait()

        valid = mask_ref[at].reshape(1, STRETCH).astype(F32)
        squares[:, at] = jnp.where(iota((8, STRETCH), 0) == 2, valid, 0.0)
        total = forward_block(
            keep, tok_all[at, :], as_column(squares[:, at])[:, 2:3], gain_ref, w_in, taps_ref, bias_ref, head_ref, skip_ref,
            normed.at[at], pre.at[block % 2], y.at[at], gated.at[at], enter.at[block], state, xs,
        )
        squares[0:1, at] = as_row(total)[0:1, :]
        for k in range(4):
            out(k, block).start()

        @pl.when(block == max(blocks - 2, 0))
        def _():
            for way in range(2):
                late.arrive(way, 0)
                if n_tp > 2:
                    late.start(way, 1)

    def swap(part, got, send, recv):
        for d in range(1, n_tp):
            remote(part, got.at[tp], send.at[d], recv.at[d], tp=(tp + d) % n_tp).start()
        got[tp] = part[...]
        for d in range(1, n_tp):
            slot = got.at[(tp + n_tp - d) % n_tp]
            remote(slot, slot, send.at[d], recv.at[d], tp=(tp + d) % n_tp).wait_recv()
        total = got[0]
        for peer in range(1, n_tp):
            total = total + got[peer]
        return total

    stats_ref[...] = swap(squares, squares_got, q_send, q_recv)

    @pl.loop(0, blocks)
    def _(block):
        at = span(block)

        grstd, _, _ = row_stats(stats_ref.at[:, at], inner)
        value = (gated[at, :] * grstd * gate_ref[...]).astype(BF16)
        gnormed[at, :] = value
        rows[at, :] = mm(value, w_out[...], NT).astype(BF16)
        out(4, block).start()
        out(5, block).start()

    chunk = per // CHUNKS
    piece = lambda index, part: chunk_of(rows, index, per, part, chunk)
    sums = LineSum(tp, n_tp, EARLY, piece, piece, o_got, o_send, o_recv)
    sums.kick()

    def gradient(block):
        at = span(block)
        value = mm(cot_all[at, :], w_out[...])
        dgn[at, :] = value
        crosses[:, at] = as_row(jnp.sum(gate_ref[...] * value * gated[at, :], axis=1, keepdims=True))
        out(6, block).start()
        out(7, block).start()

    ratio = per // STRETCH

    def gradients(index):
        for k in range(ratio):
            gradient(index * ratio + k)

    gradients(tp)
    middle = min(sums.turns, 3)
    for step in range(n_tp - 1):
        for way in range(2):
            if step > 0:
                late.arrive(way, step)
                if step + 1 < n_tp - 1:
                    late.start(way, step + 1)
        for way in range(2):
            @pl.when(late.takes(way, step))
            def _():
                gradients(tp - step - 1 if way == 0 else tp + step + 1)
        if step == max(n_tp - 3, 0):
            pl.loop(0, middle)(sums.advance)

    total = swap(crosses, crosses_got, r_send, r_recv)
    if middle < sums.turns:
        pl.loop(middle, sums.turns)(sums.advance)
    sums.settle(lambda part: mixed_out.at[pl.ds(part * chunk, chunk)])

    stats_ref[1:2, :] = total[0:1, :]
    stats_ref[2:3, :] = squares[2:3, :]

    for copy in wholes:
        copy.wait()

    @pl.loop(0, blocks)
    def _(block):
        for k in (0, 2, 3, 4, 5, 6, 7):
            out(k, block).wait()

    for block in range(max(blocks - 2, 0), blocks):
        out(1, block).wait()
    for step in range(n_tp - 1):
        for way in range(2):
            late.finish(way, step)
    sums.drain()
    for d in range(1, n_tp):
        remote(squares, squares_got.at[tp], q_send.at[d], q_recv.at[d], tp=(tp + d) % n_tp).wait_send()
        remote(crosses, crosses_got.at[tp], r_send.at[d], r_recv.at[d], tp=(tp + d) % n_tp).wait_send()


def ahead(
    openings, heads, tokens, cotangent, projections, mask, vectors, n_tp, n_fs
):
    per, width = tokens.shape
    total = per * n_tp
    count, chan = projections[0].shape
    wide = chan + 2 * STATE
    cols = chan + wide + LANES
    blocks = total // STRETCH
    chips = n_fs // 2
    dma = pltpu.SemaphoreType.DMA
    anywhere = pl.BlockSpec(memory_space=pl.ANY)
    vmem = pl.BlockSpec(memory_space=pltpu.VMEM)
    shape = jax.ShapeDtypeStruct
    return pl.pallas_call(
        functools.partial(ahead_kernel, n_tp=n_tp, n_fs=n_fs, inner=chan * n_tp),
        name="ahead",
        in_specs=[pl.BlockSpec(memory_space=pltpu.SMEM)] * 4 + [vmem] * 14,
        out_specs=[anywhere] * 10 + [vmem] * 7,
        out_shape=[
            shape((total, width), BF16), shape((total, width), BF16), shape((count * n_fs, cols), BF16),
            shape((total, width), BF16), shape((total, cols), F32), shape((total, chan), F32),
            shape((blocks, STATE, chan), F32), shape((total, chan), F32), shape((total, chan), BF16),
            shape((total, width), BF16), shape((per // CHUNKS * EARLY, width), BF16), shape((8, total), F32),
            shape((4, wide), F32), shape((1, wide), F32),
            shape((8, LANES), F32), shape((1, chan), F32), shape((1, chan), F32),
        ],
        scratch_shapes=[
            pltpu.VMEM((count, cols), BF16), pltpu.VMEM((1, width), F32),
            pltpu.VMEM((total, width), BF16), pltpu.VMEM((total, width), BF16),
            pltpu.VMEM((count * n_fs, cols), BF16), pltpu.VMEM((count * n_fs, chan), BF16),
            pltpu.VMEM((total, width), BF16), pltpu.VMEM((2, STRETCH, cols), F32), pltpu.VMEM((total, chan), F32),
            pltpu.VMEM((total, chan), F32), pltpu.VMEM((blocks, STATE, chan), F32), pltpu.VMEM((total, chan), F32),
            pltpu.VMEM((total, chan), BF16), pltpu.VMEM((total, width), BF16),
            pltpu.VMEM((STATE, chan), F32), pltpu.VMEM((STRETCH + 8, wide), F32),
            pltpu.VMEM((8, total), F32), pltpu.VMEM((8, total), F32),
            pltpu.VMEM((n_tp, 8, total), F32), pltpu.VMEM((n_tp, 8, total), F32),
            pltpu.VMEM((2, (n_tp - 1) * EARLY, per // CHUNKS, width), BF16),
            dma((4,)), dma((2, 2 * (n_tp - 1))), dma((2, 2 * (n_tp - 1))), dma((2, n_tp - 1)), dma((2, n_tp - 1)),
            dma((2, chips)), dma((2, chips)), dma((2, chips)), dma((2, chips)),
            dma((n_tp,)), dma((n_tp,)), dma((n_tp,)), dma((n_tp,)), dma((2,)), dma((8, blocks)),
            dma((2, (n_tp - 1) * EARLY)), dma((2, (n_tp - 1) * EARLY)),
        ],
        compiler_params=pltpu.CompilerParams(
            collective_id=TAGS["ahead"], has_side_effects=True, vmem_limit_bytes=63 << 20
        ),
    )(openings, *heads, tokens, cotangent, *projections, mask, *vectors)


def add_into(target, *sources):
    rows, tile = target.shape[0], 32

    @pl.loop(0, rows // tile)
    def _(i):
        at = pl.ds(pl.multiple_of(i * tile, tile), tile)
        total = sources[0][at, :].astype(F32)
        for source in sources[1:]:
            total = total + source[at, :].astype(F32)
        target[at, :] = total.astype(target.dtype)


def fill_rows(target, pieces):
    at = 0
    for source, row, start, length in pieces:
        for k in range(length // LANES):
            target[at:at + 1, :] = source[row:row + 1, start + k * LANES:start + (k + 1) * LANES]
            at += 1
    if at < target.shape[0]:
        target[at:, :] = jnp.zeros((target.shape[0] - at, LANES), F32)


def finish_kernel(
    *refs,
):
    sources, refs = refs[:10], refs[10:]
    results, copies, sem = refs[:16], refs[16:26], refs[26]
    fetches = [pltpu.make_async_copy(source, copy, sem.at[k]) for k, (source, copy) in enumerate(zip(sources, copies))]
    for fetch in fetches:
        fetch.start()
    for fetch in fetches:
        fetch.wait()
    write_results(*copies, *results)


def write_results(
    tok_ref, cot_ref, early_ref, mixed_ref, gain_ref, dn_ref, own_ref, bc_ref, mine_ref, shared_ref,
    output, grad_tokens, g_gain, g_z, g_x, g_bc, g_dt, g_taps, g_bias, g_taps_s, g_bias_s, g_log, g_step, g_skip, g_gate,
    g_out,
):
    chan, heads_here = g_z.shape[1], g_log.shape[0]
    resid = tok_ref[...].astype(F32)
    early = early_ref.shape[0]
    output[0:early, :] = (resid[0:early, :] + early_ref[...].astype(F32)).astype(BF16)
    output[early:, :] = (resid[early:, :] + mixed_ref[...].astype(F32)).astype(BF16)
    rstd = lax.rsqrt(jnp.mean(resid * resid, axis=1, keepdims=True) + EPSILON)
    scaled = dn_ref[...].astype(F32) * gain_ref[...].reshape(1, resid.shape[1])
    grad_tokens[...] = (
        cot_ref[...].astype(F32) + rstd * scaled
        - resid * (rstd * rstd * rstd) * jnp.mean(scaled * resid, axis=1, keepdims=True)
    ).astype(BF16)
    g_z[...] = own_ref[:, :chan].astype(F32)
    g_x[...] = own_ref[:, chan:2 * chan].astype(F32)
    g_dt[...] = own_ref[:, 2 * chan:2 * chan + LANES].astype(F32).T[0:heads_here, :]
    g_out[...] = own_ref[:, 2 * chan + LANES:].astype(F32)
    g_bc[...] = bc_ref[...].astype(F32)

    def row(source, at, length):
        return jnp.concatenate([source[at + k:at + k + 1, :] for k in range(length // LANES)], axis=1)

    per = chan // LANES
    for tap in range(4):
        g_taps[tap:tap + 1, :] = row(mine_ref, tap * per, chan)
        g_taps_s[tap:tap + 1, :] = row(shared_ref, tap * 2, 2 * STATE)
    g_bias[...] = row(mine_ref, 4 * per, chan).reshape(chan)
    g_gate[...] = row(mine_ref, 5 * per, chan).reshape(chan)
    skip = gather_heads(jnp.broadcast_to(row(mine_ref, 6 * per, chan), (8, chan)))
    g_skip[...] = skip[0:1, :heads_here].reshape(heads_here)
    g_log[...] = mine_ref[7 * per:7 * per + 1, :heads_here].reshape(heads_here)
    g_step[...] = mine_ref[7 * per + 1:7 * per + 2, :heads_here].reshape(heads_here)
    g_bias_s[...] = row(shared_ref, 8, 2 * STATE).reshape(2 * STATE)
    g_gain[...] = row(shared_ref, 10, g_gain.shape[0]).reshape(g_gain.shape[0])


def finish(tokens, cotangent, early, mixed, gain, dn, own, bc, mine, shared, heads_here):
    operands = (tokens, cotangent, early, mixed, gain, dn, own, bc, mine, shared)
    rows, width = tokens.shape
    count = own.shape[0]
    chan = (own.shape[1] - LANES) // 3
    vmem = pl.BlockSpec(memory_space=pltpu.VMEM)
    shape = lambda *extents: jax.ShapeDtypeStruct(extents, F32)
    outs = [
        jax.ShapeDtypeStruct((rows, width), BF16), jax.ShapeDtypeStruct((rows, width), BF16), shape(width),
        shape(count, chan), shape(count, chan), shape(count, 2 * STATE), shape(heads_here, count), shape(4, chan),
        shape(chan), shape(4, 2 * STATE), shape(2 * STATE), shape(heads_here), shape(heads_here), shape(heads_here),
        shape(chan), shape(count, chan),
    ]
    return pl.pallas_call(
        finish_kernel, name="finish", in_specs=[pl.BlockSpec(memory_space=pltpu.HBM)] * 10,
        out_specs=[vmem] * len(outs), out_shape=outs,
        scratch_shapes=[pltpu.VMEM(v.shape, v.dtype) for v in operands] + [pltpu.SemaphoreType.DMA((10,))],
        compiler_params=pltpu.CompilerParams(vmem_limit_bytes=63 << 20),
    )(*operands)


def exit_kernel(
    dn_ref, normed_ref, dpre_ref, cot_ref, gn_ref, dtaps_ref, dbias_ref, dhead_ref, dchan_ref, dgain_ref,
    dn_out, own_out, bc_out, mine_out, shared_out,
    dn, normed, dpre, cot, gn, fetch_sem,
    gin_ref, gout_ref, mine_ref, shared_ref,
    z_got, near_in, near_out, far_in, far_out, got_in, got_out, mine_got, shared_got, shared_held, shared_z,
    bc_held, bc_got,
    zs, zr, ns, nr, fs, fr, ms, mr, ss, sr, ts, tr, bs, br,
    *, n_tp, n_fs,
):
    tp, me = lax.axis_index("tp"), lax.axis_index("fsdp")
    chip, core, chips = me // 2, me % 2, n_fs // 2
    partner = chip * 2 + 1 - core
    chan = gout_ref.shape[1]
    cols = gin_ref.shape[1]
    width = gin_ref.shape[0]
    fetches = [
        pltpu.make_async_copy(source, target, fetch_sem.at[k])
        for k, (source, target) in enumerate(
            [(normed_ref, normed), (dpre_ref, dpre), (cot_ref, cot), (gn_ref, gn), (dn_ref, dn)]
        )
    ]
    for fetch in fetches:
        fetch.start()
    fill_rows(
        mine_ref, [(dtaps_ref, tap, 0, chan) for tap in range(4)] + [(dbias_ref, 0, 0, chan)]
        + [(dchan_ref, row, 0, chan) for row in range(2)] + [(dhead_ref, row, 0, LANES) for row in range(2)]
    )
    fill_rows(
        shared_ref, [(dtaps_ref, tap, chan, 2 * STATE) for tap in range(4)] + [(dbias_ref, 0, chan, 2 * STATE)]
        + [(dgain_ref, 0, 0, width)]
    )
    block, count = dn_out.shape[0], own_out.shape[0]
    greet("fsdp", [(me + d) % n_fs for d in range(1, n_fs)])
    greet("tp", [(tp + d) % n_tp for d in range(1, n_tp)])
    pl.semaphore_wait(pltpu.get_barrier_semaphore(), n_fs - 1 + n_tp - 1)

    chunk = block // CHUNKS
    sums = LineSum(
        tp, n_tp, CHUNKS, lambda index, part: chunk_of(dn, index, block, part, chunk),
        lambda index, part: chunk_of(dn_ref, index, block, part, chunk), z_got, zs, zr,
    )
    sums.kick()
    for k in (0, 1):
        fetches[k].wait()
    advance = sums.advance
    parts = (
        (gin_ref, slice(2 * chan, cols), near_in, far_in, got_in),
        (gout_ref, slice(0, chan), near_out, far_out, got_out),
        (gin_ref, slice(chan, 2 * chan), near_in, far_in, got_in),
        (gin_ref, slice(0, chan), near_in, far_in, got_in),
    )

    def near(j, d):
        source, span, held, _, _ = parts[j]
        rows = rows_at(source, ((chip + d) % chips) * 2 + 1 - core, count)
        return remote(rows.at[:, span], held.at[d, :, span], ns.at[j, d], nr.at[j, d], fsdp=partner)

    def far(j, d):
        _, span, _, held, got = parts[j]
        return remote(
            held.at[d, :, span], got.at[d, :, span], fs.at[j, d], fr.at[j, d], fsdp=((chip + d) % chips) * 2 + core
        )

    order = [d for d in range(1, chips)]

    def small(d):
        peer = (me + d) % n_fs
        return (
            remote(mine_ref, mine_got.at[me], ms.at[d], mr.at[d], fsdp=peer),
            remote(shared_ref, shared_got.at[me], ss.at[d], sr.at[d], fsdp=peer),
        )

    for d in range(1, n_fs):
        for copy in small(d):
            copy.start()
    mine_got[me] = mine_ref[...]
    shared_got[me] = shared_ref[...]

    def differentiate(j):
        _, span, *_ = parts[j]
        left, right, target = (cot, gn, gout_ref) if j == 1 else (normed, dpre, gin_ref)
        tile = 256

        @pl.loop(0, width // tile)
        def _(piece):
            at = pl.ds(pl.multiple_of(piece * tile, tile), tile)
            target[at, span] = mm(left[:, at], right[:, span], TN).astype(BF16)

        for d in order + [0]:
            near(j, d).start()

    def send_sums(j):
        source, span, held, summed, _ = parts[j]
        for d in order:
            near(j, d).wait_recv()
            rows = rows_at(source, ((chip + d) % chips) * 2 + core, count)
            add_into(summed.at[d, :, span], rows.at[:, span], held.at[d, :, span])
            far(j, d).start()
        near(j, 0).wait_recv()

    differentiate(0)
    for k in (2, 3, 4):
        fetches[k].wait()
    advance(0)
    differentiate(1)
    send_sums(0)
    advance(1)
    differentiate(2)
    send_sums(1)
    advance(2)
    differentiate(3)
    send_sums(2)
    advance(3)
    send_sums(3)
    at = 3
    turns = sums.turns
    for d in range(1, n_fs):
        for copy in small(d):
            copy.wait_recv()
    total, again = mine_got[0], shared_got[0]
    for peer in range(1, n_fs):
        total, again = total + mine_got[peer], again + shared_got[peer]
    mine_out[...] = total
    shared_held[...] = again
    shared_z[tp] = again
    for d in range(1, n_tp):
        remote(shared_held, shared_z.at[tp], ts.at[d], tr.at[d], tp=(tp + d) % n_tp).start()
    pl.loop(at + 1, turns)(advance)

    def settle(j, target, span):
        source, _, held, _, got = parts[j]
        rows = rows_at(source, me, count)
        add_into(
            target, rows.at[:, span], held.at[0, :, span], *[got.at[d, :, span] for d in order]
        )

    for d in order:
        far(0, d).wait_recv()
    settle(0, bc_held, slice(2 * chan, 2 * chan + 2 * STATE))
    bc_got[tp] = bc_held[...]
    for d in range(1, n_tp):
        remote(bc_held, bc_got.at[tp], bs.at[d], br.at[d], tp=(tp + d) % n_tp).start()
    settle(0, own_out.at[:, 2 * chan:2 * chan + LANES], slice(2 * chan + 2 * STATE, cols))
    for j in (1, 2, 3):
        for d in order:
            far(j, d).wait_recv()
    settle(1, own_out.at[:, 2 * chan + LANES:], slice(0, chan))
    settle(2, own_out.at[:, chan:2 * chan], slice(chan, 2 * chan))
    settle(3, own_out.at[:, :chan], slice(0, chan))
    for d in range(1, n_tp):
        peer = (tp + n_tp - d) % n_tp
        remote(shared_held, shared_z.at[peer], ts.at[d], tr.at[d], tp=peer).wait_recv()
        remote(bc_held, bc_got.at[peer], bs.at[d], br.at[d], tp=peer).wait_recv()
    total = shared_z[0]
    for peer in range(1, n_tp):
        total = total + shared_z[peer]
    shared_out[...] = total
    add_into(bc_out, *[bc_got.at[peer] for peer in range(n_tp)])

    sums.settle(lambda part: dn_out.at[pl.ds(part * chunk, chunk)])
    sums.drain()
    for j in range(4):
        for d in range(chips):
            near(j, d).wait_send()
        for d in order:
            far(j, d).wait_send()
    for d in range(1, n_fs):
        for copy in small(d):
            copy.wait_send()
    for d in range(1, n_tp):
        remote(shared_held, shared_z.at[tp], ts.at[d], tr.at[d], tp=(tp + d) % n_tp).wait_send()
        remote(bc_held, bc_got.at[tp], bs.at[d], br.at[d], tp=(tp + d) % n_tp).wait_send()


def leave(dn, normed, dpre, cot, gnormed, small, n_tp, n_fs):
    block, width = dn.shape[0] // n_tp, dn.shape[1]
    count, cols = width // n_fs, dpre.shape[1]
    chan = gnormed.shape[1]
    chips, steps = n_fs // 2, (n_tp - 1) * CHUNKS
    dma = pltpu.SemaphoreType.DMA
    vmem = pl.BlockSpec(memory_space=pltpu.VMEM)
    room = lambda *shape: pltpu.VMEM(shape, BF16)
    shape = lambda *extents: jax.ShapeDtypeStruct(extents, F32)
    up = lambda n: -(-n // 8) * 8
    mine = (up(7 * chan // LANES + 2), LANES)
    shared = (up((10 * STATE + width) // LANES), LANES)
    low = lambda *extents: jax.ShapeDtypeStruct(extents, BF16)
    outs = [low(block, width), low(count, 3 * chan + LANES), low(count, 2 * STATE), shape(*mine), shape(*shared)]
    return pl.pallas_call(
        functools.partial(exit_kernel, n_tp=n_tp, n_fs=n_fs),
        name="exit",
        in_specs=[pl.BlockSpec(memory_space=pl.ANY)] * 5 + [vmem] * 5,
        out_specs=[vmem] * len(outs),
        out_shape=outs,
        scratch_shapes=[
            room(*dn.shape), room(*normed.shape), room(*dpre.shape), room(*cot.shape), room(*gnormed.shape), dma((5,)),
            room(width, cols), room(width, chan), pltpu.VMEM(mine, F32), pltpu.VMEM(shared, F32),
            room(2, steps, block // CHUNKS, width),
            room(chips, count, cols), room(chips, count, chan), room(chips, count, cols), room(chips, count, chan),
            room(chips, count, cols), room(chips, count, chan),
            pltpu.VMEM((n_fs,) + mine, F32), pltpu.VMEM((n_fs,) + shared, F32),
            pltpu.VMEM(shared, F32), pltpu.VMEM((n_tp,) + shared, F32),
            room(count, 2 * STATE), room(n_tp, count, 2 * STATE),
            dma((2, steps)), dma((2, steps)), dma((4, chips)), dma((4, chips)), dma((4, chips)), dma((4, chips)),
            dma((n_fs,)), dma((n_fs,)), dma((n_fs,)), dma((n_fs,)), dma((n_tp,)), dma((n_tp,)), dma((n_tp,)),
            dma((n_tp,)),
        ],
        compiler_params=pltpu.CompilerParams(
            collective_id=TAGS["exit"], has_side_effects=True, vmem_limit_bytes=62 << 20
        ),
    )(dn, normed, dpre, cot, gnormed, *small)


def shards(
    tokens, cotangent, seq_start, token_valid, norm_gain, proj_z, proj_x, proj_bc, proj_dt, conv_chan, bias_chan,
    conv_shared, bias_shared, a_log, dt_bias, skip_gain, gate_gain, proj_out,
):
    chan, heads_here = proj_z.shape[1], proj_dt.shape[1]
    n_tp, n_fs = lax.axis_size("tp"), lax.axis_size("fsdp")
    (
        tok_all, cot_all, w_in, normed, pre, y, enter, dgn, gnormed, out_rows, early, stats, taps, bias, heads, skip,
        gate,
    ) = ahead(
        seq_start, (dt_bias, a_log, skip_gain), tokens, cotangent,
        (proj_z, proj_x, proj_bc, proj_dt.T, proj_out.T), token_valid,
        (norm_gain, conv_chan, bias_chan, conv_shared, bias_shared, gate_gain), n_tp, n_fs,
    )
    dpre, dn_rows, *small, mixed = mixer_backward(
        seq_start, tok_all, w_in, taps, bias, heads, skip, gate, pre, y, enter, dgn, stats, out_rows, chan * n_tp,
        n_tp,
    )
    sums = leave(dn_rows, normed, dpre, cot_all, gnormed, small, n_tp, n_fs)
    grads = list(finish(tokens, cotangent, early, mixed, norm_gain, *sums, heads_here))
    grads[6], grads[15] = grads[6].T, grads[15].T
    return tuple(grads)


def solution(mesh):
    in_specs = (
        P(("fsdp", "tp"), None), P(("fsdp", "tp"), None), P("fsdp"), P("fsdp"), P(), P("fsdp", "tp"),
        P("fsdp", "tp"), P("fsdp", None), P("fsdp", "tp"), P(None, "tp"), P("tp"), P(), P(), P("tp"), P("tp"),
        P("tp"), P("tp"), P("tp", "fsdp"),
    )
    out_specs = (
        P(("fsdp", "tp"), None), P(("fsdp", "tp"), None), P(), P("fsdp", "tp"), P("fsdp", "tp"), P("fsdp", None),
        P("fsdp", "tp"), P(None, "tp"), P("tp"), P(), P(), P("tp"), P("tp"), P("tp"), P("tp"), P("tp", "fsdp"),
    )
    return jax.shard_map(shards, mesh=mesh, in_specs=in_specs, out_specs=out_specs, check_vma=False)
```

```python
import functools
import jax
import jax.numpy as jnp
from jax import lax
from jax.experimental import pallas as pl
from jax.experimental.pallas import tpu as pltpu
from jax.sharding import PartitionSpec as P

HEAD = 64
STATE = 128
STRETCH = 256
LANES = 128
EPSILON = 1e-05
PLACES = 3
F32 = jnp.float32
BF16 = jnp.bfloat16
NN = (((1,), (0,)), ((), ()))
NT = (((1,), (1,)), ((), ()))
TN = (((0,), (0,)), ((), ()))


def mm(a, b, dims=NN):
    return lax.dot_general(a, b, dims, preferred_element_type=F32)


def exact(a, b):
    return lax.dot_general(a, b, NN, precision=lax.Precision.HIGHEST, preferred_element_type=F32)


def halves(v):
    high = v.astype(BF16)
    return high, (v - high.astype(F32)).astype(BF16)


def iota(shape, dim):
    return lax.broadcasted_iota(jnp.int32, shape, dim)


def spread_heads(v, chan):
    high, rest = halves(v)
    rows = iota((2 * LANES, chan), 0) & (LANES - 1)
    pick = jnp.where(rows == (iota((2 * LANES, chan), 1) >> 6), 1.0, 0.0).astype(BF16)
    return mm(jnp.concatenate([high, rest], axis=1), pick)


def gather_heads(v):
    chan = v.shape[1]
    high, rest = halves(v)
    pick = jnp.where((iota((chan, LANES), 0) >> 6) == iota((chan, LANES), 1), 1.0, 0.0).astype(BF16)
    return mm(high, pick) + mm(rest, pick)


def softplus(v):
    return jnp.maximum(v, 0.0) + jnp.log1p(jnp.exp(-jnp.abs(v)))


def sigmoid(v):
    return 1.0 / (1.0 + jnp.exp(-v))


def lower_mask():
    return iota((STRETCH, STRETCH), 0) >= iota((STRETCH, STRETCH), 1)


def convolve(xs_ref, taps_ref, bias_ref):
    total = bias_ref[...] + taps_ref[0:1, :] * xs_ref[5:5 + STRETCH, :]
    for tap in range(1, 4):
        total = total + taps_ref[tap:tap + 1, :] * xs_ref[5 + tap:5 + tap + STRETCH, :]
    return total


def decays(pre_dt, head_ref, valid):
    rates = softplus(pre_dt + head_ref[0:1, :]) * valid
    log_decay = rates * head_ref[1:2, :]
    lower = lower_mask().astype(F32)
    cumulative = exact(lower, log_decay)
    last = cumulative[STRETCH - 1:STRETCH, :]
    return rates, cumulative, jnp.exp(cumulative), jnp.exp(last - cumulative)


def weights_of(cumulative, across, head):
    return jnp.exp(jnp.minimum(cumulative[:, head:head + 1] - across[head:head + 1, :], 0.0))


def backward_kernel(
    open_ref, tok_ref, w_hbm, taps_ref, bias_ref, head_ref, skip_ref, gate_ref,
    pre_ref, halo_ref, y_ref, enter_ref, dgn_ref, stats_ref, rows_ref,
    dpre_ref, dnormed_ref, dtaps_ref, dbias_ref, dhead_ref, dchan_ref, dgain_ref, mixed_ref,
    dstate, xs, dus, rows, w_ref, o_got, fetch_sem, o_send, o_recv,
    *, inner, n_tp,
):
    chan = y_ref.shape[1]
    wide = chan + 2 * STATE
    step = pl.program_id(0)
    block = pl.num_programs(0) - 1 - step
    opening = open_ref[block] == 1
    keep = jnp.where(opening, 0.0, 1.0).astype(F32)
    tp = lax.axis_index("tp")
    per = rows.shape[0] // n_tp
    chunk = per // CHUNKS
    sums = LineSum(
        tp, n_tp, CHUNKS - EARLY, lambda index, part: chunk_of(rows, index, per, part + EARLY, chunk),
        lambda index, part: chunk_of(rows_ref, index, per, part + EARLY, chunk), o_got, o_send, o_recv,
    )

    fetches = (
        pltpu.make_async_copy(rows_ref, rows, fetch_sem.at[0]), pltpu.make_async_copy(w_hbm, w_ref, fetch_sem.at[1])
    )

    def turn(place):
        at = step * PLACES + place - 2

        @pl.when(jnp.logical_and(at >= 0, at < sums.turns))
        def _():
            sums.advance(at)

    @pl.when(step == 0)
    def _():
        for fetch in fetches:
            fetch.start()
        line_greeting(tp, n_tp)
        sums.kick()

    @pl.when(step == 0)
    def _():
        dstate[...] = jnp.zeros_like(dstate)
        dus[...] = jnp.zeros_like(dus)
        dtaps_ref[...] = jnp.zeros_like(dtaps_ref)
        dbias_ref[...] = jnp.zeros_like(dbias_ref)
        dhead_ref[...] = jnp.zeros_like(dhead_ref)
        dchan_ref[...] = jnp.zeros_like(dchan_ref)
        dgain_ref[...] = jnp.zeros_like(dgain_ref)

    grstd, cross, valid = row_stats(stats_ref, inner)
    xs[0:8, :] = halo_ref[:, chan:2 * chan + 2 * STATE] * keep
    xs[8:8 + STRETCH, :] = pre_ref[:, chan:2 * chan + 2 * STATE]
    conv = convolve(xs, taps_ref, bias_ref)
    gate_u = sigmoid(conv)
    feats = conv * gate_u
    slope = gate_u * (1.0 + conv * (1.0 - gate_u))
    x = feats[:, :chan]
    bs = feats[:, chan:chan + STATE].astype(BF16)
    cs = feats[:, chan + STATE:].astype(BF16)
    pre_dt = pre_ref[:, 2 * chan + 2 * STATE:]
    rates, cumulative, grown, to_end = decays(pre_dt, head_ref, valid)
    across = cumulative.T
    grown_e = spread_heads(grown, chan)
    rates_e = spread_heads(rates, chan)
    to_end_e = spread_heads(to_end, chan)
    leave_e = grown_e[STRETCH - 1:STRETCH, :]

    pre_z = pre_ref[:, :chan]
    gate_z = sigmoid(pre_z)
    silu_z = pre_z * gate_z * valid
    y = y_ref[...]
    mixed = y + skip_ref[...] * x
    gated = mixed * silu_z
    dgn = dgn_ref[...]
    d_gated = grstd * (gate_ref[...] * dgn) - gated * (grstd * grstd * grstd * cross * (1.0 / inner))
    d_mixed = d_gated * silu_z
    dpre_ref[:, :chan] = (
        d_gated * mixed * (valid * (gate_z * (1.0 + pre_z * (1.0 - gate_z))))
    ).astype(BF16)
    dchan_ref[0:1, :] += jnp.sum(dgn * gated * grstd, axis=0, keepdims=True)
    dchan_ref[1:2, :] += jnp.sum(d_mixed * x, axis=0, keepdims=True)

    turn(0)
    dy_b = d_mixed.astype(BF16)
    dy = dy_b.astype(F32)
    scaled = x * rates_e
    scaled_b = scaled.astype(BF16)
    entering = enter_ref[0]
    d_leaving = dstate[...]
    d_leaving_b = d_leaving.astype(BF16)
    tail = mm(bs, d_leaving_b) * to_end_e
    overlap = jnp.where(lower_mask(), mm(cs, bs, NT), 0.0)
    first = iota((STRETCH, LANES), 1) < HEAD
    d_overlap = jnp.zeros((STRETCH, STRETCH), F32)
    parts = []
    for pair in range(chan // LANES):
        cols = slice(pair * LANES, (pair + 1) * LANES)
        dy_pair = dy_b[:, cols]
        x_pair = scaled_b[:, cols]
        zero = jnp.zeros_like(dy_pair)
        sides = [jnp.where(first, dy_pair, zero), jnp.where(first, zero, dy_pair)]
        mats = []
        for side in range(2):
            weight = weights_of(cumulative, across, 2 * pair + side)
            mats.append((weight * overlap).astype(BF16))
            d_overlap = d_overlap + mm(sides[side], x_pair, NT) * weight
        parts.append(mm(jnp.concatenate(mats, axis=0), jnp.concatenate(sides, axis=0), TN))
    turn(1)
    d_scaled = jnp.concatenate(parts, axis=1) + tail
    scaled_r = scaled_b.astype(F32)
    d_cum = gather_heads(dy * y - scaled_r * d_scaled)
    d_last = jnp.sum(scaled_r * tail, axis=0, keepdims=True) + leave_e * jnp.sum(
        d_leaving * entering, axis=0, keepdims=True
    )
    d_last = gather_heads(jnp.broadcast_to(d_last, (8, chan)))[0:1, :]
    upper = (iota((STRETCH, STRETCH), 0) <= iota((STRETCH, STRETCH), 1)).astype(F32)
    d_log = exact(upper, d_cum) + d_last
    decay = head_ref[1:2, :]
    d_rates = d_log * decay + gather_heads(x * d_scaled)
    d_dt = d_rates * valid * sigmoid(pre_dt + head_ref[0:1, :])
    dhead_ref[0:1, :] += jnp.sum(d_log * rates, axis=0, keepdims=True) * decay
    dhead_ref[1:2, :] += jnp.sum(d_dt, axis=0, keepdims=True)
    dpre_ref[:, 2 * chan + 2 * STATE:] = d_dt.astype(BF16)

    d_x = d_scaled * rates_e + skip_ref[...] * d_mixed
    d_overlap_b = jnp.where(lower_mask(), d_overlap, 0.0).astype(BF16)
    dy_grown = (dy * grown_e).astype(BF16)
    x_end = (scaled * to_end_e).astype(BF16)
    d_b = mm(d_overlap_b, cs, TN) + mm(x_end, d_leaving_b, NT)
    d_c = mm(d_overlap_b, bs) + mm(dy_grown, entering.astype(BF16), NT)
    dstate[...] = (d_leaving * leave_e + mm(cs, dy_grown, TN)) * keep

    dus[0:STRETCH, :chan] = d_x * slope[:, :chan]
    dus[0:STRETCH, chan:chan + STATE] = d_b * slope[:, chan:chan + STATE]
    dus[0:STRETCH, chan + STATE:] = d_c * slope[:, chan + STATE:]
    d_conv = dus[0:STRETCH, :]
    dbias_ref[...] += jnp.sum(d_conv, axis=0, keepdims=True)
    d_pre = jnp.zeros((STRETCH, wide), F32)
    for tap in range(4):
        dtaps_ref[tap:tap + 1, :] += jnp.sum(d_conv * xs[5 + tap:5 + tap + STRETCH, :], axis=0, keepdims=True)
        d_pre = d_pre + taps_ref[tap:tap + 1, :] * dus[3 - tap:3 - tap + STRETCH, :]
    dpre_ref[:, chan:2 * chan + 2 * STATE] = d_pre.astype(BF16)
    dus[STRETCH:STRETCH + 8, :] = d_conv[0:8, :] * keep

    @pl.when(step == 0)
    def _():
        for fetch in fetches:
            fetch.wait()

    turn(2)
    d_normed = mm(dpre_ref[...], w_ref[...], NT)
    dnormed_ref[...] = d_normed.astype(BF16)
    resid = tok_ref[...].astype(F32)
    rstd = lax.rsqrt(jnp.mean(resid * resid, axis=1, keepdims=True) + EPSILON)
    dgain_ref[...] += jnp.sum(d_normed * (resid * rstd), axis=0, keepdims=True)

    @pl.when(step == pl.num_programs(0) - 1)
    def _():
        pl.loop(jnp.minimum(step * PLACES + 1, sums.turns), sums.turns)(sums.advance)
        sums.settle(lambda part: mixed_ref.at[pl.ds(part * chunk, chunk)])
        sums.drain()


def whole(shape):
    return pl.BlockSpec(shape, lambda *_: (0,) * len(shape), pipeline_mode=pl.Buffered(1))


def mixer_backward(
    openings, tok, w_in, taps, bias, heads, skip, gate, pre, y, enter, dgn, stats, out_rows, inner, n_tp
):
    tokens, width = tok.shape
    cols = w_in.shape[1]
    chan = skip.shape[1]
    blocks = tokens // STRETCH
    wide = chan + 2 * STATE
    per = STRETCH // 8
    steps = (n_tp - 1) * (CHUNKS - EARLY)
    kept = tokens // n_tp // CHUNKS * (CHUNKS - EARLY)
    rows = lambda n: pl.BlockSpec((STRETCH, n), lambda i, *_: (blocks - 1 - i, 0))
    return pl.pallas_call(
        functools.partial(backward_kernel, inner=inner, n_tp=n_tp),
        name="mixer_backward",
        grid_spec=pltpu.PrefetchScalarGridSpec(
            num_scalar_prefetch=1,
            grid=(blocks,),
            in_specs=[
                rows(width), pl.BlockSpec(memory_space=pl.ANY), whole((4, wide)), whole((1, wide)),
                whole((8, LANES)), whole((1, chan)), whole((1, chan)),
                rows(cols),
                pl.BlockSpec((8, cols), lambda i, *_: (jnp.maximum((blocks - 1 - i) * per - 1, 0), 0)),
                rows(chan),
                pl.BlockSpec((1, STATE, chan), lambda i, *_: (blocks - 1 - i, 0, 0)),
                rows(chan),
                pl.BlockSpec((8, STRETCH), lambda i, *_: (0, blocks - 1 - i)),
                pl.BlockSpec(memory_space=pl.ANY),
            ],
            out_specs=[
                rows(cols), rows(width),
                pl.BlockSpec((8, wide), lambda i, *_: (0, 0)),
                pl.BlockSpec((1, wide), lambda i, *_: (0, 0)),
                pl.BlockSpec((8, LANES), lambda i, *_: (0, 0)),
                pl.BlockSpec((8, chan), lambda i, *_: (0, 0)),
                pl.BlockSpec((1, width), lambda i, *_: (0, 0)),
                pl.BlockSpec((kept, width), lambda i, *_: (0, 0)),
            ],
            scratch_shapes=[
                pltpu.VMEM((STATE, chan), F32),
                pltpu.VMEM((STRETCH + 8, wide), F32),
                pltpu.VMEM((STRETCH + 8, wide), F32),
                pltpu.VMEM((tokens, width), BF16),
                pltpu.VMEM((width, cols), BF16),
                pltpu.VMEM((2, steps, tokens // n_tp // CHUNKS, width), BF16),
                pltpu.SemaphoreType.DMA((2,)),
                pltpu.SemaphoreType.DMA((2, steps)),
                pltpu.SemaphoreType.DMA((2, steps)),
            ],
        ),
        out_shape=[
            jax.ShapeDtypeStruct((tokens, cols), BF16),
            jax.ShapeDtypeStruct((tokens, width), BF16),
            jax.ShapeDtypeStruct((8, wide), F32),
            jax.ShapeDtypeStruct((1, wide), F32),
            jax.ShapeDtypeStruct((8, LANES), F32),
            jax.ShapeDtypeStruct((8, chan), F32),
            jax.ShapeDtypeStruct((1, width), F32),
            jax.ShapeDtypeStruct((kept, width), BF16),
        ],
        cost_estimate=pl.CostEstimate(
            flops=4 * tokens * width * cols, bytes_accessed=tokens * cols * 12, transcendentals=tokens * chan
        ),
        compiler_params=pltpu.CompilerParams(
            collective_id=TAGS["backward"], has_side_effects=True, vmem_limit_bytes=60 << 20,
            dimension_semantics=("arbitrary",),
        ),
    )(openings, tok, w_in, taps, bias, heads, skip, gate, pre, pre, y, enter, dgn, stats, out_rows)


MESH = pl.DeviceIdType.MESH
CHUNKS = 4
EARLY = 1
LARGE = (0, 1, 3, 4, 5, 15)
TAGS = {"ahead": 1, "backward": 2, "exit": 3}


def remote(source, target, send, recv, **where):
    return pltpu.make_async_remote_copy(
        src_ref=source, dst_ref=target, send_sem=send, recv_sem=recv, device_id=where, device_id_type=MESH
    )


def rows_at(ref, index, count):
    return ref.at[pl.ds(pl.multiple_of(index * count, count), count)]


def greet(axis, peers):
    barrier = pltpu.get_barrier_semaphore()
    for peer in peers:
        pl.semaphore_signal(barrier, inc=1, device_id={axis: peer}, device_id_type=MESH)


class Line:
    def __init__(self, tp, n_tp, own, whole_ref, send, recv, split=1):
        self.tp, self.n, self.own, self.whole_ref, self.send, self.recv = tp, n_tp, own, whole_ref, send, recv
        self.count = own.shape[0]
        self.split, self.part = split, own.shape[0] // split

    def piece(self, index, step):
        return self.whole_ref.at[
            pl.ds(pl.multiple_of(index * self.count + step % self.split * self.part, self.part), self.part)
        ]

    def copy(self, way, step, own=False):
        shift = -1 if way == 0 else 1
        slot = self.piece(self.tp + shift * (step // self.split), step)
        source = self.own.at[pl.ds(step % self.split * self.part, self.part)] if own else slot
        return remote(source, slot, self.send.at[way, step], self.recv.at[way, step], tp=self.tp - shift)

    def sends(self, way, step):
        step = step // self.split
        if way == 0:
            return jnp.logical_and(self.tp < self.n - 1, self.tp >= step)
        return jnp.logical_and(self.tp > 0, self.tp + step <= self.n - 1)

    def takes(self, way, step):
        step = step // self.split
        return self.tp >= step + 1 if way == 0 else self.tp + step + 1 <= self.n - 1

    def start(self, way, step):
        @pl.when(self.sends(way, step))
        def _():
            self.copy(way, step, own=step < self.split).start()

    def arrive(self, way, step):
        @pl.when(self.takes(way, step))
        def _():
            shift = -1 if way == 0 else 1
            slot = self.piece(self.tp + shift * (step // self.split + 1), step)
            remote(
                slot, slot, self.send.at[way, step], self.recv.at[way, step], tp=self.tp + shift
            ).wait_recv()

    def finish(self, way, step):
        @pl.when(self.sends(way, step))
        def _():
            self.copy(way, step, own=step < self.split).wait_send()


class LineSum:
    def __init__(self, tp, n_tp, per, local, origin, got, send, recv):
        self.tp, self.n, self.per, self.local_of, self.origin = tp, n_tp, per, local, origin
        self.got, self.send, self.recv = got, send, recv
        self.steps = (n_tp - 1) * per
        self.paced = max(n_tp - 2, 0) * per
        self.turns = self.paced + max(n_tp - 3, 0)

    def ahead(self, way, step):
        return self.n - 1 - step // self.per if way == 0 else step // self.per

    def passes(self, way, step):
        return self.ahead(way, step) > self.tp if way == 0 else self.ahead(way, step) < self.tp

    def first(self, way):
        return self.tp == 0 if way == 0 else self.tp == self.n - 1

    def local(self, way, step):
        return self.local_of(self.ahead(way, step), step % self.per)

    def copy(self, way, step, direct):
        source = (self.origin if direct else self.local_of)(self.ahead(way, step), step % self.per)
        return remote(
            source, self.got.at[way, step], self.send.at[way, step], self.recv.at[way, step],
            tp=self.tp + 1 if way == 0 else self.tp - 1,
        )

    def kick(self):
        for way in range(2):
            @pl.when(self.first(way))
            def _():
                for step in range(min(3, self.steps) if self.paced else self.steps):
                    self.copy(way, step, True).start()

    def advance(self, turn):
        for way in range(2):
            lag = jnp.maximum(self.tp - 1 if way == 0 else self.n - 2 - self.tp, 0)
            step = turn - lag
            live = jnp.logical_and(step >= 0, step < self.paced)

            @pl.when(jnp.logical_and(self.first(way), live))
            def _():
                self.copy(way, step, True).wait_send()

                @pl.when(step + 3 < self.steps)
                def _():
                    self.copy(way, step + 3, True).start()

                @pl.when(step == self.paced - 1)
                def _():
                    for rest in range(self.paced + 3, self.steps):
                        self.copy(way, rest, True).start()

            @pl.when(jnp.logical_and(jnp.logical_and(self.passes(way, step), live), jnp.logical_not(self.first(way))))
            def _():
                copy = self.copy(way, step, False)
                copy.wait_recv()
                add_into(self.local(way, step), self.local(way, step), self.got.at[way, step])
                copy.start()

    def settle(self, target):
        for way in range(2):
            for step in range(self.steps):
                @pl.when(jnp.logical_and(self.ahead(way, step) == self.tp, jnp.logical_not(self.first(way))))
                def _():
                    self.copy(way, step, False).wait_recv()

        for value in range(self.n):
            @pl.when(self.tp == value)
            def _():
                for part in range(self.per):
                    incoming = []
                    if value > 0:
                        incoming.append(self.got.at[0, (self.n - 1 - value) * self.per + part])
                    if value < self.n - 1:
                        incoming.append(self.got.at[1, value * self.per + part])
                    add_into(target(part), self.local_of(value, part), *incoming)

    def drain(self):
        for way in range(2):
            @pl.when(self.first(way))
            def _():
                for step in range(self.paced, self.steps):
                    self.copy(way, step, True).wait_send()

            for step in range(self.steps):
                @pl.when(jnp.logical_and(self.passes(way, step), jnp.logical_not(self.first(way))))
                def _():
                    self.copy(way, step, False).wait_send()


def chunk_of(ref, block, rows, part, chunk):
    return ref.at[pl.ds(pl.multiple_of(block * rows + part * chunk, chunk), chunk)]


def line_greeting(tp, n_tp):
    barrier = pltpu.get_barrier_semaphore()
    for near, there in ((tp - 1, tp > 0), (tp + 1, tp < n_tp - 1)):
        @pl.when(there)
        def _():
            pl.semaphore_signal(barrier, inc=1, device_id={"tp": near}, device_id_type=MESH)
    pl.semaphore_wait(barrier, jnp.where(tp > 0, 1, 0) + jnp.where(tp < n_tp - 1, 1, 0))


def forward_block(keep, tok, valid, gain_ref, w_ref, taps_ref, bias_ref, head_ref, skip_ref,
                  normed_ref, pre_ref, y_ref, gated_ref, enter_ref, state, xs):
    chan = y_ref.shape[1]
    xs[0:8, :] = xs[STRETCH:STRETCH + 8, :] * keep
    resid = tok.astype(F32)
    rstd = lax.rsqrt(jnp.mean(resid * resid, axis=1, keepdims=True) + EPSILON)
    normed = (resid * rstd * gain_ref[...]).astype(BF16)
    normed_ref[...] = normed
    pre_ref[...] = mm(normed, w_ref[...])
    xs[8:8 + STRETCH, :] = pre_ref[:, chan:2 * chan + 2 * STATE]
    conv = convolve(xs, taps_ref, bias_ref)
    feats = conv * sigmoid(conv)
    x = feats[:, :chan]
    bs = feats[:, chan:chan + STATE].astype(BF16)
    cs = feats[:, chan + STATE:].astype(BF16)
    rates, cumulative, grown, to_end = decays(pre_ref[:, 2 * chan + 2 * STATE:], head_ref, valid)
    across = cumulative.T
    grown_e = spread_heads(grown, chan)
    scaled = x * spread_heads(rates, chan)
    entering = state[...] * keep
    enter_ref[...] = entering
    y_ref[...] = mm(cs, entering.astype(BF16)) * grown_e
    state[...] = entering * grown_e[STRETCH - 1:STRETCH, :] + mm(
        bs, (scaled * spread_heads(to_end, chan)).astype(BF16), TN
    )
    overlap = jnp.where(lower_mask(), mm(cs, bs, NT), 0.0)
    scaled_b = scaled.astype(BF16)
    first = iota((STRETCH, LANES), 1) < HEAD
    for pair in range(chan // LANES):
        cols = slice(pair * LANES, (pair + 1) * LANES)
        both = scaled_b[:, cols]
        mats = [
            (weights_of(cumulative, across, 2 * pair + side) * overlap).astype(BF16) for side in range(2)
        ]
        zero = jnp.zeros_like(both)
        y_ref[:, cols] += mm(
            jnp.concatenate(mats, axis=1),
            jnp.concatenate([jnp.where(first, both, zero), jnp.where(first, zero, both)], axis=0),
        )
    pre_z = pre_ref[:, :chan]
    gated = (y_ref[...] + skip_ref[...] * x) * (pre_z * sigmoid(pre_z)) * valid
    gated_ref[...] = gated
    return jnp.sum(gated * gated, axis=1, keepdims=True)


def as_row(column):
    lane = iota((STRETCH, LANES), 1)
    return jnp.where(lane == 0, column, 0.0).T[0:8, :]


def as_column(row):
    return jnp.concatenate([row, jnp.zeros((LANES - 8, STRETCH), F32)], axis=0).T


def row_stats(stats_ref, inner):
    filled = as_column(stats_ref[...])
    return lax.rsqrt(filled[:, 0:1] * (1.0 / inner) + EPSILON), filled[:, 1:2], filled[:, 2:3]


def ahead_kernel(
    open_ref, step_bias, log_rate, direct, tok_ref, cot_ref, pz_ref, px_ref, pbc_ref, pdt_ref, pout_ref, mask_ref,
    norm_gain, conv_chan, bias_chan, conv_shared, bias_shared, gate_gain,
    tok_out, cot_out, win_out, normed_out, pre_out, y_out, enter_out, dgn_out, gn_out, rows_out, mixed_out, stats_ref,
    taps_ref, bias_ref, head_ref, skip_ref, gate_ref,
    pin_ref, gain_ref, tok_all, cot_all, w_in, w_out, normed, pre, y, gated, enter, dgn, gnormed, rows, state, xs, squares, crosses,
    squares_got, crosses_got, o_got,
    own_sem, z_send, z_recv, c_send, c_recv, f_send, f_recv, p_send, p_recv, q_send, q_recv, r_send, r_recv,
    all_sem, out_sem, o_send, o_recv,
    *, n_tp, n_fs, inner,
):
    tp, me = lax.axis_index("tp"), lax.axis_index("fsdp")
    chip, core, chips = me // 2, me % 2, n_fs // 2
    partner = chip * 2 + 1 - core
    blocks = tok_all.shape[0] // STRETCH
    per = tok_ref.shape[0]
    chan = pout_ref.shape[1]
    greet("fsdp", [((chip + d) % chips) * 2 + core for d in range(1, chips)] + [partner])
    greet("tp", [(tp + d) % n_tp for d in range(1, n_tp)])
    pin_ref[:, :chan] = pz_ref[...]
    pin_ref[:, chan:2 * chan] = px_ref[...]
    pin_ref[:, 2 * chan:2 * chan + 2 * STATE] = pbc_ref[...]
    heads_here, rows_dt = pdt_ref.shape
    pin_ref[:, 2 * chan + 2 * STATE:] = jnp.concatenate(
        [pdt_ref[...].astype(F32), jnp.zeros((LANES - heads_here, rows_dt), F32)], axis=0
    ).T.astype(BF16)
    pl.semaphore_wait(pltpu.get_barrier_semaphore(), chips + n_tp - 1)

    packs = ((pin_ref, w_in), (pout_ref, w_out))
    count = pin_ref.shape[0]
    line = Line(tp, n_tp, tok_ref, tok_all, z_send, z_recv, split=2)
    late = Line(tp, n_tp, cot_ref, cot_all, c_send, c_recv)
    for way in range(2):
        line.start(way, 0)
    for j, (pack, full) in enumerate(packs):
        for d in range(1, chips):
            remote(
                pack, rows_at(full, me, count), f_send.at[j, d], f_recv.at[j, d], fsdp=((chip + d) % chips) * 2 + core
            ).start()
        remote(pack, rows_at(full, me, count), p_send.at[j, 0], p_recv.at[j, 0], fsdp=partner).start()
    own = [
        pltpu.make_async_copy(tok_ref, rows_at(tok_all, tp, per), own_sem.at[0]),
        pltpu.make_async_copy(pin_ref, rows_at(w_in, me, count), own_sem.at[1]),
        pltpu.make_async_copy(pout_ref, rows_at(w_out, me, count), own_sem.at[2]),
        pltpu.make_async_copy(cot_ref, rows_at(cot_all, tp, per), own_sem.at[3]),
    ]
    for copy in own:
        copy.start()
    state[...] = jnp.zeros_like(state)
    xs[...] = jnp.zeros_like(xs)
    lane = iota((8, LANES), 1)
    place = iota((8, LANES), 0)
    step_row, rate_row, skip_row = (
        sum(jnp.where(lane == head, source[head], 0.0) for head in range(heads_here))
        for source in (step_bias, log_rate, direct)
    )
    live = lane < heads_here
    head_ref[...] = jnp.where(
        place == 0, jnp.where(live, step_row, -100.0), jnp.where(live & (place == 1), -jnp.exp(rate_row), 0.0)
    )
    skip_ref[...] = spread_heads(skip_row, chan)[0:1, :]
    gain_ref[...] = norm_gain[...].reshape(gain_ref.shape)
    gate_ref[...] = gate_gain[...].reshape(gate_ref.shape)
    taps_ref[:, :chan] = conv_chan[...]
    taps_ref[:, chan:] = conv_shared[...]
    bias_ref[:, :chan] = bias_chan[...].reshape(1, chan)
    bias_ref[:, chan:] = bias_shared[...].reshape(1, 2 * STATE)
    last = 2 * (n_tp - 1)
    for step in range(1, last):
        for way in range(2):
            if step >= 2:
                line.arrive(way, step - 2)
            line.finish(way, step - 1)
            line.start(way, step)
    for j, (pack, full) in enumerate(packs):
        for d in range(1, chips):
            slot = rows_at(full, ((chip + chips - d) % chips) * 2 + core, count)
            remote(slot, slot, f_send.at[j, d], f_recv.at[j, d], fsdp=partner).wait_recv()
            remote(slot, slot, p_send.at[j, d], p_recv.at[j, d], fsdp=partner).start()
    for way in range(2):
        line.finish(way, last - 1)
        late.start(way, 0)
    for way in range(2):
        line.arrive(way, last - 2)
        line.arrive(way, last - 1)
    for j, (pack, full) in enumerate(packs):
        for d in range(chips):
            slot = rows_at(full, ((chip + chips - d) % chips) * 2 + 1 - core, count)
            remote(slot, slot, p_send.at[j, d], p_recv.at[j, d], fsdp=partner).wait()
        for d in range(1, chips):
            remote(pack, rows_at(full, me, count), f_send.at[j, d], f_recv.at[j, d], fsdp=partner).wait_send()
    for copy in own:
        copy.wait()
    wholes = [
        pltpu.make_async_copy(tok_all, tok_out, all_sem.at[0]), pltpu.make_async_copy(w_in, win_out, all_sem.at[1]),
    ]
    for copy in wholes:
        copy.start()

    def span(block):
        return pl.ds(pl.multiple_of(block * STRETCH, STRETCH), STRETCH)

    def out(k, block):
        at = span(block)
        chunk = per // CHUNKS * EARLY
        kept = pl.ds(pl.multiple_of(block * STRETCH + chunk, chunk), STRETCH - chunk)
        pairs = (
            (normed.at[at], normed_out.at[at]), (pre.at[block % 2], pre_out.at[at]), (y.at[at], y_out.at[at]),
            (enter.at[block], enter_out.at[block]), (gnormed.at[at], gn_out.at[at]),
            (rows.at[kept], rows_out.at[kept]), (dgn.at[at], dgn_out.at[at]), (cot_all.at[at], cot_out.at[at]),
        )
        return pltpu.make_async_copy(*pairs[k], out_sem.at[k, block])

    @pl.loop(0, blocks)
    def _(block):
        at = span(block)
        keep = jnp.where(open_ref[block] == 1, 0.0, 1.0).astype(F32)

        @pl.when(block >= 2)
        def _():
            out(1, block - 2).wait()

        valid = mask_ref[at].reshape(1, STRETCH).astype(F32)
        squares[:, at] = jnp.where(iota((8, STRETCH), 0) == 2, valid, 0.0)
        total = forward_block(
            keep, tok_all[at, :], as_column(squares[:, at])[:, 2:3], gain_ref, w_in, taps_ref, bias_ref, head_ref, skip_ref,
            normed.at[at], pre.at[block % 2], y.at[at], gated.at[at], enter.at[block], state, xs,
        )
        squares[0:1, at] = as_row(total)[0:1, :]
        for k in range(4):
            out(k, block).start()

        @pl.when(block == max(blocks - 2, 0))
        def _():
            for way in range(2):
                late.arrive(way, 0)
                if n_tp > 2:
                    late.start(way, 1)

    def swap(part, got, send, recv):
        for d in range(1, n_tp):
            remote(part, got.at[tp], send.at[d], recv.at[d], tp=(tp + d) % n_tp).start()
        got[tp] = part[...]
        for d in range(1, n_tp):
            slot = got.at[(tp + n_tp - d) % n_tp]
            remote(slot, slot, send.at[d], recv.at[d], tp=(tp + d) % n_tp).wait_recv()
        total = got[0]
        for peer in range(1, n_tp):
            total = total + got[peer]
        return total

    stats_ref[...] = swap(squares, squares_got, q_send, q_recv)

    @pl.loop(0, blocks)
    def _(block):
        at = span(block)

        grstd, _, _ = row_stats(stats_ref.at[:, at], inner)
        value = (gated[at, :] * grstd * gate_ref[...]).astype(BF16)
        gnormed[at, :] = value
        rows[at, :] = mm(value, w_out[...], NT).astype(BF16)
        out(4, block).start()
        out(5, block).start()

    chunk = per // CHUNKS
    piece = lambda index, part: chunk_of(rows, index, per, part, chunk)
    sums = LineSum(tp, n_tp, EARLY, piece, piece, o_got, o_send, o_recv)
    sums.kick()

    def gradient(block):
        at = span(block)
        value = mm(cot_all[at, :], w_out[...])
        dgn[at, :] = value
        crosses[:, at] = as_row(jnp.sum(gate_ref[...] * value * gated[at, :], axis=1, keepdims=True))
        out(6, block).start()
        out(7, block).start()

    ratio = per // STRETCH

    def gradients(index):
        for k in range(ratio):
            gradient(index * ratio + k)

    gradients(tp)
    middle = min(sums.turns, 3)
    for step in range(n_tp - 1):
        for way in range(2):
            if step > 0:
                late.arrive(way, step)
                if step + 1 < n_tp - 1:
                    late.start(way, step + 1)
        for way in range(2):
            @pl.when(late.takes(way, step))
            def _():
                gradients(tp - step - 1 if way == 0 else tp + step + 1)
        if step == max(n_tp - 3, 0):
            pl.loop(0, middle)(sums.advance)

    total = swap(crosses, crosses_got, r_send, r_recv)
    if middle < sums.turns:
        pl.loop(middle, sums.turns)(sums.advance)
    sums.settle(lambda part: mixed_out.at[pl.ds(part * chunk, chunk)])

    stats_ref[1:2, :] = total[0:1, :]
    stats_ref[2:3, :] = squares[2:3, :]

    for copy in wholes:
        copy.wait()

    @pl.loop(0, blocks)
    def _(block):
        for k in (0, 2, 3, 4, 5, 6, 7):
            out(k, block).wait()

    for block in range(max(blocks - 2, 0), blocks):
        out(1, block).wait()
    for step in range(n_tp - 1):
        for way in range(2):
            late.finish(way, step)
    sums.drain()
    for d in range(1, n_tp):
        remote(squares, squares_got.at[tp], q_send.at[d], q_recv.at[d], tp=(tp + d) % n_tp).wait_send()
        remote(crosses, crosses_got.at[tp], r_send.at[d], r_recv.at[d], tp=(tp + d) % n_tp).wait_send()


def ahead(
    openings, heads, tokens, cotangent, projections, mask, vectors, n_tp, n_fs
):
    per, width = tokens.shape
    total = per * n_tp
    count, chan = projections[0].shape
    wide = chan + 2 * STATE
    cols = chan + wide + LANES
    blocks = total // STRETCH
    chips = n_fs // 2
    dma = pltpu.SemaphoreType.DMA
    anywhere = pl.BlockSpec(memory_space=pl.ANY)
    vmem = pl.BlockSpec(memory_space=pltpu.VMEM)
    shape = jax.ShapeDtypeStruct
    return pl.pallas_call(
        functools.partial(ahead_kernel, n_tp=n_tp, n_fs=n_fs, inner=chan * n_tp),
        name="ahead",
        in_specs=[pl.BlockSpec(memory_space=pltpu.SMEM)] * 4 + [vmem] * 14,
        out_specs=[anywhere] * 10 + [vmem] * 7,
        out_shape=[
            shape((total, width), BF16), shape((total, width), BF16), shape((count * n_fs, cols), BF16),
            shape((total, width), BF16), shape((total, cols), F32), shape((total, chan), F32),
            shape((blocks, STATE, chan), F32), shape((total, chan), F32), shape((total, chan), BF16),
            shape((total, width), BF16), shape((per // CHUNKS * EARLY, width), BF16), shape((8, total), F32),
            shape((4, wide), F32), shape((1, wide), F32),
            shape((8, LANES), F32), shape((1, chan), F32), shape((1, chan), F32),
        ],
        scratch_shapes=[
            pltpu.VMEM((count, cols), BF16), pltpu.VMEM((1, width), F32),
            pltpu.VMEM((total, width), BF16), pltpu.VMEM((total, width), BF16),
            pltpu.VMEM((count * n_fs, cols), BF16), pltpu.VMEM((count * n_fs, chan), BF16),
            pltpu.VMEM((total, width), BF16), pltpu.VMEM((2, STRETCH, cols), F32), pltpu.VMEM((total, chan), F32),
            pltpu.VMEM((total, chan), F32), pltpu.VMEM((blocks, STATE, chan), F32), pltpu.VMEM((total, chan), F32),
            pltpu.VMEM((total, chan), BF16), pltpu.VMEM((total, width), BF16),
            pltpu.VMEM((STATE, chan), F32), pltpu.VMEM((STRETCH + 8, wide), F32),
            pltpu.VMEM((8, total), F32), pltpu.VMEM((8, total), F32),
            pltpu.VMEM((n_tp, 8, total), F32), pltpu.VMEM((n_tp, 8, total), F32),
            pltpu.VMEM((2, (n_tp - 1) * EARLY, per // CHUNKS, width), BF16),
            dma((4,)), dma((2, 2 * (n_tp - 1))), dma((2, 2 * (n_tp - 1))), dma((2, n_tp - 1)), dma((2, n_tp - 1)),
            dma((2, chips)), dma((2, chips)), dma((2, chips)), dma((2, chips)),
            dma((n_tp,)), dma((n_tp,)), dma((n_tp,)), dma((n_tp,)), dma((2,)), dma((8, blocks)),
            dma((2, (n_tp - 1) * EARLY)), dma((2, (n_tp - 1) * EARLY)),
        ],
        compiler_params=pltpu.CompilerParams(
            collective_id=TAGS["ahead"], has_side_effects=True, vmem_limit_bytes=63 << 20
        ),
    )(openings, *heads, tokens, cotangent, *projections, mask, *vectors)


def add_into(target, *sources):
    rows, tile = target.shape[0], 32

    @pl.loop(0, rows // tile)
    def _(i):
        at = pl.ds(pl.multiple_of(i * tile, tile), tile)
        total = sources[0][at, :].astype(F32)
        for source in sources[1:]:
            total = total + source[at, :].astype(F32)
        target[at, :] = total.astype(target.dtype)


def fill_rows(target, pieces):
    at = 0
    for source, row, start, length in pieces:
        for k in range(length // LANES):
            target[at:at + 1, :] = source[row:row + 1, start + k * LANES:start + (k + 1) * LANES]
            at += 1
    if at < target.shape[0]:
        target[at:, :] = jnp.zeros((target.shape[0] - at, LANES), F32)


def finish_kernel(
    *refs,
):
    sources, refs = refs[:10], refs[10:]
    results, copies, held, sem, out_sem = list(refs[:16]), refs[16:26], refs[26:32], refs[32], refs[33]
    fetches = [pltpu.make_async_copy(source, copy, sem.at[k]) for k, (source, copy) in enumerate(zip(sources, copies))]
    for k in (6, 7, 8, 9, 5, 0, 1, 2, 3, 4):
        fetches[k].start()
    stores = [pltpu.make_async_copy(held[k], results[n], out_sem.at[k]) for k, n in enumerate(LARGE)]
    for k, n in enumerate(LARGE):
        results[n] = held[k]
    for k in (6, 7, 8, 9):
        fetches[k].wait()
    write_grads(*copies[6:], *results[3:])
    for store in stores[2:]:
        store.start()
    for k in range(6):
        fetches[k].wait()
    write_tokens(*copies[:6], *results[:2])
    for store in stores[:2]:
        store.start()
    results[2][...] = jnp.concatenate(
        [copies[9][10 + k:11 + k, :] for k in range(results[2].shape[0] // LANES)], axis=1
    ).reshape(results[2].shape[0])
    for store in stores:
        store.wait()


def write_grads(
    own_ref, bc_ref, mine_ref, shared_ref,
    g_z, g_x, g_bc, g_dt, g_taps, g_bias, g_taps_s, g_bias_s, g_log, g_step, g_skip, g_gate, g_out,
):
    chan, heads_here = g_z.shape[1], g_log.shape[0]
    g_z[...] = own_ref[:, :chan].astype(F32)
    g_x[...] = own_ref[:, chan:2 * chan].astype(F32)
    g_dt[...] = own_ref[:, 2 * chan:2 * chan + LANES].astype(F32).T[0:heads_here, :]
    g_out[...] = own_ref[:, 2 * chan + LANES:].astype(F32)
    g_bc[...] = bc_ref[...].astype(F32)

    def row(source, at, length):
        return jnp.concatenate([source[at + k:at + k + 1, :] for k in range(length // LANES)], axis=1)

    per = chan // LANES
    for tap in range(4):
        g_taps[tap:tap + 1, :] = row(mine_ref, tap * per, chan)
        g_taps_s[tap:tap + 1, :] = row(shared_ref, tap * 2, 2 * STATE)
    g_bias[...] = row(mine_ref, 4 * per, chan).reshape(chan)
    g_gate[...] = row(mine_ref, 5 * per, chan).reshape(chan)
    skip = gather_heads(jnp.broadcast_to(row(mine_ref, 6 * per, chan), (8, chan)))
    g_skip[...] = skip[0:1, :heads_here].reshape(heads_here)
    g_log[...] = mine_ref[7 * per:7 * per + 1, :heads_here].reshape(heads_here)
    g_step[...] = mine_ref[7 * per + 1:7 * per + 2, :heads_here].reshape(heads_here)
    g_bias_s[...] = row(shared_ref, 8, 2 * STATE).reshape(2 * STATE)


def write_tokens(tok_ref, cot_ref, early_ref, mixed_ref, gain_ref, dn_ref, output, grad_tokens):
    resid = tok_ref[...].astype(F32)
    early = early_ref.shape[0]
    output[0:early, :] = (resid[0:early, :] + early_ref[...].astype(F32)).astype(BF16)
    output[early:, :] = (resid[early:, :] + mixed_ref[...].astype(F32)).astype(BF16)
    rstd = lax.rsqrt(jnp.mean(resid * resid, axis=1, keepdims=True) + EPSILON)
    scaled = dn_ref[...].astype(F32) * gain_ref[...].reshape(1, resid.shape[1])
    grad_tokens[...] = (
        cot_ref[...].astype(F32) + rstd * scaled
        - resid * (rstd * rstd * rstd) * jnp.mean(scaled * resid, axis=1, keepdims=True)
    ).astype(BF16)


def finish(tokens, cotangent, early, mixed, gain, dn, own, bc, mine, shared, heads_here):
    operands = (tokens, cotangent, early, mixed, gain, dn, own, bc, mine, shared)
    rows, width = tokens.shape
    count = own.shape[0]
    chan = (own.shape[1] - LANES) // 3
    vmem = pl.BlockSpec(memory_space=pltpu.VMEM)
    shape = lambda *extents: jax.ShapeDtypeStruct(extents, F32)
    outs = [
        jax.ShapeDtypeStruct((rows, width), BF16), jax.ShapeDtypeStruct((rows, width), BF16), shape(width),
        shape(count, chan), shape(count, chan), shape(count, 2 * STATE), shape(heads_here, count), shape(4, chan),
        shape(chan), shape(4, 2 * STATE), shape(2 * STATE), shape(heads_here), shape(heads_here), shape(heads_here),
        shape(chan), shape(count, chan),
    ]
    return pl.pallas_call(
        finish_kernel, name="finish", in_specs=[pl.BlockSpec(memory_space=pltpu.HBM)] * 10,
        out_specs=[pl.BlockSpec(memory_space=pl.ANY) if n in LARGE else vmem for n in range(len(outs))], out_shape=outs,
        scratch_shapes=[pltpu.VMEM(v.shape, v.dtype) for v in operands]
        + [pltpu.VMEM(outs[n].shape, outs[n].dtype) for n in LARGE]
        + [pltpu.SemaphoreType.DMA((10,)), pltpu.SemaphoreType.DMA((6,))],
        compiler_params=pltpu.CompilerParams(vmem_limit_bytes=63 << 20),
    )(*operands)


def exit_kernel(
    dn_ref, normed_ref, dpre_ref, cot_ref, gn_ref, dtaps_ref, dbias_ref, dhead_ref, dchan_ref, dgain_ref,
    dn_out, own_out, bc_out, mine_out, shared_out,
    dn, normed, dpre, cot, gn, fetch_sem,
    gin_ref, gout_ref, mine_ref, shared_ref,
    z_got, near_in, near_out, far_in, far_out, got_in, got_out, mine_got, shared_got, shared_held, shared_z,
    bc_held, bc_got,
    zs, zr, ns, nr, fs, fr, ms, mr, ss, sr, ts, tr, bs, br,
    *, n_tp, n_fs,
):
    tp, me = lax.axis_index("tp"), lax.axis_index("fsdp")
    chip, core, chips = me // 2, me % 2, n_fs // 2
    partner = chip * 2 + 1 - core
    greet("fsdp", [(me + d) % n_fs for d in range(1, n_fs)])
    greet("tp", [(tp + d) % n_tp for d in range(1, n_tp)])
    chan = gout_ref.shape[1]
    cols = gin_ref.shape[1]
    width = gin_ref.shape[0]
    fetches = [
        pltpu.make_async_copy(source, target, fetch_sem.at[k])
        for k, (source, target) in enumerate(
            [(normed_ref, normed), (dpre_ref, dpre), (cot_ref, cot), (gn_ref, gn), (dn_ref, dn)]
        )
    ]
    for fetch in fetches:
        fetch.start()
    fill_rows(
        mine_ref, [(dtaps_ref, tap, 0, chan) for tap in range(4)] + [(dbias_ref, 0, 0, chan)]
        + [(dchan_ref, row, 0, chan) for row in range(2)] + [(dhead_ref, row, 0, LANES) for row in range(2)]
    )
    fill_rows(
        shared_ref, [(dtaps_ref, tap, chan, 2 * STATE) for tap in range(4)] + [(dbias_ref, 0, chan, 2 * STATE)]
        + [(dgain_ref, 0, 0, width)]
    )
    block, count = dn_out.shape[0], own_out.shape[0]
    pl.semaphore_wait(pltpu.get_barrier_semaphore(), n_fs - 1 + n_tp - 1)

    chunk = block // CHUNKS
    sums = LineSum(
        tp, n_tp, CHUNKS, lambda index, part: chunk_of(dn, index, block, part, chunk),
        lambda index, part: chunk_of(dn_ref, index, block, part, chunk), z_got, zs, zr,
    )
    sums.kick()
    for k in (0, 1):
        fetches[k].wait()
    advance = sums.advance
    parts = (
        (gin_ref, slice(2 * chan, cols), near_in, far_in, got_in),
        (gout_ref, slice(0, chan), near_out, far_out, got_out),
        (gin_ref, slice(chan, 2 * chan), near_in, far_in, got_in),
        (gin_ref, slice(0, chan), near_in, far_in, got_in),
    )

    def near(j, d):
        source, span, held, _, _ = parts[j]
        rows = rows_at(source, ((chip + d) % chips) * 2 + 1 - core, count)
        return remote(rows.at[:, span], held.at[d, :, span], ns.at[j, d], nr.at[j, d], fsdp=partner)

    def far(j, d):
        _, span, _, held, got = parts[j]
        return remote(
            held.at[d, :, span], got.at[d, :, span], fs.at[j, d], fr.at[j, d], fsdp=((chip + d) % chips) * 2 + core
        )

    order = [d for d in range(1, chips)]

    def small(d):
        peer = (me + d) % n_fs
        return (
            remote(mine_ref, mine_got.at[me], ms.at[d], mr.at[d], fsdp=peer),
            remote(shared_ref, shared_got.at[me], ss.at[d], sr.at[d], fsdp=peer),
        )

    for d in range(1, n_fs):
        for copy in small(d):
            copy.start()
    mine_got[me] = mine_ref[...]
    shared_got[me] = shared_ref[...]

    def differentiate(j):
        _, span, *_ = parts[j]
        left, right, target = (cot, gn, gout_ref) if j == 1 else (normed, dpre, gin_ref)
        tile = 256

        @pl.loop(0, width // tile)
        def _(piece):
            at = pl.ds(pl.multiple_of(piece * tile, tile), tile)
            target[at, span] = mm(left[:, at], right[:, span], TN).astype(BF16)

        for d in order + [0]:
            near(j, d).start()

    def send_sums(j):
        source, span, held, summed, _ = parts[j]
        for d in order:
            near(j, d).wait_recv()
            rows = rows_at(source, ((chip + d) % chips) * 2 + core, count)
            add_into(summed.at[d, :, span], rows.at[:, span], held.at[d, :, span])
            far(j, d).start()
        near(j, 0).wait_recv()

    differentiate(0)
    for k in (2, 3, 4):
        fetches[k].wait()
    advance(0)
    differentiate(1)
    send_sums(0)
    advance(1)
    differentiate(2)
    send_sums(1)
    advance(2)
    differentiate(3)
    send_sums(2)
    advance(3)
    send_sums(3)
    at = 3
    turns = sums.turns
    for d in range(1, n_fs):
        for copy in small(d):
            copy.wait_recv()
    total, again = mine_got[0], shared_got[0]
    for peer in range(1, n_fs):
        total, again = total + mine_got[peer], again + shared_got[peer]
    mine_out[...] = total
    shared_held[...] = again
    shared_z[tp] = again
    for d in range(1, n_tp):
        remote(shared_held, shared_z.at[tp], ts.at[d], tr.at[d], tp=(tp + d) % n_tp).start()
    pl.loop(at + 1, turns)(advance)

    def settle(j, target, span):
        source, _, held, _, got = parts[j]
        rows = rows_at(source, me, count)
        add_into(
            target, rows.at[:, span], held.at[0, :, span], *[got.at[d, :, span] for d in order]
        )

    for d in order:
        far(0, d).wait_recv()
    settle(0, bc_held, slice(2 * chan, 2 * chan + 2 * STATE))
    bc_got[tp] = bc_held[...]
    for d in range(1, n_tp):
        remote(bc_held, bc_got.at[tp], bs.at[d], br.at[d], tp=(tp + d) % n_tp).start()
    settle(0, own_out.at[:, 2 * chan:2 * chan + LANES], slice(2 * chan + 2 * STATE, cols))
    for j in (1, 2, 3):
        for d in order:
            far(j, d).wait_recv()
    settle(1, own_out.at[:, 2 * chan + LANES:], slice(0, chan))
    settle(2, own_out.at[:, chan:2 * chan], slice(chan, 2 * chan))
    settle(3, own_out.at[:, :chan], slice(0, chan))
    for d in range(1, n_tp):
        peer = (tp + n_tp - d) % n_tp
        remote(shared_held, shared_z.at[peer], ts.at[d], tr.at[d], tp=peer).wait_recv()
        remote(bc_held, bc_got.at[peer], bs.at[d], br.at[d], tp=peer).wait_recv()
    total = shared_z[0]
    for peer in range(1, n_tp):
        total = total + shared_z[peer]
    shared_out[...] = total
    add_into(bc_out, *[bc_got.at[peer] for peer in range(n_tp)])

    sums.settle(lambda part: dn_out.at[pl.ds(part * chunk, chunk)])
    sums.drain()
    for j in range(4):
        for d in range(chips):
            near(j, d).wait_send()
        for d in order:
            far(j, d).wait_send()
    for d in range(1, n_fs):
        for copy in small(d):
            copy.wait_send()
    for d in range(1, n_tp):
        remote(shared_held, shared_z.at[tp], ts.at[d], tr.at[d], tp=(tp + d) % n_tp).wait_send()
        remote(bc_held, bc_got.at[tp], bs.at[d], br.at[d], tp=(tp + d) % n_tp).wait_send()


def leave(dn, normed, dpre, cot, gnormed, small, n_tp, n_fs):
    block, width = dn.shape[0] // n_tp, dn.shape[1]
    count, cols = width // n_fs, dpre.shape[1]
    chan = gnormed.shape[1]
    chips, steps = n_fs // 2, (n_tp - 1) * CHUNKS
    dma = pltpu.SemaphoreType.DMA
    vmem = pl.BlockSpec(memory_space=pltpu.VMEM)
    room = lambda *shape: pltpu.VMEM(shape, BF16)
    shape = lambda *extents: jax.ShapeDtypeStruct(extents, F32)
    up = lambda n: -(-n // 8) * 8
    mine = (up(7 * chan // LANES + 2), LANES)
    shared = (up((10 * STATE + width) // LANES), LANES)
    low = lambda *extents: jax.ShapeDtypeStruct(extents, BF16)
    outs = [low(block, width), low(count, 3 * chan + LANES), low(count, 2 * STATE), shape(*mine), shape(*shared)]
    return pl.pallas_call(
        functools.partial(exit_kernel, n_tp=n_tp, n_fs=n_fs),
        name="exit",
        in_specs=[pl.BlockSpec(memory_space=pl.ANY)] * 5 + [vmem] * 5,
        out_specs=[vmem] * len(outs),
        out_shape=outs,
        scratch_shapes=[
            room(*dn.shape), room(*normed.shape), room(*dpre.shape), room(*cot.shape), room(*gnormed.shape), dma((5,)),
            room(width, cols), room(width, chan), pltpu.VMEM(mine, F32), pltpu.VMEM(shared, F32),
            room(2, steps, block // CHUNKS, width),
            room(chips, count, cols), room(chips, count, chan), room(chips, count, cols), room(chips, count, chan),
            room(chips, count, cols), room(chips, count, chan),
            pltpu.VMEM((n_fs,) + mine, F32), pltpu.VMEM((n_fs,) + shared, F32),
            pltpu.VMEM(shared, F32), pltpu.VMEM((n_tp,) + shared, F32),
            room(count, 2 * STATE), room(n_tp, count, 2 * STATE),
            dma((2, steps)), dma((2, steps)), dma((4, chips)), dma((4, chips)), dma((4, chips)), dma((4, chips)),
            dma((n_fs,)), dma((n_fs,)), dma((n_fs,)), dma((n_fs,)), dma((n_tp,)), dma((n_tp,)), dma((n_tp,)),
            dma((n_tp,)),
        ],
        compiler_params=pltpu.CompilerParams(
            collective_id=TAGS["exit"], has_side_effects=True, vmem_limit_bytes=62 << 20
        ),
    )(dn, normed, dpre, cot, gnormed, *small)


def shards(
    tokens, cotangent, seq_start, token_valid, norm_gain, proj_z, proj_x, proj_bc, proj_dt, conv_chan, bias_chan,
    conv_shared, bias_shared, a_log, dt_bias, skip_gain, gate_gain, proj_out,
):
    chan, heads_here = proj_z.shape[1], proj_dt.shape[1]
    n_tp, n_fs = lax.axis_size("tp"), lax.axis_size("fsdp")
    (
        tok_all, cot_all, w_in, normed, pre, y, enter, dgn, gnormed, out_rows, early, stats, taps, bias, heads, skip,
        gate,
    ) = ahead(
        seq_start, (dt_bias, a_log, skip_gain), tokens, cotangent,
        (proj_z, proj_x, proj_bc, proj_dt.T, proj_out.T), token_valid,
        (norm_gain, conv_chan, bias_chan, conv_shared, bias_shared, gate_gain), n_tp, n_fs,
    )
    dpre, dn_rows, *small, mixed = mixer_backward(
        seq_start, tok_all, w_in, taps, bias, heads, skip, gate, pre, y, enter, dgn, stats, out_rows, chan * n_tp,
        n_tp,
    )
    sums = leave(dn_rows, normed, dpre, cot_all, gnormed, small, n_tp, n_fs)
    grads = list(finish(tokens, cotangent, early, mixed, norm_gain, *sums, heads_here))
    grads[6], grads[15] = grads[6].T, grads[15].T
    return tuple(grads)


def solution(mesh):
    in_specs = (
        P(("fsdp", "tp"), None), P(("fsdp", "tp"), None), P("fsdp"), P("fsdp"), P(), P("fsdp", "tp"),
        P("fsdp", "tp"), P("fsdp", None), P("fsdp", "tp"), P(None, "tp"), P("tp"), P(), P(), P("tp"), P("tp"),
        P("tp"), P("tp"), P("tp", "fsdp"),
    )
    out_specs = (
        P(("fsdp", "tp"), None), P(("fsdp", "tp"), None), P(), P("fsdp", "tp"), P("fsdp", "tp"), P("fsdp", None),
        P("fsdp", "tp"), P(None, "tp"), P("tp"), P(), P(), P("tp"), P("tp"), P("tp"), P("tp"), P("tp", "fsdp"),
    )
    return jax.shard_map(shards, mesh=mesh, in_specs=in_specs, out_specs=out_specs, check_vma=False)
```
